32 devices in a mesh: ep: 2 (over core), cp: 8 (over z, x), tp: 2 (over y).
Axes of the slice: x: 2, y: 2, z: 4, core: 2. Of those that a mesh axis runs over, the one named last changes fastest.
Arguments:
- activations: bfloat16 [4, 1024, 1536], P('ep', 'cp')
- cotangent: bfloat16 [4, 1024, 1536], P('ep', 'cp'), may hold values from -6 to 6
- positions: int32 [4, 1024], P('ep', 'cp'), may hold values from 0 to 1023, as said below
- routes: int32 [4, 1024, 8], P('ep', 'cp'), may hold values from 0 to 15, all different within a row
- w_query: bfloat16 [1536, 1536], P(None, 'tp'), may hold values from -0.15625 to 0.15625
- w_key: bfloat16 [1536, 512], P(None, 'tp'), may hold values from -0.15625 to 0.15625
- value_weight: bfloat16 [1536, 512], P(None, 'tp'), may hold values from -0.15625 to 0.15625
- w_out: bfloat16 [1536, 1536], P(None, 'tp'), may hold values from -1.25 to 1.25
- gain_attn: float32 [1536], replicated, may hold values from 0.5 to 1.5
- gain_moe: float32 [1536], replicated, may hold values from 0.5 to 1.5
- w_router: bfloat16 [1536, 16], replicated, may hold values from -0.3125 to 0.3125
- w_gate_up: bfloat16 [16, 1536, 2, 512], P('ep', None, None, 'tp'), may hold values from -0.15625 to 0.15625
- w_down: bfloat16 [16, 1536, 512], P('ep', None, 'tp'), may hold values from -0.75 to 0.75
Outputs:
- output: float32 [4, 1024, 1536], P('ep', 'cp')
- input_grad: float32 [4, 1024, 1536], P('ep', 'cp')
- query_grad: float32 [1536, 1536], P(('ep', 'cp'), 'tp')
- key_grad: float32 [1536, 512], P(('ep', 'cp'), 'tp')
- value_grad: float32 [1536, 512], P(('ep', 'cp'), 'tp')
- out_proj_grad: float32 [1536, 1536], P(('ep', 'cp'), 'tp')
- gain_attn_grad: float32 [1536], P(('ep', 'cp'))
- gain_moe_grad: float32 [1536], P(('ep', 'cp'))
- router_grad: float32 [1536, 16], P(('ep', 'cp'))
- gate_up_grad: float32 [16, 1536, 2, 512], P('ep', 'cp', None, 'tp')
- down_grad: float32 [16, 1536, 512], P('ep', 'cp', 'tp')
The draws below stay inside these ranges and needn't reach their ends.
Inputs may be any that keep to these rules, and one draw needn't show every extreme that they name: `positions`: along each sequence a position is 0 where a document starts and rises by one with each row; the first sequence is a single document. `routes`: each token names 8 different experts.
All inputs are finite; a program needn't handle non-finite values.
Results may differ from the reference program's by a relative error of at most 0.035.
Values may be sent and summed in bfloat16 or wider, within the bound.
A program may use at most 192 MiB of HBM per device.

```python
import math
import jax
import jax.numpy as jnp
from jax import lax

MODEL_DIM = 1536
QUERY_HEADS = 24
KEY_VALUE_HEADS = 8
HEAD_SIZE = 64
FF = 512
TOPK = 8
EXPERTS = 16
SEQS = 4
LEN = 1024
N_TP = 2


def draw_activations(key, part):
    random_subkeys = jax.random.split(key, 3)
    base_draw = jax.random.normal(random_subkeys[0], (SEQS, LEN, MODEL_DIM), jnp.float32)
    row_scale = jnp.exp(jax.random.uniform(random_subkeys[1], (SEQS, LEN, 1), jnp.float32, math.log(0.3), math.log(3.0)))
    column_scale = jnp.exp(jax.random.uniform(random_subkeys[2], (1, 1, MODEL_DIM), jnp.float32, math.log(0.5), math.log(2.0)))
    return jnp.clip(base_draw * row_scale * column_scale, -40.0, 40.0).astype(jnp.bfloat16)


def draw_positions(key, part):
    row_index = jnp.arange(LEN, dtype=jnp.int32)[None, :]
    seq_index = jnp.arange(SEQS, dtype=jnp.int32)[:, None]
    marks = jax.random.randint(key, (SEQS, LEN), 0, LEN)
    starts = (marks < 3) & (seq_index > 0) | (row_index == 0)
    begins = lax.cummax(jnp.where(starts, row_index, 0), axis=1)
    return row_index - begins


def spiked(result, stream_key, source, target, shards_of, factor):
    owner, partner = [(jnp.arange(result.shape[axis_at]) // (result.shape[axis_at] // shards_of)).reshape([-1 if axis == axis_at else 1 for axis in range(result.ndim)]) for axis_at in (source, target)]
    chosen = jax.random.permutation(stream_key, shards_of)[partner]
    strong = (owner == chosen) | (owner == (partner + shards_of // 2) % shards_of)
    return jnp.where(strong, factor * result, result)


def levels(stream_key, shape, cuts, low, top_value):
    level = 1.0
    for dim, parts in cuts:
        heights = jax.random.uniform(jax.random.fold_in(jax.random.fold_in(stream_key, 6), dim), (parts,), jnp.float32, low / len(cuts), top_value / len(cuts))
        level = level * jnp.repeat(jnp.exp(heights), shape[dim] // parts).reshape((-1,) + (1,) * (len(shape) - 1 - dim))
    return level


def different_ones(rng, rows, count, top, lift):
    sequence = jax.random.permutation(jax.random.fold_in(rng, 1), count)
    pull = sequence
    for power in range(3):
        pull = pull * pull // count
    pull = pull * lift // count
    tickets = jax.random.randint(jax.random.fold_in(rng, 2), (rows, count), 0, 4096) + pull
    fixed_rows = jax.random.permutation(jax.random.fold_in(rng, 3), rows)[jnp.arange(count) % rows]
    tickets = jnp.where(jnp.arange(rows)[:, None] == fixed_rows[None, :], 1 << 14, tickets)
    score = tickets * count + jnp.arange(count)
    return lax.top_k(score.astype(jnp.int32), top)[1].astype(jnp.int32)


def bell_draw(key, dims, scale, most, cuts=(), kind=jnp.bfloat16):
    values = scale * jax.random.normal(key, dims, jnp.float32)
    if cuts:
        values = values * levels(key, dims, cuts, -0.22, 0.18)
    return jnp.clip(values, -most, most).astype(kind)


def gaussian_with(rng, dims, deviation, bound, pieces, heavy, kind=jnp.bfloat16):
    values = deviation * jax.random.normal(rng, dims, jnp.float32)
    if pieces:
        values = values * levels(rng, dims, pieces, -0.22, 0.18)
    return jnp.clip(spiked(values, jax.random.fold_in(rng, 3), *heavy), -bound, bound).astype(kind)


def setup_inputs(seed: int = 0) -> dict:
    key_of = jax.random.split(jax.random.key(seed), 14)
    return {
        "activations": draw_activations(jax.random.fold_in(key_of[13], 71), 0),
        "cotangent": gaussian_with(key_of[1], (SEQS, LEN, MODEL_DIM), 1.0, 6.0, ((0, 2), (1, 8)), (1, 2, 8, 2.0)),
        "positions": draw_positions(jax.random.fold_in(key_of[13], 71), 0),
        "routes": different_ones(key_of[3], SEQS * LEN, EXPERTS, TOPK, 8192).reshape((SEQS, LEN, TOPK)),
        "w_query": bell_draw(key_of[4], (MODEL_DIM, QUERY_HEADS * HEAD_SIZE), MODEL_DIM ** -0.5, 0.15625, ((1, 2),)),
        "w_key": bell_draw(key_of[5], (MODEL_DIM, KEY_VALUE_HEADS * HEAD_SIZE), MODEL_DIM ** -0.5, 0.15625, ((1, 2),)),
        "value_weight": bell_draw(key_of[6], (MODEL_DIM, KEY_VALUE_HEADS * HEAD_SIZE), MODEL_DIM ** -0.5, 0.15625, ((1, 2),)),
        "w_out": bell_draw(key_of[7], (MODEL_DIM, QUERY_HEADS * HEAD_SIZE), (QUERY_HEADS * HEAD_SIZE // 64) ** -0.5, 1.25, ((1, 2),)),
        "gain_attn": jnp.clip(1.0 + 0.1 * jax.random.normal(key_of[8], (MODEL_DIM,), jnp.float32), 0.5, 1.5),
        "gain_moe": jnp.clip(1.0 + 0.1 * jax.random.normal(key_of[9], (MODEL_DIM,), jnp.float32), 0.5, 1.5),
        "w_router": bell_draw(key_of[10], (MODEL_DIM, EXPERTS), (MODEL_DIM // 4) ** -0.5, 0.3125),
        "w_gate_up": bell_draw(key_of[11], (EXPERTS, MODEL_DIM, 2, FF), MODEL_DIM ** -0.5, 0.15625, ((0, 2), (3, 2))),
        "w_down": bell_draw(key_of[12], (EXPERTS, MODEL_DIM, FF), (FF // 8) ** -0.5, 0.75, ((0, 2), (2, 2))),
    }


UPPER_PRECISION = lax.Precision.HIGHEST
EPS = 1e-06
NEG = -1e+30

@jax.custom_vjp
def low(v):
    return lax.optimization_barrier(v.astype(jnp.bfloat16)).astype(jnp.float32)

@jax.custom_vjp
def low_back(v):
    return v

def low_keep(v):
    return (low(v), None)

def low_pass(kept, grad):
    return (grad,)

def back_keep(v):
    return (v, None)

def back_low(kept, grad):
    return (low(grad),)
low.defvjp(low_keep, low_pass)
low_back.defvjp(back_keep, back_low)

def norm_rows(values, gain):
    scale = lax.rsqrt(lax.optimization_barrier(jnp.mean(values * values, axis=-1, keepdims=True)) + EPS)
    return values * scale * gain

def rope_table(places, head_width):
    frequency = jnp.power(10000.0, -(jnp.arange(head_width // 2, dtype=jnp.float32) * 2.0 / head_width))
    angles = places.astype(jnp.float32)[..., None] * frequency
    cosine = jnp.cos(angles)
    sine_table = jnp.sin(angles)
    return (jnp.concatenate([cosine, cosine], -1), jnp.concatenate([sine_table, sine_table], -1))

def rotate(values, cosine, sine_table):
    half_width = values.shape[-1] // 2
    turned = jnp.concatenate([-values[..., half_width:], values[..., :half_width]], -1)
    return values * cosine + turned * sine_table

def attend_sequence(packed):
    queries, key_rows, projected_value_rows, places = packed
    sequence_length, key_value_count, group_size, head_width = queries.shape
    block_size = math.gcd(sequence_length, 512)
    block_count = sequence_length // block_size
    key_index = jnp.arange(sequence_length, dtype=jnp.int32)

    def one_block(block_input):
        query_block, place_block, first_row = block_input
        query_index = first_row + jnp.arange(block_size, dtype=jnp.int32)
        distance = query_index[:, None] - key_index[None, :]
        allowed = (distance >= 0) & (distance <= place_block[:, None])
        scores = low_back(jnp.einsum('qhgd,khd->hgqk', query_block, key_rows, precision=UPPER_PRECISION) * 0.125)
        scores = jnp.where(allowed[None, None], scores, NEG)
        weights = jax.nn.softmax(scores, axis=-1)
        return jnp.einsum('hgqk,khd->qhgd', low(weights), projected_value_rows, precision=UPPER_PRECISION)
    starts = jnp.arange(block_count, dtype=jnp.int32) * block_size
    results = lax.map(jax.checkpoint(one_block), (queries.reshape(block_count, block_size, key_value_count, group_size, head_width), places.reshape(block_count, block_size), starts))
    return results.reshape(sequence_length, key_value_count, group_size, head_width)

def expert_mix(token_rows, spread, wt_gate_up, wt_down, group_count):
    row_total, model_width = token_rows.shape
    block_size = math.gcd(row_total, 4096)
    block_count = row_total // block_size
    group_width = wt_down.shape[2] // group_count

    def token_block(block_input):
        rows_block, weight_block = block_input

        def one_expert(running, expert_input):
            gate_up_one, down_one, weight_one = expert_input
            summed = jnp.zeros_like(rows_block)
            for group_index in range(group_count):
                low_edge = group_index * group_width
                high_edge = low_edge + group_width
                inputs = low_back(rows_block)
                gate_up = low_back(jnp.einsum('nd,dgf->ngf', inputs, gate_up_one[:, :, low_edge:high_edge], precision=UPPER_PRECISION))
                hidden = low(jax.nn.silu(gate_up[:, 0]) * gate_up[:, 1])
                summed = summed + low(jnp.einsum('nf,df->nd', hidden, down_one[:, low_edge:high_edge], precision=UPPER_PRECISION))
            return (running + weight_one[:, None] * low_back(summed), None)
        mixture, unused = lax.scan(jax.checkpoint(one_expert), jnp.zeros_like(rows_block), (wt_gate_up, wt_down, weight_block.T))
        return mixture
    results = lax.map(jax.checkpoint(token_block), (token_rows.reshape(block_count, block_size, model_width), spread.reshape(block_count, block_size, spread.shape[1])))
    return results.reshape(row_total, model_width)

def layer(inputs, query_weight_cast, key_weight_cast, value_weight_cast, output_weight_cast, gain_one, gain_two, router_weight_cast, wt_gate_up, wt_down, positions, routes):
    sequence_total, sequence_length, model_width = inputs.shape
    head_count = query_weight_cast.shape[1] // HEAD_SIZE
    key_value_count = key_weight_cast.shape[1] // HEAD_SIZE
    group_size = head_count // key_value_count
    expert_count = router_weight_cast.shape[1]
    first_normed_rows = low(norm_rows(inputs, gain_one))
    cosine, sine_table = rope_table(positions, HEAD_SIZE)
    cosine = cosine[:, :, None, :]
    sine_table = sine_table[:, :, None, :]
    query_before_rotation = low_back(jnp.einsum('ugq,qy->ugy', first_normed_rows, query_weight_cast, precision=UPPER_PRECISION))
    queries = low(rotate(query_before_rotation.reshape(sequence_total, sequence_length, head_count, HEAD_SIZE), cosine, sine_table))
    key_before_rotation = low_back(jnp.einsum('ugq,qy->ugy', first_normed_rows, key_weight_cast, precision=UPPER_PRECISION))
    key_rows = low(rotate(key_before_rotation.reshape(sequence_total, sequence_length, key_value_count, HEAD_SIZE), cosine, sine_table))
    projected_value_rows = low(low_back(jnp.einsum('ugq,qy->ugy', first_normed_rows, value_weight_cast, precision=UPPER_PRECISION))).reshape(sequence_total, sequence_length, key_value_count, HEAD_SIZE)
    attention_output = lax.map(jax.checkpoint(attend_sequence), (queries.reshape(sequence_total, sequence_length, key_value_count, group_size, HEAD_SIZE), key_rows, projected_value_rows, positions))
    attention_output = low(low_back(attention_output.reshape(sequence_total, sequence_length, head_count * HEAD_SIZE)))
    residual_branch = low_back(jnp.einsum('eby,ty->ebt', attention_output, output_weight_cast, precision=UPPER_PRECISION))
    middle = inputs + residual_branch
    second_normed_rows = low(norm_rows(middle, gain_two))
    router_logits = jnp.einsum('ypw,wj->ypj', second_normed_rows, router_weight_cast, precision=UPPER_PRECISION)
    one_hot = (routes[..., None] == jnp.arange(expert_count, dtype=jnp.int32)).astype(jnp.float32)
    chosen = jnp.einsum('slke,sle->slk', one_hot, router_logits, precision=UPPER_PRECISION)
    gate_probs = jax.nn.softmax(chosen, axis=-1)
    spread = jnp.einsum('slk,slke->sle', gate_probs, one_hot, precision=UPPER_PRECISION)
    mixture = expert_mix(second_normed_rows.reshape(sequence_total * sequence_length, model_width), spread.reshape(sequence_total * sequence_length, expert_count), wt_gate_up, wt_down, N_TP)
    return middle + mixture.reshape(sequence_total, sequence_length, model_width)

def reference(activations, cotangent, positions, routes, w_query, w_key, value_weight, w_out, gain_attn, gain_moe, w_router, w_gate_up, w_down):

    def closed(inputs, query_weight_cast, key_weight_cast, value_weight_cast, output_weight_cast, gain_one, gain_two, router_weight_cast, wt_gate_up, wt_down):
        return layer(inputs, query_weight_cast, key_weight_cast, value_weight_cast, output_weight_cast, gain_one, gain_two, router_weight_cast, wt_gate_up, wt_down, positions, routes)
    output, pullback = jax.vjp(closed, activations.astype(jnp.float32), w_query.astype(jnp.float32), w_key.astype(jnp.float32), value_weight.astype(jnp.float32), w_out.astype(jnp.float32), gain_attn.astype(jnp.float32), gain_moe.astype(jnp.float32), w_router.astype(jnp.float32), w_gate_up.astype(jnp.float32), w_down.astype(jnp.float32))
    gradients = pullback(cotangent.astype(jnp.float32))
    return (output, gradients[0], gradients[1], gradients[2], gradients[3], gradients[4], gradients[5], gradients[6], gradients[7], gradients[8], gradients[9])
```

```python
import functools

import jax
import jax.numpy as jnp
from jax import lax
from jax.experimental import pallas as pl
from jax.experimental.pallas import tpu as pltpu
from jax.sharding import PartitionSpec as P

HEAD = 64
EPS = 1e-06
NEG = -1e30
SCALE = 0.125
LANES = 128
KEY_CHUNK = 1024
F32 = jnp.float32
BF16 = jnp.bfloat16


def mm(a, b):
    return lax.dot_general(a, b, (((1,), (0,)), ((), ())), preferred_element_type=F32)


def mm_t(a, b):
    return lax.dot_general(a, b, (((1,), (1,)), ((), ())), preferred_element_type=F32)


def t_mm(a, b):
    return lax.dot_general(a, b, (((0,), (0,)), ((), ())), preferred_element_type=F32)


def two_parts(v):
    high = v.astype(BF16)
    return high, (v - high.astype(F32)).astype(BF16)


def halves_turned(v, back):
    width = v.shape[1]
    ahead = pltpu.roll(v, width - HEAD // 2, 1)
    behind = pltpu.roll(v, HEAD // 2, 1)
    first = lax.broadcasted_iota(jnp.int32, v.shape, 1) % HEAD < HEAD // 2
    if back:
        return jnp.where(first, ahead, -behind)
    return jnp.where(first, -ahead, behind)


def rope(v, cosine, sine):
    return v * cosine + halves_turned(v, False) * sine


def rope_back(v, cosine, sine):
    return v * cosine + halves_turned(v * sine, True)


def widen(table, width):
    return jnp.concatenate([table] * (width // table.shape[1]), axis=1)


def unit_rows(v):
    scale = lax.rsqrt(jnp.mean(v * v, axis=-1, keepdims=True) + EPS)
    return v * scale, scale


def shape_of(shape, dtype):
    return jax.ShapeDtypeStruct(shape, dtype)


def params(**kw):
    return pltpu.CompilerParams(vmem_limit_bytes=60 * 2**20, **kw)


def cost(flops, moved):
    return pl.CostEstimate(flops=int(flops), bytes_accessed=int(moved), transcendentals=0)


def project_body(act, gain, wq, wk, wv, cosine, sine, normed, q, kv):
    unit, _ = unit_rows(act[...].astype(F32))
    low = (unit * gain[...]).astype(BF16)
    normed[...] = low
    qf = mm(low, wq[...])
    q[...] = rope(qf, widen(cosine[...], qf.shape[1]), widen(sine[...], qf.shape[1])).astype(BF16)
    kf = mm(low, wk[...])
    width = kf.shape[1]
    kv[:, :width] = rope(kf, widen(cosine[...], width), widen(sine[...], width)).astype(BF16)
    kv[:, width:] = mm(low, wv[...]).astype(BF16)


def project(act, gain, wq, wk, wv, cosine, sine):
    rows, model = act.shape
    total = wq.shape[1] + 2 * wk.shape[1]
    return pl.pallas_call(
        project_body,
        out_shape=(
            shape_of((rows, model), BF16),
            shape_of((rows, wq.shape[1]), BF16),
            shape_of((rows, 2 * wk.shape[1]), BF16),
        ),
        compiler_params=params(),
        cost_estimate=cost(2 * rows * model * total, 2 * model * total + 6 * rows * model),
        name="project",
    )(act, gain, wq, wk, wv, cosine, sine)


def fill_keys(first_ref, offset_ref, place, slots, keys, bias, rows):
    at = 0
    query = lax.broadcasted_iota(jnp.int32, (rows, rows), 1) + offset_ref[0]
    for slot in slots:
        for one in range(slot.shape[0]):
            keys[at * rows : (at + 1) * rows, :] = slot[one, 0]
            key = lax.broadcasted_iota(jnp.int32, (rows, rows), 0) + first_ref[at]
            distance = query - key
            seen = (distance >= 0) & (distance <= place)
            bias[at * rows : (at + 1) * rows, :] = jnp.where(seen, 0.0, NEG)
            at += 1


def group_rows(block, head, group):
    return jnp.concatenate(
        [block[:, (head * group + g) * HEAD : (head * group + g + 1) * HEAD] for g in range(group)], axis=0
    )


def attend_body(group, count, first_ref, offset_ref, q_ref, place_ref, *refs):
    slots = refs[:count]
    low_ref, out_ref, lse_ref, keys, bias = refs[count:]
    rows = q_ref.shape[1]
    fill_keys(first_ref, offset_ref, place_ref[0], slots, keys, bias, rows)
    total, width = keys.shape[0], keys.shape[1] // 2
    chunk = min(total, KEY_CHUNK)
    q = (q_ref[0].astype(F32) * SCALE).astype(BF16)
    pieces = []
    for head in range(width // HEAD):
        q3 = group_rows(q, head, group)
        top = run = out = None
        for low in range(0, total, chunk):
            k = keys[low : low + chunk, head * HEAD : (head + 1) * HEAD]
            v = keys[low : low + chunk, width + head * HEAD : width + (head + 1) * HEAD]
            s = mm_t(k, q3) + widen(bias[low : low + chunk, :], group * rows)
            here = jnp.max(s, axis=0, keepdims=True)
            new = here if top is None else jnp.maximum(top, here)
            p = jnp.exp(s - new)
            part = jnp.sum(p, axis=0, keepdims=True)
            o = t_mm(v, p.astype(BF16))
            if top is None:
                run, out = part, o
            else:
                shrink = jnp.exp(top - new)
                run, out = run * shrink + part, out * shrink + o
            top = new
        out = jnp.transpose(out / run)
        pieces += [out[g * rows : (g + 1) * rows] for g in range(group)]
        lse_ref[0, head : head + 1, :] = top + jnp.log(run)
    whole = jnp.concatenate(pieces, axis=1)
    out_ref[0] = whole
    low_ref[0] = whole.astype(BF16)


def seq_block(shape):
    return pl.BlockSpec((1,) + shape[1:], lambda s, *_: (s,) + (0,) * (len(shape) - 1))


def slot_block(shape):
    return pl.BlockSpec((shape[0], 1) + shape[2:], lambda s, *_: (0, s, 0, 0))


def attend(q, place, slots, first, offset, group):
    seqs, rows, wide = q.shape
    both = slots[0].shape[-1]
    total = rows * sum(slot.shape[0] for slot in slots)
    heads = wide // HEAD // group
    outs = (
        shape_of(q.shape, BF16),
        shape_of(q.shape, F32),
        shape_of((seqs, heads, group * rows), F32),
    )
    return pl.pallas_call(
        functools.partial(attend_body, group, len(slots)),
        out_shape=outs,
        grid_spec=pltpu.PrefetchScalarGridSpec(
            num_scalar_prefetch=2,
            grid=(seqs,),
            in_specs=[seq_block(q.shape), seq_block(place.shape)] + [slot_block(s.shape) for s in slots],
            out_specs=tuple(seq_block(o.shape) for o in outs),
            scratch_shapes=[pltpu.VMEM((total, both), BF16), pltpu.VMEM((total, rows), F32)],
        ),
        compiler_params=params(),
        cost_estimate=cost(2e9 * 4, 20e6),
        name="attend",
    )(first, offset, q, place, *slots)


def attend_back_body(
    group, count, first_ref, offset_ref, q_ref, place_ref, grad_ref, out_ref, lse_ref, cos_ref, sin_ref, *refs
):
    slots = refs[:count]
    dq_ref = refs[count]
    grads = refs[count + 1 : 2 * count + 1]
    keys, bias = refs[2 * count + 1 :]
    rows = q_ref.shape[1]
    fill_keys(first_ref, offset_ref, place_ref[0], slots, keys, bias, rows)
    total, width = keys.shape[0], keys.shape[1] // 2
    chunk = min(total, KEY_CHUNK)
    q = (q_ref[0].astype(F32) * SCALE).astype(BF16)
    go = grad_ref[0]
    products = go.astype(F32) * out_ref[0]
    ones = jnp.ones((8, HEAD), F32)
    heads = width // HEAD
    q3s = [group_rows(q, head, group) for head in range(heads)]
    g3s = [group_rows(go, head, group) for head in range(heads)]
    deltas = [
        lax.dot_general(
            ones,
            group_rows(products, head, group),
            (((1,), (1,)), ((), ())),
            preferred_element_type=F32,
            precision=lax.Precision.HIGHEST,
        )[:1]
        for head in range(heads)
    ]
    dq = [None] * heads
    for low in range(0, total, chunk):
        dks, dvs = [], []
        for head in range(heads):
            k = keys[low : low + chunk, head * HEAD : (head + 1) * HEAD]
            v = keys[low : low + chunk, width + head * HEAD : width + (head + 1) * HEAD]
            s = mm_t(k, q3s[head]) + widen(bias[low : low + chunk, :], group * rows)
            p = jnp.exp(s - lse_ref[0, head : head + 1, :])
            dp = mm_t(v, g3s[head])
            ds = (p * (dp - deltas[head])).astype(BF16)
            dks.append(mm(ds, q3s[head]))
            dvs.append(mm(p.astype(BF16), g3s[head]))
            part = t_mm(k, ds)
            dq[head] = part if dq[head] is None else dq[head] + part
        both = jnp.concatenate(dks + dvs, axis=1).astype(BF16)
        at = low // rows
        done = 0
        for ref in grads:
            for one in range(ref.shape[0]):
                if at <= done < at + chunk // rows:
                    ref[one, 0] = both[(done - at) * rows : (done - at + 1) * rows]
                done += 1
    pieces = []
    for head in range(heads):
        back = jnp.transpose(dq[head] * SCALE)
        pieces += [back[g * rows : (g + 1) * rows] for g in range(group)]
    whole = jnp.concatenate(pieces, axis=1)
    cosine, sine = widen(cos_ref[0], whole.shape[1]), widen(sin_ref[0], whole.shape[1])
    dq_ref[0] = rope_back(whole, cosine, sine).astype(BF16)


def attend_back(q, place, grad, out, lse, cosine, sine, slots, first, offset, group):
    seqs, rows, _ = q.shape
    both = slots[0].shape[-1]
    total = rows * sum(slot.shape[0] for slot in slots)
    outs = (shape_of(q.shape, BF16),) + tuple(shape_of(s.shape, BF16) for s in slots)
    ins = (q, place, grad, out, lse, cosine, sine)
    got = pl.pallas_call(
        functools.partial(attend_back_body, group, len(slots)),
        out_shape=outs,
        grid_spec=pltpu.PrefetchScalarGridSpec(
            num_scalar_prefetch=2,
            grid=(seqs,),
            in_specs=[seq_block(a.shape) for a in ins] + [slot_block(s.shape) for s in slots],
            out_specs=(seq_block(outs[0].shape),) + tuple(slot_block(s.shape) for s in slots),
            scratch_shapes=[pltpu.VMEM((total, both), BF16), pltpu.VMEM((total, rows), F32)],
        ),
        compiler_params=params(),
        cost_estimate=cost(2e9 * 8, 30e6),
        name="attend_back",
    )(first, offset, *ins, *slots)
    return got[0], got[1:]


def out_body(low, w_out, part):
    part[...] = mm_t(low[...], w_out[...]).astype(BF16)


def out_project(low, w_out):
    rows, model = low.shape[0], w_out.shape[0]
    return pl.pallas_call(
        out_body,
        out_shape=shape_of((rows, model), BF16),
        compiler_params=params(),
        cost_estimate=cost(2 * rows * model * low.shape[1], 4e6),
        name="out_project",
    )(low, w_out)


def middle_body(act, part, other, gain, router, hot, middle, normed, gates):
    mid = act[...].astype(F32) + (part[...].astype(F32) + other[...].astype(F32))
    middle[...] = mid
    unit, _ = unit_rows(mid)
    low = (unit * gain[...]).astype(BF16)
    normed[...] = low
    chosen = hot[...] > 0.5
    logits = jnp.where(chosen, mm(low, router[...]), NEG)
    up = jnp.where(chosen, jnp.exp(logits - jnp.max(logits, axis=-1, keepdims=True)), 0.0)
    gates[...] = up / jnp.sum(up, axis=-1, keepdims=True)


def middle_of(act, part, other, gain, router, hot):
    rows, model = act.shape
    return pl.pallas_call(
        middle_body,
        out_shape=(shape_of((rows, model), F32), shape_of((rows, model), BF16), shape_of((rows, LANES), F32)),
        compiler_params=params(),
        cost_estimate=cost(2 * rows * model * LANES, 12 * rows * model),
        name="middle",
    )(act, part, other, gain, router, hot)


def experts_body(
    lo, hi, per, fresh, where_ref, x_own, x_par, dy_own, dy_par, dy_turned, g_own, g_par, *refs
):
    steps = hi - lo
    refs = list(refs)
    carried = None if fresh else [refs.pop(0) for _ in range(4)]
    x_turned_in = None if fresh else refs.pop(0)
    wg, wu, wd = refs[:3]
    refs = refs[3:]
    outs = refs[: 2 * (steps // per)]
    refs = refs[2 * (steps // per) :]
    own_back, par_back, own_mix, par_mix = refs[:4]
    refs = refs[4:]
    x_turned = refs.pop(0) if fresh else x_turned_in
    x_all, dy_all, back, mix, pulls, spread = refs
    step = pl.program_id(0)
    rows, model = x_own.shape
    wide = own_back.shape[1] - model

    @pl.when(step == 0)
    def _():
        x_all[:rows] = x_own[...]
        x_all[rows:] = x_par[...]
        dy_all[:rows] = dy_own[...]
        dy_all[rows:] = dy_par[...]
        if fresh:
            x_turned[...] = jnp.transpose(x_all[...])
            back[...] = jnp.zeros_like(back)
            mix[...] = jnp.zeros_like(mix)
            pulls[...] = jnp.zeros_like(pulls)
        else:
            back[:rows] = carried[0][:, :model].astype(F32)
            back[rows:] = carried[1][:, :model].astype(F32)
            pulls[:rows] = carried[0][:, model:].astype(F32)
            pulls[rows:] = carried[1][:, model:].astype(F32)
            mix[:rows] = carried[2][...].astype(F32)
            mix[rows:] = carried[3][...].astype(F32)

    lane = lax.broadcasted_iota(jnp.int32, (2 * rows, wide), 1) == where_ref[0] + lo + step
    gate_rows = jnp.concatenate([g_own[...], g_par[...]], axis=0)
    gate = jnp.sum(jnp.where(lane, gate_rows, 0.0), axis=-1, keepdims=True)
    x, dy = x_all[...], dy_all[...]
    w_g, w_u, w_d = wg[0], wu[0], wd[0]
    g, u = mm(x, w_g), mm(x, w_u)
    pull = mm(dy, w_d)
    sig = 1.0 / (1.0 + jnp.exp(-g))
    act = g * sig
    hidden = (act * u).astype(BF16).astype(F32)
    pulls[...] += jnp.where(lane, jnp.sum(hidden * pull, axis=-1, keepdims=True), 0.0)
    weighted = (gate * hidden).astype(BF16)
    pull = gate * pull
    d_g = (pull * u * sig * (1.0 + g * (1.0 - sig))).astype(BF16)
    d_u = (pull * act).astype(BF16)
    back[...] += mm_t(d_g, w_g) + mm_t(d_u, w_u)
    mix[...] += mm_t(weighted, w_d)
    blocks, depth, _ = spread.shape
    half = g.shape[1]
    turned = x_turned[...]
    spread[:, :, :half] = mm(turned, d_g).astype(BF16).reshape(blocks, depth, half)
    spread[:, :, half : 2 * half] = mm(turned, d_u).astype(BF16).reshape(blocks, depth, half)
    spread[:, :, 2 * half :] = mm(dy_turned[...], weighted).astype(BF16).reshape(blocks, depth, half)
    side = where_ref[1]
    for i in range(steps // per):

        @pl.when(step // per == i)
        def _(i=i):
            for z in range(blocks // 2):
                outs[2 * i][z, 0] = spread[2 * z + side]
                outs[2 * i + 1][z, 0] = spread[2 * z + 1 - side]

    @pl.when(step == steps - 1)
    def _():
        own_back[:, :model] = back[:rows].astype(BF16)
        par_back[:, :model] = back[rows:].astype(BF16)
        own_back[:, model:] = pulls[:rows].astype(BF16)
        par_back[:, model:] = pulls[rows:].astype(BF16)
        own_mix[...] = mix[:rows].astype(BF16)
        par_mix[...] = mix[rows:].astype(BF16)


def experts(lo, hi, per, blocks, where, x_own, x_par, dy_own, dy_par, dy_turned, g_own, g_par, carried, wg, wu, wd):
    rows, model = x_own.shape
    half = wg.shape[2]
    depth = model // blocks
    fresh = carried is None
    pairs = (hi - lo) // per
    once = lambda shape: pl.BlockSpec(shape, lambda e, *_: (0,) * len(shape))
    wspec = pl.BlockSpec((1, model, half), lambda e, *_: (lo + e, 0, 0))

    def out_spec(i):
        return pl.BlockSpec(
            (blocks // 2, 1, depth, 3 * half), lambda e, *_: (0, jnp.clip(e - i * per, 0, per - 1), 0, 0)
        )

    ins = [x_own, x_par, dy_own, dy_par, dy_turned, g_own, g_par] + ([] if fresh else list(carried))
    outs, specs = [], []
    for i in range(pairs):
        outs += [shape_of((blocks // 2, per, depth, 3 * half), BF16)] * 2
        specs += [out_spec(i)] * 2
    tail = [shape_of((rows, model + LANES), BF16)] * 2 + [shape_of((rows, model), BF16)] * 2
    if fresh:
        tail.append(shape_of((model, 2 * rows), BF16))
    outs += tail
    specs += [once(t.shape) for t in tail]
    n = hi - lo
    got = pl.pallas_call(
        functools.partial(experts_body, lo, hi, per, fresh),
        out_shape=tuple(outs),
        grid_spec=pltpu.PrefetchScalarGridSpec(
            num_scalar_prefetch=1,
            grid=(n,),
            in_specs=[once(a.shape) for a in ins] + [wspec] * 3,
            out_specs=tuple(specs),
            scratch_shapes=[
                pltpu.VMEM((2 * rows, model), BF16),
                pltpu.VMEM((2 * rows, model), BF16),
                pltpu.VMEM((2 * rows, model), F32),
                pltpu.VMEM((2 * rows, model), F32),
                pltpu.VMEM((2 * rows, LANES), F32),
                pltpu.VMEM((blocks, depth, 3 * half), BF16),
            ],
        ),
        compiler_params=params(),
        cost_estimate=cost(n * 18 * 2 * rows * model * half, n * 12 * model * half),
        name="experts",
    )(where, *ins, wg, wu, wd)
    chunks = [(got[2 * i], got[2 * i + 1]) for i in range(pairs)]
    return chunks, got[2 * pairs :]


def middle_back_body(mine, other, middle, dy, gates, router, gain, w_out, normed, grad, low, heads, small):
    model = middle.shape[1]
    total = mine[...].astype(F32) + other[...].astype(F32)
    gate, pulls = gates[...], total[:, model:]
    chosen = gate * (pulls - jnp.sum(gate * pulls, axis=-1, keepdims=True))
    high, rest = two_parts(chosen)
    grad_two = total[:, :model] + (mm_t(high, router[...]) + mm_t(rest, router[...]))
    unit, scale = unit_rows(middle[...])
    small[:LANES, :] = t_mm(high, normed[...]) + t_mm(rest, normed[...])
    small[LANES : LANES + 8, :] = jnp.broadcast_to(jnp.sum(grad_two * unit, axis=0, keepdims=True), (8, model))
    scaled = grad_two * gain[...]
    out = dy[...].astype(F32) + scale * (scaled - unit * jnp.mean(scaled * unit, axis=-1, keepdims=True))
    grad[...] = out
    rounded = out.astype(BF16)
    low[...] = rounded
    heads[...] = mm(rounded, w_out[...]).astype(BF16)


def middle_back(mine, other, middle, dy, gates, router, gain, w_out, normed):
    rows, model = middle.shape
    return pl.pallas_call(
        middle_back_body,
        out_shape=(
            shape_of((rows, model), F32),
            shape_of((rows, model), BF16),
            shape_of((rows, w_out.shape[1]), BF16),
            shape_of((LANES + 8, model), F32),
        ),
        compiler_params=params(),
        cost_estimate=cost(2 * rows * model * (w_out.shape[1] + 4 * LANES), 10e6),
        name="middle_back",
    )(mine, other, middle, dy, gates, router, gain, w_out, normed)


def project_back_body(width, act, dq, a, b, c, cosine, sine, wq, wk, wv, part, dkv, gain_row):
    total = a[...].astype(F32) + b[...].astype(F32) + c[...].astype(F32)
    dk = rope_back(total[:, :width], widen(cosine[...], width), widen(sine[...], width)).astype(BF16)
    dv = total[:, width:].astype(BF16)
    dkv[:, :width] = dk
    dkv[:, width:] = dv
    full = mm_t(dq[...], wq[...]) + mm_t(dk, wk[...]) + mm_t(dv, wv[...])
    part[...] = full.astype(BF16)
    unit, _ = unit_rows(act[...].astype(F32))
    gain_row[...] = jnp.broadcast_to(jnp.sum(full * unit, axis=0, keepdims=True), gain_row.shape)


def project_back(act, dq, a, b, c, cosine, sine, wq, wk, wv):
    rows, model = act.shape
    width = wk.shape[1]
    return pl.pallas_call(
        functools.partial(project_back_body, width),
        out_shape=(
            shape_of((rows, model), BF16),
            shape_of((rows, 2 * width), BF16),
            shape_of((8, model), F32),
        ),
        compiler_params=params(),
        cost_estimate=cost(2 * rows * model * (wq.shape[1] + 2 * width), 8e6),
        name="project_back",
    )(act, dq, a, b, c, cosine, sine, wq, wk, wv)


def input_body(act, grad, mine, other, gain, out):
    unit, scale = unit_rows(act[...].astype(F32))
    scaled = (mine[...].astype(F32) + other[...].astype(F32)) * gain[...]
    out[...] = grad[...] + scale * (scaled - unit * jnp.mean(scaled * unit, axis=-1, keepdims=True))


def input_of(act, grad, mine, other, gain):
    return pl.pallas_call(
        input_body,
        out_shape=shape_of(act.shape, F32),
        compiler_params=params(),
        cost_estimate=cost(0, 12 * act.shape[0] * act.shape[1]),
        name="input_grad",
    )(act, grad, mine, other, gain)


def weights_body(blocks, count, where_ref, *refs):
    lefts = refs[:count]
    rights = refs[count : 2 * count]
    extra = refs[2 * count : -3]
    keep, send, whole = refs[-3:]
    parts = [t_mm(a[...], b[...]).astype(BF16) for a, b in zip(lefts, rights)]
    parts += [jnp.transpose(e[...]).astype(BF16) for e in extra]
    at = 0
    for part in parts:
        width = part.shape[1]
        whole[:, :, at : at + width] = part.reshape(2 * blocks, -1, width)
        at += width
    mine, side = where_ref[0], where_ref[1]
    for half, ref in ((mine, keep), (1 - mine, send)):
        for z in range(blocks // 2):
            ref[0, z] = whole[half * blocks + 2 * z + side]
            ref[1, z] = whole[half * blocks + 2 * z + 1 - side]


def weights(where, blocks, pairs, extra=()):
    model = pairs[0][0].shape[1]
    rows = pairs[0][0].shape[0]
    depth = model // (2 * blocks)
    columns = sum(b.shape[1] for _, b in pairs) + sum(e.shape[0] for e in extra)
    shape = (2, blocks // 2, depth, columns)
    ins = [a for a, _ in pairs] + [b for _, b in pairs] + list(extra)
    full = lambda a: pl.BlockSpec(a.shape, lambda i, *_: (0,) * len(a.shape))
    return pl.pallas_call(
        functools.partial(weights_body, blocks, len(pairs)),
        out_shape=(shape_of(shape, BF16),) * 2,
        grid_spec=pltpu.PrefetchScalarGridSpec(
            num_scalar_prefetch=1,
            grid=(1,),
            in_specs=[full(a) for a in ins],
            out_specs=(pl.BlockSpec(shape, lambda i, *_: (0, 0, 0, 0)),) * 2,
            scratch_shapes=[pltpu.VMEM((2 * blocks, depth, columns), BF16)],
        ),
        compiler_params=params(),
        cost_estimate=cost(2 * rows * model * columns, 4 * model * columns),
        name="weights",
    )(where, *ins)


def swap(v, axis):
    size = lax.axis_size(axis)
    return lax.ppermute(v, axis, [(i, i ^ 1) for i in range(size)])


def up(v, low, high):
    return lax.ppermute(v, "cp", [(2 * z + s, 2 * z + 2 + s) for z in range(low, high) for s in range(2)])


def down(v, low, high):
    return lax.ppermute(v, "cp", [(2 * z + s, 2 * z - 2 + s) for z in range(low, high) for s in range(2)])


def total_of(terms):
    return functools.reduce(lambda a, b: a + b, [t.astype(F32) for t in terms])


def line_sum(parts, z, length):
    def own(d):
        return [lax.dynamic_index_in_dim(p, jnp.clip(d, 0, length - 1), 0, keepdims=False) for p in parts]

    if length > 4:
        mine = total_of(parts).astype(BF16)
        side = lax.axis_index("cp") % 2
        full = jnp.where(jnp.arange(2).reshape((1, 2) + (1,) * (mine.ndim - 1)) == side, mine[:, None], 0)
        full = full.reshape((2 * length,) + mine.shape[1:])
        return lax.psum_scatter(full, "cp", scatter_dimension=0, tiled=True)[0].astype(F32)
    right = left = None
    for k in range(length - 1):
        far = length - 1 - k
        terms = own(z + far) + ([] if right is None else [right])
        right = up(total_of(terms).astype(BF16), 0, k + 1)
        terms = own(z - far) + ([] if left is None else [left])
        left = down(total_of(terms).astype(BF16), far, length)
    return total_of(own(z) + ([right, left] if length > 1 else []))


def on_device(
    activations,
    cotangent,
    positions,
    routes,
    w_query,
    w_key,
    value_weight,
    w_out,
    gain_attn,
    gain_moe,
    w_router,
    w_gate_up,
    w_down,
):
    seqs, rows, model = activations.shape
    total = seqs * rows
    width = w_key.shape[1]
    group = w_query.shape[1] // width
    expert_count = w_router.shape[1]
    local = w_gate_up.shape[0]
    half = w_down.shape[2]
    blocks = lax.axis_size("cp")
    length = blocks // 2
    here = lax.axis_index("cp")
    z, side = here // 2, here % 2
    mine = lax.axis_index("ep")
    act = activations.reshape(total, model)
    dy = cotangent.reshape(total, model)
    gain_one, gain_two = gain_attn.reshape(1, model), gain_moe.reshape(1, model)

    frequency = jnp.power(10000.0, -(jnp.arange(HEAD // 2, dtype=F32) * 2.0 / HEAD))
    angles = positions.reshape(total, 1).astype(F32) * frequency
    cosine = jnp.tile(jnp.cos(angles), (1, 2 * LANES // HEAD))
    sine = jnp.tile(jnp.sin(angles), (1, 2 * LANES // HEAD))

    normed, q, kv = project(act, gain_one, w_query, w_key, value_weight, cosine, sine)
    q = q.reshape(seqs, rows, -1)
    kv = kv.reshape(1, seqs, rows, 2 * width)
    offset = (here * rows).astype(jnp.int32).reshape(1)
    if length == 4:
        slots, homes = [kv, swap(kv, "cp")], [(z, side), (z, 1 - side)]
        travel = kv
        for r in range(1, length):
            travel = up(travel, r - 1, length - 1)
            slots += [travel, swap(travel, "cp")]
            homes += [(z - r, side), (z - r, 1 - side)]
        first = jnp.stack([jnp.where(a >= 0, (2 * a + b) * rows, 2**24) for a, b in homes]).astype(jnp.int32)
    else:
        slots = [lax.all_gather(kv, "cp", axis=0, tiled=True)]
        first = jnp.arange(blocks, dtype=jnp.int32) * rows
    place = positions.reshape(seqs, 1, rows)

    dy_par = swap(dy, "ep")
    dy_turned = jnp.concatenate([dy, dy_par], axis=0).T
    w_g, w_u = w_gate_up[:, :, 0, :], w_gate_up[:, :, 1, :]
    lanes = jnp.arange(LANES, dtype=jnp.int32)
    hot = jnp.sum((routes.reshape(total, -1, 1) == lanes).astype(F32), axis=1)
    router = jnp.pad(w_router, ((0, 0), (0, LANES - expert_count)))

    low, attended, lse = attend(q, place, slots, first, offset, group)
    low = low.reshape(total, -1)
    part = out_project(low, w_out)
    middle, normed_two, gates = middle_of(act, part, swap(part, "tp"), gain_two, router, hot)
    x_par, gates_par = swap(normed_two, "ep"), swap(gates, "ep")

    where = jnp.stack([mine * local, side]).astype(jnp.int32)
    args = (blocks, where, normed_two, x_par, dy, dy_par, dy_turned, gates, gates_par)
    cut = 2
    chunks, carried = experts(0, cut, 2, *args, None, w_g, w_u, w_down)
    more, (own_back, par_back, own_mix, par_mix) = experts(cut, local, 2, *args, carried, w_g, w_u, w_down)
    chunks = chunks + more

    back = total_of([own_back, swap(par_back, "ep")]).astype(BF16)
    grad_middle, branch, grad_heads, small = middle_back(
        back, swap(back, "tp"), middle, dy, gates, router, gain_two, w_out, normed_two
    )
    dq, grads = attend_back(
        q,
        place,
        grad_heads.reshape(q.shape),
        attended,
        lse,
        cosine.reshape(seqs, rows, -1),
        sine.reshape(seqs, rows, -1),
        slots,
        first,
        offset,
        group,
    )
    dq = dq.reshape(total, -1)
    if length == 4:
        arriving = None
        for r in range(length - 1, 0, -1):
            terms = [grads[2 * r], swap(grads[2 * r + 1], "cp")] + ([] if arriving is None else [arriving])
            arriving = down(total_of(terms).astype(BF16), r, length)
        kv_terms = [grads[0], swap(grads[1], "cp"), arriving]
    else:
        kv_sum = lax.psum_scatter(grads[0], "cp", scatter_dimension=0, tiled=True)
        kv_terms = [kv_sum, jnp.zeros_like(kv_sum), jnp.zeros_like(kv_sum)]
    kv_terms = [t.reshape(total, 2 * width) for t in kv_terms]

    spots = jnp.stack([mine, side]).astype(jnp.int32)
    big = weights(spots, blocks, [(branch, low), (normed, dq)])
    normed_part, dkv, gain_row = project_back(
        act, dq, *kv_terms, cosine, sine, w_query, w_key, value_weight
    )
    small = jnp.concatenate([small[:expert_count], small[LANES : LANES + 1], gain_row[:1]], axis=0)
    small = jnp.pad(small, ((0, LANES - small.shape[0]), (0, 0)))
    little = weights(spots, blocks, [(normed, dkv)], (small,))
    input_grad = input_of(act, grad_middle, normed_part, swap(normed_part, "tp"), gain_one)

    mix = total_of([own_mix, swap(par_mix, "ep")]).astype(BF16)
    output = middle + total_of([mix, swap(mix, "tp")])

    def spread_sum(keep, send):
        both = total_of([keep, swap(send, "ep")]).astype(BF16)
        return line_sum([both[0], swap(both[1], "cp")], z, length)

    sums = [line_sum([keep, swap(send, "cp")], z, length) for keep, send in chunks]
    expert_grad = jnp.concatenate(sums, axis=0)
    gate_up_grad = expert_grad[:, :, : 2 * half].reshape(local, -1, 2, half)
    down_grad = expert_grad[:, :, 2 * half :]
    big = spread_sum(*big)
    little = spread_sum(*little)
    wide = w_query.shape[1]
    gain_part = little[:, 2 * width + expert_count + 1]
    return (
        output.reshape(activations.shape),
        input_grad.reshape(activations.shape),
        big[:, wide:],
        little[:, :width],
        little[:, width : 2 * width],
        big[:, :wide],
        gain_part + swap(gain_part, "tp"),
        little[:, 2 * width + expert_count],
        little[:, 2 * width : 2 * width + expert_count],
        gate_up_grad,
        down_grad,
    )


def solution(mesh):
    in_specs = (
        P("ep", "cp", None),
        P("ep", "cp", None),
        P("ep", "cp"),
        P("ep", "cp", None),
        P(None, "tp"),
        P(None, "tp"),
        P(None, "tp"),
        P(None, "tp"),
        P(),
        P(),
        P(),
        P("ep", None, None, "tp"),
        P("ep", None, "tp"),
    )
    out_specs = (
        P("ep", "cp", None),
        P("ep", "cp", None),
        P(("ep", "cp"), "tp"),
        P(("ep", "cp"), "tp"),
        P(("ep", "cp"), "tp"),
        P(("ep", "cp"), "tp"),
        P(("ep", "cp")),
        P(("ep", "cp")),
        P(("ep", "cp"), None),
        P("ep", "cp", None, "tp"),
        P("ep", "cp", "tp"),
    )
    return jax.shard_map(
        on_device, mesh=mesh, in_specs=in_specs, out_specs=out_specs, check_vma=False
    )
```

```python
import functools

import jax
import jax.numpy as jnp
from jax import lax
from jax.experimental import pallas as pl
from jax.experimental.pallas import tpu as pltpu
from jax.sharding import PartitionSpec as P

HEAD = 64
EPS = 1e-06
NEG = -1e30
SCALE = 0.125
LANES = 128
KEY_CHUNK = 1024
F32 = jnp.float32
BF16 = jnp.bfloat16


def mm(a, b):
    return lax.dot_general(a, b, (((1,), (0,)), ((), ())), preferred_element_type=F32)


def mm_t(a, b):
    return lax.dot_general(a, b, (((1,), (1,)), ((), ())), preferred_element_type=F32)


def t_mm(a, b):
    return lax.dot_general(a, b, (((0,), (0,)), ((), ())), preferred_element_type=F32)


def two_parts(v):
    high = v.astype(BF16)
    return high, (v - high.astype(F32)).astype(BF16)


def halves_turned(v, back):
    width = v.shape[1]
    ahead = pltpu.roll(v, width - HEAD // 2, 1)
    behind = pltpu.roll(v, HEAD // 2, 1)
    first = lax.broadcasted_iota(jnp.int32, v.shape, 1) % HEAD < HEAD // 2
    if back:
        return jnp.where(first, ahead, -behind)
    return jnp.where(first, -ahead, behind)


def rope(v, cosine, sine):
    return v * cosine + halves_turned(v, False) * sine


def rope_back(v, cosine, sine):
    return v * cosine + halves_turned(v * sine, True)


def widen(table, width):
    return jnp.concatenate([table] * (width // table.shape[1]), axis=1)


def unit_rows(v):
    scale = lax.rsqrt(jnp.mean(v * v, axis=-1, keepdims=True) + EPS)
    return v * scale, scale


def shape_of(shape, dtype):
    return jax.ShapeDtypeStruct(shape, dtype)


def params(**kw):
    return pltpu.CompilerParams(vmem_limit_bytes=60 * 2**20, **kw)


def cost(flops, moved):
    return pl.CostEstimate(flops=int(flops), bytes_accessed=int(moved), transcendentals=0)


def project_body(act, gain, wq, wk, wv, cosine, sine, normed, q, kv):
    unit, _ = unit_rows(act[...].astype(F32))
    low = (unit * gain[...]).astype(BF16)
    normed[...] = low
    qf = mm(low, wq[...])
    q[...] = rope(qf, widen(cosine[...], qf.shape[1]), widen(sine[...], qf.shape[1])).astype(BF16)
    kf = mm(low, wk[...])
    width = kf.shape[1]
    kv[:, :width] = rope(kf, widen(cosine[...], width), widen(sine[...], width)).astype(BF16)
    kv[:, width:] = mm(low, wv[...]).astype(BF16)


def project(act, gain, wq, wk, wv, cosine, sine):
    rows, model = act.shape
    total = wq.shape[1] + 2 * wk.shape[1]
    return pl.pallas_call(
        project_body,
        out_shape=(
            shape_of((rows, model), BF16),
            shape_of((rows, wq.shape[1]), BF16),
            shape_of((rows, 2 * wk.shape[1]), BF16),
        ),
        compiler_params=params(),
        cost_estimate=cost(2 * rows * model * total, 2 * model * total + 6 * rows * model),
        name="project",
    )(act, gain, wq, wk, wv, cosine, sine)


def fill_keys(first_ref, offset_ref, place, slots, keys, bias, rows):
    at = 0
    query = lax.broadcasted_iota(jnp.int32, (rows, rows), 1) + offset_ref[0]
    for slot in slots:
        for one in range(slot.shape[0]):
            keys[at * rows : (at + 1) * rows, :] = slot[one, 0]
            key = lax.broadcasted_iota(jnp.int32, (rows, rows), 0) + first_ref[at]
            distance = query - key
            seen = (distance >= 0) & (distance <= place)
            bias[at * rows : (at + 1) * rows, :] = jnp.where(seen, 0.0, NEG)
            at += 1


def group_rows(block, head, group):
    return jnp.concatenate(
        [block[:, (head * group + g) * HEAD : (head * group + g + 1) * HEAD] for g in range(group)], axis=0
    )


def attend_body(group, count, first_ref, offset_ref, q_ref, place_ref, *refs):
    slots = refs[:count]
    low_ref, out_ref, lse_ref, keys, bias = refs[count:]
    rows = q_ref.shape[1]
    fill_keys(first_ref, offset_ref, place_ref[0], slots, keys, bias, rows)
    total, width = keys.shape[0], keys.shape[1] // 2
    chunk = min(total, KEY_CHUNK)
    q = (q_ref[0].astype(F32) * SCALE).astype(BF16)
    pieces = []
    for head in range(width // HEAD):
        q3 = group_rows(q, head, group)
        top = run = out = None
        for low in range(0, total, chunk):
            k = keys[low : low + chunk, head * HEAD : (head + 1) * HEAD]
            v = keys[low : low + chunk, width + head * HEAD : width + (head + 1) * HEAD]
            s = mm_t(k, q3) + widen(bias[low : low + chunk, :], group * rows)
            here = jnp.max(s, axis=0, keepdims=True)
            new = here if top is None else jnp.maximum(top, here)
            p = jnp.exp(s - new)
            part = jnp.sum(p, axis=0, keepdims=True)
            o = t_mm(v, p.astype(BF16))
            if top is None:
                run, out = part, o
            else:
                shrink = jnp.exp(top - new)
                run, out = run * shrink + part, out * shrink + o
            top = new
        out = jnp.transpose(out / run)
        pieces += [out[g * rows : (g + 1) * rows] for g in range(group)]
        lse_ref[0, head : head + 1, :] = top + jnp.log(run)
    whole = jnp.concatenate(pieces, axis=1)
    out_ref[0] = whole
    low_ref[0] = whole.astype(BF16)


def seq_block(shape):
    return pl.BlockSpec((1,) + shape[1:], lambda s, *_: (s,) + (0,) * (len(shape) - 1))


def slot_block(shape):
    return pl.BlockSpec((shape[0], 1) + shape[2:], lambda s, *_: (0, s, 0, 0))


def attend(q, place, slots, first, offset, group):
    seqs, rows, wide = q.shape
    both = slots[0].shape[-1]
    total = rows * sum(slot.shape[0] for slot in slots)
    heads = wide // HEAD // group
    outs = (
        shape_of(q.shape, BF16),
        shape_of(q.shape, F32),
        shape_of((seqs, heads, group * rows), F32),
    )
    return pl.pallas_call(
        functools.partial(attend_body, group, len(slots)),
        out_shape=outs,
        grid_spec=pltpu.PrefetchScalarGridSpec(
            num_scalar_prefetch=2,
            grid=(seqs,),
            in_specs=[seq_block(q.shape), seq_block(place.shape)] + [slot_block(s.shape) for s in slots],
            out_specs=tuple(seq_block(o.shape) for o in outs),
            scratch_shapes=[pltpu.VMEM((total, both), BF16), pltpu.VMEM((total, rows), F32)],
        ),
        compiler_params=params(),
        cost_estimate=cost(2e9 * 4, 20e6),
        name="attend",
    )(first, offset, q, place, *slots)


def attend_back_body(
    group, count, first_ref, offset_ref, q_ref, place_ref, grad_ref, out_ref, lse_ref, cos_ref, sin_ref, *refs
):
    slots = refs[:count]
    dq_ref = refs[count]
    grads = refs[count + 1 : 2 * count + 1]
    keys, bias = refs[2 * count + 1 :]
    rows = q_ref.shape[1]
    fill_keys(first_ref, offset_ref, place_ref[0], slots, keys, bias, rows)
    total, width = keys.shape[0], keys.shape[1] // 2
    chunk = min(total, KEY_CHUNK)
    q = (q_ref[0].astype(F32) * SCALE).astype(BF16)
    go = grad_ref[0]
    products = go.astype(F32) * out_ref[0]
    ones = jnp.ones((8, HEAD), F32)
    heads = width // HEAD
    q3s = [group_rows(q, head, group) for head in range(heads)]
    g3s = [group_rows(go, head, group) for head in range(heads)]
    deltas = [
        lax.dot_general(
            ones,
            group_rows(products, head, group),
            (((1,), (1,)), ((), ())),
            preferred_element_type=F32,
            precision=lax.Precision.HIGHEST,
        )[:1]
        for head in range(heads)
    ]
    dq = [None] * heads
    for low in range(0, total, chunk):
        dks, dvs = [], []
        for head in range(heads):
            k = keys[low : low + chunk, head * HEAD : (head + 1) * HEAD]
            v = keys[low : low + chunk, width + head * HEAD : width + (head + 1) * HEAD]
            s = mm_t(k, q3s[head]) + widen(bias[low : low + chunk, :], group * rows)
            p = jnp.exp(s - lse_ref[0, head : head + 1, :])
            dp = mm_t(v, g3s[head])
            ds = (p * (dp - deltas[head])).astype(BF16)
            dks.append(mm(ds, q3s[head]))
            dvs.append(mm(p.astype(BF16), g3s[head]))
            part = t_mm(k, ds)
            dq[head] = part if dq[head] is None else dq[head] + part
        both = jnp.concatenate(dks + dvs, axis=1).astype(BF16)
        at = low // rows
        done = 0
        for ref in grads:
            for one in range(ref.shape[0]):
                if at <= done < at + chunk // rows:
                    ref[one, 0] = both[(done - at) * rows : (done - at + 1) * rows]
                done += 1
    pieces = []
    for head in range(heads):
        back = jnp.transpose(dq[head] * SCALE)
        pieces += [back[g * rows : (g + 1) * rows] for g in range(group)]
    whole = jnp.concatenate(pieces, axis=1)
    cosine, sine = widen(cos_ref[0], whole.shape[1]), widen(sin_ref[0], whole.shape[1])
    dq_ref[0] = rope_back(whole, cosine, sine).astype(BF16)


def attend_back(q, place, grad, out, lse, cosine, sine, slots, first, offset, group):
    seqs, rows, _ = q.shape
    both = slots[0].shape[-1]
    total = rows * sum(slot.shape[0] for slot in slots)
    outs = (shape_of(q.shape, BF16),) + tuple(shape_of(s.shape, BF16) for s in slots)
    ins = (q, place, grad, out, lse, cosine, sine)
    got = pl.pallas_call(
        functools.partial(attend_back_body, group, len(slots)),
        out_shape=outs,
        grid_spec=pltpu.PrefetchScalarGridSpec(
            num_scalar_prefetch=2,
            grid=(seqs,),
            in_specs=[seq_block(a.shape) for a in ins] + [slot_block(s.shape) for s in slots],
            out_specs=(seq_block(outs[0].shape),) + tuple(slot_block(s.shape) for s in slots),
            scratch_shapes=[pltpu.VMEM((total, both), BF16), pltpu.VMEM((total, rows), F32)],
        ),
        compiler_params=params(),
        cost_estimate=cost(2e9 * 8, 30e6),
        name="attend_back",
    )(first, offset, *ins, *slots)
    return got[0], got[1:]


def out_body(low, w_out, part):
    part[...] = mm_t(low[...], w_out[...]).astype(BF16)


def out_project(low, w_out):
    rows, model = low.shape[0], w_out.shape[0]
    return pl.pallas_call(
        out_body,
        out_shape=shape_of((rows, model), BF16),
        compiler_params=params(),
        cost_estimate=cost(2 * rows * model * low.shape[1], 4e6),
        name="out_project",
    )(low, w_out)


def middle_body(act, part, other, gain, router, hot, middle, normed, gates):
    mid = act[...].astype(F32) + (part[...].astype(F32) + other[...].astype(F32))
    middle[...] = mid
    unit, _ = unit_rows(mid)
    low = (unit * gain[...]).astype(BF16)
    normed[...] = low
    chosen = hot[...] > 0.5
    logits = jnp.where(chosen, mm(low, router[...]), NEG)
    up = jnp.where(chosen, jnp.exp(logits - jnp.max(logits, axis=-1, keepdims=True)), 0.0)
    gates[...] = up / jnp.sum(up, axis=-1, keepdims=True)


def middle_of(act, part, other, gain, router, hot):
    rows, model = act.shape
    return pl.pallas_call(
        middle_body,
        out_shape=(shape_of((rows, model), F32), shape_of((rows, model), BF16), shape_of((rows, LANES), F32)),
        compiler_params=params(),
        cost_estimate=cost(2 * rows * model * LANES, 12 * rows * model),
        name="middle",
    )(act, part, other, gain, router, hot)


def experts_body(
    lo, hi, per, fresh, where_ref, x_own, x_par, dy_own, dy_par, dy_turned, g_own, g_par, *refs
):
    steps = hi - lo
    refs = list(refs)
    carried = None if fresh else [refs.pop(0) for _ in range(4)]
    x_turned_in = None if fresh else refs.pop(0)
    wg, wu, wd = refs[:3]
    refs = refs[3:]
    outs = refs[: 2 * (steps // per)]
    refs = refs[2 * (steps // per) :]
    own_back, par_back, own_mix, par_mix = refs[:4]
    refs = refs[4:]
    x_turned = refs.pop(0) if fresh else x_turned_in
    x_all, dy_all, back, mix, pulls, spread = refs
    step = pl.program_id(0)
    rows, model = x_own.shape
    wide = own_back.shape[1] - model

    @pl.when(step == 0)
    def _():
        x_all[:rows] = x_own[...]
        x_all[rows:] = x_par[...]
        dy_all[:rows] = dy_own[...]
        dy_all[rows:] = dy_par[...]
        if fresh:
            x_turned[...] = jnp.transpose(x_all[...])
            back[...] = jnp.zeros_like(back)
            mix[...] = jnp.zeros_like(mix)
            pulls[...] = jnp.zeros_like(pulls)
        else:
            back[:rows] = carried[0][:, :model].astype(F32)
            back[rows:] = carried[1][:, :model].astype(F32)
            pulls[:rows] = carried[0][:, model:].astype(F32)
            pulls[rows:] = carried[1][:, model:].astype(F32)
            mix[:rows] = carried[2][...].astype(F32)
            mix[rows:] = carried[3][...].astype(F32)

    lane = lax.broadcasted_iota(jnp.int32, (2 * rows, wide), 1) == where_ref[0] + lo + step
    gate_rows = jnp.concatenate([g_own[...], g_par[...]], axis=0)
    gate = jnp.sum(jnp.where(lane, gate_rows, 0.0), axis=-1, keepdims=True)
    x, dy = x_all[...], dy_all[...]
    w_g, w_u, w_d = wg[0], wu[0], wd[0]
    g, u = mm(x, w_g), mm(x, w_u)
    pull = mm(dy, w_d)
    sig = 1.0 / (1.0 + jnp.exp(-g))
    act = g * sig
    hidden = (act * u).astype(BF16).astype(F32)
    pulls[...] += jnp.where(lane, jnp.sum(hidden * pull, axis=-1, keepdims=True), 0.0)
    weighted = (gate * hidden).astype(BF16)
    pull = gate * pull
    d_g = (pull * u * sig * (1.0 + g * (1.0 - sig))).astype(BF16)
    d_u = (pull * act).astype(BF16)
    back[...] += mm_t(d_g, w_g) + mm_t(d_u, w_u)
    mix[...] += mm_t(weighted, w_d)
    blocks, depth, _ = spread.shape
    half = g.shape[1]
    turned = x_turned[...]
    spread[:, :, :half] = mm(turned, d_g).astype(BF16).reshape(blocks, depth, half)
    spread[:, :, half : 2 * half] = mm(turned, d_u).astype(BF16).reshape(blocks, depth, half)
    spread[:, :, 2 * half :] = mm(dy_turned[...], weighted).astype(BF16).reshape(blocks, depth, half)
    side = where_ref[1]
    for i in range(steps // per):

        @pl.when(step // per == i)
        def _(i=i):
            for z in range(blocks // 2):
                outs[2 * i][z, 0] = spread[2 * z + side]
                outs[2 * i + 1][z, 0] = spread[2 * z + 1 - side]

    @pl.when(step == steps - 1)
    def _():
        own_back[:, :model] = back[:rows].astype(BF16)
        par_back[:, :model] = back[rows:].astype(BF16)
        own_back[:, model:] = pulls[:rows].astype(BF16)
        par_back[:, model:] = pulls[rows:].astype(BF16)
        own_mix[...] = mix[:rows].astype(BF16)
        par_mix[...] = mix[rows:].astype(BF16)


def experts(lo, hi, per, blocks, where, x_own, x_par, dy_own, dy_par, dy_turned, g_own, g_par, carried, wg, wu, wd):
    rows, model = x_own.shape
    half = wg.shape[2]
    depth = model // blocks
    fresh = carried is None
    pairs = (hi - lo) // per
    once = lambda shape: pl.BlockSpec(shape, lambda e, *_: (0,) * len(shape))
    wspec = pl.BlockSpec((1, model, half), lambda e, *_: (lo + e, 0, 0))

    def out_spec(i):
        return pl.BlockSpec(
            (blocks // 2, 1, depth, 3 * half), lambda e, *_: (0, jnp.clip(e - i * per, 0, per - 1), 0, 0)
        )

    ins = [x_own, x_par, dy_own, dy_par, dy_turned, g_own, g_par] + ([] if fresh else list(carried))
    outs, specs = [], []
    for i in range(pairs):
        outs += [shape_of((blocks // 2, per, depth, 3 * half), BF16)] * 2
        specs += [out_spec(i)] * 2
    tail = [shape_of((rows, model + LANES), BF16)] * 2 + [shape_of((rows, model), BF16)] * 2
    if fresh:
        tail.append(shape_of((model, 2 * rows), BF16))
    outs += tail
    specs += [once(t.shape) for t in tail]
    n = hi - lo
    got = pl.pallas_call(
        functools.partial(experts_body, lo, hi, per, fresh),
        out_shape=tuple(outs),
        grid_spec=pltpu.PrefetchScalarGridSpec(
            num_scalar_prefetch=1,
            grid=(n,),
            in_specs=[once(a.shape) for a in ins] + [wspec] * 3,
            out_specs=tuple(specs),
            scratch_shapes=[
                pltpu.VMEM((2 * rows, model), BF16),
                pltpu.VMEM((2 * rows, model), BF16),
                pltpu.VMEM((2 * rows, model), F32),
                pltpu.VMEM((2 * rows, model), F32),
                pltpu.VMEM((2 * rows, LANES), F32),
                pltpu.VMEM((blocks, depth, 3 * half), BF16),
            ],
        ),
        compiler_params=params(),
        cost_estimate=cost(n * 18 * 2 * rows * model * half, n * 12 * model * half),
        name="experts",
    )(where, *ins, wg, wu, wd)
    chunks = [(got[2 * i], got[2 * i + 1]) for i in range(pairs)]
    return chunks, got[2 * pairs :]


def middle_back_body(mine, other, middle, dy, gates, router, gain, w_out, normed, grad, low, heads, small):
    model = middle.shape[1]
    total = mine[...].astype(F32) + other[...].astype(F32)
    gate, pulls = gates[...], total[:, model:]
    chosen = gate * (pulls - jnp.sum(gate * pulls, axis=-1, keepdims=True))
    high, rest = two_parts(chosen)
    grad_two = total[:, :model] + (mm_t(high, router[...]) + mm_t(rest, router[...]))
    unit, scale = unit_rows(middle[...])
    small[:LANES, :] = t_mm(high, normed[...]) + t_mm(rest, normed[...])
    small[LANES : LANES + 8, :] = jnp.broadcast_to(jnp.sum(grad_two * unit, axis=0, keepdims=True), (8, model))
    scaled = grad_two * gain[...]
    out = dy[...].astype(F32) + scale * (scaled - unit * jnp.mean(scaled * unit, axis=-1, keepdims=True))
    grad[...] = out
    rounded = out.astype(BF16)
    low[...] = rounded
    heads[...] = mm(rounded, w_out[...]).astype(BF16)


def middle_back(mine, other, middle, dy, gates, router, gain, w_out, normed):
    rows, model = middle.shape
    return pl.pallas_call(
        middle_back_body,
        out_shape=(
            shape_of((rows, model), F32),
            shape_of((rows, model), BF16),
            shape_of((rows, w_out.shape[1]), BF16),
            shape_of((LANES + 8, model), F32),
        ),
        compiler_params=params(),
        cost_estimate=cost(2 * rows * model * (w_out.shape[1] + 4 * LANES), 10e6),
        name="middle_back",
    )(mine, other, middle, dy, gates, router, gain, w_out, normed)


def project_back_body(width, act, dq, a, b, c, cosine, sine, wq, wk, wv, part, dkv, gain_row):
    total = a[...].astype(F32) + b[...].astype(F32) + c[...].astype(F32)
    dk = rope_back(total[:, :width], widen(cosine[...], width), widen(sine[...], width)).astype(BF16)
    dv = total[:, width:].astype(BF16)
    dkv[:, :width] = dk
    dkv[:, width:] = dv
    full = mm_t(dq[...], wq[...]) + mm_t(dk, wk[...]) + mm_t(dv, wv[...])
    part[...] = full.astype(BF16)
    unit, _ = unit_rows(act[...].astype(F32))
    gain_row[...] = jnp.broadcast_to(jnp.sum(full * unit, axis=0, keepdims=True), gain_row.shape)


def project_back(act, dq, a, b, c, cosine, sine, wq, wk, wv):
    rows, model = act.shape
    width = wk.shape[1]
    return pl.pallas_call(
        functools.partial(project_back_body, width),
        out_shape=(
            shape_of((rows, model), BF16),
            shape_of((rows, 2 * width), BF16),
            shape_of((8, model), F32),
        ),
        compiler_params=params(),
        cost_estimate=cost(2 * rows * model * (wq.shape[1] + 2 * width), 8e6),
        name="project_back",
    )(act, dq, a, b, c, cosine, sine, wq, wk, wv)


def input_body(act, grad, mine, other, gain, out):
    unit, scale = unit_rows(act[...].astype(F32))
    scaled = (mine[...].astype(F32) + other[...].astype(F32)) * gain[...]
    out[...] = grad[...] + scale * (scaled - unit * jnp.mean(scaled * unit, axis=-1, keepdims=True))


def input_of(act, grad, mine, other, gain):
    return pl.pallas_call(
        input_body,
        out_shape=shape_of(act.shape, F32),
        compiler_params=params(),
        cost_estimate=cost(0, 12 * act.shape[0] * act.shape[1]),
        name="input_grad",
    )(act, grad, mine, other, gain)


def weights_body(blocks, count, stacked, where_ref, *refs):
    lefts = refs[:count]
    rights = refs[count : 2 * count]
    extra = refs[2 * count : -3]
    keep, send, whole = refs[-3:]
    parts = [t_mm(a[...], b[...]).astype(BF16) for a, b in zip(lefts, rights)]
    parts += [jnp.transpose(e[...]).astype(BF16) for e in extra]
    at = down = 0
    for part in parts:
        block = part.reshape(2 * blocks, -1, part.shape[1])
        whole[:, down : down + block.shape[1], at : at + part.shape[1]] = block
        if stacked:
            down += block.shape[1]
        else:
            at += part.shape[1]
    mine, side = where_ref[0], where_ref[1]
    for half, ref in ((mine, keep), (1 - mine, send)):
        for z in range(blocks // 2):
            ref[0, z] = whole[half * blocks + 2 * z + side]
            ref[1, z] = whole[half * blocks + 2 * z + 1 - side]


def weights(where, blocks, pairs, extra=(), stacked=False):
    model = pairs[0][0].shape[1]
    rows = pairs[0][0].shape[0]
    depth = model // (2 * blocks)
    columns = sum(b.shape[1] for _, b in pairs) + sum(e.shape[0] for e in extra)
    tall, wide = (depth * len(pairs), pairs[0][1].shape[1]) if stacked else (depth, columns)
    shape = (2, blocks // 2, tall, wide)
    ins = [a for a, _ in pairs] + [b for _, b in pairs] + list(extra)
    full = lambda a: pl.BlockSpec(a.shape, lambda i, *_: (0,) * len(a.shape))
    return pl.pallas_call(
        functools.partial(weights_body, blocks, len(pairs), stacked),
        out_shape=(shape_of(shape, BF16),) * 2,
        grid_spec=pltpu.PrefetchScalarGridSpec(
            num_scalar_prefetch=1,
            grid=(1,),
            in_specs=[full(a) for a in ins],
            out_specs=(pl.BlockSpec(shape, lambda i, *_: (0, 0, 0, 0)),) * 2,
            scratch_shapes=[pltpu.VMEM((2 * blocks, tall, wide), BF16)],
        ),
        compiler_params=params(),
        cost_estimate=cost(2 * rows * model * columns, 4 * model * columns),
        name="weights",
    )(where, *ins)


def swap(v, axis):
    size = lax.axis_size(axis)
    return lax.ppermute(v, axis, [(i, i ^ 1) for i in range(size)])


def up(v, low, high):
    return lax.ppermute(v, "cp", [(2 * z + s, 2 * z + 2 + s) for z in range(low, high) for s in range(2)])


def down(v, low, high):
    return lax.ppermute(v, "cp", [(2 * z + s, 2 * z - 2 + s) for z in range(low, high) for s in range(2)])


def total_of(terms):
    return functools.reduce(lambda a, b: a + b, [t.astype(F32) for t in terms])


def line_sum(parts, z, length):
    def own(d):
        return [lax.dynamic_index_in_dim(p, jnp.clip(d, 0, length - 1), 0, keepdims=False) for p in parts]

    if length > 4:
        mine = total_of(parts).astype(BF16)
        side = lax.axis_index("cp") % 2
        full = jnp.where(jnp.arange(2).reshape((1, 2) + (1,) * (mine.ndim - 1)) == side, mine[:, None], 0)
        full = full.reshape((2 * length,) + mine.shape[1:])
        return lax.psum_scatter(full, "cp", scatter_dimension=0, tiled=True)[0].astype(F32)
    right = left = None
    for k in range(length - 1):
        far = length - 1 - k
        terms = own(z + far) + ([] if right is None else [right])
        right = up(total_of(terms).astype(BF16), 0, k + 1)
        terms = own(z - far) + ([] if left is None else [left])
        left = down(total_of(terms).astype(BF16), far, length)
    return total_of(own(z) + ([right, left] if length > 1 else []))


MESH = pl.DeviceIdType.MESH
LINE = 4


def add_to(ref, at, *others):
    total = ref[at].astype(F32)
    for other in others:
        total = total + other.astype(F32)
    ref[at] = total.astype(BF16)


class Place:
    def __init__(self):
        self.cp = lax.axis_index("cp")
        self.z, self.side = self.cp // 2, self.cp % 2
        self.ep, self.tp = lax.axis_index("ep"), lax.axis_index("tp")

    def to(self, way):
        if way == "x":
            return {"cp": self.cp + 1 - 2 * self.side}
        if way == "up":
            return {"cp": self.cp + 2}
        if way == "down":
            return {"cp": self.cp - 2}
        return {way: 1 - (self.ep if way == "ep" else self.tp)}

    def greet(self, ways):
        barrier = pltpu.get_barrier_semaphore()
        count = len(ways)
        for way in ways:
            pl.semaphore_signal(barrier, inc=1, device_id=self.to(way), device_id_type=MESH)
        if self.line:
            count = count + jnp.where(self.z > 0, 1, 0) + jnp.where(self.z < LINE - 1, 1, 0)

            @pl.when(self.z > 0)
            def _():
                pl.semaphore_signal(barrier, inc=1, device_id=self.to("down"), device_id_type=MESH)

            @pl.when(self.z < LINE - 1)
            def _():
                pl.semaphore_signal(barrier, inc=1, device_id=self.to("up"), device_id_type=MESH)

        pl.semaphore_wait(barrier, count)

    line = True

    def copy(self, way, src, dst, send, recv):
        return pltpu.make_async_remote_copy(
            src_ref=src, dst_ref=dst, send_sem=send, recv_sem=recv, device_id=self.to(way), device_id_type=MESH
        )


class Flow:
    def __init__(self, place, held, rights, lefts, send, recv):
        self.p, self.held, self.rights, self.lefts, self.send, self.recv = place, held, rights, lefts, send, recv

    def right(self, d):
        return self.p.copy("up", self.held.at[d], self.rights.at[d - 1], self.send.at[d - 1], self.recv.at[d - 1])

    def left(self, d):
        return self.p.copy("down", self.held.at[d], self.lefts.at[d], self.send.at[d + 3], self.recv.at[d + 3])

    def open(self):
        @pl.when(self.p.z == 0)
        def _():
            for d in (3, 2, 1):
                self.right(d).start()

        @pl.when(self.p.z == 3)
        def _():
            for d in (0, 1, 2):
                self.left(d).start()

    def pass_right(self, d):
        self.right(d).wait_recv()
        add_to(self.held, d, self.rights[d - 1])
        self.right(d).start()

    def pass_left(self, d):
        self.left(d).wait_recv()
        add_to(self.held, d, self.lefts[d])
        self.left(d).start()

    def second(self):
        @pl.when(self.p.z == 1)
        def _():
            self.pass_right(3)
            self.pass_right(2)

        @pl.when(self.p.z == 2)
        def _():
            self.pass_left(0)
            self.pass_left(1)

    def third(self):
        @pl.when(self.p.z == 2)
        def _():
            self.pass_right(3)

        @pl.when(self.p.z == 1)
        def _():
            self.pass_left(0)

    def close(self, finish):
        for z in range(LINE):

            @pl.when(self.p.z == z)
            def _(z=z):
                blocks = [self.held[z]]
                if z > 0:
                    self.right(z).wait_recv()
                    blocks.append(self.rights[z - 1])
                if z < LINE - 1:
                    self.left(z).wait_recv()
                    blocks.append(self.lefts[z])
                finish(blocks)

    def drain(self):
        for z in range(LINE):

            @pl.when(self.p.z == z)
            def _(z=z):
                for d in range(z + 1, LINE):
                    self.right(d).wait_send()
                for d in range(z):
                    self.left(d).wait_send()


def sums_body(groups, per, zfirst, *refs):
    count = groups * per
    sends, keeps = refs[:groups], refs[groups : 2 * groups]
    big_keep, big_send, little_keep, little_send = refs[2 * groups : 2 * groups + 4]
    experts_out, big_out, little_out = refs[2 * groups + 4 : 2 * groups + 7]
    (
        held, rights, lefts, kept, crossing, big_here, big_came, big_x, little_here, little_came, little_x,
        little_rights, little_lefts, xs, xr, zs, zr, ks, es, er, ls,
    ) = refs[2 * groups + 7 :]
    p = Place()
    big, little = count, count + 1

    def piece(arrays, e):
        return arrays[e // per].at[:, e % per]

    def load_keep(e):
        return pltpu.make_async_copy(piece(keeps, e), kept.at[e % 2], ks.at[e % 2])

    def x_copy(e):
        return p.copy("x", piece(sends, e), held.at[e], xs.at[e], xr.at[e])

    order = [e for e in range(count) if e not in zfirst]
    for e in order[:2]:
        load_keep(e).start()
    pltpu.make_async_copy(big_keep, big_here, ls.at[0]).start()
    pltpu.make_async_copy(little_keep, little_here, ls.at[1]).start()
    p.greet(("x", "ep"))
    p.copy("ep", big_send, big_came, es.at[0], er.at[0]).start()
    p.copy("ep", little_send, little_came, es.at[1], er.at[1]).start()
    for e in order:
        x_copy(e).start()

    flows = [Flow(p, held.at[e], rights.at[e], lefts.at[e], zs.at[e], zr.at[e]) for e in range(count + 1)]
    flows.append(Flow(p, little_x, little_rights, little_lefts, zs.at[little], zr.at[little]))

    def opened(e):
        if e == little:
            p.copy("x", little_here.at[1], little_x, xs.at[little], xr.at[little]).wait_recv()
            for d in range(LINE):
                add_to(little_x, d, little_here[0, d])
        elif e == big:
            p.copy("x", big_here.at[1], held.at[big], xs.at[big], xr.at[big]).wait_recv()
            for d in range(LINE):
                add_to(held.at[big], d, big_here[0, d])
        else:
            load_keep(e).wait()
            x_copy(e).wait_recv()
            for d in range(LINE):
                add_to(held.at[e], d, kept[e % 2, d])
            after = order.index(e) + 2
            if after < len(order):
                load_keep(order[after]).start()
        flows[e].open()

    def across_cores():
        for slot, (here, came, keep) in enumerate(
            ((big_here, big_came, big_keep), (little_here, little_came, little_keep))
        ):
            pltpu.make_async_copy(keep, here, ls.at[slot]).wait()
            p.copy("ep", big_send if slot == 0 else little_send, came, es.at[slot], er.at[slot]).wait_recv()
            for s in range(2):
                for d in range(LINE):
                    add_to(here.at[s], d, came[s, d])
        p.copy("x", big_here.at[1], held.at[big], xs.at[big], xr.at[big]).start()
        p.copy("x", little_here.at[1], little_x, xs.at[little], xr.at[little]).start()

    def closed(e):
        def finish(blocks):
            total = total_of(blocks)
            if e == little:
                little_out[...] = total
            elif e == big:
                big_out[...] = total
            else:
                experts_out[e] = total

        flows[e].close(finish)

    line = order + [big, little]
    across_cores()
    for step in range(len(line) + 3):
        if step < len(line):
            opened(line[step])
        if 0 <= step - 1 < len(line):
            flows[line[step - 1]].second()
        if 0 <= step - 2 < len(line):
            flows[line[step - 2]].third()
        if 0 <= step - 3 < len(line):
            closed(line[step - 3])
    for e in order:
        x_copy(e).wait_send()
    p.copy("x", big_here.at[1], held.at[big], xs.at[big], xr.at[big]).wait_send()
    p.copy("x", little_here.at[1], little_x, xs.at[little], xr.at[little]).wait_send()
    p.copy("ep", big_send, big_came, es.at[0], er.at[0]).wait_send()
    p.copy("ep", little_send, little_came, es.at[1], er.at[1]).wait_send()
    for e in line:
        flows[e].drain()


def chip_sums(chunks, big, little):
    groups = len(chunks)
    length, per, depth, wide = chunks[0][0].shape
    count = groups * per
    small = little[0].shape
    block = (length, depth, wide)
    anywhere = pl.BlockSpec(memory_space=pl.ANY)
    inside = pl.BlockSpec(memory_space=pltpu.VMEM)
    dma = pltpu.SemaphoreType.DMA
    scratch = [
        pltpu.VMEM((count + 1,) + block, BF16),
        pltpu.VMEM((count + 1, 3, depth, wide), BF16),
        pltpu.VMEM((count + 1, 3, depth, wide), BF16),
        pltpu.VMEM((2,) + block, BF16),
        pltpu.VMEM((depth, wide), BF16),
        pltpu.VMEM((2,) + block, BF16),
        pltpu.VMEM((2,) + block, BF16),
        pltpu.VMEM((8, 128), BF16),
        pltpu.VMEM(small, BF16),
        pltpu.VMEM(small, BF16),
        pltpu.VMEM(small[1:], BF16),
        pltpu.VMEM((3,) + small[2:], BF16),
        pltpu.VMEM((3,) + small[2:], BF16),
        dma((count + 2,)),
        dma((count + 2,)),
        dma((count + 2, 6)),
        dma((count + 2, 6)),
        dma((2,)),
        dma((2,)),
        dma((2,)),
        dma((2,)),
    ]
    return pl.pallas_call(
        functools.partial(sums_body, groups, per, ()),
        out_shape=(
            shape_of((count, depth, wide), F32),
            shape_of((depth, wide), F32),
            shape_of(small[2:], F32),
        ),
        in_specs=[anywhere] * (2 * groups + 4),
        out_specs=(inside,) * 3,
        scratch_shapes=scratch,
        compiler_params=pltpu.CompilerParams(
            collective_id=1, has_side_effects=True, vmem_limit_bytes=62 * 2**20
        ),
        name="chip_sums",
    )(*[s for _, s in chunks], *[k for k, _ in chunks], *big, *little)


def on_device(
    activations,
    cotangent,
    positions,
    routes,
    w_query,
    w_key,
    value_weight,
    w_out,
    gain_attn,
    gain_moe,
    w_router,
    w_gate_up,
    w_down,
):
    seqs, rows, model = activations.shape
    total = seqs * rows
    width = w_key.shape[1]
    group = w_query.shape[1] // width
    expert_count = w_router.shape[1]
    local = w_gate_up.shape[0]
    half = w_down.shape[2]
    blocks = lax.axis_size("cp")
    length = blocks // 2
    here = lax.axis_index("cp")
    z, side = here // 2, here % 2
    mine = lax.axis_index("ep")
    act = activations.reshape(total, model)
    dy = cotangent.reshape(total, model)
    gain_one, gain_two = gain_attn.reshape(1, model), gain_moe.reshape(1, model)

    frequency = jnp.power(10000.0, -(jnp.arange(HEAD // 2, dtype=F32) * 2.0 / HEAD))
    angles = positions.reshape(total, 1).astype(F32) * frequency
    cosine = jnp.tile(jnp.cos(angles), (1, 2 * LANES // HEAD))
    sine = jnp.tile(jnp.sin(angles), (1, 2 * LANES // HEAD))

    normed, q, kv = project(act, gain_one, w_query, w_key, value_weight, cosine, sine)
    q = q.reshape(seqs, rows, -1)
    kv = kv.reshape(1, seqs, rows, 2 * width)
    offset = (here * rows).astype(jnp.int32).reshape(1)
    if length == 4:
        slots, homes = [kv, swap(kv, "cp")], [(z, side), (z, 1 - side)]
        travel = kv
        for r in range(1, length):
            travel = up(travel, r - 1, length - 1)
            slots += [travel, swap(travel, "cp")]
            homes += [(z - r, side), (z - r, 1 - side)]
        first = jnp.stack([jnp.where(a >= 0, (2 * a + b) * rows, 2**24) for a, b in homes]).astype(jnp.int32)
    else:
        slots = [lax.all_gather(kv, "cp", axis=0, tiled=True)]
        first = jnp.arange(blocks, dtype=jnp.int32) * rows
    place = positions.reshape(seqs, 1, rows)

    dy_par = swap(dy, "ep")
    dy_turned = jnp.concatenate([dy, dy_par], axis=0).T
    w_g, w_u = w_gate_up[:, :, 0, :], w_gate_up[:, :, 1, :]
    lanes = jnp.arange(LANES, dtype=jnp.int32)
    hot = jnp.sum((routes.reshape(total, -1, 1) == lanes).astype(F32), axis=1)
    router = jnp.pad(w_router, ((0, 0), (0, LANES - expert_count)))

    low, attended, lse = attend(q, place, slots, first, offset, group)
    low = low.reshape(total, -1)
    part = out_project(low, w_out)
    middle, normed_two, gates = middle_of(act, part, swap(part, "tp"), gain_two, router, hot)
    x_par, gates_par = swap(normed_two, "ep"), swap(gates, "ep")

    where = jnp.stack([mine * local, side]).astype(jnp.int32)
    args = (blocks, where, normed_two, x_par, dy, dy_par, dy_turned, gates, gates_par)
    cut = 2
    chunks, carried = experts(0, cut, 2, *args, None, w_g, w_u, w_down)
    more, (own_back, par_back, own_mix, par_mix) = experts(cut, local, 2, *args, carried, w_g, w_u, w_down)
    chunks = chunks + more

    back = total_of([own_back, swap(par_back, "ep")]).astype(BF16)
    grad_middle, branch, grad_heads, small = middle_back(
        back, swap(back, "tp"), middle, dy, gates, router, gain_two, w_out, normed_two
    )
    dq, grads = attend_back(
        q,
        place,
        grad_heads.reshape(q.shape),
        attended,
        lse,
        cosine.reshape(seqs, rows, -1),
        sine.reshape(seqs, rows, -1),
        slots,
        first,
        offset,
        group,
    )
    dq = dq.reshape(total, -1)
    if length == 4:
        arriving = None
        for r in range(length - 1, 0, -1):
            terms = [grads[2 * r], swap(grads[2 * r + 1], "cp")] + ([] if arriving is None else [arriving])
            arriving = down(total_of(terms).astype(BF16), r, length)
        kv_terms = [grads[0], swap(grads[1], "cp"), arriving]
    else:
        kv_sum = lax.psum_scatter(grads[0], "cp", scatter_dimension=0, tiled=True)
        kv_terms = [kv_sum, jnp.zeros_like(kv_sum), jnp.zeros_like(kv_sum)]
    kv_terms = [t.reshape(total, 2 * width) for t in kv_terms]

    spots = jnp.stack([mine, side]).astype(jnp.int32)
    big = weights(spots, blocks, [(branch, low), (normed, dq)], stacked=True)
    normed_part, dkv, gain_row = project_back(
        act, dq, *kv_terms, cosine, sine, w_query, w_key, value_weight
    )
    small = jnp.concatenate([small[:expert_count], small[LANES : LANES + 1], gain_row[:1]], axis=0)
    small = jnp.pad(small, ((0, LANES - small.shape[0]), (0, 0)))
    little = weights(spots, blocks, [(normed, dkv)], (small,))
    input_grad = input_of(act, grad_middle, normed_part, swap(normed_part, "tp"), gain_one)

    mix = total_of([own_mix, swap(par_mix, "ep")]).astype(BF16)
    output = middle + total_of([mix, swap(mix, "tp")])

    def spread_sum(keep, send):
        both = total_of([keep, swap(send, "ep")]).astype(BF16)
        return line_sum([both[0], swap(both[1], "cp")], z, length)

    if length == LINE:
        expert_grad, big, little = chip_sums(chunks, big, little)
    else:
        sums = [line_sum([keep, swap(send, "cp")], z, length) for keep, send in chunks]
        expert_grad = jnp.concatenate(sums, axis=0)
        big, little = spread_sum(*big), spread_sum(*little)
    gate_up_grad = expert_grad[:, :, : 2 * half].reshape(local, -1, 2, half)
    down_grad = expert_grad[:, :, 2 * half :]
    tall = big.shape[0] // 2
    gain_part = little[:, 2 * width + expert_count + 1]
    return (
        output.reshape(activations.shape),
        input_grad.reshape(activations.shape),
        big[tall:],
        little[:, :width],
        little[:, width : 2 * width],
        big[:tall],
        gain_part + swap(gain_part, "tp"),
        little[:, 2 * width + expert_count],
        little[:, 2 * width : 2 * width + expert_count],
        gate_up_grad,
        down_grad,
    )


def solution(mesh):
    in_specs = (
        P("ep", "cp", None),
        P("ep", "cp", None),
        P("ep", "cp"),
        P("ep", "cp", None),
        P(None, "tp"),
        P(None, "tp"),
        P(None, "tp"),
        P(None, "tp"),
        P(),
        P(),
        P(),
        P("ep", None, None, "tp"),
        P("ep", None, "tp"),
    )
    out_specs = (
        P("ep", "cp", None),
        P("ep", "cp", None),
        P(("ep", "cp"), "tp"),
        P(("ep", "cp"), "tp"),
        P(("ep", "cp"), "tp"),
        P(("ep", "cp"), "tp"),
        P(("ep", "cp")),
        P(("ep", "cp")),
        P(("ep", "cp"), None),
        P("ep", "cp", None, "tp"),
        P("ep", "cp", "tp"),
    )
    return jax.shard_map(
        on_device, mesh=mesh, in_specs=in_specs, out_specs=out_specs, check_vma=False
    )
```

```python
import functools

import jax
import jax.numpy as jnp
from jax import lax
from jax.experimental import pallas as pl
from jax.experimental.pallas import tpu as pltpu
from jax.sharding import PartitionSpec as P

HEAD = 64
EPS = 1e-06
NEG = -1e30
SCALE = 0.125
LANES = 128
KEY_CHUNK = 1024
F32 = jnp.float32
BF16 = jnp.bfloat16
MESH = pl.DeviceIdType.MESH


def mm(a, b):
    return lax.dot_general(a, b, (((1,), (0,)), ((), ())), preferred_element_type=F32)


def mm_t(a, b):
    return lax.dot_general(a, b, (((1,), (1,)), ((), ())), preferred_element_type=F32)


def t_mm(a, b):
    return lax.dot_general(a, b, (((0,), (0,)), ((), ())), preferred_element_type=F32)


def two_parts(v):
    high = v.astype(BF16)
    return high, (v - high.astype(F32)).astype(BF16)


def halves_turned(v, back):
    width = v.shape[1]
    ahead = pltpu.roll(v, width - HEAD // 2, 1)
    behind = pltpu.roll(v, HEAD // 2, 1)
    first = lax.broadcasted_iota(jnp.int32, v.shape, 1) % HEAD < HEAD // 2
    if back:
        return jnp.where(first, ahead, -behind)
    return jnp.where(first, -ahead, behind)


def rope(v, cosine, sine):
    return v * cosine + halves_turned(v, False) * sine


def rope_back(v, cosine, sine):
    return v * cosine + halves_turned(v * sine, True)


def widen(table, width):
    return jnp.concatenate([table] * (width // table.shape[1]), axis=1)


def unit_rows(v):
    scale = lax.rsqrt(jnp.mean(v * v, axis=-1, keepdims=True) + EPS)
    return v * scale, scale


def shape_of(shape, dtype):
    return jax.ShapeDtypeStruct(shape, dtype)


def params(**kw):
    return pltpu.CompilerParams(vmem_limit_bytes=60 * 2**20, **kw)


def cost(flops, moved):
    return pl.CostEstimate(flops=int(flops), bytes_accessed=int(moved), transcendentals=0)


def project_body(act, gain, wq, wk, wv, cosine, sine, normed, q, kv):
    unit, _ = unit_rows(act[...].astype(F32))
    low = (unit * gain[...]).astype(BF16)
    normed[...] = low
    qf = mm(low, wq[...])
    q[...] = rope(qf, widen(cosine[...], qf.shape[1]), widen(sine[...], qf.shape[1])).astype(BF16)
    kf = mm(low, wk[...])
    width = kf.shape[1]
    kv[:, :width] = rope(kf, widen(cosine[...], width), widen(sine[...], width)).astype(BF16)
    kv[:, width:] = mm(low, wv[...]).astype(BF16)


def project(act, gain, wq, wk, wv, cosine, sine):
    rows, model = act.shape
    total = wq.shape[1] + 2 * wk.shape[1]
    return pl.pallas_call(
        project_body,
        out_shape=(
            shape_of((rows, model), BF16),
            shape_of((rows, wq.shape[1]), BF16),
            shape_of((rows, 2 * wk.shape[1]), BF16),
        ),
        compiler_params=params(),
        cost_estimate=cost(2 * rows * model * total, 2 * model * total + 6 * rows * model),
        name="project",
    )(act, gain, wq, wk, wv, cosine, sine)


def fill_keys(firsts, offset, place, slots, keys, bias, rows):
    query = lax.broadcasted_iota(jnp.int32, (rows, rows), 1) + offset
    for at, slot in enumerate(slots):
        keys[at * rows : (at + 1) * rows, :] = slot[...]
        key = lax.broadcasted_iota(jnp.int32, (rows, rows), 0) + firsts[at]
        distance = query - key
        seen = (distance >= 0) & (distance <= place)
        bias[at * rows : (at + 1) * rows, :] = jnp.where(seen, 0.0, NEG)


def single_slots(slots):
    return [slot.at[one, 0] for slot in slots for one in range(slot.shape[0])]


def group_rows(block, head, group):
    return jnp.concatenate(
        [block[:, (head * group + g) * HEAD : (head * group + g + 1) * HEAD] for g in range(group)], axis=0
    )


def attend_body(group, count, first_ref, offset_ref, q_ref, place_ref, *refs):
    slots = refs[:count]
    low_ref, out_ref, lse_ref, keys, bias = refs[count:]
    rows = q_ref.shape[1]
    singles = single_slots(slots)
    fill_keys([first_ref[i] for i in range(len(singles))], offset_ref[0], place_ref[0], singles, keys, bias, rows)
    total, width = keys.shape[0], keys.shape[1] // 2
    chunk = min(total, KEY_CHUNK)
    q = (q_ref[0].astype(F32) * SCALE).astype(BF16)
    pieces = []
    for head in range(width // HEAD):
        q3 = group_rows(q, head, group)
        top = run = out = None
        for low in range(0, total, chunk):
            k = keys[low : low + chunk, head * HEAD : (head + 1) * HEAD]
            v = keys[low : low + chunk, width + head * HEAD : width + (head + 1) * HEAD]
            s = mm_t(k, q3) + widen(bias[low : low + chunk, :], group * rows)
            here = jnp.max(s, axis=0, keepdims=True)
            new = here if top is None else jnp.maximum(top, here)
            p = jnp.exp(s - new)
            part = jnp.sum(p, axis=0, keepdims=True)
            o = t_mm(v, p.astype(BF16))
            if top is None:
                run, out = part, o
            else:
                shrink = jnp.exp(top - new)
                run, out = run * shrink + part, out * shrink + o
            top = new
        out = jnp.transpose(out / run)
        pieces += [out[g * rows : (g + 1) * rows] for g in range(group)]
        lse_ref[0, head : head + 1, :] = top + jnp.log(run)
    whole = jnp.concatenate(pieces, axis=1)
    out_ref[0] = whole
    low_ref[0] = whole.astype(BF16)


def seq_block(shape):
    return pl.BlockSpec((1,) + shape[1:], lambda s, *_: (s,) + (0,) * (len(shape) - 1))


def slot_block(shape):
    return pl.BlockSpec((shape[0], 1) + shape[2:], lambda s, *_: (0, s, 0, 0))


def attend(q, place, slots, first, offset, group):
    seqs, rows, wide = q.shape
    both = slots[0].shape[-1]
    total = rows * sum(slot.shape[0] for slot in slots)
    heads = wide // HEAD // group
    outs = (
        shape_of(q.shape, BF16),
        shape_of(q.shape, F32),
        shape_of((seqs, heads, group * rows), F32),
    )
    return pl.pallas_call(
        functools.partial(attend_body, group, len(slots)),
        out_shape=outs,
        grid_spec=pltpu.PrefetchScalarGridSpec(
            num_scalar_prefetch=2,
            grid=(seqs,),
            in_specs=[seq_block(q.shape), seq_block(place.shape)] + [slot_block(s.shape) for s in slots],
            out_specs=tuple(seq_block(o.shape) for o in outs),
            scratch_shapes=[pltpu.VMEM((total, both), BF16), pltpu.VMEM((total, rows), F32)],
        ),
        compiler_params=params(),
        cost_estimate=cost(2e9 * 4, 20e6),
        name="attend",
    )(first, offset, q, place, *slots)


def attend_back_core(
    group, q, place, go, out, lse_ref, cosine, sine, slots, firsts, offset, keys, bias, keep_grad, most
):
    rows = q.shape[0]
    fill_keys(firsts, offset, place, slots, keys, bias, rows)
    total, width = keys.shape[0], keys.shape[1] // 2
    chunk = min(total, most)
    q = (q.astype(F32) * SCALE).astype(BF16)
    products = go.astype(F32) * out
    ones = jnp.ones((8, HEAD), F32)
    heads = width // HEAD
    q3s = [group_rows(q, head, group) for head in range(heads)]
    g3s = [group_rows(go, head, group) for head in range(heads)]
    deltas = [
        lax.dot_general(
            ones,
            group_rows(products, head, group),
            (((1,), (1,)), ((), ())),
            preferred_element_type=F32,
            precision=lax.Precision.HIGHEST,
        )[:1]
        for head in range(heads)
    ]
    dq = [None] * heads
    for low in range(0, total, chunk):
        dks, dvs = [], []
        for head in range(heads):
            k = keys[low : low + chunk, head * HEAD : (head + 1) * HEAD]
            v = keys[low : low + chunk, width + head * HEAD : width + (head + 1) * HEAD]
            s = mm_t(k, q3s[head]) + widen(bias[low : low + chunk, :], group * rows)
            p = jnp.exp(s - lse_ref[head : head + 1, :])
            dp = mm_t(v, g3s[head])
            ds = (p * (dp - deltas[head])).astype(BF16)
            dks.append(mm(ds, q3s[head]))
            dvs.append(mm(p.astype(BF16), g3s[head]))
            part = t_mm(k, ds)
            dq[head] = part if dq[head] is None else dq[head] + part
        both = jnp.concatenate(dks + dvs, axis=1).astype(BF16)
        for one in range(chunk // rows):
            keep_grad(low // rows + one, both[one * rows : (one + 1) * rows])
    pieces = []
    for head in range(heads):
        back = jnp.transpose(dq[head] * SCALE)
        pieces += [back[g * rows : (g + 1) * rows] for g in range(group)]
    whole = jnp.concatenate(pieces, axis=1)
    return rope_back(whole, widen(cosine, whole.shape[1]), widen(sine, whole.shape[1])).astype(BF16)


def attend_back_body(
    group, count, first_ref, offset_ref, q_ref, place_ref, grad_ref, out_ref, lse_ref, cos_ref, sin_ref, *refs
):
    slots = single_slots(refs[:count])
    dq_ref = refs[count]
    grads = single_slots(refs[count + 1 : 2 * count + 1])
    keys, bias = refs[2 * count + 1 :]

    def keep_grad(at, value):
        grads[at][...] = value

    dq_ref[0] = attend_back_core(
        group,
        q_ref[0],
        place_ref[0],
        grad_ref[0],
        out_ref[0],
        lse_ref.at[0],
        cos_ref[0],
        sin_ref[0],
        slots,
        [first_ref[i] for i in range(len(slots))],
        offset_ref[0],
        keys,
        bias,
        keep_grad,
        KEY_CHUNK,
    )


def attend_back(q, place, grad, out, lse, cosine, sine, slots, first, offset, group):
    seqs, rows, _ = q.shape
    both = slots[0].shape[-1]
    total = rows * sum(slot.shape[0] for slot in slots)
    outs = (shape_of(q.shape, BF16),) + tuple(shape_of(s.shape, BF16) for s in slots)
    ins = (q, place, grad, out, lse, cosine, sine)
    got = pl.pallas_call(
        functools.partial(attend_back_body, group, len(slots)),
        out_shape=outs,
        grid_spec=pltpu.PrefetchScalarGridSpec(
            num_scalar_prefetch=2,
            grid=(seqs,),
            in_specs=[seq_block(a.shape) for a in ins] + [slot_block(s.shape) for s in slots],
            out_specs=(seq_block(outs[0].shape),) + tuple(slot_block(s.shape) for s in slots),
            scratch_shapes=[pltpu.VMEM((total, both), BF16), pltpu.VMEM((total, rows), F32)],
        ),
        compiler_params=params(),
        cost_estimate=cost(2e9 * 8, 30e6),
        name="attend_back",
    )(first, offset, *ins, *slots)
    return got[0], got[1:]


def out_body(low, w_out, part):
    part[...] = mm_t(low[...], w_out[...]).astype(BF16)


def out_project(low, w_out):
    rows, model = low.shape[0], w_out.shape[0]
    return pl.pallas_call(
        out_body,
        out_shape=shape_of((rows, model), BF16),
        compiler_params=params(),
        cost_estimate=cost(2 * rows * model * low.shape[1], 4e6),
        name="out_project",
    )(low, w_out)


def middle_body(act, part, other, gain, router, hot, middle, normed, gates):
    mid = act[...].astype(F32) + (part[...].astype(F32) + other[...].astype(F32))
    middle[...] = mid
    unit, _ = unit_rows(mid)
    low = (unit * gain[...]).astype(BF16)
    normed[...] = low
    chosen = hot[...] > 0.5
    logits = jnp.where(chosen, mm(low, router[...]), NEG)
    up = jnp.where(chosen, jnp.exp(logits - jnp.max(logits, axis=-1, keepdims=True)), 0.0)
    gates[...] = up / jnp.sum(up, axis=-1, keepdims=True)


def middle_of(act, part, other, gain, router, hot):
    rows, model = act.shape
    return pl.pallas_call(
        middle_body,
        out_shape=(shape_of((rows, model), F32), shape_of((rows, model), BF16), shape_of((rows, LANES), F32)),
        compiler_params=params(),
        cost_estimate=cost(2 * rows * model * LANES, 12 * rows * model),
        name="middle",
    )(act, part, other, gain, router, hot)


EARLY = 2


def experts_body(early, x_own, x_par, dy_own, dy_par, dy_turned, g_own, g_par, w_in, w_out, keep, send, *refs):
    refs = list(refs)
    came = refs.pop(0) if early else None
    own_back, par_back, own_mix, par_mix, x_turned, x_all, dy_all, back, mix, pulls, spread = refs[:11]
    leaving, es, er = refs[11:] if early else (None, None, None)
    step, steps = pl.program_id(0), pl.num_programs(0)
    rows, model = x_own.shape
    wide = own_back.shape[1] - model
    side = lax.axis_index("cp") % 2

    def early_copy(i):
        return pltpu.make_async_remote_copy(
            src_ref=leaving.at[i],
            dst_ref=came.at[i],
            send_sem=es.at[i],
            recv_sem=er.at[i],
            device_id={"cp": lax.axis_index("cp") + 1 - 2 * side},
            device_id_type=MESH,
        )

    @pl.when(step == 0)
    def _():
        if early:
            barrier = pltpu.get_barrier_semaphore()
            pl.semaphore_signal(
                barrier, inc=1, device_id={"cp": lax.axis_index("cp") + 1 - 2 * side}, device_id_type=MESH
            )
            pl.semaphore_wait(barrier, 1)
        x_all[:rows] = x_own[...]
        x_all[rows:] = x_par[...]
        dy_all[:rows] = dy_own[...]
        dy_all[rows:] = dy_par[...]
        x_turned[...] = jnp.transpose(x_all[...])
        back[...] = jnp.zeros_like(back)
        mix[...] = jnp.zeros_like(mix)
        pulls[...] = jnp.zeros_like(pulls)

    expert = lax.axis_index("ep") * steps + step
    lane = lax.broadcasted_iota(jnp.int32, (2 * rows, wide), 1) == expert
    gate_rows = jnp.concatenate([g_own[...], g_par[...]], axis=0)
    gate = jnp.sum(jnp.where(lane, gate_rows, 0.0), axis=-1, keepdims=True)
    x, dy = x_all[...], dy_all[...]
    w_gu, w_d = w_in[0], w_out[0]
    both = mm(x, w_gu)
    half = both.shape[1] // 2
    g, u = both[:, :half], both[:, half:]
    pull = mm(dy, w_d)
    sig = 1.0 / (1.0 + jnp.exp(-g))
    act = g * sig
    hidden = (act * u).astype(BF16).astype(F32)
    pulls[...] += jnp.where(lane, jnp.sum(hidden * pull, axis=-1, keepdims=True), 0.0)
    weighted = (gate * hidden).astype(BF16)
    pull = gate * pull
    d_g = (pull * u * sig * (1.0 + g * (1.0 - sig))).astype(BF16)
    d_u = (pull * act).astype(BF16)
    d_gu = jnp.concatenate([d_g, d_u], axis=1)
    blocks, depth, _ = spread.shape
    spread[:, :, : 2 * half] = mm(x_turned[...], d_gu).astype(BF16).reshape(blocks, depth, 2 * half)
    spread[:, :, 2 * half :] = mm(dy_turned[...], weighted).astype(BF16).reshape(blocks, depth, half)
    for z in range(blocks // 2):
        keep[0, z] = spread[2 * z + side]
        send[0, z] = spread[2 * z + 1 - side]
    for i in range(early):

        @pl.when(step == i)
        def _(i=i):
            for z in range(blocks // 2):
                leaving[i, z] = spread[2 * z + 1 - side]
            early_copy(i).start()

    back[...] += mm_t(d_gu, w_gu)
    mix[...] += mm_t(weighted, w_d)

    @pl.when(step == steps - 1)
    def _():
        own_back[:, :model] = back[:rows].astype(BF16)
        par_back[:, :model] = back[rows:].astype(BF16)
        own_back[:, model:] = pulls[:rows].astype(BF16)
        par_back[:, model:] = pulls[rows:].astype(BF16)
        own_mix[...] = mix[:rows].astype(BF16)
        par_mix[...] = mix[rows:].astype(BF16)
        for i in range(early):
            early_copy(i).wait()


def experts(early, blocks, x_own, x_par, dy_own, dy_par, dy_turned, g_own, g_par, w_in, w_out):
    rows, model = x_own.shape
    count, _, half = w_out.shape
    depth = model // blocks
    once = lambda shape: pl.BlockSpec(shape, lambda e: (0,) * len(shape))
    whole = (blocks // 2, depth, 3 * half)
    ins = [x_own, x_par, dy_own, dy_par, dy_turned, g_own, g_par]
    tail = [shape_of((rows, model + LANES), BF16)] * 2 + [shape_of((rows, model), BF16)] * 2
    outs = [shape_of((count,) + whole, BF16), shape_of((count - early,) + whole, BF16)]
    specs = [
        pl.BlockSpec((1,) + whole, lambda e: (e, 0, 0, 0)),
        pl.BlockSpec((1,) + whole, lambda e: (jnp.maximum(e - early, 0), 0, 0, 0)),
    ]
    scratch = [
        pltpu.VMEM((model, 2 * rows), BF16),
        pltpu.VMEM((2 * rows, model), BF16),
        pltpu.VMEM((2 * rows, model), BF16),
        pltpu.VMEM((2 * rows, model), F32),
        pltpu.VMEM((2 * rows, model), F32),
        pltpu.VMEM((2 * rows, LANES), F32),
        pltpu.VMEM((blocks, depth, 3 * half), BF16),
    ]
    kind = params()
    if early:
        outs.append(shape_of((early,) + whole, BF16))
        specs.append(pl.BlockSpec(memory_space=pl.ANY))
        scratch += [pltpu.VMEM((early,) + whole, BF16)] + [pltpu.SemaphoreType.DMA((early,))] * 2
        kind = params(collective_id=2, has_side_effects=True)
    got = pl.pallas_call(
        functools.partial(experts_body, early),
        out_shape=tuple(outs + tail),
        grid=(count,),
        in_specs=[once(a.shape) for a in ins]
        + [
            pl.BlockSpec((1, model, 2 * half), lambda e: (e, 0, 0)),
            pl.BlockSpec((1, model, half), lambda e: (e, 0, 0)),
        ],
        out_specs=tuple(specs + [once(t.shape) for t in tail]),
        scratch_shapes=scratch,
        compiler_params=kind,
        cost_estimate=cost(count * 18 * 2 * rows * model * half, count * 12 * model * half),
        name="experts",
    )(*ins, w_in, w_out)
    return got[: len(outs)], got[len(outs) :]


def middle_back_body(mine, other, middle, dy, gates, router, gain, w_out, normed, grad, low, heads, small):
    model = middle.shape[1]
    total = mine[...].astype(F32) + other[...].astype(F32)
    gate, pulls = gates[...], total[:, model:]
    chosen = gate * (pulls - jnp.sum(gate * pulls, axis=-1, keepdims=True))
    high, rest = two_parts(chosen)
    grad_two = total[:, :model] + (mm_t(high, router[...]) + mm_t(rest, router[...]))
    unit, scale = unit_rows(middle[...])
    small[:LANES, :] = t_mm(high, normed[...]) + t_mm(rest, normed[...])
    small[LANES : LANES + 8, :] = jnp.broadcast_to(jnp.sum(grad_two * unit, axis=0, keepdims=True), (8, model))
    scaled = grad_two * gain[...]
    out = dy[...].astype(F32) + scale * (scaled - unit * jnp.mean(scaled * unit, axis=-1, keepdims=True))
    grad[...] = out
    rounded = out.astype(BF16)
    low[...] = rounded
    heads[...] = mm(rounded, w_out[...]).astype(BF16)


def middle_back(mine, other, middle, dy, gates, router, gain, w_out, normed):
    rows, model = middle.shape
    return pl.pallas_call(
        middle_back_body,
        out_shape=(
            shape_of((rows, model), F32),
            shape_of((rows, model), BF16),
            shape_of((rows, w_out.shape[1]), BF16),
            shape_of((LANES + 8, model), F32),
        ),
        compiler_params=params(),
        cost_estimate=cost(2 * rows * model * (w_out.shape[1] + 4 * LANES), 10e6),
        name="middle_back",
    )(mine, other, middle, dy, gates, router, gain, w_out, normed)


def project_back_body(width, act, dq, a, b, c, cosine, sine, wq, wk, wv, part, dkv, gain_row):
    total = a[...].astype(F32) + b[...].astype(F32) + c[...].astype(F32)
    dk = rope_back(total[:, :width], widen(cosine[...], width), widen(sine[...], width)).astype(BF16)
    dv = total[:, width:].astype(BF16)
    dkv[:, :width] = dk
    dkv[:, width:] = dv
    full = mm_t(dq[...], wq[...]) + mm_t(dk, wk[...]) + mm_t(dv, wv[...])
    part[...] = full.astype(BF16)
    unit, _ = unit_rows(act[...].astype(F32))
    gain_row[...] = jnp.broadcast_to(jnp.sum(full * unit, axis=0, keepdims=True), gain_row.shape)


def project_back(act, dq, a, b, c, cosine, sine, wq, wk, wv):
    rows, model = act.shape
    width = wk.shape[1]
    return pl.pallas_call(
        functools.partial(project_back_body, width),
        out_shape=(
            shape_of((rows, model), BF16),
            shape_of((rows, 2 * width), BF16),
            shape_of((8, model), F32),
        ),
        compiler_params=params(),
        cost_estimate=cost(2 * rows * model * (wq.shape[1] + 2 * width), 8e6),
        name="project_back",
    )(act, dq, a, b, c, cosine, sine, wq, wk, wv)


def input_body(act, grad, mine, other, gain, out):
    unit, scale = unit_rows(act[...].astype(F32))
    scaled = (mine[...].astype(F32) + other[...].astype(F32)) * gain[...]
    out[...] = grad[...] + scale * (scaled - unit * jnp.mean(scaled * unit, axis=-1, keepdims=True))


def input_of(act, grad, mine, other, gain):
    return pl.pallas_call(
        input_body,
        out_shape=shape_of(act.shape, F32),
        compiler_params=params(),
        cost_estimate=cost(0, 12 * act.shape[0] * act.shape[1]),
        name="input_grad",
    )(act, grad, mine, other, gain)


def weights_body(blocks, count, stacked, where_ref, *refs):
    lefts = refs[:count]
    rights = refs[count : 2 * count]
    extra = refs[2 * count : -3]
    keep, send, whole = refs[-3:]
    parts = [t_mm(a[...], b[...]).astype(BF16) for a, b in zip(lefts, rights)]
    parts += [jnp.transpose(e[...]).astype(BF16) for e in extra]
    at = down = 0
    for part in parts:
        block = part.reshape(2 * blocks, -1, part.shape[1])
        whole[:, down : down + block.shape[1], at : at + part.shape[1]] = block
        if stacked:
            down += block.shape[1]
        else:
            at += part.shape[1]
    mine, side = where_ref[0], where_ref[1]
    for half, ref in ((mine, keep), (1 - mine, send)):
        for z in range(blocks // 2):
            ref[0, z] = whole[half * blocks + 2 * z + side]
            ref[1, z] = whole[half * blocks + 2 * z + 1 - side]


def weights(where, blocks, pairs, extra=(), stacked=False):
    model = pairs[0][0].shape[1]
    rows = pairs[0][0].shape[0]
    depth = model // (2 * blocks)
    columns = sum(b.shape[1] for _, b in pairs) + sum(e.shape[0] for e in extra)
    tall, wide = (depth * len(pairs), pairs[0][1].shape[1]) if stacked else (depth, columns)
    shape = (2, blocks // 2, tall, wide)
    ins = [a for a, _ in pairs] + [b for _, b in pairs] + list(extra)
    full = lambda a: pl.BlockSpec(a.shape, lambda i, *_: (0,) * len(a.shape))
    return pl.pallas_call(
        functools.partial(weights_body, blocks, len(pairs), stacked),
        out_shape=(shape_of(shape, BF16),) * 2,
        grid_spec=pltpu.PrefetchScalarGridSpec(
            num_scalar_prefetch=1,
            grid=(1,),
            in_specs=[full(a) for a in ins],
            out_specs=(pl.BlockSpec(shape, lambda i, *_: (0, 0, 0, 0)),) * 2,
            scratch_shapes=[pltpu.VMEM((2 * blocks, tall, wide), BF16)],
        ),
        compiler_params=params(),
        cost_estimate=cost(2 * rows * model * columns, 4 * model * columns),
        name="weights",
    )(where, *ins)


def swap(v, axis):
    size = lax.axis_size(axis)
    return lax.ppermute(v, axis, [(i, i ^ 1) for i in range(size)])


def up(v, low, high):
    return lax.ppermute(v, "cp", [(2 * z + s, 2 * z + 2 + s) for z in range(low, high) for s in range(2)])


def down(v, low, high):
    return lax.ppermute(v, "cp", [(2 * z + s, 2 * z - 2 + s) for z in range(low, high) for s in range(2)])


def total_of(terms):
    return functools.reduce(lambda a, b: a + b, [t.astype(F32) for t in terms])


def line_sum(parts, z, length):
    def own(d):
        return [lax.dynamic_index_in_dim(p, jnp.clip(d, 0, length - 1), 0, keepdims=False) for p in parts]

    if length > 4:
        mine = total_of(parts).astype(BF16)
        side = lax.axis_index("cp") % 2
        full = jnp.where(jnp.arange(2).reshape((1, 2) + (1,) * (mine.ndim - 1)) == side, mine[:, None], 0)
        full = full.reshape((2 * length,) + mine.shape[1:])
        return lax.psum_scatter(full, "cp", scatter_dimension=0, tiled=True)[0].astype(F32)
    right = left = None
    for k in range(length - 1):
        far = length - 1 - k
        terms = own(z + far) + ([] if right is None else [right])
        right = up(total_of(terms).astype(BF16), 0, k + 1)
        terms = own(z - far) + ([] if left is None else [left])
        left = down(total_of(terms).astype(BF16), far, length)
    return total_of(own(z) + ([right, left] if length > 1 else []))


LINE = 4
RING = 6


def add_to(ref, at, other):
    ref[at] = (ref[at].astype(F32) + other.astype(F32)).astype(BF16)


class Place:
    def __init__(self):
        self.cp = lax.axis_index("cp")
        self.z, self.side = self.cp // 2, self.cp % 2
        self.ep, self.tp = lax.axis_index("ep"), lax.axis_index("tp")

    def to(self, way):
        if way == "x":
            return {"cp": self.cp + 1 - 2 * self.side}
        if way == "up":
            return {"cp": self.cp + 2}
        if way == "down":
            return {"cp": self.cp - 2}
        return {way: 1 - (self.ep if way == "ep" else self.tp)}

    def signal(self, sem, way):
        pl.semaphore_signal(sem, inc=1, device_id=self.to(way), device_id_type=MESH)

    def signal_line(self, to_down, to_up):
        @pl.when(self.z > 0)
        def _():
            self.signal(to_down, "down")

        @pl.when(self.z < LINE - 1)
        def _():
            self.signal(to_up, "up")

    def greet(self, ways):
        barrier = pltpu.get_barrier_semaphore()
        for way in ways:
            self.signal(barrier, way)
        self.signal_line(barrier, barrier)
        both = jnp.where(self.z > 0, 1, 0) + jnp.where(self.z < LINE - 1, 1, 0)
        pl.semaphore_wait(barrier, len(ways) + both)

    def copy(self, way, src, dst, send, recv):
        return pltpu.make_async_remote_copy(
            src_ref=src, dst_ref=dst, send_sem=send, recv_sem=recv, device_id=self.to(way), device_id_type=MESH
        )

    def at(self, z):
        return pl.when(self.z == z)


LEFT_SPOT = (3, 4, 0)


class Flow:
    def __init__(self, place, held, spots, send, recv, credit=None):
        self.p, self.held, self.spots, self.send, self.recv, self.credit = place, held, spots, send, recv, credit

    def right(self, d):
        return self.p.copy("up", self.held.at[d], self.spots.at[d - 1], self.send.at[d - 1], self.recv.at[d - 1])

    def left(self, d):
        spot = LEFT_SPOT[d]
        return self.p.copy("down", self.held.at[d], self.spots.at[spot], self.send.at[d + 3], self.recv.at[d + 3])

    def allowed(self, way):
        if self.credit is not None:
            pl.semaphore_wait(self.credit[way], 1)

    def open(self):
        @self.p.at(0)
        def _():
            self.allowed("up")
            for d in (3, 2, 1):
                self.right(d).start()

        @self.p.at(3)
        def _():
            self.allowed("down")
            for d in (0, 1, 2):
                self.left(d).start()

    def pass_right(self, d):
        self.right(d).wait_recv()
        add_to(self.held, d, self.spots[d - 1])
        self.right(d).start()

    def pass_left(self, d):
        self.left(d).wait_recv()
        add_to(self.held, d, self.spots[LEFT_SPOT[d]])
        self.left(d).start()

    def second(self):
        @self.p.at(1)
        def _():
            self.allowed("up")
            self.pass_right(3)
            self.pass_right(2)

        @self.p.at(2)
        def _():
            self.allowed("down")
            self.pass_left(0)
            self.pass_left(1)

    def third(self):
        @self.p.at(2)
        def _():
            self.allowed("up")
            self.pass_right(3)

        @self.p.at(1)
        def _():
            self.allowed("down")
            self.pass_left(0)

    def close(self, finish):
        for z in range(LINE):

            @self.p.at(z)
            def _(z=z):
                blocks = [self.held[z]]
                if z > 0:
                    self.right(z).wait_recv()
                    blocks.append(self.spots[z - 1])
                if z < LINE - 1:
                    self.left(z).wait_recv()
                    blocks.append(self.spots[LEFT_SPOT[z]])
                finish(blocks)

    def drain(self):
        for z in range(LINE):

            @self.p.at(z)
            def _(z=z):
                for d in range(z + 1, LINE):
                    self.right(d).wait_send()
                for d in range(z):
                    self.left(d).wait_send()


class Names:
    pass


def named(names, refs):
    out = Names()
    for name, ref in zip(names, refs, strict=True):
        setattr(out, name, ref)
    return out


BACK_INS = (
    "own_back", "par_back", "own_mix", "par_mix", "middle", "dy", "router", "w_out", "x2", "q", "attended",
    "act", "normed", "low", "wq", "wk", "wv", "gates", "gain_two", "gain_one", "place", "lse", "cosine",
    "sine",
)
BACK_IN_PLACE = 7
BACK_OUTS = (
    "grad", "mix", "experts", "big_out", "little_out",
)
BACK_SCRATCH = (
    "back", "other_ep", "other_tp", "mid_dy", "mid_x2", "wide_w", "branch", "heads", "small", "qs", "atts",
    "slots", "kv_x", "kv_z", "keys", "bias", "dq", "lows", "wks", "wvs", "routers", "dkv", "part", "part_in",
    "mix_ep", "mix_tp", "held", "spots", "kept", "staged", "whole", "came", "lit",
    "lit_came", "lit_x", "lit_spots", "ls", "ks", "xs", "xr", "zs", "zr", "es", "er", "ts", "tr", "kxs",
    "kxr", "kzs", "kzr", "os", "free_x", "free_up", "free_down",
)


def back_body(group, *refs):
    n_in = len(BACK_INS) + 2 * LINE + 3
    ins = named(BACK_INS, refs[: len(BACK_INS)])
    slots_in = refs[len(BACK_INS) : n_in - 3]
    keeps, sends, arrived = refs[n_in - 3 : n_in]
    o = named(BACK_OUTS, refs[n_in : n_in + len(BACK_OUTS)])
    s = named(BACK_SCRATCH, refs[n_in + len(BACK_OUTS) :])
    p = Place()
    count, early = keeps.shape[0], arrived.shape[0]
    seqs, rows, _ = ins.q.shape
    model = ins.middle.shape[1]
    width = ins.wk.shape[1]
    part_of = lambda i: pl.ds(i * rows, rows)

    ring = [("here", e) for e in range(early)] + [("x", e) for e in range(early, count)] + [("big", count)]
    index_of = {item: i for i, item in enumerate(ring)}
    crosses = lambda item: item[0] in ("x", "big")

    def flow(item):
        if item == "little":
            return Flow(p, s.lit_x, s.lit_spots, s.zs.at[len(ring)], s.zr.at[len(ring)])
        i = index_of[item]
        credit = {"up": s.free_up, "down": s.free_down} if i >= RING else None
        return Flow(p, s.held.at[i % RING], s.spots.at[i % RING], s.zs.at[i], s.zr.at[i], credit)

    def x_copy(item):
        if item == "little":
            return p.copy("x", s.lit.at[p.ep, :, 1 - p.side], s.lit_x, s.xs.at[len(ring)], s.xr.at[len(ring)])
        i = index_of[item]
        src = s.whole.at[p.ep, :, 1 - p.side] if item[0] == "big" else sends.at[item[1] - early]
        return p.copy("x", src, s.held.at[i % RING], s.xs.at[i], s.xr.at[i])

    def cross(item):
        if item != "little" and index_of[item] >= RING:
            pl.semaphore_wait(s.free_x, 1)
        x_copy(item).start()

    def load_keep(e):
        return pltpu.make_async_copy(keeps.at[e], s.kept, s.ks.at[0])

    def load_arrived(e):
        return pltpu.make_async_copy(arrived.at[e], s.held.at[e], s.ks.at[1 + e])

    def opened(item):
        if item == "little":
            x_copy(item).wait_recv()
            for d in range(LINE):
                add_to(s.lit_x, d, s.lit[p.ep, d, p.side])
        else:
            held = s.held.at[index_of[item] % RING]
            if item[0] == "here":
                load_arrived(item[1]).wait()
            else:
                x_copy(item).wait_recv()
            if item[0] == "big":
                for d in range(LINE):
                    add_to(held, d, s.whole[p.ep, d, p.side])
            else:
                load_keep(item[1]).wait()
                for d in range(LINE):
                    add_to(held, d, s.kept[d])
                if item[1] + 1 < count:
                    load_keep(item[1] + 1).start()
        flow(item).open()

    stored = []

    def store(e):
        return pltpu.make_async_copy(s.staged.at[e % 2], o.experts.at[e], s.os.at[e])

    def finish_expert(e, make):
        if len(stored) >= 2 and e % 2 in [k % 2 for k in stored[-2:]]:
            last = [k for k in stored if k % 2 == e % 2][-1]
            store(last).wait()
            waited.add(last)
        make()
        store(e).start()
        stored.append(e)

    waited = set()

    def closed(item):
        if item == "little":
            def finish(blocks):
                o.little_out[...] = total_of(blocks)

            flow(item).close(finish)
        elif item[0] == "big":
            def finish(blocks):
                o.big_out[...] = total_of(blocks)

            flow(item).close(finish)
        else:
            def finish(blocks):
                s.staged[item[1] % 2] = total_of(blocks)

            finish_expert(item[1], lambda: flow(item).close(finish))

    def freed(item):
        flow(item).drain()
        if item == "little":
            return
        after = index_of[item] + RING
        if after < len(ring):
            if crosses(item):
                x_copy(item).wait_send()
            if crosses(ring[after]):
                p.signal(s.free_x, "x")
            p.signal_line(s.free_up, s.free_down)

    loads = {}

    def load(name, src, dst):
        copy = pltpu.make_async_copy(src, dst, s.ls.at[len(loads)])
        copy.start()
        loads[name] = copy

    def got(*names):
        for name in names:
            loads[name].wait()

    load("back", ins.own_back, s.back)
    load_keep(0).start()
    for e in range(early):
        load_arrived(e).start()
    load("grad", ins.middle, o.grad)
    load("dy", ins.dy, s.mid_dy)
    load("router", ins.router, s.routers)
    load("x2", ins.x2, s.mid_x2)
    load("w_out", ins.w_out, s.wide_w)
    load("mix", ins.own_mix, o.mix)
    load("q", ins.q, s.qs)
    load("attended", ins.attended, s.atts)
    for j in range(2 * LINE):
        load(f"slot{j}", slots_in[j].at[0], s.slots.at[:, j // 2, j % 2])
    load("low", ins.low, s.lows)
    load("wk", ins.wk, s.wks)
    load("wv", ins.wv, s.wvs)

    p.greet(("x", "ep", "tp"))
    ep_back = p.copy("ep", ins.par_back, s.other_ep, s.es.at[0], s.er.at[0])
    ep_back.start()
    ep_mix = p.copy("ep", ins.par_mix, s.mix_ep, s.es.at[1], s.er.at[1])
    ep_mix.start()
    queue = ring[early:] + ["little"]
    cross(queue.pop(0))
    cross(queue.pop(0))

    got("back")
    ep_back.wait_recv()
    for i in range(seqs):
        s.back[part_of(i)] = (
            s.back[part_of(i)].astype(F32) + s.other_ep[part_of(i)].astype(F32)
        ).astype(BF16)
    tp_back = p.copy("tp", s.back, s.other_tp, s.ts.at[0], s.tr.at[0])
    tp_back.start()
    got("mix")
    ep_mix.wait_recv()
    for i in range(seqs):
        o.mix[part_of(i)] = (o.mix[part_of(i)].astype(F32) + s.mix_ep[part_of(i)].astype(F32)).astype(BF16)

    def step_middle():
        got("grad", "dy", "router", "x2", "w_out")
        tp_back.wait_recv()
        for i in range(seqs):
            at = part_of(i)
            total = s.back[at].astype(F32) + s.other_tp[at].astype(F32)
            gate, pulls = ins.gates[at], total[:, model:]
            chosen = gate * (pulls - jnp.sum(gate * pulls, axis=-1, keepdims=True))
            high, rest = two_parts(chosen)
            grad_two = total[:, :model] + (mm_t(high, s.routers[...]) + mm_t(rest, s.routers[...]))
            unit, scale = unit_rows(o.grad[at])
            routed = t_mm(high, s.mid_x2[at]) + t_mm(rest, s.mid_x2[at])
            gain_row = jnp.sum(grad_two * unit, axis=0, keepdims=True)
            if i == 0:
                s.small[...] = routed
                s.small[LANES - 1 :, :] = gain_row
            else:
                s.small[: LANES - 1, :] += routed[: LANES - 1]
                s.small[LANES - 1 :, :] += gain_row
            scaled = grad_two * ins.gain_two[...]
            out = s.mid_dy[at].astype(F32) + scale * (
                scaled - unit * jnp.mean(scaled * unit, axis=-1, keepdims=True)
            )
            o.grad[at] = out
            rounded = out.astype(BF16)
            s.branch[at] = rounded
            s.heads[at] = mm(rounded, s.wide_w[...]).astype(BF16)
        load("wq", ins.wq, s.wide_w)
        load("act", ins.act, s.mid_dy)
        load("normed", ins.normed, s.mid_x2)

    tp_mix = p.copy("tp", o.mix, s.mix_tp, s.ts.at[1], s.tr.at[1])

    def step_attend(i):
        if i == 0:
            got("q", "attended", *[f"slot{j}" for j in range(2 * LINE)])
        homes = [(p.z - r, side) for r in range(LINE) for side in (p.side, 1 - p.side)]
        firsts = [jnp.where(a >= 0, (2 * a + b) * rows, 2**24) for a, b in homes]

        def keep_grad(j, value):
            s.slots[i, j // 2, j % 2] = value

        s.dq[i] = attend_back_core(
            group,
            s.qs[i],
            ins.place[i],
            s.heads[part_of(i)],
            s.atts[i],
            ins.lse.at[i],
            ins.cosine[i],
            ins.sine[i],
            [s.slots.at[i, j // 2, j % 2] for j in range(2 * LINE)],
            firsts,
            p.cp * rows,
            s.keys,
            s.bias,
            keep_grad,
            512,
        )
        kv_cross(i).start()

    def kv_cross(i):
        return p.copy("x", s.slots.at[i, :, 1], s.kv_x.at[i], s.kxs.at[i], s.kxr.at[i])

    def kv_down(i, r):
        return p.copy("down", s.slots.at[i, r, 0], s.kv_z.at[i, r - 1], s.kzs.at[i, r - 1], s.kzr.at[i, r - 1])

    def kv_take(i, r):
        kv_down(i, r + 1).wait_recv()
        s.slots[i, r, 0] = (s.slots[i, r, 0].astype(F32) + s.kv_z[i, r].astype(F32)).astype(BF16)

    def step_keys(i):
        kv_cross(i).wait_recv()
        for r in range(LINE):
            s.slots[i, r, 0] = (s.slots[i, r, 0].astype(F32) + s.kv_x[i, r].astype(F32)).astype(BF16)
        for z in range(LINE - 1, -1, -1):

            @p.at(z)
            def _(z=z):
                for r in range(z, 0, -1):
                    if z < LINE - 1:
                        kv_take(i, r)
                    kv_down(i, r).start()
                if z < LINE - 1:
                    kv_take(i, 0)

    def part_copy(i):
        return p.copy("tp", s.part.at[part_of(i)], s.part_in.at[part_of(i)], s.ts.at[2 + i], s.tr.at[2 + i])

    def step_project(i):
        if i == 0:
            got("wq", "wk", "wv", "act", "normed")
        at = part_of(i)
        total = s.slots[i, 0, 0].astype(F32)
        dk = rope_back(total[:, :width], widen(ins.cosine[i], width), widen(ins.sine[i], width)).astype(BF16)
        dv = total[:, width:].astype(BF16)
        s.dkv[at, :width] = dk
        s.dkv[at, width:] = dv
        full = mm_t(s.dq[i], s.wide_w[...]) + mm_t(dk, s.wks[...]) + mm_t(dv, s.wvs[...])
        s.part[at] = full.astype(BF16)
        part_copy(i).start()
        unit, _ = unit_rows(s.mid_dy[at].astype(F32))
        gain_row = jnp.sum(full * unit, axis=0, keepdims=True)
        if i == 0:
            s.small[LANES - 2 : LANES - 1, :] = gain_row
        else:
            s.small[LANES - 2 : LANES - 1, :] += gain_row

    tall = model // 4

    def weight_pieces(left, right, ref, keep):
        for piece_at in range(4):
            got_piece = t_mm(left[:, piece_at * tall : (piece_at + 1) * tall], right).astype(BF16)
            block = got_piece.reshape(-1, model // 16, right.shape[1])
            for b in range(4):
                whole = 4 * piece_at + b
                keep(whole // 8, whole % 8 // 2, whole % 2, block[b])

    def big_part(row):
        def keep(half, z, side, value):
            s.whole[half, z, side, row : row + value.shape[0], :] = value

        return keep

    def little_part(column):
        def keep(half, z, side, value):
            s.lit[half, z, side, :, column : column + value.shape[1]] = value

        return keep

    ep_big = p.copy("ep", s.whole.at[1 - p.ep], s.came, s.es.at[2], s.er.at[2])
    ep_lit = p.copy("ep", s.lit.at[1 - p.ep], s.lit_came, s.es.at[3], s.er.at[3])

    def step_out_weight():
        got("low")
        weight_pieces(s.branch[...], s.lows[...], s.whole, big_part(0))

    def step_query_weight():
        got("normed")
        loads["normed"] = Done()
        query = jnp.concatenate([s.dq[i] for i in range(seqs)], axis=0)
        weight_pieces(s.mid_x2[...], query, s.whole, big_part(model // 16))
        ep_big.start()

    def step_key_weight():
        weight_pieces(s.mid_x2[...], s.dkv[...], s.lit, little_part(0))
        for piece_at in range(4):
            turned = jnp.transpose(s.small[:, piece_at * tall : (piece_at + 1) * tall]).astype(BF16)
            block = turned.reshape(-1, model // 16, LANES)
            for b in range(4):
                whole = 4 * piece_at + b
                little_part(2 * width)(whole // 8, whole % 8 // 2, whole % 2, block[b])
        ep_lit.start()

    def step_big_cores():
        ep_big.wait_recv()
        for d in range(LINE):
            for side in range(2):
                s.whole[p.ep, d, side] = (
                    s.whole[p.ep, d, side].astype(F32) + s.came[d, side].astype(F32)
                ).astype(BF16)

    def step_little_cores():
        ep_lit.wait_recv()
        for d in range(LINE):
            for side in range(2):
                s.lit[p.ep, d, side] = (
                    s.lit[p.ep, d, side].astype(F32) + s.lit_came[d, side].astype(F32)
                ).astype(BF16)

    def step_input():
        for i in range(seqs):
            at = part_of(i)
            part_copy(i).wait_recv()
            unit, scale = unit_rows(s.mid_dy[at].astype(F32))
            scaled = (s.part[at].astype(F32) + s.part_in[at].astype(F32)) * ins.gain_one[...]
            o.grad[at] = o.grad[at] + scale * (scaled - unit * jnp.mean(scaled * unit, axis=-1, keepdims=True))

    def step_mix():
        tp_mix.wait_recv()
        tp_mix.wait_send()
        for i in range(seqs):
            o.mix[part_of(i)] = (o.mix[part_of(i)].astype(F32) + s.mix_tp[part_of(i)].astype(F32)).astype(BF16)

    line = list(ring) + ["little"]
    stage = {item: 0 for item in line}

    def advance(at, to):
        if not 0 <= at < len(line):
            return
        item = line[at]
        while stage[item] < to:
            now = stage[item]
            if now == 0:
                opened(item)
            elif now == 1:
                flow(item).second()
            elif now == 2:
                flow(item).third()
            elif now == 3:
                closed(item)
            elif now == 4:
                freed(item)
            stage[item] = now + 1

    def turn(at):
        for back in (4, 3, 2, 1, 0):
            advance(at - back, back + 1)

    tp_mix.start()
    turn(0)
    turn(1)
    step_middle()
    advance(0, 3)
    advance(1, 2)
    step_attend(0)
    turn(2)
    step_attend(1)
    cross(queue.pop(0))
    advance(0, 4)
    advance(1, 3)
    advance(2, 2)
    step_out_weight()
    step_query_weight()
    turn(3)
    cross(queue.pop(0))
    step_keys(0)
    advance(2, 3)
    advance(3, 2)
    step_keys(1)
    step_project(0)
    step_project(1)
    advance(0, 5)
    advance(1, 4)
    advance(2, 4)
    advance(3, 3)
    step_key_weight()
    step_big_cores()
    step_mix()
    extra = [step_little_cores, step_input]
    for at in range(4, len(line) + 4):
        turn(at)
        if queue:
            cross(queue.pop(0))
        if extra:
            extra.pop(0)()
    for e in stored:
        if e not in waited:
            store(e).wait()
    for item in line:
        if item == "little" or (crosses(item) and index_of[item] + RING >= len(ring)):
            x_copy(item).wait_send()
    for i in range(seqs):
        kv_cross(i).wait_send()
        part_copy(i).wait_send()
        for z in range(1, LINE):

            @p.at(z)
            def _(z=z):
                for r in range(z, 0, -1):
                    kv_down(i, r).wait_send()

    tp_back.wait_send()
    for copy in (ep_back, ep_mix, ep_big, ep_lit):
        copy.wait_send()


class Done:
    def wait(self):
        return None


def back_and_sums(ins, slots, chunks, group):
    keeps, _, arrived = chunks
    count, length, depth, wide = keeps.shape
    early = arrived.shape[0]
    block = (length, depth, wide)
    v = dict(zip(BACK_INS, ins, strict=True))
    rows, model = v["middle"].shape
    seqs, each, heads = v["q"].shape
    width = v["wk"].shape[1]
    both = 2 * width
    small = (length, 2, model // 16, both + LANES)
    n_ring = count + 1
    anywhere = pl.BlockSpec(memory_space=pl.ANY)
    inside = pl.BlockSpec(memory_space=pltpu.VMEM)
    dma, vm = pltpu.SemaphoreType.DMA, pltpu.VMEM
    flag = pltpu.SemaphoreType.REGULAR
    scratch = dict(
        back=vm((rows, model + LANES), BF16),
        other_ep=vm((rows, model + LANES), BF16),
        other_tp=vm((rows, model + LANES), BF16),
        mid_dy=vm((rows, model), BF16),
        mid_x2=vm((rows, model), BF16),
        wide_w=vm((model, heads), BF16),
        branch=vm((rows, model), BF16),
        heads=vm((rows, heads), BF16),
        small=vm((LANES, model), F32),
        qs=vm((seqs, each, heads), BF16),
        atts=vm((seqs, each, heads), F32),
        slots=vm((seqs, LINE, 2, each, both), BF16),
        kv_x=vm((seqs, LINE, each, both), BF16),
        kv_z=vm((seqs, LINE - 1, each, both), BF16),
        keys=vm((2 * LINE * each, both), BF16),
        bias=vm((2 * LINE * each, each), F32),
        dq=vm((seqs, each, heads), BF16),
        lows=vm((rows, heads), BF16),
        wks=vm((model, width), BF16),
        wvs=vm((model, width), BF16),
        routers=vm((model, LANES), BF16),
        dkv=vm((rows, both), BF16),
        part=vm((rows, model), BF16),
        part_in=vm((rows, model), BF16),
        mix_ep=vm((rows, model), BF16),
        mix_tp=vm((rows, model), BF16),
        held=vm((RING,) + block, BF16),
        spots=vm((RING, 5, depth, wide), BF16),
        kept=vm(block, BF16),
        staged=vm((2, depth, wide), F32),
        whole=vm((2, length, 2, depth, wide), BF16),
        came=vm((length, 2, depth, wide), BF16),
        lit=vm((2,) + small, BF16),
        lit_came=vm(small, BF16),
        lit_x=vm((small[0],) + small[2:], BF16),
        lit_spots=vm((5,) + small[2:], BF16),
        ls=dma((28,)),
        ks=dma((1 + early,)),
        xs=dma((n_ring + 1,)),
        xr=dma((n_ring + 1,)),
        zs=dma((n_ring + 1, 6)),
        zr=dma((n_ring + 1, 6)),
        es=dma((4,)),
        er=dma((4,)),
        ts=dma((4,)),
        tr=dma((4,)),
        kxs=dma((2,)),
        kxr=dma((2,)),
        kzs=dma((2, 3)),
        kzr=dma((2, 3)),
        os=dma((count,)),
        free_x=flag,
        free_up=flag,
        free_down=flag,
    )
    return pl.pallas_call(
        functools.partial(back_body, group),
        out_shape=(
            shape_of((rows, model), F32),
            shape_of((rows, model), BF16),
            shape_of((count, depth, wide), F32),
            shape_of((depth, wide), F32),
            shape_of(small[2:], F32),
        ),
        in_specs=[anywhere] * (len(BACK_INS) - BACK_IN_PLACE)
        + [inside] * BACK_IN_PLACE
        + [anywhere] * (2 * LINE + 3),
        out_specs=(inside, inside, anywhere, inside, inside),
        scratch_shapes=[scratch[name] for name in BACK_SCRATCH],
        compiler_params=pltpu.CompilerParams(
            collective_id=1, has_side_effects=True, vmem_limit_bytes=67_043_328
        ),
        name="back_and_sums",
    )(*ins, *slots, *chunks)


def on_device(
    activations,
    cotangent,
    positions,
    routes,
    w_query,
    w_key,
    value_weight,
    w_out,
    gain_attn,
    gain_moe,
    w_router,
    w_gate_up,
    w_down,
):
    seqs, rows, model = activations.shape
    total = seqs * rows
    width = w_key.shape[1]
    group = w_query.shape[1] // width
    expert_count = w_router.shape[1]
    local = w_gate_up.shape[0]
    half = w_down.shape[2]
    blocks = lax.axis_size("cp")
    length = blocks // 2
    here = lax.axis_index("cp")
    z, side = here // 2, here % 2
    mine = lax.axis_index("ep")
    act = activations.reshape(total, model)
    dy = cotangent.reshape(total, model)
    gain_one, gain_two = gain_attn.reshape(1, model), gain_moe.reshape(1, model)

    frequency = jnp.power(10000.0, -(jnp.arange(HEAD // 2, dtype=F32) * 2.0 / HEAD))
    angles = positions.reshape(total, 1).astype(F32) * frequency
    cosine = jnp.tile(jnp.cos(angles), (1, 2 * LANES // HEAD))
    sine = jnp.tile(jnp.sin(angles), (1, 2 * LANES // HEAD))

    normed, q, kv = project(act, gain_one, w_query, w_key, value_weight, cosine, sine)
    q = q.reshape(seqs, rows, -1)
    kv = kv.reshape(1, seqs, rows, 2 * width)
    offset = (here * rows).astype(jnp.int32).reshape(1)
    if length == 4:
        slots, homes = [kv, swap(kv, "cp")], [(z, side), (z, 1 - side)]
        travel = kv
        for r in range(1, length):
            travel = up(travel, r - 1, length - 1)
            slots += [travel, swap(travel, "cp")]
            homes += [(z - r, side), (z - r, 1 - side)]
        first = jnp.stack([jnp.where(a >= 0, (2 * a + b) * rows, 2**24) for a, b in homes]).astype(jnp.int32)
    else:
        slots = [lax.all_gather(kv, "cp", axis=0, tiled=True)]
        first = jnp.arange(blocks, dtype=jnp.int32) * rows
    place = positions.reshape(seqs, 1, rows)

    dy_par = swap(dy, "ep")
    dy_turned = jnp.concatenate([dy, dy_par], axis=0).T
    w_in = w_gate_up.reshape(local, model, 2 * half)
    lanes = jnp.arange(LANES, dtype=jnp.int32)
    hot = jnp.sum((routes.reshape(total, -1, 1) == lanes).astype(F32), axis=1)
    router = jnp.pad(w_router, ((0, 0), (0, LANES - expert_count)))

    slots, w_in, dy_turned, hot, router = lax.optimization_barrier((slots, w_in, dy_turned, hot, router))
    low, attended, lse = attend(q, place, slots, first, offset, group)
    low = low.reshape(total, -1)
    part = out_project(low, w_out)
    middle, normed_two, gates = middle_of(act, part, swap(part, "tp"), gain_two, router, hot)
    x_par, gates_par = swap(normed_two, "ep"), swap(gates, "ep")

    early = EARLY if length == LINE else 0
    args = (normed_two, x_par, dy, dy_par, dy_turned, gates, gates_par, w_in, w_down)
    chunks, (own_back, par_back, own_mix, par_mix) = experts(early, blocks, *args)
    seq_cosine, seq_sine = cosine.reshape(seqs, rows, -1), sine.reshape(seqs, rows, -1)
    if length == LINE:
        ins = (
            own_back, par_back, own_mix, par_mix, middle, dy, router, w_out, normed_two, q, attended, act, normed,
            low, w_query, w_key, value_weight, gates, gain_two, gain_one, place, lse, seq_cosine, seq_sine,
        )
        input_grad, mix, expert_grad, big, little = back_and_sums(ins, slots, chunks, group)
        output = middle + mix.astype(F32)
        gain_two_at, gain_one_at = LANES - 1, LANES - 2
    else:
        gain_two_at, gain_one_at = expert_count, expert_count + 1
        back = total_of([own_back, swap(par_back, "ep")]).astype(BF16)
        grad_middle, branch, grad_heads, small = middle_back(
            back, swap(back, "tp"), middle, dy, gates, router, gain_two, w_out, normed_two
        )
        dq, grads = attend_back(
            q, place, grad_heads.reshape(q.shape), attended, lse, seq_cosine, seq_sine, slots, first, offset, group
        )
        dq = dq.reshape(total, -1)
        kv_sum = lax.psum_scatter(grads[0], "cp", scatter_dimension=0, tiled=True)
        kv_terms = [kv_sum, jnp.zeros_like(kv_sum), jnp.zeros_like(kv_sum)]
        kv_terms = [t.reshape(total, 2 * width) for t in kv_terms]
        spots = jnp.stack([mine, side]).astype(jnp.int32)
        big = weights(spots, blocks, [(branch, low), (normed, dq)], stacked=True)
        normed_part, dkv, gain_row = project_back(act, dq, *kv_terms, cosine, sine, w_query, w_key, value_weight)
        small = jnp.concatenate([small[:expert_count], small[LANES : LANES + 1], gain_row[:1]], axis=0)
        small = jnp.pad(small, ((0, LANES - small.shape[0]), (0, 0)))
        little = weights(spots, blocks, [(normed, dkv)], (small,))
        input_grad = input_of(act, grad_middle, normed_part, swap(normed_part, "tp"), gain_one)
        mix = total_of([own_mix, swap(par_mix, "ep")]).astype(BF16)
        output = middle + total_of([mix, swap(mix, "tp")])

        def spread_sum(keep, send):
            both = total_of([keep, swap(send, "ep")]).astype(BF16)
            return line_sum([both[0], swap(both[1], "cp")], z, length)

        turned = [jnp.swapaxes(v, 0, 1) for v in (chunks[0], swap(chunks[1], "cp"))]
        expert_grad = line_sum(turned, z, length)
        big, little = spread_sum(*big), spread_sum(*little)
    gate_up_grad = expert_grad[:, :, : 2 * half].reshape(local, -1, 2, half)
    down_grad = expert_grad[:, :, 2 * half :]
    tall = big.shape[0] // 2
    gain_part = little[:, 2 * width + gain_one_at]
    return (
        output.reshape(activations.shape),
        input_grad.reshape(activations.shape),
        big[tall:],
        little[:, :width],
        little[:, width : 2 * width],
        big[:tall],
        gain_part + swap(gain_part, "tp"),
        little[:, 2 * width + gain_two_at],
        little[:, 2 * width : 2 * width + expert_count],
        gate_up_grad,
        down_grad,
    )


def solution(mesh):
    in_specs = (
        P("ep", "cp", None),
        P("ep", "cp", None),
        P("ep", "cp"),
        P("ep", "cp", None),
        P(None, "tp"),
        P(None, "tp"),
        P(None, "tp"),
        P(None, "tp"),
        P(),
        P(),
        P(),
        P("ep", None, None, "tp"),
        P("ep", None, "tp"),
    )
    out_specs = (
        P("ep", "cp", None),
        P("ep", "cp", None),
        P(("ep", "cp"), "tp"),
        P(("ep", "cp"), "tp"),
        P(("ep", "cp"), "tp"),
        P(("ep", "cp"), "tp"),
        P(("ep", "cp")),
        P(("ep", "cp")),
        P(("ep", "cp"), None),
        P("ep", "cp", None, "tp"),
        P("ep", "cp", "tp"),
    )
    return jax.shard_map(
        on_device, mesh=mesh, in_specs=in_specs, out_specs=out_specs, check_vma=False
    )
```

```python
import functools

import jax
import jax.numpy as jnp
from jax import lax
from jax.experimental import pallas as pl
from jax.experimental.pallas import tpu as pltpu
from jax.sharding import PartitionSpec as P

HEAD = 64
EPS = 1e-06
NEG = -1e30
SCALE = 0.125
LANES = 128
KEY_CHUNK = 1024
F32 = jnp.float32
BF16 = jnp.bfloat16
MESH = pl.DeviceIdType.MESH


def mm(a, b):
    return lax.dot_general(a, b, (((1,), (0,)), ((), ())), preferred_element_type=F32)


def mm_t(a, b):
    return lax.dot_general(a, b, (((1,), (1,)), ((), ())), preferred_element_type=F32)


def t_mm(a, b):
    return lax.dot_general(a, b, (((0,), (0,)), ((), ())), preferred_element_type=F32)


def two_parts(v):
    high = v.astype(BF16)
    return high, (v - high.astype(F32)).astype(BF16)


def halves_turned(v, back):
    width = v.shape[1]
    ahead = pltpu.roll(v, width - HEAD // 2, 1)
    behind = pltpu.roll(v, HEAD // 2, 1)
    first = lax.broadcasted_iota(jnp.int32, v.shape, 1) % HEAD < HEAD // 2
    if back:
        return jnp.where(first, ahead, -behind)
    return jnp.where(first, -ahead, behind)


def rope(v, cosine, sine):
    return v * cosine + halves_turned(v, False) * sine


def rope_back(v, cosine, sine):
    return v * cosine + halves_turned(v * sine, True)


def widen(table, width):
    return jnp.concatenate([table] * (width // table.shape[1]), axis=1)


def unit_rows(v):
    scale = lax.rsqrt(jnp.mean(v * v, axis=-1, keepdims=True) + EPS)
    return v * scale, scale


def shape_of(shape, dtype):
    return jax.ShapeDtypeStruct(shape, dtype)


def params(**kw):
    return pltpu.CompilerParams(vmem_limit_bytes=60 * 2**20, **kw)


def cost(flops, moved):
    return pl.CostEstimate(flops=int(flops), bytes_accessed=int(moved), transcendentals=0)


def project_body(act, gain, wq, wk, wv, cosine, sine, normed, q, kv):
    unit, _ = unit_rows(act[...].astype(F32))
    low = (unit * gain[...]).astype(BF16)
    normed[...] = low
    qf = mm(low, wq[...])
    q[...] = rope(qf, widen(cosine[...], qf.shape[1]), widen(sine[...], qf.shape[1])).astype(BF16)
    kf = mm(low, wk[...])
    width = kf.shape[1]
    kv[:, :width] = rope(kf, widen(cosine[...], width), widen(sine[...], width)).astype(BF16)
    kv[:, width:] = mm(low, wv[...]).astype(BF16)


def project(act, gain, wq, wk, wv, cosine, sine):
    rows, model = act.shape
    total = wq.shape[1] + 2 * wk.shape[1]
    return pl.pallas_call(
        project_body,
        out_shape=(
            shape_of((rows, model), BF16),
            shape_of((rows, wq.shape[1]), BF16),
            shape_of((rows, 2 * wk.shape[1]), BF16),
        ),
        compiler_params=params(),
        cost_estimate=cost(2 * rows * model * total, 2 * model * total + 6 * rows * model),
        name="project",
    )(act, gain, wq, wk, wv, cosine, sine)


def fill_keys(firsts, offset, place, slots, keys, bias, rows):
    query = lax.broadcasted_iota(jnp.int32, (rows, rows), 1) + offset
    for at, slot in enumerate(slots):
        keys[at * rows : (at + 1) * rows, :] = slot[...]
        key = lax.broadcasted_iota(jnp.int32, (rows, rows), 0) + firsts[at]
        distance = query - key
        seen = (distance >= 0) & (distance <= place)
        bias[at * rows : (at + 1) * rows, :] = jnp.where(seen, 0.0, NEG)


def single_slots(slots):
    return [slot.at[one, 0] for slot in slots for one in range(slot.shape[0])]


def group_rows(block, head, group):
    return jnp.concatenate(
        [block[:, (head * group + g) * HEAD : (head * group + g + 1) * HEAD] for g in range(group)], axis=0
    )


def attend_body(group, count, first_ref, offset_ref, q_ref, place_ref, *refs):
    slots = refs[:count]
    low_ref, out_ref, lse_ref, keys, bias = refs[count:]
    rows = q_ref.shape[1]
    singles = single_slots(slots)
    fill_keys([first_ref[i] for i in range(len(singles))], offset_ref[0], place_ref[0], singles, keys, bias, rows)
    total, width = keys.shape[0], keys.shape[1] // 2
    chunk = min(total, KEY_CHUNK)
    q = (q_ref[0].astype(F32) * SCALE).astype(BF16)
    pieces = []
    for head in range(width // HEAD):
        q3 = group_rows(q, head, group)
        top = run = out = None
        for low in range(0, total, chunk):
            k = keys[low : low + chunk, head * HEAD : (head + 1) * HEAD]
            v = keys[low : low + chunk, width + head * HEAD : width + (head + 1) * HEAD]
            s = mm_t(k, q3) + widen(bias[low : low + chunk, :], group * rows)
            here = jnp.max(s, axis=0, keepdims=True)
            new = here if top is None else jnp.maximum(top, here)
            p = jnp.exp(s - new)
            part = jnp.sum(p, axis=0, keepdims=True)
            o = t_mm(v, p.astype(BF16))
            if top is None:
                run, out = part, o
            else:
                shrink = jnp.exp(top - new)
                run, out = run * shrink + part, out * shrink + o
            top = new
        out = jnp.transpose(out / run)
        pieces += [out[g * rows : (g + 1) * rows] for g in range(group)]
        lse_ref[0, head : head + 1, :] = top + jnp.log(run)
    whole = jnp.concatenate(pieces, axis=1)
    out_ref[0] = whole
    low_ref[0] = whole.astype(BF16)


def seq_block(shape):
    return pl.BlockSpec((1,) + shape[1:], lambda s, *_: (s,) + (0,) * (len(shape) - 1))


def slot_block(shape):
    return pl.BlockSpec((shape[0], 1) + shape[2:], lambda s, *_: (0, s, 0, 0))


def attend(q, place, slots, first, offset, group):
    seqs, rows, wide = q.shape
    both = slots[0].shape[-1]
    total = rows * sum(slot.shape[0] for slot in slots)
    heads = wide // HEAD // group
    outs = (
        shape_of(q.shape, BF16),
        shape_of(q.shape, F32),
        shape_of((seqs, heads, group * rows), F32),
    )
    return pl.pallas_call(
        functools.partial(attend_body, group, len(slots)),
        out_shape=outs,
        grid_spec=pltpu.PrefetchScalarGridSpec(
            num_scalar_prefetch=2,
            grid=(seqs,),
            in_specs=[seq_block(q.shape), seq_block(place.shape)] + [slot_block(s.shape) for s in slots],
            out_specs=tuple(seq_block(o.shape) for o in outs),
            scratch_shapes=[pltpu.VMEM((total, both), BF16), pltpu.VMEM((total, rows), F32)],
        ),
        compiler_params=params(),
        cost_estimate=cost(2e9 * 4, 20e6),
        name="attend",
    )(first, offset, q, place, *slots)


def attend_back_core(
    group, q, place, go, out, lse_ref, cosine, sine, slots, firsts, offset, keys, bias, keep_grad, most
):
    rows = q.shape[0]
    fill_keys(firsts, offset, place, slots, keys, bias, rows)
    total, width = keys.shape[0], keys.shape[1] // 2
    chunk = min(total, most)
    q = (q.astype(F32) * SCALE).astype(BF16)
    products = go.astype(F32) * out
    ones = jnp.ones((8, HEAD), F32)
    heads = width // HEAD
    q3s = [group_rows(q, head, group) for head in range(heads)]
    g3s = [group_rows(go, head, group) for head in range(heads)]
    deltas = [
        lax.dot_general(
            ones,
            group_rows(products, head, group),
            (((1,), (1,)), ((), ())),
            preferred_element_type=F32,
            precision=lax.Precision.HIGHEST,
        )[:1]
        for head in range(heads)
    ]
    dq = [None] * heads
    for low in range(0, total, chunk):
        dks, dvs = [], []
        for head in range(heads):
            k = keys[low : low + chunk, head * HEAD : (head + 1) * HEAD]
            v = keys[low : low + chunk, width + head * HEAD : width + (head + 1) * HEAD]
            s = mm_t(k, q3s[head]) + widen(bias[low : low + chunk, :], group * rows)
            p = jnp.exp(s - lse_ref[head : head + 1, :])
            dp = mm_t(v, g3s[head])
            ds = (p * (dp - deltas[head])).astype(BF16)
            dks.append(mm(ds, q3s[head]))
            dvs.append(mm(p.astype(BF16), g3s[head]))
            part = t_mm(k, ds)
            dq[head] = part if dq[head] is None else dq[head] + part
        both = jnp.concatenate(dks + dvs, axis=1).astype(BF16)
        for one in range(chunk // rows):
            keep_grad(low // rows + one, both[one * rows : (one + 1) * rows])
    pieces = []
    for head in range(heads):
        back = jnp.transpose(dq[head] * SCALE)
        pieces += [back[g * rows : (g + 1) * rows] for g in range(group)]
    whole = jnp.concatenate(pieces, axis=1)
    return rope_back(whole, widen(cosine, whole.shape[1]), widen(sine, whole.shape[1])).astype(BF16)


def attend_back_body(
    group, count, first_ref, offset_ref, q_ref, place_ref, grad_ref, out_ref, lse_ref, cos_ref, sin_ref, *refs
):
    slots = single_slots(refs[:count])
    dq_ref = refs[count]
    grads = single_slots(refs[count + 1 : 2 * count + 1])
    keys, bias = refs[2 * count + 1 :]

    def keep_grad(at, value):
        grads[at][...] = value

    dq_ref[0] = attend_back_core(
        group,
        q_ref[0],
        place_ref[0],
        grad_ref[0],
        out_ref[0],
        lse_ref.at[0],
        cos_ref[0],
        sin_ref[0],
        slots,
        [first_ref[i] for i in range(len(slots))],
        offset_ref[0],
        keys,
        bias,
        keep_grad,
        KEY_CHUNK,
    )


def attend_back(q, place, grad, out, lse, cosine, sine, slots, first, offset, group):
    seqs, rows, _ = q.shape
    both = slots[0].shape[-1]
    total = rows * sum(slot.shape[0] for slot in slots)
    outs = (shape_of(q.shape, BF16),) + tuple(shape_of(s.shape, BF16) for s in slots)
    ins = (q, place, grad, out, lse, cosine, sine)
    got = pl.pallas_call(
        functools.partial(attend_back_body, group, len(slots)),
        out_shape=outs,
        grid_spec=pltpu.PrefetchScalarGridSpec(
            num_scalar_prefetch=2,
            grid=(seqs,),
            in_specs=[seq_block(a.shape) for a in ins] + [slot_block(s.shape) for s in slots],
            out_specs=(seq_block(outs[0].shape),) + tuple(slot_block(s.shape) for s in slots),
            scratch_shapes=[pltpu.VMEM((total, both), BF16), pltpu.VMEM((total, rows), F32)],
        ),
        compiler_params=params(),
        cost_estimate=cost(2e9 * 8, 30e6),
        name="attend_back",
    )(first, offset, *ins, *slots)
    return got[0], got[1:]


def out_body(low, w_out, part):
    part[...] = mm_t(low[...], w_out[...]).astype(BF16)


def out_project(low, w_out):
    rows, model = low.shape[0], w_out.shape[0]
    return pl.pallas_call(
        out_body,
        out_shape=shape_of((rows, model), BF16),
        compiler_params=params(),
        cost_estimate=cost(2 * rows * model * low.shape[1], 4e6),
        name="out_project",
    )(low, w_out)


def middle_body(act, part, other, gain, router, hot, middle, normed, gates):
    mid = act[...].astype(F32) + (part[...].astype(F32) + other[...].astype(F32))
    middle[...] = mid
    unit, _ = unit_rows(mid)
    low = (unit * gain[...]).astype(BF16)
    normed[...] = low
    chosen = hot[...] > 0.5
    logits = jnp.where(chosen, mm(low, router[...]), NEG)
    up = jnp.where(chosen, jnp.exp(logits - jnp.max(logits, axis=-1, keepdims=True)), 0.0)
    gates[...] = up / jnp.sum(up, axis=-1, keepdims=True)


def middle_of(act, part, other, gain, router, hot):
    rows, model = act.shape
    return pl.pallas_call(
        middle_body,
        out_shape=(shape_of((rows, model), F32), shape_of((rows, model), BF16), shape_of((rows, LANES), F32)),
        compiler_params=params(),
        cost_estimate=cost(2 * rows * model * LANES, 12 * rows * model),
        name="middle",
    )(act, part, other, gain, router, hot)


EARLY = 2
FIRST = 1


def experts_body(early, first, x_own, x_par, dy_own, dy_par, dy_turned, g_own, g_par, w_in, w_out, keep, send, *refs):
    refs = list(refs)
    came, z_kept, z_sent = (refs.pop(0), refs.pop(0), refs.pop(0)) if early else (None, None, None)
    own_back, par_back, own_mix, par_mix, x_turned, dy_order, x_all, dy_all, back, mix, pulls, blocks_of = refs[:12]
    step, steps = pl.program_id(0), pl.num_programs(0)
    rows, model = x_own.shape
    wide = own_back.shape[1] - model
    blocks, depth, _ = blocks_of.shape
    side = lax.axis_index("cp") % 2
    if early:
        leaving, held, spots, es, er, zs, zr = refs[12:]
        p = Place()
        flows = [Flow(p, held.at[i], spots.at[i], zs.at[i], zr.at[i]) for i in range(2)]

    def early_copy(i):
        return p.copy("x", leaving.at[i], came.at[i], es.at[i], er.at[i])

    @pl.when(step == 0)
    def _():
        if early:
            p.greet(("x",))
        x_all[:rows] = x_own[...]
        x_all[rows:] = x_par[...]
        dy_all[:rows] = dy_own[...]
        dy_all[rows:] = dy_par[...]
        blocks_of[...] = jnp.transpose(x_all[...]).reshape(blocks_of.shape)
        for z in range(blocks // 2):
            x_turned[z] = blocks_of[2 * z + side]
            x_turned[blocks // 2 + z] = blocks_of[2 * z + 1 - side]
            dy_order[z] = dy_turned[2 * z + side]
            dy_order[blocks // 2 + z] = dy_turned[2 * z + 1 - side]
        back[...] = jnp.zeros_like(back)
        mix[...] = jnp.zeros_like(mix)
        pulls[...] = jnp.zeros_like(pulls)

    expert = lax.axis_index("ep") * steps + step
    lane = lax.broadcasted_iota(jnp.int32, (2 * rows, wide), 1) == expert
    gate_rows = jnp.concatenate([g_own[...], g_par[...]], axis=0)
    gate = jnp.sum(jnp.where(lane, gate_rows, 0.0), axis=-1, keepdims=True)
    x, dy = x_all[...], dy_all[...]
    w_gu, w_d = w_in[0], w_out[0]
    both = mm(x, w_gu)
    half = both.shape[1] // 2
    g, u = both[:, :half], both[:, half:]
    pull = mm(dy, w_d)
    sig = 1.0 / (1.0 + jnp.exp(-g))
    act = g * sig
    hidden = (act * u).astype(BF16).astype(F32)
    pulls[...] += jnp.where(lane, jnp.sum(hidden * pull, axis=-1, keepdims=True), 0.0)
    weighted = (gate * hidden).astype(BF16)
    pull = gate * pull
    d_g = (pull * u * sig * (1.0 + g * (1.0 - sig))).astype(BF16)
    d_u = (pull * act).astype(BF16)
    d_gu = jnp.concatenate([d_g, d_u], axis=1)
    for i, out in enumerate((keep, send)):
        at = pl.ds(i * (blocks // 2), blocks // 2)
        shape = (model // 2, 2 * rows)
        to = (blocks // 2, depth, -1)
        out[0, :, :, : 2 * half] = mm(x_turned[at].reshape(shape), d_gu).astype(BF16).reshape(to)
        out[0, :, :, 2 * half :] = mm(dy_order[at].reshape(shape), weighted).astype(BF16).reshape(to)
    if early:

        @pl.when(step == 0)
        def _():
            held[0] = keep[0]
            held[1] = send[0]
            for flow in flows:
                flow.open()

        for i in range(early):

            @pl.when(step == first + i)
            def _(i=i):
                leaving[i] = send[0]
                early_copy(i).start()

        for at, work in ((2, flows[0].second), (3, flows[0].third), (4, flows[1].second), (5, flows[1].third)):

            @pl.when(step == at)
            def _(work=work):
                work()

    back[...] += mm_t(d_gu, w_gu)
    mix[...] += mm_t(weighted, w_d)

    @pl.when(step == steps - 1)
    def _():
        own_back[:, :model] = back[:rows].astype(BF16)
        par_back[:, :model] = back[rows:].astype(BF16)
        own_back[:, model:] = pulls[:rows].astype(BF16)
        par_back[:, model:] = pulls[rows:].astype(BF16)
        own_mix[...] = mix[:rows].astype(BF16)
        par_mix[...] = mix[rows:].astype(BF16)
        if early:
            for flow, out in zip(flows, (z_kept, z_sent)):

                def finish(parts, out=out):
                    out[...] = total_of(parts).astype(out.dtype)

                flow.close(finish)
                flow.drain()
            for i in range(early):
                early_copy(i).wait()


def experts(early, first, blocks, x_own, x_par, dy_own, dy_par, dy_turned, g_own, g_par, w_in, w_out):
    rows, model = x_own.shape
    count, _, half = w_out.shape
    depth = model // blocks
    once = lambda shape: pl.BlockSpec(shape, lambda e: (0,) * len(shape))
    whole = (blocks // 2, depth, 3 * half)
    ins = [x_own, x_par, dy_own, dy_par, dy_turned, g_own, g_par]
    tail = [shape_of((rows, model + LANES), BF16)] * 2 + [shape_of((rows, model), BF16)] * 2
    outs = [shape_of((count - first,) + whole, BF16), shape_of((count - first - early,) + whole, BF16)]
    specs = [
        pl.BlockSpec((1,) + whole, lambda e: (jnp.maximum(e - first, 0), 0, 0, 0)),
        pl.BlockSpec((1,) + whole, lambda e: (jnp.maximum(e - first - early, 0), 0, 0, 0)),
    ]
    turned = (blocks, depth, 2 * rows)
    scratch = [
        pltpu.VMEM(turned, BF16),
        pltpu.VMEM(turned, BF16),
        pltpu.VMEM((2 * rows, model), BF16),
        pltpu.VMEM((2 * rows, model), BF16),
        pltpu.VMEM((2 * rows, model), F32),
        pltpu.VMEM((2 * rows, model), F32),
        pltpu.VMEM((2 * rows, LANES), F32),
        pltpu.VMEM(turned, BF16),
    ]
    kind = params()
    if early:
        dma = pltpu.SemaphoreType.DMA
        sums = [shape_of(whole[1:], F32), shape_of(whole[1:], BF16)]
        outs += [shape_of((early,) + whole, BF16)] + sums
        specs += [pl.BlockSpec(memory_space=pl.ANY)] + [once(t.shape) for t in sums]
        scratch += [
            pltpu.VMEM((early,) + whole, BF16),
            pltpu.VMEM((2,) + whole, BF16),
            pltpu.VMEM((2, 5) + whole[1:], BF16),
            dma((early,)),
            dma((early,)),
            dma((2, 6)),
            dma((2, 6)),
        ]
        kind = params(collective_id=2, has_side_effects=True)
    got = pl.pallas_call(
        functools.partial(experts_body, early, first),
        out_shape=tuple(outs + tail),
        grid=(count,),
        in_specs=[once(a.shape) for a in ins]
        + [
            pl.BlockSpec((1, model, 2 * half), lambda e: (e, 0, 0)),
            pl.BlockSpec((1, model, half), lambda e: (e, 0, 0)),
        ],
        out_specs=tuple(specs + [once(t.shape) for t in tail]),
        scratch_shapes=scratch,
        compiler_params=kind,
        cost_estimate=cost(count * 18 * 2 * rows * model * half, count * 12 * model * half),
        name="experts",
    )(*ins, w_in, w_out)
    return got[: len(outs)], got[len(outs) :]


def middle_back_body(mine, other, middle, dy, gates, router, gain, w_out, normed, grad, low, heads, small):
    model = middle.shape[1]
    total = mine[...].astype(F32) + other[...].astype(F32)
    gate, pulls = gates[...], total[:, model:]
    chosen = gate * (pulls - jnp.sum(gate * pulls, axis=-1, keepdims=True))
    high, rest = two_parts(chosen)
    grad_two = total[:, :model] + (mm_t(high, router[...]) + mm_t(rest, router[...]))
    unit, scale = unit_rows(middle[...])
    small[:LANES, :] = t_mm(high, normed[...]) + t_mm(rest, normed[...])
    small[LANES : LANES + 8, :] = jnp.broadcast_to(jnp.sum(grad_two * unit, axis=0, keepdims=True), (8, model))
    scaled = grad_two * gain[...]
    out = dy[...].astype(F32) + scale * (scaled - unit * jnp.mean(scaled * unit, axis=-1, keepdims=True))
    grad[...] = out
    rounded = out.astype(BF16)
    low[...] = rounded
    heads[...] = mm(rounded, w_out[...]).astype(BF16)


def middle_back(mine, other, middle, dy, gates, router, gain, w_out, normed):
    rows, model = middle.shape
    return pl.pallas_call(
        middle_back_body,
        out_shape=(
            shape_of((rows, model), F32),
            shape_of((rows, model), BF16),
            shape_of((rows, w_out.shape[1]), BF16),
            shape_of((LANES + 8, model), F32),
        ),
        compiler_params=params(),
        cost_estimate=cost(2 * rows * model * (w_out.shape[1] + 4 * LANES), 10e6),
        name="middle_back",
    )(mine, other, middle, dy, gates, router, gain, w_out, normed)


def project_back_body(width, act, dq, a, b, c, cosine, sine, wq, wk, wv, part, dkv, gain_row):
    total = a[...].astype(F32) + b[...].astype(F32) + c[...].astype(F32)
    dk = rope_back(total[:, :width], widen(cosine[...], width), widen(sine[...], width)).astype(BF16)
    dv = total[:, width:].astype(BF16)
    dkv[:, :width] = dk
    dkv[:, width:] = dv
    full = mm_t(dq[...], wq[...]) + mm_t(dk, wk[...]) + mm_t(dv, wv[...])
    part[...] = full.astype(BF16)
    unit, _ = unit_rows(act[...].astype(F32))
    gain_row[...] = jnp.broadcast_to(jnp.sum(full * unit, axis=0, keepdims=True), gain_row.shape)


def project_back(act, dq, a, b, c, cosine, sine, wq, wk, wv):
    rows, model = act.shape
    width = wk.shape[1]
    return pl.pallas_call(
        functools.partial(project_back_body, width),
        out_shape=(
            shape_of((rows, model), BF16),
            shape_of((rows, 2 * width), BF16),
            shape_of((8, model), F32),
        ),
        compiler_params=params(),
        cost_estimate=cost(2 * rows * model * (wq.shape[1] + 2 * width), 8e6),
        name="project_back",
    )(act, dq, a, b, c, cosine, sine, wq, wk, wv)


def input_body(act, grad, mine, other, gain, out):
    unit, scale = unit_rows(act[...].astype(F32))
    scaled = (mine[...].astype(F32) + other[...].astype(F32)) * gain[...]
    out[...] = grad[...] + scale * (scaled - unit * jnp.mean(scaled * unit, axis=-1, keepdims=True))


def input_of(act, grad, mine, other, gain):
    return pl.pallas_call(
        input_body,
        out_shape=shape_of(act.shape, F32),
        compiler_params=params(),
        cost_estimate=cost(0, 12 * act.shape[0] * act.shape[1]),
        name="input_grad",
    )(act, grad, mine, other, gain)


def weights_body(blocks, count, stacked, where_ref, *refs):
    lefts = refs[:count]
    rights = refs[count : 2 * count]
    extra = refs[2 * count : -3]
    keep, send, whole = refs[-3:]
    parts = [t_mm(a[...], b[...]).astype(BF16) for a, b in zip(lefts, rights)]
    parts += [jnp.transpose(e[...]).astype(BF16) for e in extra]
    at = down = 0
    for part in parts:
        block = part.reshape(2 * blocks, -1, part.shape[1])
        whole[:, down : down + block.shape[1], at : at + part.shape[1]] = block
        if stacked:
            down += block.shape[1]
        else:
            at += part.shape[1]
    mine, side = where_ref[0], where_ref[1]
    for half, ref in ((mine, keep), (1 - mine, send)):
        for z in range(blocks // 2):
            ref[0, z] = whole[half * blocks + 2 * z + side]
            ref[1, z] = whole[half * blocks + 2 * z + 1 - side]


def weights(where, blocks, pairs, extra=(), stacked=False):
    model = pairs[0][0].shape[1]
    rows = pairs[0][0].shape[0]
    depth = model // (2 * blocks)
    columns = sum(b.shape[1] for _, b in pairs) + sum(e.shape[0] for e in extra)
    tall, wide = (depth * len(pairs), pairs[0][1].shape[1]) if stacked else (depth, columns)
    shape = (2, blocks // 2, tall, wide)
    ins = [a for a, _ in pairs] + [b for _, b in pairs] + list(extra)
    full = lambda a: pl.BlockSpec(a.shape, lambda i, *_: (0,) * len(a.shape))
    return pl.pallas_call(
        functools.partial(weights_body, blocks, len(pairs), stacked),
        out_shape=(shape_of(shape, BF16),) * 2,
        grid_spec=pltpu.PrefetchScalarGridSpec(
            num_scalar_prefetch=1,
            grid=(1,),
            in_specs=[full(a) for a in ins],
            out_specs=(pl.BlockSpec(shape, lambda i, *_: (0, 0, 0, 0)),) * 2,
            scratch_shapes=[pltpu.VMEM((2 * blocks, tall, wide), BF16)],
        ),
        compiler_params=params(),
        cost_estimate=cost(2 * rows * model * columns, 4 * model * columns),
        name="weights",
    )(where, *ins)


def swap(v, axis):
    size = lax.axis_size(axis)
    return lax.ppermute(v, axis, [(i, i ^ 1) for i in range(size)])


def up(v, low, high):
    return lax.ppermute(v, "cp", [(2 * z + s, 2 * z + 2 + s) for z in range(low, high) for s in range(2)])


def down(v, low, high):
    return lax.ppermute(v, "cp", [(2 * z + s, 2 * z - 2 + s) for z in range(low, high) for s in range(2)])


def total_of(terms):
    return functools.reduce(lambda a, b: a + b, [t.astype(F32) for t in terms])


def line_sum(parts, z, length):
    def own(d):
        return [lax.dynamic_index_in_dim(p, jnp.clip(d, 0, length - 1), 0, keepdims=False) for p in parts]

    if length > 4:
        mine = total_of(parts).astype(BF16)
        side = lax.axis_index("cp") % 2
        full = jnp.where(jnp.arange(2).reshape((1, 2) + (1,) * (mine.ndim - 1)) == side, mine[:, None], 0)
        full = full.reshape((2 * length,) + mine.shape[1:])
        return lax.psum_scatter(full, "cp", scatter_dimension=0, tiled=True)[0].astype(F32)
    right = left = None
    for k in range(length - 1):
        far = length - 1 - k
        terms = own(z + far) + ([] if right is None else [right])
        right = up(total_of(terms).astype(BF16), 0, k + 1)
        terms = own(z - far) + ([] if left is None else [left])
        left = down(total_of(terms).astype(BF16), far, length)
    return total_of(own(z) + ([right, left] if length > 1 else []))


LINE = 4
RING = 6


def add_to(ref, at, other):
    ref[at] = (ref[at].astype(F32) + other.astype(F32)).astype(BF16)


class Place:
    def __init__(self):
        self.cp = lax.axis_index("cp")
        self.z, self.side = self.cp // 2, self.cp % 2
        self.ep, self.tp = lax.axis_index("ep"), lax.axis_index("tp")

    def to(self, way):
        if way == "x":
            return {"cp": self.cp + 1 - 2 * self.side}
        if way == "up":
            return {"cp": self.cp + 2}
        if way == "down":
            return {"cp": self.cp - 2}
        return {way: 1 - (self.ep if way == "ep" else self.tp)}

    def signal(self, sem, way):
        pl.semaphore_signal(sem, inc=1, device_id=self.to(way), device_id_type=MESH)

    def signal_line(self, to_down, to_up):
        @pl.when(self.z > 0)
        def _():
            self.signal(to_down, "down")

        @pl.when(self.z < LINE - 1)
        def _():
            self.signal(to_up, "up")

    def greet(self, ways):
        barrier = pltpu.get_barrier_semaphore()
        for way in ways:
            self.signal(barrier, way)
        self.signal_line(barrier, barrier)
        both = jnp.where(self.z > 0, 1, 0) + jnp.where(self.z < LINE - 1, 1, 0)
        pl.semaphore_wait(barrier, len(ways) + both)

    def copy(self, way, src, dst, send, recv):
        return pltpu.make_async_remote_copy(
            src_ref=src, dst_ref=dst, send_sem=send, recv_sem=recv, device_id=self.to(way), device_id_type=MESH
        )

    def at(self, z):
        return pl.when(self.z == z)


LEFT_SPOT = (3, 4, 0)


class Flow:
    def __init__(self, place, held, spots, send, recv, credit=None):
        self.p, self.held, self.spots, self.send, self.recv, self.credit = place, held, spots, send, recv, credit

    def right(self, d):
        return self.p.copy("up", self.held.at[d], self.spots.at[d - 1], self.send.at[d - 1], self.recv.at[d - 1])

    def left(self, d):
        spot = LEFT_SPOT[d]
        return self.p.copy("down", self.held.at[d], self.spots.at[spot], self.send.at[d + 3], self.recv.at[d + 3])

    def allowed(self, way):
        if self.credit is not None:
            pl.semaphore_wait(self.credit[way], 1)

    def open(self):
        @self.p.at(0)
        def _():
            self.allowed("up")
            for d in (3, 2, 1):
                self.right(d).start()

        @self.p.at(3)
        def _():
            self.allowed("down")
            for d in (0, 1, 2):
                self.left(d).start()

    def pass_right(self, d):
        self.right(d).wait_recv()
        add_to(self.held, d, self.spots[d - 1])
        self.right(d).start()

    def pass_left(self, d):
        self.left(d).wait_recv()
        add_to(self.held, d, self.spots[LEFT_SPOT[d]])
        self.left(d).start()

    def second(self):
        @self.p.at(1)
        def _():
            self.allowed("up")
            self.pass_right(3)
            self.pass_right(2)

        @self.p.at(2)
        def _():
            self.allowed("down")
            self.pass_left(0)
            self.pass_left(1)

    def third(self):
        @self.p.at(2)
        def _():
            self.allowed("up")
            self.pass_right(3)

        @self.p.at(1)
        def _():
            self.allowed("down")
            self.pass_left(0)

    def close(self, finish):
        for z in range(LINE):

            @self.p.at(z)
            def _(z=z):
                blocks = [self.held[z]]
                if z > 0:
                    self.right(z).wait_recv()
                    blocks.append(self.spots[z - 1])
                if z < LINE - 1:
                    self.left(z).wait_recv()
                    blocks.append(self.spots[LEFT_SPOT[z]])
                finish(blocks)

    def drain(self):
        for z in range(LINE):

            @self.p.at(z)
            def _(z=z):
                for d in range(z + 1, LINE):
                    self.right(d).wait_send()
                for d in range(z):
                    self.left(d).wait_send()


class Names:
    pass


def named(names, refs):
    out = Names()
    for name, ref in zip(names, refs, strict=True):
        setattr(out, name, ref)
    return out


BACK_INS = (
    "own_back", "par_back", "own_mix", "par_mix", "middle", "dy", "router", "w_out", "x2", "q", "attended",
    "act", "normed", "low", "wq", "wk", "wv", "gates", "gain_two", "gain_one", "place", "lse", "cosine",
    "sine",
)
BACK_IN_PLACE = 7
BACK_OUTS = (
    "grad", "mix", "experts", "big_out", "little_out",
)
BACK_SCRATCH = (
    "back", "other_ep", "other_tp", "mid_dy", "mid_x2", "wide_w", "branch", "heads", "small", "qs", "atts",
    "slots", "kv_x", "kv_z", "keys", "bias", "dq", "lows", "wks", "wvs", "routers", "dkv", "part", "part_in",
    "mix_ep", "mix_tp", "held", "spots", "kept", "staged", "zero_in", "whole", "came", "lit",
    "lit_came", "lit_x", "lit_spots", "ls", "ks", "xs", "xr", "zs", "zr", "es", "er", "ts", "tr", "kxs",
    "kxr", "kzs", "kzr", "os", "free_x", "free_up", "free_down",
)


def back_body(group, *refs):
    n_in = len(BACK_INS) + 2 * LINE + 5
    ins = named(BACK_INS, refs[: len(BACK_INS)])
    slots_in = refs[len(BACK_INS) : n_in - 5]
    keeps, sends, arrived, z_kept, z_sent = refs[n_in - 5 : n_in]
    o = named(BACK_OUTS, refs[n_in : n_in + len(BACK_OUTS)])
    s = named(BACK_SCRATCH, refs[n_in + len(BACK_OUTS) :])
    p = Place()
    early = arrived.shape[0]
    first = FIRST
    count = first + keeps.shape[0]
    seqs, rows, _ = ins.q.shape
    model = ins.middle.shape[1]
    width = ins.wk.shape[1]
    part_of = lambda i: pl.ds(i * rows, rows)

    ring = [("here", e) for e in range(first, first + early)]
    ring += [("x", e) for e in range(first + early, count)] + [("big", count)]
    index_of = {item: i for i, item in enumerate(ring)}
    crosses = lambda item: item[0] in ("x", "big")

    def flow(item):
        if item == "little":
            return Flow(p, s.lit_x, s.lit_spots, s.zs.at[len(ring)], s.zr.at[len(ring)])
        i = index_of[item]
        credit = {"up": s.free_up, "down": s.free_down} if i >= RING else None
        return Flow(p, s.held.at[i % RING], s.spots.at[i % RING], s.zs.at[i], s.zr.at[i], credit)

    def x_copy(item):
        if item == "little":
            return p.copy("x", s.lit.at[p.ep, :, 1 - p.side], s.lit_x, s.xs.at[len(ring)], s.xr.at[len(ring)])
        i = index_of[item]
        src = s.whole.at[p.ep, :, 1 - p.side] if item[0] == "big" else sends.at[item[1] - first - early]
        return p.copy("x", src, s.held.at[i % RING], s.xs.at[i], s.xr.at[i])

    def cross(item):
        if item != "little" and index_of[item] >= RING:
            pl.semaphore_wait(s.free_x, 1)
        x_copy(item).start()

    def load_keep(e):
        return pltpu.make_async_copy(keeps.at[e - first], s.kept, s.ks.at[0])

    def load_arrived(e):
        return pltpu.make_async_copy(arrived.at[e - first], s.held.at[e - first], s.ks.at[1 + e - first])

    def opened(item):
        if item == "little":
            x_copy(item).wait_recv()
            for d in range(LINE):
                add_to(s.lit_x, d, s.lit[p.ep, d, p.side])
        else:
            held = s.held.at[index_of[item] % RING]
            if item[0] == "here":
                load_arrived(item[1]).wait()
            else:
                x_copy(item).wait_recv()
            if item[0] == "big":
                for d in range(LINE):
                    add_to(held, d, s.whole[p.ep, d, p.side])
            else:
                load_keep(item[1]).wait()
                for d in range(LINE):
                    add_to(held, d, s.kept[d])
                if item[1] + 1 < count:
                    load_keep(item[1] + 1).start()
        flow(item).open()

    stored = []

    def store(e):
        return pltpu.make_async_copy(s.staged.at[e % 2], o.experts.at[e], s.os.at[e])

    def finish_expert(e, make):
        if len(stored) >= 2 and e % 2 in [k % 2 for k in stored[-2:]]:
            last = [k for k in stored if k % 2 == e % 2][-1]
            store(last).wait()
            waited.add(last)
        make()
        store(e).start()
        stored.append(e)

    waited = set()

    def closed(item):
        if item == "little":
            def finish(blocks):
                o.little_out[...] = total_of(blocks)

            flow(item).close(finish)
        elif item[0] == "big":
            def finish(blocks):
                o.big_out[...] = total_of(blocks)

            flow(item).close(finish)
        else:
            def finish(blocks):
                s.staged[item[1] % 2] = total_of(blocks)

            finish_expert(item[1], lambda: flow(item).close(finish))

    def freed(item):
        flow(item).drain()
        if item == "little":
            return
        after = index_of[item] + RING
        if after < len(ring):
            if crosses(item):
                x_copy(item).wait_send()
            if crosses(ring[after]):
                p.signal(s.free_x, "x")
            p.signal_line(s.free_up, s.free_down)

    loads = {}

    def load(name, src, dst):
        copy = pltpu.make_async_copy(src, dst, s.ls.at[len(loads)])
        copy.start()
        loads[name] = copy

    def got(*names):
        for name in names:
            loads[name].wait()

    load("back", ins.own_back, s.back)
    load_keep(first).start()
    for e in range(first, first + early):
        load_arrived(e).start()
    load("zero", z_kept, s.staged.at[0])
    load("grad", ins.middle, o.grad)
    load("dy", ins.dy, s.mid_dy)
    load("router", ins.router, s.routers)
    load("x2", ins.x2, s.mid_x2)
    load("w_out", ins.w_out, s.wide_w)
    load("mix", ins.own_mix, o.mix)
    load("q", ins.q, s.qs)
    load("attended", ins.attended, s.atts)
    for j in range(2 * LINE):
        load(f"slot{j}", slots_in[j].at[0], s.slots.at[:, j // 2, j % 2])
    load("low", ins.low, s.lows)
    load("wk", ins.wk, s.wks)
    load("wv", ins.wv, s.wvs)

    p.greet(("x", "ep", "tp"))
    ep_back = p.copy("ep", ins.par_back, s.other_ep, s.es.at[0], s.er.at[0])
    ep_back.start()
    ep_mix = p.copy("ep", ins.par_mix, s.mix_ep, s.es.at[1], s.er.at[1])
    ep_mix.start()
    queue = ring[early:] + ["little"]
    zero_copy = p.copy("x", z_sent, s.zero_in, s.xs.at[len(ring) + 1], s.xr.at[len(ring) + 1])
    zero_copy.start()
    cross(queue.pop(0))
    cross(queue.pop(0))

    got("back")
    ep_back.wait_recv()
    for i in range(seqs):
        s.back[part_of(i)] = (
            s.back[part_of(i)].astype(F32) + s.other_ep[part_of(i)].astype(F32)
        ).astype(BF16)
    tp_back = p.copy("tp", s.back, s.other_tp, s.ts.at[0], s.tr.at[0])
    tp_back.start()
    got("mix")
    ep_mix.wait_recv()
    for i in range(seqs):
        o.mix[part_of(i)] = (o.mix[part_of(i)].astype(F32) + s.mix_ep[part_of(i)].astype(F32)).astype(BF16)

    def step_middle():
        got("grad", "dy", "router", "x2", "w_out")
        tp_back.wait_recv()
        for i in range(seqs):
            at = part_of(i)
            total = s.back[at].astype(F32) + s.other_tp[at].astype(F32)
            gate, pulls = ins.gates[at], total[:, model:]
            chosen = gate * (pulls - jnp.sum(gate * pulls, axis=-1, keepdims=True))
            high, rest = two_parts(chosen)
            grad_two = total[:, :model] + (mm_t(high, s.routers[...]) + mm_t(rest, s.routers[...]))
            unit, scale = unit_rows(o.grad[at])
            routed = t_mm(high, s.mid_x2[at]) + t_mm(rest, s.mid_x2[at])
            gain_row = jnp.sum(grad_two * unit, axis=0, keepdims=True)
            if i == 0:
                s.small[...] = routed
                s.small[LANES - 1 :, :] = gain_row
            else:
                s.small[: LANES - 1, :] += routed[: LANES - 1]
                s.small[LANES - 1 :, :] += gain_row
            scaled = grad_two * ins.gain_two[...]
            out = s.mid_dy[at].astype(F32) + scale * (
                scaled - unit * jnp.mean(scaled * unit, axis=-1, keepdims=True)
            )
            o.grad[at] = out
            rounded = out.astype(BF16)
            s.branch[at] = rounded
            s.heads[at] = mm(rounded, s.wide_w[...]).astype(BF16)
        load("wq", ins.wq, s.wide_w)
        load("act", ins.act, s.mid_dy)
        load("normed", ins.normed, s.mid_x2)

    tp_mix = p.copy("tp", o.mix, s.mix_tp, s.ts.at[1], s.tr.at[1])

    def step_attend(i):
        if i == 0:
            got("q", "attended", *[f"slot{j}" for j in range(2 * LINE)])
        homes = [(p.z - r, side) for r in range(LINE) for side in (p.side, 1 - p.side)]
        firsts = [jnp.where(a >= 0, (2 * a + b) * rows, 2**24) for a, b in homes]

        def keep_grad(j, value):
            s.slots[i, j // 2, j % 2] = value

        s.dq[i] = attend_back_core(
            group,
            s.qs[i],
            ins.place[i],
            s.heads[part_of(i)],
            s.atts[i],
            ins.lse.at[i],
            ins.cosine[i],
            ins.sine[i],
            [s.slots.at[i, j // 2, j % 2] for j in range(2 * LINE)],
            firsts,
            p.cp * rows,
            s.keys,
            s.bias,
            keep_grad,
            512,
        )
        kv_cross(i).start()

    def kv_cross(i):
        return p.copy("x", s.slots.at[i, :, 1], s.kv_x.at[i], s.kxs.at[i], s.kxr.at[i])

    def kv_down(i, r):
        return p.copy("down", s.slots.at[i, r, 0], s.kv_z.at[i, r - 1], s.kzs.at[i, r - 1], s.kzr.at[i, r - 1])

    def kv_take(i, r):
        kv_down(i, r + 1).wait_recv()
        s.slots[i, r, 0] = (s.slots[i, r, 0].astype(F32) + s.kv_z[i, r].astype(F32)).astype(BF16)

    def step_keys(i):
        kv_cross(i).wait_recv()
        for r in range(LINE):
            s.slots[i, r, 0] = (s.slots[i, r, 0].astype(F32) + s.kv_x[i, r].astype(F32)).astype(BF16)
        for z in range(LINE - 1, -1, -1):

            @p.at(z)
            def _(z=z):
                for r in range(z, 0, -1):
                    if z < LINE - 1:
                        kv_take(i, r)
                    kv_down(i, r).start()
                if z < LINE - 1:
                    kv_take(i, 0)

    def part_copy(i):
        return p.copy("tp", s.part.at[part_of(i)], s.part_in.at[part_of(i)], s.ts.at[2 + i], s.tr.at[2 + i])

    def step_project(i):
        if i == 0:
            got("wq", "wk", "wv", "act", "normed")
        at = part_of(i)
        total = s.slots[i, 0, 0].astype(F32)
        dk = rope_back(total[:, :width], widen(ins.cosine[i], width), widen(ins.sine[i], width)).astype(BF16)
        dv = total[:, width:].astype(BF16)
        s.dkv[at, :width] = dk
        s.dkv[at, width:] = dv
        full = mm_t(s.dq[i], s.wide_w[...]) + mm_t(dk, s.wks[...]) + mm_t(dv, s.wvs[...])
        s.part[at] = full.astype(BF16)
        part_copy(i).start()
        unit, _ = unit_rows(s.mid_dy[at].astype(F32))
        gain_row = jnp.sum(full * unit, axis=0, keepdims=True)
        if i == 0:
            s.small[LANES - 2 : LANES - 1, :] = gain_row
        else:
            s.small[LANES - 2 : LANES - 1, :] += gain_row

    tall = model // 4

    def weight_pieces(left, right, ref, keep):
        for piece_at in range(4):
            got_piece = t_mm(left[:, piece_at * tall : (piece_at + 1) * tall], right).astype(BF16)
            block = got_piece.reshape(-1, model // 16, right.shape[1])
            for b in range(4):
                whole = 4 * piece_at + b
                keep(whole // 8, whole % 8 // 2, whole % 2, block[b])

    def big_part(row):
        def keep(half, z, side, value):
            s.whole[half, z, side, row : row + value.shape[0], :] = value

        return keep

    def little_part(column):
        def keep(half, z, side, value):
            s.lit[half, z, side, :, column : column + value.shape[1]] = value

        return keep

    ep_big = p.copy("ep", s.whole.at[1 - p.ep], s.came, s.es.at[2], s.er.at[2])
    ep_lit = p.copy("ep", s.lit.at[1 - p.ep], s.lit_came, s.es.at[3], s.er.at[3])

    def step_out_weight():
        got("low")
        weight_pieces(s.branch[...], s.lows[...], s.whole, big_part(0))

    def step_query_weight():
        got("normed")
        loads["normed"] = Done()
        query = jnp.concatenate([s.dq[i] for i in range(seqs)], axis=0)
        weight_pieces(s.mid_x2[...], query, s.whole, big_part(model // 16))
        ep_big.start()

    def step_key_weight():
        weight_pieces(s.mid_x2[...], s.dkv[...], s.lit, little_part(0))
        for piece_at in range(4):
            turned = jnp.transpose(s.small[:, piece_at * tall : (piece_at + 1) * tall]).astype(BF16)
            block = turned.reshape(-1, model // 16, LANES)
            for b in range(4):
                whole = 4 * piece_at + b
                little_part(2 * width)(whole // 8, whole % 8 // 2, whole % 2, block[b])
        ep_lit.start()

    def step_big_cores():
        ep_big.wait_recv()
        for d in range(LINE):
            for side in range(2):
                s.whole[p.ep, d, side] = (
                    s.whole[p.ep, d, side].astype(F32) + s.came[d, side].astype(F32)
                ).astype(BF16)

    def step_little_cores():
        ep_lit.wait_recv()
        for d in range(LINE):
            for side in range(2):
                s.lit[p.ep, d, side] = (
                    s.lit[p.ep, d, side].astype(F32) + s.lit_came[d, side].astype(F32)
                ).astype(BF16)

    def step_input():
        for i in range(seqs):
            at = part_of(i)
            part_copy(i).wait_recv()
            unit, scale = unit_rows(s.mid_dy[at].astype(F32))
            scaled = (s.part[at].astype(F32) + s.part_in[at].astype(F32)) * ins.gain_one[...]
            o.grad[at] = o.grad[at] + scale * (scaled - unit * jnp.mean(scaled * unit, axis=-1, keepdims=True))

    def step_mix():
        tp_mix.wait_recv()
        tp_mix.wait_send()
        for i in range(seqs):
            o.mix[part_of(i)] = (o.mix[part_of(i)].astype(F32) + s.mix_tp[part_of(i)].astype(F32)).astype(BF16)

    line = list(ring) + ["little"]
    stage = {item: 0 for item in line}

    def advance(at, to):
        if not 0 <= at < len(line):
            return
        item = line[at]
        while stage[item] < to:
            now = stage[item]
            if now == 0:
                opened(item)
            elif now == 1:
                flow(item).second()
            elif now == 2:
                flow(item).third()
            elif now == 3:
                closed(item)
            elif now == 4:
                freed(item)
            stage[item] = now + 1

    def turn(at):
        for back in (4, 3, 2, 1, 0):
            advance(at - back, back + 1)

    def add_zero():
        got("zero")
        zero_copy.wait_recv()
        s.staged[0] = s.staged[0] + s.zero_in[...].astype(F32)

    tp_mix.start()
    turn(0)
    finish_expert(0, add_zero)
    turn(1)
    step_middle()
    advance(0, 3)
    advance(1, 2)
    step_attend(0)
    turn(2)
    step_attend(1)
    cross(queue.pop(0))
    advance(0, 4)
    advance(1, 3)
    advance(2, 2)
    step_out_weight()
    step_query_weight()
    turn(3)
    cross(queue.pop(0))
    step_keys(0)
    advance(2, 3)
    advance(3, 2)
    step_keys(1)
    step_project(0)
    step_project(1)
    advance(0, 5)
    advance(1, 4)
    advance(2, 4)
    advance(3, 3)
    step_key_weight()
    step_big_cores()
    step_mix()
    extra = [step_little_cores, step_input]
    for at in range(4, len(line) + 4):
        turn(at)
        if queue:
            cross(queue.pop(0))
        if extra:
            extra.pop(0)()
    for e in stored:
        if e not in waited:
            store(e).wait()
    for item in line:
        if item == "little" or (crosses(item) and index_of[item] + RING >= len(ring)):
            x_copy(item).wait_send()
    for i in range(seqs):
        kv_cross(i).wait_send()
        part_copy(i).wait_send()
        for z in range(1, LINE):

            @p.at(z)
            def _(z=z):
                for r in range(z, 0, -1):
                    kv_down(i, r).wait_send()

    tp_back.wait_send()
    zero_copy.wait_send()
    for copy in (ep_back, ep_mix, ep_big, ep_lit):
        copy.wait_send()


class Done:
    def wait(self):
        return None


def back_and_sums(ins, slots, chunks, group):
    keeps, _, arrived, *_ = chunks
    _, length, depth, wide = keeps.shape
    early, count = arrived.shape[0], FIRST + keeps.shape[0]
    block = (length, depth, wide)
    v = dict(zip(BACK_INS, ins, strict=True))
    rows, model = v["middle"].shape
    seqs, each, heads = v["q"].shape
    width = v["wk"].shape[1]
    both = 2 * width
    small = (length, 2, model // 16, both + LANES)
    n_ring = count - FIRST + 1
    anywhere = pl.BlockSpec(memory_space=pl.ANY)
    inside = pl.BlockSpec(memory_space=pltpu.VMEM)
    dma, vm = pltpu.SemaphoreType.DMA, pltpu.VMEM
    flag = pltpu.SemaphoreType.REGULAR
    scratch = dict(
        back=vm((rows, model + LANES), BF16),
        other_ep=vm((rows, model + LANES), BF16),
        other_tp=vm((rows, model + LANES), BF16),
        mid_dy=vm((rows, model), BF16),
        mid_x2=vm((rows, model), BF16),
        wide_w=vm((model, heads), BF16),
        branch=vm((rows, model), BF16),
        heads=vm((rows, heads), BF16),
        small=vm((LANES, model), F32),
        qs=vm((seqs, each, heads), BF16),
        atts=vm((seqs, each, heads), F32),
        slots=vm((seqs, LINE, 2, each, both), BF16),
        kv_x=vm((seqs, LINE, each, both), BF16),
        kv_z=vm((seqs, LINE - 1, each, both), BF16),
        keys=vm((2 * LINE * each, both), BF16),
        bias=vm((2 * LINE * each, each), F32),
        dq=vm((seqs, each, heads), BF16),
        lows=vm((rows, heads), BF16),
        wks=vm((model, width), BF16),
        wvs=vm((model, width), BF16),
        routers=vm((model, LANES), BF16),
        dkv=vm((rows, both), BF16),
        part=vm((rows, model), BF16),
        part_in=vm((rows, model), BF16),
        mix_ep=vm((rows, model), BF16),
        mix_tp=vm((rows, model), BF16),
        held=vm((RING,) + block, BF16),
        spots=vm((RING, 5, depth, wide), BF16),
        kept=vm(block, BF16),
        staged=vm((2, depth, wide), F32),
        zero_in=vm((depth, wide), BF16),
        whole=vm((2, length, 2, depth, wide), BF16),
        came=vm((length, 2, depth, wide), BF16),
        lit=vm((2,) + small, BF16),
        lit_came=vm(small, BF16),
        lit_x=vm((small[0],) + small[2:], BF16),
        lit_spots=vm((5,) + small[2:], BF16),
        ls=dma((28,)),
        ks=dma((1 + early,)),
        xs=dma((n_ring + 2,)),
        xr=dma((n_ring + 2,)),
        zs=dma((n_ring + 1, 6)),
        zr=dma((n_ring + 1, 6)),
        es=dma((4,)),
        er=dma((4,)),
        ts=dma((4,)),
        tr=dma((4,)),
        kxs=dma((2,)),
        kxr=dma((2,)),
        kzs=dma((2, 3)),
        kzr=dma((2, 3)),
        os=dma((count,)),
        free_x=flag,
        free_up=flag,
        free_down=flag,
    )
    return pl.pallas_call(
        functools.partial(back_body, group),
        out_shape=(
            shape_of((rows, model), F32),
            shape_of((rows, model), BF16),
            shape_of((count, depth, wide), F32),
            shape_of((depth, wide), F32),
            shape_of(small[2:], F32),
        ),
        in_specs=[anywhere] * (len(BACK_INS) - BACK_IN_PLACE)
        + [inside] * BACK_IN_PLACE
        + [anywhere] * (2 * LINE + 5),
        out_specs=(inside, inside, anywhere, inside, inside),
        scratch_shapes=[scratch[name] for name in BACK_SCRATCH],
        compiler_params=pltpu.CompilerParams(
            collective_id=1, has_side_effects=True, vmem_limit_bytes=67_043_328
        ),
        name="back_and_sums",
    )(*ins, *slots, *chunks)


def on_device(
    activations,
    cotangent,
    positions,
    routes,
    w_query,
    w_key,
    value_weight,
    w_out,
    gain_attn,
    gain_moe,
    w_router,
    w_gate_up,
    w_down,
):
    seqs, rows, model = activations.shape
    total = seqs * rows
    width = w_key.shape[1]
    group = w_query.shape[1] // width
    expert_count = w_router.shape[1]
    local = w_gate_up.shape[0]
    half = w_down.shape[2]
    blocks = lax.axis_size("cp")
    length = blocks // 2
    here = lax.axis_index("cp")
    z, side = here // 2, here % 2
    mine = lax.axis_index("ep")
    act = activations.reshape(total, model)
    dy = cotangent.reshape(total, model)
    gain_one, gain_two = gain_attn.reshape(1, model), gain_moe.reshape(1, model)

    frequency = jnp.power(10000.0, -(jnp.arange(HEAD // 2, dtype=F32) * 2.0 / HEAD))
    angles = positions.reshape(total, 1).astype(F32) * frequency
    cosine = jnp.tile(jnp.cos(angles), (1, 2 * LANES // HEAD))
    sine = jnp.tile(jnp.sin(angles), (1, 2 * LANES // HEAD))

    normed, q, kv = project(act, gain_one, w_query, w_key, value_weight, cosine, sine)
    q = q.reshape(seqs, rows, -1)
    kv = kv.reshape(1, seqs, rows, 2 * width)
    offset = (here * rows).astype(jnp.int32).reshape(1)
    if length == 4:
        slots, homes = [kv, swap(kv, "cp")], [(z, side), (z, 1 - side)]
        travel = kv
        for r in range(1, length):
            travel = up(travel, r - 1, length - 1)
            slots += [travel, swap(travel, "cp")]
            homes += [(z - r, side), (z - r, 1 - side)]
        first = jnp.stack([jnp.where(a >= 0, (2 * a + b) * rows, 2**24) for a, b in homes]).astype(jnp.int32)
    else:
        slots = [lax.all_gather(kv, "cp", axis=0, tiled=True)]
        first = jnp.arange(blocks, dtype=jnp.int32) * rows
    place = positions.reshape(seqs, 1, rows)

    dy_par = swap(dy, "ep")
    dy_turned = jnp.concatenate([dy, dy_par], axis=0).T.reshape(blocks, -1, 2 * total)
    lanes = jnp.arange(LANES, dtype=jnp.int32)
    hot = jnp.sum((routes.reshape(total, -1, 1) == lanes).astype(F32), axis=1)
    router = jnp.pad(w_router, ((0, 0), (0, LANES - expert_count)))

    slots, dy_turned, hot, router = lax.optimization_barrier((slots, dy_turned, hot, router))
    low, attended, lse = attend(q, place, slots, first, offset, group)
    low = low.reshape(total, -1)
    part = out_project(low, w_out)
    part, w_in = lax.optimization_barrier((part, w_gate_up))
    w_in = w_in.reshape(local, model, 2 * half)
    middle, normed_two, gates = middle_of(act, part, swap(part, "tp"), gain_two, router, hot)
    x_par, gates_par = swap(normed_two, "ep"), swap(gates, "ep")

    early, apart = (EARLY, FIRST) if length == LINE else (0, 0)
    args = (normed_two, x_par, dy, dy_par, dy_turned, gates, gates_par, w_in, w_down)
    chunks, (own_back, par_back, own_mix, par_mix) = experts(early, apart, blocks, *args)
    seq_cosine, seq_sine = cosine.reshape(seqs, rows, -1), sine.reshape(seqs, rows, -1)
    if length == LINE:
        ins = (
            own_back, par_back, own_mix, par_mix, middle, dy, router, w_out, normed_two, q, attended, act, normed,
            low, w_query, w_key, value_weight, gates, gain_two, gain_one, place, lse, seq_cosine, seq_sine,
        )
        input_grad, mix, expert_grad, big, little = back_and_sums(ins, slots, chunks, group)
        output = middle + mix.astype(F32)
        gain_two_at, gain_one_at = LANES - 1, LANES - 2
    else:
        gain_two_at, gain_one_at = expert_count, expert_count + 1
        back = total_of([own_back, swap(par_back, "ep")]).astype(BF16)
        grad_middle, branch, grad_heads, small = middle_back(
            back, swap(back, "tp"), middle, dy, gates, router, gain_two, w_out, normed_two
        )
        dq, grads = attend_back(
            q, place, grad_heads.reshape(q.shape), attended, lse, seq_cosine, seq_sine, slots, first, offset, group
        )
        dq = dq.reshape(total, -1)
        kv_sum = lax.psum_scatter(grads[0], "cp", scatter_dimension=0, tiled=True)
        kv_terms = [kv_sum, jnp.zeros_like(kv_sum), jnp.zeros_like(kv_sum)]
        kv_terms = [t.reshape(total, 2 * width) for t in kv_terms]
        spots = jnp.stack([mine, side]).astype(jnp.int32)
        big = weights(spots, blocks, [(branch, low), (normed, dq)], stacked=True)
        normed_part, dkv, gain_row = project_back(act, dq, *kv_terms, cosine, sine, w_query, w_key, value_weight)
        small = jnp.concatenate([small[:expert_count], small[LANES : LANES + 1], gain_row[:1]], axis=0)
        small = jnp.pad(small, ((0, LANES - small.shape[0]), (0, 0)))
        little = weights(spots, blocks, [(normed, dkv)], (small,))
        input_grad = input_of(act, grad_middle, normed_part, swap(normed_part, "tp"), gain_one)
        mix = total_of([own_mix, swap(par_mix, "ep")]).astype(BF16)
        output = middle + total_of([mix, swap(mix, "tp")])

        def spread_sum(keep, send):
            both = total_of([keep, swap(send, "ep")]).astype(BF16)
            return line_sum([both[0], swap(both[1], "cp")], z, length)

        turned = [jnp.swapaxes(v, 0, 1) for v in (chunks[0], swap(chunks[1], "cp"))]
        expert_grad = line_sum(turned, z, length)
        big, little = spread_sum(*big), spread_sum(*little)
    gate_up_grad = expert_grad[:, :, : 2 * half].reshape(local, -1, 2, half)
    down_grad = expert_grad[:, :, 2 * half :]
    tall = big.shape[0] // 2
    gain_part = little[:, 2 * width + gain_one_at]
    return (
        output.reshape(activations.shape),
        input_grad.reshape(activations.shape),
        big[tall:],
        little[:, :width],
        little[:, width : 2 * width],
        big[:tall],
        gain_part + swap(gain_part, "tp"),
        little[:, 2 * width + gain_two_at],
        little[:, 2 * width : 2 * width + expert_count],
        gate_up_grad,
        down_grad,
    )


def solution(mesh):
    in_specs = (
        P("ep", "cp", None),
        P("ep", "cp", None),
        P("ep", "cp"),
        P("ep", "cp", None),
        P(None, "tp"),
        P(None, "tp"),
        P(None, "tp"),
        P(None, "tp"),
        P(),
        P(),
        P(),
        P("ep", None, None, "tp"),
        P("ep", None, "tp"),
    )
    out_specs = (
        P("ep", "cp", None),
        P("ep", "cp", None),
        P(("ep", "cp"), "tp"),
        P(("ep", "cp"), "tp"),
        P(("ep", "cp"), "tp"),
        P(("ep", "cp"), "tp"),
        P(("ep", "cp")),
        P(("ep", "cp")),
        P(("ep", "cp"), None),
        P("ep", "cp", None, "tp"),
        P("ep", "cp", "tp"),
    )
    return jax.shard_map(
        on_device, mesh=mesh, in_specs=in_specs, out_specs=out_specs, check_vma=False
    )
```

```python
import functools
from typing import Any, NamedTuple

import jax
import jax.numpy as jnp
from jax import lax
from jax.experimental import pallas as pl
from jax.experimental.pallas import tpu as pltpu
from jax.sharding import PartitionSpec as P

HEAD = 64
EPS = 1e-06
NEG = -1e30
SCALE = 0.125
LANES = 128
KEY_CHUNK = 1024
F32 = jnp.float32
BF16 = jnp.bfloat16
MESH = pl.DeviceIdType.MESH


def mm(a, b):
    return lax.dot_general(a, b, (((1,), (0,)), ((), ())), preferred_element_type=F32)


def mm_t(a, b):
    return lax.dot_general(a, b, (((1,), (1,)), ((), ())), preferred_element_type=F32)


def t_mm(a, b):
    return lax.dot_general(a, b, (((0,), (0,)), ((), ())), preferred_element_type=F32)


def two_parts(v):
    high = v.astype(BF16)
    return high, (v - high.astype(F32)).astype(BF16)


def halves_turned(v, back):
    width = v.shape[1]
    ahead = pltpu.roll(v, width - HEAD // 2, 1)
    behind = pltpu.roll(v, HEAD // 2, 1)
    first = lax.broadcasted_iota(jnp.int32, v.shape, 1) % HEAD < HEAD // 2
    if back:
        return jnp.where(first, ahead, -behind)
    return jnp.where(first, -ahead, behind)


def rope(v, cosine, sine):
    return v * cosine + halves_turned(v, False) * sine


def rope_back(v, cosine, sine):
    return v * cosine + halves_turned(v * sine, True)


def widen(table, width):
    return jnp.concatenate([table] * (width // table.shape[1]), axis=1)


def unit_rows(v):
    scale = lax.rsqrt(jnp.mean(v * v, axis=-1, keepdims=True) + EPS)
    return v * scale, scale


def shape_of(shape, dtype):
    return jax.ShapeDtypeStruct(shape, dtype)


def params(**kw):
    return pltpu.CompilerParams(vmem_limit_bytes=60 * 2**20, **kw)


def cost(flops, moved):
    return pl.CostEstimate(flops=int(flops), bytes_accessed=int(moved), transcendentals=0)


def project_body(act, gain, wq, wk, wv, cosine, sine, normed, q, kv):
    unit, _ = unit_rows(act[...].astype(F32))
    low = (unit * gain[...]).astype(BF16)
    normed[...] = low
    qf = mm(low, wq[...])
    q[...] = rope(qf, widen(cosine[...], qf.shape[1]), widen(sine[...], qf.shape[1])).astype(BF16)
    kf = mm(low, wk[...])
    width = kf.shape[1]
    kv[:, :width] = rope(kf, widen(cosine[...], width), widen(sine[...], width)).astype(BF16)
    kv[:, width:] = mm(low, wv[...]).astype(BF16)


def project(act, gain, wq, wk, wv, cosine, sine):
    rows, model = act.shape
    total = wq.shape[1] + 2 * wk.shape[1]
    return pl.pallas_call(
        project_body,
        out_shape=(
            shape_of((rows, model), BF16),
            shape_of((rows, wq.shape[1]), BF16),
            shape_of((rows, 2 * wk.shape[1]), BF16),
        ),
        compiler_params=params(),
        cost_estimate=cost(2 * rows * model * total, 2 * model * total + 6 * rows * model),
        name="project",
    )(act, gain, wq, wk, wv, cosine, sine)


def fill_keys(firsts, offset, place, slots, keys, bias, rows):
    query = lax.broadcasted_iota(jnp.int32, (rows, rows), 1) + offset
    for at, slot in enumerate(slots):
        keys[at * rows : (at + 1) * rows, :] = slot[...]
        key = lax.broadcasted_iota(jnp.int32, (rows, rows), 0) + firsts[at]
        distance = query - key
        seen = (distance >= 0) & (distance <= place)
        bias[at * rows : (at + 1) * rows, :] = jnp.where(seen, 0.0, NEG)


def single_slots(slots):
    return [slot.at[one, 0] for slot in slots for one in range(slot.shape[0])]


def group_rows(block, head, group):
    return jnp.concatenate(
        [block[:, (head * group + g) * HEAD : (head * group + g + 1) * HEAD] for g in range(group)], axis=0
    )


def attend_core(group, q, place, slots, firsts, offset, keys, bias, lse_ref, most):
    rows = q.shape[0]
    fill_keys(firsts, offset, place, slots, keys, bias, rows)
    total, width = keys.shape[0], keys.shape[1] // 2
    chunk = min(total, most)
    q = (q.astype(F32) * SCALE).astype(BF16)
    pieces = []
    for head in range(width // HEAD):
        q3 = group_rows(q, head, group)
        top = run = out = None
        for low in range(0, total, chunk):
            k = keys[low : low + chunk, head * HEAD : (head + 1) * HEAD]
            v = keys[low : low + chunk, width + head * HEAD : width + (head + 1) * HEAD]
            s = mm_t(k, q3) + widen(bias[low : low + chunk, :], group * rows)
            here = jnp.max(s, axis=0, keepdims=True)
            new = here if top is None else jnp.maximum(top, here)
            p = jnp.exp(s - new)
            part = jnp.sum(p, axis=0, keepdims=True)
            o = t_mm(v, p.astype(BF16))
            if top is None:
                run, out = part, o
            else:
                shrink = jnp.exp(top - new)
                run, out = run * shrink + part, out * shrink + o
            top = new
        out = jnp.transpose(out / run)
        pieces += [out[g * rows : (g + 1) * rows] for g in range(group)]
        lse_ref[head : head + 1, :] = top + jnp.log(run)
    return jnp.concatenate(pieces, axis=1)


def attend_body(group, count, first_ref, offset_ref, q_ref, place_ref, *refs):
    slots = single_slots(refs[:count])
    low_ref, out_ref, lse_ref, keys, bias = refs[count:]
    firsts = [first_ref[i] for i in range(len(slots))]
    whole = attend_core(
        group, q_ref[0], place_ref[0], slots, firsts, offset_ref[0], keys, bias, lse_ref.at[0], KEY_CHUNK
    )
    out_ref[0] = whole
    low_ref[0] = whole.astype(BF16)


def seq_block(shape):
    return pl.BlockSpec((1,) + shape[1:], lambda s, *_: (s,) + (0,) * (len(shape) - 1))


def slot_block(shape):
    return pl.BlockSpec((shape[0], 1) + shape[2:], lambda s, *_: (0, s, 0, 0))


def attend(q, place, slots, first, offset, group):
    seqs, rows, wide = q.shape
    both = slots[0].shape[-1]
    total = rows * sum(slot.shape[0] for slot in slots)
    heads = wide // HEAD // group
    outs = (
        shape_of(q.shape, BF16),
        shape_of(q.shape, F32),
        shape_of((seqs, heads, group * rows), F32),
    )
    return pl.pallas_call(
        functools.partial(attend_body, group, len(slots)),
        out_shape=outs,
        grid_spec=pltpu.PrefetchScalarGridSpec(
            num_scalar_prefetch=2,
            grid=(seqs,),
            in_specs=[seq_block(q.shape), seq_block(place.shape)] + [slot_block(s.shape) for s in slots],
            out_specs=tuple(seq_block(o.shape) for o in outs),
            scratch_shapes=[pltpu.VMEM((total, both), BF16), pltpu.VMEM((total, rows), F32)],
        ),
        compiler_params=params(),
        cost_estimate=cost(2e9 * 4, 20e6),
        name="attend",
    )(first, offset, q, place, *slots)


def attend_back_core(
    group, q, place, go, out, lse_ref, cosine, sine, slots, firsts, offset, keys, bias, keep_grad, most
):
    rows = q.shape[0]
    fill_keys(firsts, offset, place, slots, keys, bias, rows)
    total, width = keys.shape[0], keys.shape[1] // 2
    chunk = min(total, most)
    q = (q.astype(F32) * SCALE).astype(BF16)
    products = go.astype(F32) * out
    ones = jnp.ones((8, HEAD), F32)
    heads = width // HEAD
    q3s = [group_rows(q, head, group) for head in range(heads)]
    g3s = [group_rows(go, head, group) for head in range(heads)]
    deltas = [
        lax.dot_general(
            ones,
            group_rows(products, head, group),
            (((1,), (1,)), ((), ())),
            preferred_element_type=F32,
            precision=lax.Precision.HIGHEST,
        )[:1]
        for head in range(heads)
    ]
    dq = [None] * heads
    for low in range(0, total, chunk):
        dks, dvs = [], []
        for head in range(heads):
            k = keys[low : low + chunk, head * HEAD : (head + 1) * HEAD]
            v = keys[low : low + chunk, width + head * HEAD : width + (head + 1) * HEAD]
            s = mm_t(k, q3s[head]) + widen(bias[low : low + chunk, :], group * rows)
            p = jnp.exp(s - lse_ref[head : head + 1, :])
            dp = mm_t(v, g3s[head])
            ds = (p * (dp - deltas[head])).astype(BF16)
            dks.append(mm(ds, q3s[head]))
            dvs.append(mm(p.astype(BF16), g3s[head]))
            part = t_mm(k, ds)
            dq[head] = part if dq[head] is None else dq[head] + part
        both = jnp.concatenate(dks + dvs, axis=1).astype(BF16)
        for one in range(chunk // rows):
            keep_grad(low // rows + one, both[one * rows : (one + 1) * rows])
    pieces = []
    for head in range(heads):
        back = jnp.transpose(dq[head] * SCALE)
        pieces += [back[g * rows : (g + 1) * rows] for g in range(group)]
    whole = jnp.concatenate(pieces, axis=1)
    return rope_back(whole, widen(cosine, whole.shape[1]), widen(sine, whole.shape[1])).astype(BF16)


def attend_back_body(
    group, count, first_ref, offset_ref, q_ref, place_ref, grad_ref, out_ref, lse_ref, cos_ref, sin_ref, *refs
):
    slots = single_slots(refs[:count])
    dq_ref = refs[count]
    grads = single_slots(refs[count + 1 : 2 * count + 1])
    keys, bias = refs[2 * count + 1 :]

    def keep_grad(at, value):
        grads[at][...] = value

    dq_ref[0] = attend_back_core(
        group,
        q_ref[0],
        place_ref[0],
        grad_ref[0],
        out_ref[0],
        lse_ref.at[0],
        cos_ref[0],
        sin_ref[0],
        slots,
        [first_ref[i] for i in range(len(slots))],
        offset_ref[0],
        keys,
        bias,
        keep_grad,
        KEY_CHUNK,
    )


def attend_back(q, place, grad, out, lse, cosine, sine, slots, first, offset, group):
    seqs, rows, _ = q.shape
    both = slots[0].shape[-1]
    total = rows * sum(slot.shape[0] for slot in slots)
    outs = (shape_of(q.shape, BF16),) + tuple(shape_of(s.shape, BF16) for s in slots)
    ins = (q, place, grad, out, lse, cosine, sine)
    got = pl.pallas_call(
        functools.partial(attend_back_body, group, len(slots)),
        out_shape=outs,
        grid_spec=pltpu.PrefetchScalarGridSpec(
            num_scalar_prefetch=2,
            grid=(seqs,),
            in_specs=[seq_block(a.shape) for a in ins] + [slot_block(s.shape) for s in slots],
            out_specs=(seq_block(outs[0].shape),) + tuple(slot_block(s.shape) for s in slots),
            scratch_shapes=[pltpu.VMEM((total, both), BF16), pltpu.VMEM((total, rows), F32)],
        ),
        compiler_params=params(),
        cost_estimate=cost(2e9 * 8, 30e6),
        name="attend_back",
    )(first, offset, *ins, *slots)
    return got[0], got[1:]


def out_body(low, w_out, part):
    part[...] = mm_t(low[...], w_out[...]).astype(BF16)


def out_project(low, w_out):
    rows, model = low.shape[0], w_out.shape[0]
    return pl.pallas_call(
        out_body,
        out_shape=shape_of((rows, model), BF16),
        compiler_params=params(),
        cost_estimate=cost(2 * rows * model * low.shape[1], 4e6),
        name="out_project",
    )(low, w_out)


def route(mid, gain, router, hot):
    unit, _ = unit_rows(mid)
    low = (unit * gain).astype(BF16)
    chosen = hot > 0.5
    logits = jnp.where(chosen, mm(low, router), NEG)
    up = jnp.where(chosen, jnp.exp(logits - jnp.max(logits, axis=-1, keepdims=True)), 0.0)
    return low, up / jnp.sum(up, axis=-1, keepdims=True)


def middle_body(act, part, other, gain, router, hot, middle, normed, gates):
    mid = act[...].astype(F32) + (part[...].astype(F32) + other[...].astype(F32))
    middle[...] = mid
    normed[...], gates[...] = route(mid, gain[...], router[...], hot[...])


def middle_of(act, part, other, gain, router, hot):
    rows, model = act.shape
    return pl.pallas_call(
        middle_body,
        out_shape=(shape_of((rows, model), F32), shape_of((rows, model), BF16), shape_of((rows, LANES), F32)),
        compiler_params=params(),
        cost_estimate=cost(2 * rows * model * LANES, 12 * rows * model),
        name="middle",
    )(act, part, other, gain, router, hot)


EARLY = 2
FIRST = 1
HALF = 2


def experts_body(early, first, x_own, x_par, dy_own, dy_par, g_own, g_par, w_in, w_out, keep, send, *refs):
    refs = list(refs)
    came, z_kept, z_sent = (refs.pop(0), refs.pop(0), refs.pop(0)) if early else (None, None, None)
    own_back, par_back, own_mix, par_mix, x_turned, dy_order, x_all, dy_all, back, mix, pulls, blocks_of = refs[:12]
    step, steps = pl.program_id(0), pl.num_programs(0)
    rows, model = x_own.shape
    wide = own_back.shape[1] - model
    blocks, depth, _ = blocks_of.shape
    side = lax.axis_index("cp") % 2
    if early:
        leaving, held, spots, es, er, zs, zr = refs[12:]
        p = Place()
        flows = [Flow(p, held.at[i], spots.at[i], zs.at[i], zr.at[i]) for i in range(2)]

    def early_copy(i):
        some = pl.ds(0, blocks // 2 if i < early - 1 else HALF)
        return p.copy("x", leaving.at[i, some], came.at[i, some], es.at[i], er.at[i])

    @pl.when(step == 0)
    def _():
        if early:
            p.greet(("x",))
        x_all[:rows] = x_own[...]
        x_all[rows:] = x_par[...]
        dy_all[:rows] = dy_own[...]
        dy_all[rows:] = dy_par[...]
        for rows_of, ordered in ((x_all, x_turned), (dy_all, dy_order)):
            blocks_of[...] = jnp.transpose(rows_of[...]).reshape(blocks_of.shape)
            for z in range(blocks // 2):
                ordered[z] = blocks_of[2 * z + side]
                ordered[blocks // 2 + z] = blocks_of[2 * z + 1 - side]
        back[...] = jnp.zeros_like(back)
        mix[...] = jnp.zeros_like(mix)
        pulls[...] = jnp.zeros_like(pulls)

    expert = lax.axis_index("ep") * steps + step
    lane = lax.broadcasted_iota(jnp.int32, (2 * rows, wide), 1) == expert
    gate_rows = jnp.concatenate([g_own[...], g_par[...]], axis=0)
    gate = jnp.sum(jnp.where(lane, gate_rows, 0.0), axis=-1, keepdims=True)
    x, dy = x_all[...], dy_all[...]
    w_gu, w_d = w_in[0], w_out[0]
    both = mm(x, w_gu)
    half = both.shape[1] // 2
    g, u = both[:, :half], both[:, half:]
    pull = mm(dy, w_d)
    sig = 1.0 / (1.0 + jnp.exp(-g))
    act = g * sig
    hidden = (act * u).astype(BF16).astype(F32)
    pulls[...] += jnp.where(lane, jnp.sum(hidden * pull, axis=-1, keepdims=True), 0.0)
    weighted = (gate * hidden).astype(BF16)
    pull = gate * pull
    d_g = (pull * u * sig * (1.0 + g * (1.0 - sig))).astype(BF16)
    d_u = (pull * act).astype(BF16)
    d_gu = jnp.concatenate([d_g, d_u], axis=1)
    for i, out in enumerate((keep, send)):
        at = pl.ds(i * (blocks // 2), blocks // 2)
        shape = (model // 2, 2 * rows)
        to = (blocks // 2, depth, -1)
        out[0, :, :, : 2 * half] = mm(x_turned[at].reshape(shape), d_gu).astype(BF16).reshape(to)
        out[0, :, :, 2 * half :] = mm(dy_order[at].reshape(shape), weighted).astype(BF16).reshape(to)
    if early:

        @pl.when(step == 0)
        def _():
            held[0] = keep[0]
            held[1] = send[0]
            for flow in flows:
                flow.open()

        for i in range(early):

            @pl.when(step == first + i)
            def _(i=i):
                leaving[i] = send[0]
                early_copy(i).start()

        for at, work in (
            (2, [lambda: flows[0].second(0)]),
            (3, [lambda: flows[0].second(1)]),
            (4, [flows[0].third]),
            (5, [lambda: flows[1].second(0)]),
            (6, [lambda: flows[1].second(1), flows[1].third]),
        ):

            @pl.when(step == at)
            def _(work=work):
                for one in work:
                    one()

    back[...] += mm_t(d_gu, w_gu)
    mix[...] += mm_t(weighted, w_d)

    @pl.when(step == steps - 1)
    def _():
        own_back[:, :model] = back[:rows].astype(BF16)
        par_back[:, :model] = back[rows:].astype(BF16)
        own_back[:, model:] = pulls[:rows].astype(BF16)
        par_back[:, model:] = pulls[rows:].astype(BF16)
        own_mix[...] = mix[:rows].astype(BF16)
        par_mix[...] = mix[rows:].astype(BF16)
        if early:
            for flow, out in zip(flows, (z_kept, z_sent)):

                def finish(parts, out=out):
                    out[...] = total_of(parts).astype(out.dtype)

                flow.close(finish)
                flow.drain()
            for i in range(early):
                early_copy(i).wait()


def experts(early, first, blocks, x_own, x_par, dy_own, dy_par, g_own, g_par, w_in, w_out):
    rows, model = x_own.shape
    count, _, half = w_out.shape
    depth = model // blocks
    once = lambda shape: pl.BlockSpec(shape, lambda e: (0,) * len(shape))
    whole = (blocks // 2, depth, 3 * half)
    ins = [x_own, x_par, dy_own, dy_par, g_own, g_par]
    apart = first + max(early - 1, 0)
    tail = [shape_of((rows, model + LANES), BF16)] * 2 + [shape_of((rows, model), BF16)] * 2
    outs = [shape_of((count - first,) + whole, BF16), shape_of((count - apart,) + whole, BF16)]
    specs = [
        pl.BlockSpec((1,) + whole, lambda e: (jnp.maximum(e - first, 0), 0, 0, 0)),
        pl.BlockSpec((1,) + whole, lambda e: (jnp.maximum(e - apart, 0), 0, 0, 0)),
    ]
    turned = (blocks, depth, 2 * rows)
    scratch = [
        pltpu.VMEM(turned, BF16),
        pltpu.VMEM(turned, BF16),
        pltpu.VMEM((2 * rows, model), BF16),
        pltpu.VMEM((2 * rows, model), BF16),
        pltpu.VMEM((2 * rows, model), F32),
        pltpu.VMEM((2 * rows, model), F32),
        pltpu.VMEM((2 * rows, LANES), F32),
        pltpu.VMEM(turned, BF16),
    ]
    kind = params()
    if early:
        dma = pltpu.SemaphoreType.DMA
        sums = [shape_of(whole[1:], F32), shape_of(whole[1:], BF16)]
        outs += [shape_of((early,) + whole, BF16)] + sums
        specs += [pl.BlockSpec(memory_space=pl.ANY)] + [once(t.shape) for t in sums]
        scratch += [
            pltpu.VMEM((early,) + whole, BF16),
            pltpu.VMEM((2,) + whole, BF16),
            pltpu.VMEM((2, 5) + whole[1:], BF16),
            dma((early,)),
            dma((early,)),
            dma((2, 6)),
            dma((2, 6)),
        ]
        kind = params(collective_id=2, has_side_effects=True)
    got = pl.pallas_call(
        functools.partial(experts_body, early, first),
        out_shape=tuple(outs + tail),
        grid=(count,),
        in_specs=[once(a.shape) for a in ins]
        + [
            pl.BlockSpec((1, model, 2 * half), lambda e: (e, 0, 0)),
            pl.BlockSpec((1, model, half), lambda e: (e, 0, 0)),
        ],
        out_specs=tuple(specs + [once(t.shape) for t in tail]),
        scratch_shapes=scratch,
        compiler_params=kind,
        cost_estimate=cost(count * 18 * 2 * rows * model * half, count * 12 * model * half),
        name="experts",
    )(*ins, w_in, w_out)
    return got[: len(outs)], got[len(outs) :]


def middle_back_body(mine, other, middle, dy, gates, router, gain, w_out, normed, grad, low, heads, small):
    model = middle.shape[1]
    total = mine[...].astype(F32) + other[...].astype(F32)
    gate, pulls = gates[...], total[:, model:]
    chosen = gate * (pulls - jnp.sum(gate * pulls, axis=-1, keepdims=True))
    high, rest = two_parts(chosen)
    grad_two = total[:, :model] + (mm_t(high, router[...]) + mm_t(rest, router[...]))
    unit, scale = unit_rows(middle[...])
    small[:LANES, :] = t_mm(high, normed[...]) + t_mm(rest, normed[...])
    small[LANES : LANES + 8, :] = jnp.broadcast_to(jnp.sum(grad_two * unit, axis=0, keepdims=True), (8, model))
    scaled = grad_two * gain[...]
    out = dy[...].astype(F32) + scale * (scaled - unit * jnp.mean(scaled * unit, axis=-1, keepdims=True))
    grad[...] = out
    rounded = out.astype(BF16)
    low[...] = rounded
    heads[...] = mm(rounded, w_out[...]).astype(BF16)


def middle_back(mine, other, middle, dy, gates, router, gain, w_out, normed):
    rows, model = middle.shape
    return pl.pallas_call(
        middle_back_body,
        out_shape=(
            shape_of((rows, model), F32),
            shape_of((rows, model), BF16),
            shape_of((rows, w_out.shape[1]), BF16),
            shape_of((LANES + 8, model), F32),
        ),
        compiler_params=params(),
        cost_estimate=cost(2 * rows * model * (w_out.shape[1] + 4 * LANES), 10e6),
        name="middle_back",
    )(mine, other, middle, dy, gates, router, gain, w_out, normed)


def project_back_body(width, act, dq, a, b, c, cosine, sine, wq, wk, wv, part, dkv, gain_row):
    total = a[...].astype(F32) + b[...].astype(F32) + c[...].astype(F32)
    dk = rope_back(total[:, :width], widen(cosine[...], width), widen(sine[...], width)).astype(BF16)
    dv = total[:, width:].astype(BF16)
    dkv[:, :width] = dk
    dkv[:, width:] = dv
    full = mm_t(dq[...], wq[...]) + mm_t(dk, wk[...]) + mm_t(dv, wv[...])
    part[...] = full.astype(BF16)
    unit, _ = unit_rows(act[...].astype(F32))
    gain_row[...] = jnp.broadcast_to(jnp.sum(full * unit, axis=0, keepdims=True), gain_row.shape)


def project_back(act, dq, a, b, c, cosine, sine, wq, wk, wv):
    rows, model = act.shape
    width = wk.shape[1]
    return pl.pallas_call(
        functools.partial(project_back_body, width),
        out_shape=(
            shape_of((rows, model), BF16),
            shape_of((rows, 2 * width), BF16),
            shape_of((8, model), F32),
        ),
        compiler_params=params(),
        cost_estimate=cost(2 * rows * model * (wq.shape[1] + 2 * width), 8e6),
        name="project_back",
    )(act, dq, a, b, c, cosine, sine, wq, wk, wv)


def input_body(act, grad, mine, other, gain, out):
    unit, scale = unit_rows(act[...].astype(F32))
    scaled = (mine[...].astype(F32) + other[...].astype(F32)) * gain[...]
    out[...] = grad[...] + scale * (scaled - unit * jnp.mean(scaled * unit, axis=-1, keepdims=True))


def input_of(act, grad, mine, other, gain):
    return pl.pallas_call(
        input_body,
        out_shape=shape_of(act.shape, F32),
        compiler_params=params(),
        cost_estimate=cost(0, 12 * act.shape[0] * act.shape[1]),
        name="input_grad",
    )(act, grad, mine, other, gain)


def weights_body(blocks, count, stacked, where_ref, *refs):
    lefts = refs[:count]
    rights = refs[count : 2 * count]
    extra = refs[2 * count : -3]
    keep, send, whole = refs[-3:]
    parts = [t_mm(a[...], b[...]).astype(BF16) for a, b in zip(lefts, rights)]
    parts += [jnp.transpose(e[...]).astype(BF16) for e in extra]
    at = down = 0
    for part in parts:
        block = part.reshape(2 * blocks, -1, part.shape[1])
        whole[:, down : down + block.shape[1], at : at + part.shape[1]] = block
        if stacked:
            down += block.shape[1]
        else:
            at += part.shape[1]
    mine, side = where_ref[0], where_ref[1]
    for half, ref in ((mine, keep), (1 - mine, send)):
        for z in range(blocks // 2):
            ref[0, z] = whole[half * blocks + 2 * z + side]
            ref[1, z] = whole[half * blocks + 2 * z + 1 - side]


def weights(where, blocks, pairs, extra=(), stacked=False):
    model = pairs[0][0].shape[1]
    rows = pairs[0][0].shape[0]
    depth = model // (2 * blocks)
    columns = sum(b.shape[1] for _, b in pairs) + sum(e.shape[0] for e in extra)
    tall, wide = (depth * len(pairs), pairs[0][1].shape[1]) if stacked else (depth, columns)
    shape = (2, blocks // 2, tall, wide)
    ins = [a for a, _ in pairs] + [b for _, b in pairs] + list(extra)
    full = lambda a: pl.BlockSpec(a.shape, lambda i, *_: (0,) * len(a.shape))
    return pl.pallas_call(
        functools.partial(weights_body, blocks, len(pairs), stacked),
        out_shape=(shape_of(shape, BF16),) * 2,
        grid_spec=pltpu.PrefetchScalarGridSpec(
            num_scalar_prefetch=1,
            grid=(1,),
            in_specs=[full(a) for a in ins],
            out_specs=(pl.BlockSpec(shape, lambda i, *_: (0, 0, 0, 0)),) * 2,
            scratch_shapes=[pltpu.VMEM((2 * blocks, tall, wide), BF16)],
        ),
        compiler_params=params(),
        cost_estimate=cost(2 * rows * model * columns, 4 * model * columns),
        name="weights",
    )(where, *ins)


def swap(v, axis):
    size = lax.axis_size(axis)
    return lax.ppermute(v, axis, [(i, i ^ 1) for i in range(size)])


def up(v, low, high):
    return lax.ppermute(v, "cp", [(2 * z + s, 2 * z + 2 + s) for z in range(low, high) for s in range(2)])


def down(v, low, high):
    return lax.ppermute(v, "cp", [(2 * z + s, 2 * z - 2 + s) for z in range(low, high) for s in range(2)])


def total_of(terms):
    return functools.reduce(lambda a, b: a + b, [t.astype(F32) for t in terms])


def line_sum(parts, z, length):
    def own(d):
        return [lax.dynamic_index_in_dim(p, jnp.clip(d, 0, length - 1), 0, keepdims=False) for p in parts]

    if length > 4:
        mine = total_of(parts).astype(BF16)
        side = lax.axis_index("cp") % 2
        full = jnp.where(jnp.arange(2).reshape((1, 2) + (1,) * (mine.ndim - 1)) == side, mine[:, None], 0)
        full = full.reshape((2 * length,) + mine.shape[1:])
        return lax.psum_scatter(full, "cp", scatter_dimension=0, tiled=True)[0].astype(F32)
    right = left = None
    for k in range(length - 1):
        far = length - 1 - k
        terms = own(z + far) + ([] if right is None else [right])
        right = up(total_of(terms).astype(BF16), 0, k + 1)
        terms = own(z - far) + ([] if left is None else [left])
        left = down(total_of(terms).astype(BF16), far, length)
    return total_of(own(z) + ([right, left] if length > 1 else []))


LINE = 4
RING = 6


def add_to(ref, at, other):
    ref[at] = (ref[at].astype(F32) + other.astype(F32)).astype(BF16)


class Place:
    def __init__(self):
        self.cp = lax.axis_index("cp")
        self.z, self.side = self.cp // 2, self.cp % 2
        self.ep, self.tp = lax.axis_index("ep"), lax.axis_index("tp")

    def to(self, way):
        if way == "x":
            return {"cp": self.cp + 1 - 2 * self.side}
        if way == "up":
            return {"cp": self.cp + 2}
        if way == "down":
            return {"cp": self.cp - 2}
        return {way: 1 - (self.ep if way == "ep" else self.tp)}

    def signal(self, sem, way):
        pl.semaphore_signal(sem, inc=1, device_id=self.to(way), device_id_type=MESH)

    def signal_line(self, to_down, to_up):
        @pl.when(self.z > 0)
        def _():
            self.signal(to_down, "down")

        @pl.when(self.z < LINE - 1)
        def _():
            self.signal(to_up, "up")

    def greet(self, ways):
        barrier = pltpu.get_barrier_semaphore()
        for way in ways:
            self.signal(barrier, way)
        self.signal_line(barrier, barrier)
        both = jnp.where(self.z > 0, 1, 0) + jnp.where(self.z < LINE - 1, 1, 0)
        pl.semaphore_wait(barrier, len(ways) + both)

    def copy(self, way, src, dst, send, recv):
        return pltpu.make_async_remote_copy(
            src_ref=src, dst_ref=dst, send_sem=send, recv_sem=recv, device_id=self.to(way), device_id_type=MESH
        )

    def at(self, z):
        return pl.when(self.z == z)


LEFT_SPOT = (3, 4, 0)


class Flow:
    def __init__(self, place, held, spots, send, recv, credit=None):
        self.p, self.held, self.spots, self.send, self.recv, self.credit = place, held, spots, send, recv, credit

    def right(self, d):
        return self.p.copy("up", self.held.at[d], self.spots.at[d - 1], self.send.at[d - 1], self.recv.at[d - 1])

    def left(self, d):
        spot = LEFT_SPOT[d]
        return self.p.copy("down", self.held.at[d], self.spots.at[spot], self.send.at[d + 3], self.recv.at[d + 3])

    def allowed(self, way):
        if self.credit is not None:
            pl.semaphore_wait(self.credit[way], 1)

    def open(self):
        @self.p.at(0)
        def _():
            self.allowed("up")
            for d in (3, 2, 1):
                self.right(d).start()

        @self.p.at(3)
        def _():
            self.allowed("down")
            for d in (0, 1, 2):
                self.left(d).start()

    def pass_right(self, d):
        self.right(d).wait_recv()
        add_to(self.held, d, self.spots[d - 1])
        self.right(d).start()

    def pass_left(self, d):
        self.left(d).wait_recv()
        add_to(self.held, d, self.spots[LEFT_SPOT[d]])
        self.left(d).start()

    def second(self, only=None):
        @self.p.at(1)
        def _():
            if only != 1:
                self.allowed("up")
                self.pass_right(3)
            if only != 0:
                self.pass_right(2)

        @self.p.at(2)
        def _():
            if only != 1:
                self.allowed("down")
                self.pass_left(0)
            if only != 0:
                self.pass_left(1)

    def third(self):
        @self.p.at(2)
        def _():
            self.allowed("up")
            self.pass_right(3)

        @self.p.at(1)
        def _():
            self.allowed("down")
            self.pass_left(0)

    def close(self, finish):
        for z in range(LINE):

            @self.p.at(z)
            def _(z=z):
                blocks = [self.held[z]]
                if z > 0:
                    self.right(z).wait_recv()
                    blocks.append(self.spots[z - 1])
                if z < LINE - 1:
                    self.left(z).wait_recv()
                    blocks.append(self.spots[LEFT_SPOT[z]])
                finish(blocks)

    def drain(self):
        for z in range(LINE):

            @self.p.at(z)
            def _(z=z):
                for d in range(z + 1, LINE):
                    self.right(d).wait_send()
                for d in range(z):
                    self.left(d).wait_send()


class BackIns(NamedTuple):
    own_back: Any
    par_back: Any
    own_mix: Any
    par_mix: Any
    middle: Any
    dy: Any
    router: Any
    w_out: Any
    x2: Any
    q: Any
    attended: Any
    act: Any
    normed: Any
    low: Any
    wq: Any
    wk: Any
    wv: Any
    gates: Any
    gain_two: Any
    gain_one: Any
    place: Any
    lse: Any
    cosine: Any
    sine: Any


BACK_IN_PLACE = 7
class BackOuts(NamedTuple):
    grad: Any
    mix: Any
    experts: Any
    big_out: Any
    little_out: Any


class BackScratch(NamedTuple):
    back: Any
    other_ep: Any
    other_tp: Any
    mid_dy: Any
    mid_x2: Any
    wide_w: Any
    branch: Any
    heads: Any
    small: Any
    qs: Any
    atts: Any
    slots: Any
    kv_x: Any
    kv_z: Any
    keys: Any
    bias: Any
    dq: Any
    lows: Any
    wks: Any
    wvs: Any
    routers: Any
    dkv: Any
    part: Any
    part_in: Any
    mix_ep: Any
    mix_tp: Any
    held: Any
    spots: Any
    kept: Any
    staged: Any
    zero_in: Any
    whole: Any
    came: Any
    lit: Any
    lit_came: Any
    lit_x: Any
    lit_spots: Any
    ls: Any
    ks: Any
    xs: Any
    xr: Any
    zs: Any
    zr: Any
    es: Any
    er: Any
    ts: Any
    tr: Any
    kxs: Any
    kxr: Any
    kzs: Any
    kzr: Any
    os: Any
    free_x: Any
    free_up: Any
    free_down: Any


def back_body(group, *refs):
    n_in = len(BackIns._fields) + 6
    ins = BackIns(*refs[: len(BackIns._fields)])
    slots_in = refs[n_in - 6]
    keeps, sends, arrived, z_kept, z_sent = refs[n_in - 5 : n_in]
    o = BackOuts(*refs[n_in : n_in + len(BackOuts._fields)])
    s = BackScratch(*refs[n_in + len(BackOuts._fields) :])
    p = Place()
    early = arrived.shape[0]
    first = FIRST
    count = first + keeps.shape[0]
    seqs, rows, _ = ins.q.shape
    model = ins.middle.shape[1]
    width = ins.wk.shape[1]
    part_of = lambda i: pl.ds(i * rows, rows)

    whole_early = early - 1
    ring = [("here", e) for e in range(first, first + whole_early)] + [("half", first + whole_early)]
    ring += [("x", e) for e in range(first + early, count)] + [("big", count)]
    index_of = {item: i for i, item in enumerate(ring)}
    crosses = lambda item: item[0] != "here"

    def flow(item):
        if item == "little":
            return Flow(p, s.lit_x, s.lit_spots, s.zs.at[len(ring)], s.zr.at[len(ring)])
        i = index_of[item]
        credit = {"up": s.free_up, "down": s.free_down} if i >= RING else None
        return Flow(p, s.held.at[i % RING], s.spots.at[i % RING], s.zs.at[i], s.zr.at[i], credit)

    def x_copy(item):
        if item == "little":
            return p.copy("x", s.lit.at[p.ep, :, 1 - p.side], s.lit_x, s.xs.at[len(ring)], s.xr.at[len(ring)])
        i = index_of[item]
        if item[0] == "half":
            some = pl.ds(HALF, LINE - HALF)
            return p.copy("x", sends.at[0, some], s.held.at[i, some], s.xs.at[i], s.xr.at[i])
        src = s.whole.at[p.ep, :, 1 - p.side] if item[0] == "big" else sends.at[item[1] - first - whole_early]
        return p.copy("x", src, s.held.at[i % RING], s.xs.at[i], s.xr.at[i])

    def cross(item):
        if item != "little" and index_of[item] >= RING:
            pl.semaphore_wait(s.free_x, 1)
        x_copy(item).start()

    def load_keep(e):
        return pltpu.make_async_copy(keeps.at[e - first], s.kept, s.ks.at[0])

    def load_arrived(e):
        if e == first + whole_early:
            some = pl.ds(0, HALF)
            return pltpu.make_async_copy(
                arrived.at[e - first, some], s.held.at[e - first, some], s.ks.at[1 + e - first]
            )
        return pltpu.make_async_copy(arrived.at[e - first], s.held.at[e - first], s.ks.at[1 + e - first])

    def opened(item):
        if item == "little":
            x_copy(item).wait_recv()
            for d in range(LINE):
                add_to(s.lit_x, d, s.lit[p.ep, d, p.side])
        else:
            held = s.held.at[index_of[item] % RING]
            if item[0] in ("here", "half"):
                load_arrived(item[1]).wait()
            if item[0] != "here":
                x_copy(item).wait_recv()
            if item[0] == "big":
                for d in range(LINE):
                    add_to(held, d, s.whole[p.ep, d, p.side])
            else:
                load_keep(item[1]).wait()
                for d in range(LINE):
                    add_to(held, d, s.kept[d])
                if item[1] + 1 < count:
                    load_keep(item[1] + 1).start()
        flow(item).open()

    stored = []

    def store(e):
        return pltpu.make_async_copy(s.staged.at[e % 2], o.experts.at[e], s.os.at[e])

    def finish_expert(e, make):
        if len(stored) >= 2 and e % 2 in [k % 2 for k in stored[-2:]]:
            last = [k for k in stored if k % 2 == e % 2][-1]
            store(last).wait()
            waited.add(last)
        make()
        store(e).start()
        stored.append(e)

    waited = set()

    def closed(item):
        if item == "little":
            def finish(blocks):
                o.little_out[...] = total_of(blocks)

            flow(item).close(finish)
        elif item[0] == "big":
            def finish(blocks):
                o.big_out[...] = total_of(blocks)

            flow(item).close(finish)
        else:
            def finish(blocks):
                s.staged[item[1] % 2] = total_of(blocks)

            finish_expert(item[1], lambda: flow(item).close(finish))

    def freed(item):
        flow(item).drain()
        if item == "little":
            return
        after = index_of[item] + RING
        if after < len(ring):
            if crosses(item):
                x_copy(item).wait_send()
            if crosses(ring[after]):
                p.signal(s.free_x, "x")
            p.signal_line(s.free_up, s.free_down)

    loads = {}

    def load(name, src, dst):
        copy = pltpu.make_async_copy(src, dst, s.ls.at[len(loads)])
        copy.start()
        loads[name] = copy

    def got(*names):
        for name in names:
            loads[name].wait()

    load("back", ins.own_back, s.back)
    load_keep(first).start()
    for e in range(first, first + early):
        load_arrived(e).start()
    load("zero", z_kept, s.staged.at[0])
    load("grad", ins.middle, o.grad)
    load("dy", ins.dy, s.mid_dy)
    load("router", ins.router, s.routers)
    load("x2", ins.x2, s.mid_x2)
    load("w_out", ins.w_out, s.wide_w)
    load("mix", ins.own_mix, o.mix)
    load("q", ins.q, s.qs)
    load("attended", ins.attended, s.atts)
    load("slots", slots_in, s.slots)
    load("low", ins.low, s.lows)
    load("wk", ins.wk, s.wks)
    load("wv", ins.wv, s.wvs)

    p.greet(("x", "ep", "tp"))
    ep_back = p.copy("ep", ins.par_back, s.other_ep, s.es.at[0], s.er.at[0])
    ep_back.start()
    ep_mix = p.copy("ep", ins.par_mix, s.mix_ep, s.es.at[1], s.er.at[1])
    ep_mix.start()
    queue = ring[whole_early:] + ["little"]
    zero_copy = p.copy("x", z_sent, s.zero_in, s.xs.at[len(ring) + 1], s.xr.at[len(ring) + 1])
    zero_copy.start()
    for _ in range(3):
        cross(queue.pop(0))

    got("back")
    ep_back.wait_recv()
    for i in range(seqs):
        s.back[part_of(i)] = (
            s.back[part_of(i)].astype(F32) + s.other_ep[part_of(i)].astype(F32)
        ).astype(BF16)
    tp_back = p.copy("tp", s.back, s.other_tp, s.ts.at[0], s.tr.at[0])
    tp_back.start()
    got("mix")
    ep_mix.wait_recv()
    for i in range(seqs):
        o.mix[part_of(i)] = (o.mix[part_of(i)].astype(F32) + s.mix_ep[part_of(i)].astype(F32)).astype(BF16)

    def step_middle():
        got("grad", "dy", "router", "x2", "w_out")
        tp_back.wait_recv()
        for i in range(seqs):
            at = part_of(i)
            total = s.back[at].astype(F32) + s.other_tp[at].astype(F32)
            gate, pulls = ins.gates[at], total[:, model:]
            chosen = gate * (pulls - jnp.sum(gate * pulls, axis=-1, keepdims=True))
            high, rest = two_parts(chosen)
            grad_two = total[:, :model] + (mm_t(high, s.routers[...]) + mm_t(rest, s.routers[...]))
            unit, scale = unit_rows(o.grad[at])
            routed = t_mm(high, s.mid_x2[at]) + t_mm(rest, s.mid_x2[at])
            gain_row = jnp.sum(grad_two * unit, axis=0, keepdims=True)
            if i == 0:
                s.small[...] = routed
                s.small[LANES - 1 :, :] = gain_row
            else:
                s.small[: LANES - 1, :] += routed[: LANES - 1]
                s.small[LANES - 1 :, :] += gain_row
            scaled = grad_two * ins.gain_two[...]
            out = s.mid_dy[at].astype(F32) + scale * (
                scaled - unit * jnp.mean(scaled * unit, axis=-1, keepdims=True)
            )
            o.grad[at] = out
            rounded = out.astype(BF16)
            s.branch[at] = rounded
            s.heads[at] = mm(rounded, s.wide_w[...]).astype(BF16)
        load("wq", ins.wq, s.wide_w)
        load("act", ins.act, s.mid_dy)
        load("normed", ins.normed, s.mid_x2)

    tp_mix = p.copy("tp", o.mix, s.mix_tp, s.ts.at[1], s.tr.at[1])

    def step_attend(i):
        if i == 0:
            got("q", "attended", "slots")
        homes = [(p.z - r, side) for r in range(LINE) for side in (p.side, 1 - p.side)]
        firsts = [jnp.where(a >= 0, (2 * a + b) * rows, 2**24) for a, b in homes]

        def keep_grad(j, value):
            s.slots[i, j // 2, j % 2] = value

        s.dq[i] = attend_back_core(
            group,
            s.qs[i],
            ins.place[i],
            s.heads[part_of(i)],
            s.atts[i],
            ins.lse.at[i],
            ins.cosine[part_of(i)],
            ins.sine[part_of(i)],
            [s.slots.at[i, j // 2, j % 2] for j in range(2 * LINE)],
            firsts,
            p.cp * rows,
            s.keys,
            s.bias,
            keep_grad,
            512,
        )

        @p.at(LINE - 1)
        def _():
            for r in range(LINE - 1, 0, -1):
                kv_down(i, r).start()

    def kv_cross(i):
        return p.copy("x", s.slots.at[i, 0, 1], s.kv_x.at[i], s.kxs.at[i], s.kxr.at[i])

    def kv_down(i, r):
        return p.copy("down", s.slots.at[i, r], s.kv_z.at[i, r - 1], s.kzs.at[i, r - 1], s.kzr.at[i, r - 1])

    def kv_take(i, r):
        kv_down(i, r + 1).wait_recv()
        for way in range(2):
            s.slots[i, r, way] = (s.slots[i, r, way].astype(F32) + s.kv_z[i, r, way].astype(F32)).astype(BF16)

    def keys_pass(i, z):
        @p.at(z)
        def _():
            for r in range(z, 0, -1):
                kv_take(i, r)
                kv_down(i, r).start()

    def keys_cross(i):
        @pl.when(p.z < LINE - 1)
        def _():
            kv_take(i, 0)

        kv_cross(i).start()

    def keys_close(i):
        kv_cross(i).wait_recv()
        s.slots[i, 0, 0] = (s.slots[i, 0, 0].astype(F32) + s.kv_x[i].astype(F32)).astype(BF16)

    def part_copy(i):
        return p.copy("tp", s.part.at[part_of(i)], s.part_in.at[part_of(i)], s.ts.at[2 + i], s.tr.at[2 + i])

    def step_project(i):
        if i == 0:
            got("wq", "wk", "wv", "act", "normed")
        at = part_of(i)
        total = s.slots[i, 0, 0].astype(F32)
        dk = rope_back(total[:, :width], widen(ins.cosine[at], width), widen(ins.sine[at], width)).astype(BF16)
        dv = total[:, width:].astype(BF16)
        s.dkv[at, :width] = dk
        s.dkv[at, width:] = dv
        full = mm_t(s.dq[i], s.wide_w[...]) + mm_t(dk, s.wks[...]) + mm_t(dv, s.wvs[...])
        s.part[at] = full.astype(BF16)
        part_copy(i).start()

    tall = model // 4

    def weight_pieces(left, right, ref, keep):
        for piece_at in range(4):
            got_piece = t_mm(left[:, piece_at * tall : (piece_at + 1) * tall], right).astype(BF16)
            block = got_piece.reshape(-1, model // 16, right.shape[1])
            for b in range(4):
                whole = 4 * piece_at + b
                keep(whole // 8, whole % 8 // 2, whole % 2, block[b])

    def big_part(row):
        def keep(half, z, side, value):
            s.whole[half, z, side, row : row + value.shape[0], :] = value

        return keep

    def little_part(column):
        def keep(half, z, side, value):
            s.lit[half, z, side, :, column : column + value.shape[1]] = value

        return keep

    ep_big = p.copy("ep", s.whole.at[1 - p.ep], s.came, s.es.at[2], s.er.at[2])
    ep_lit = p.copy("ep", s.lit.at[1 - p.ep], s.lit_came, s.es.at[3], s.er.at[3])

    def step_out_weight():
        got("low")
        weight_pieces(s.branch[...], s.lows[...], s.whole, big_part(0))

    def step_query_weight():
        got("normed")
        loads["normed"] = Done()
        query = jnp.concatenate([s.dq[i] for i in range(seqs)], axis=0)
        weight_pieces(s.mid_x2[...], query, s.whole, big_part(model // 16))
        ep_big.start()

    def step_key_weight():
        weight_pieces(s.mid_x2[...], s.dkv[...], s.lit, little_part(0))
        for piece_at in range(4):
            turned = jnp.transpose(s.small[:, piece_at * tall : (piece_at + 1) * tall]).astype(BF16)
            block = turned.reshape(-1, model // 16, LANES)
            for b in range(4):
                whole = 4 * piece_at + b
                little_part(2 * width)(whole // 8, whole % 8 // 2, whole % 2, block[b])
        ep_lit.start()

    def step_big_cores():
        ep_big.wait_recv()
        for d in range(LINE):
            for side in range(2):
                s.whole[p.ep, d, side] = (
                    s.whole[p.ep, d, side].astype(F32) + s.came[d, side].astype(F32)
                ).astype(BF16)

    def step_little_cores():
        ep_lit.wait_recv()
        for d in range(LINE):
            for side in range(2):
                s.lit[p.ep, d, side] = (
                    s.lit[p.ep, d, side].astype(F32) + s.lit_came[d, side].astype(F32)
                ).astype(BF16)

    def step_input():
        for i in range(seqs):
            at = part_of(i)
            part_copy(i).wait_recv()
            unit, scale = unit_rows(s.mid_dy[at].astype(F32))
            whole = s.part[at].astype(F32) + s.part_in[at].astype(F32)
            gain_row = jnp.sum(whole * unit, axis=0, keepdims=True)
            if i == 0:
                s.small[LANES - 2 : LANES - 1, :] = gain_row
            else:
                s.small[LANES - 2 : LANES - 1, :] += gain_row
            scaled = whole * ins.gain_one[...]
            o.grad[at] = o.grad[at] + scale * (scaled - unit * jnp.mean(scaled * unit, axis=-1, keepdims=True))

    def step_mix():
        tp_mix.wait_recv()
        tp_mix.wait_send()
        for i in range(seqs):
            o.mix[part_of(i)] = (o.mix[part_of(i)].astype(F32) + s.mix_tp[part_of(i)].astype(F32)).astype(BF16)

    line = list(ring) + ["little"]
    stage = {item: 0 for item in line}

    def advance(at, to):
        if not 0 <= at < len(line):
            return
        item = line[at]
        while stage[item] < to:
            now = stage[item]
            if now == 0:
                opened(item)
            elif now == 1:
                flow(item).second()
            elif now == 2:
                flow(item).third()
            elif now == 3:
                closed(item)
            elif now == 4:
                freed(item)
            stage[item] = now + 1

    def turn(at):
        for back in (4, 3, 2, 1, 0):
            advance(at - back, back + 1)

    def add_zero():
        got("zero")
        zero_copy.wait_recv()
        s.staged[0] = s.staged[0] + s.zero_in[...].astype(F32)

    tp_mix.start()
    turn(0)
    finish_expert(0, add_zero)
    turn(1)
    step_middle()
    advance(0, 3)
    advance(1, 2)
    step_attend(0)
    step_attend(1)
    cross(queue.pop(0))
    step_out_weight()
    step_query_weight()
    turn(2)
    keys_pass(0, 2)
    advance(0, 4)
    advance(1, 3)
    keys_pass(1, 2)
    advance(2, 2)
    step_big_cores()
    step_mix()
    keys_pass(0, 1)
    keys_pass(1, 1)
    turn(3)
    keys_cross(0)
    keys_cross(1)
    cross(queue.pop(0))
    turn(4)
    cross(queue.pop(0))
    keys_close(0)
    step_project(0)
    keys_close(1)
    step_project(1)
    advance(2, 4)
    advance(3, 3)
    advance(4, 2)
    step_input()
    step_key_weight()
    turn(5)
    cross(queue.pop(0))
    step_little_cores()
    for at in range(6, len(line) + 4):
        turn(at)
        if queue:
            cross(queue.pop(0))
    for e in stored:
        if e not in waited:
            store(e).wait()
    for item in line:
        if item == "little" or (crosses(item) and index_of[item] + RING >= len(ring)):
            x_copy(item).wait_send()
    for i in range(seqs):
        kv_cross(i).wait_send()
        part_copy(i).wait_send()
        for z in range(1, LINE):

            @p.at(z)
            def _(z=z):
                for r in range(z, 0, -1):
                    kv_down(i, r).wait_send()

    tp_back.wait_send()
    zero_copy.wait_send()
    for copy in (ep_back, ep_mix, ep_big, ep_lit):
        copy.wait_send()


class Done:
    def wait(self):
        return None


def back_and_sums(ins, slots, chunks, group):
    keeps, _, arrived, *_ = chunks
    _, length, depth, wide = keeps.shape
    early, count = arrived.shape[0], FIRST + keeps.shape[0]
    block = (length, depth, wide)
    v = BackIns(*ins)
    rows, model = v.middle.shape
    seqs, each, heads = v.q.shape
    width = v.wk.shape[1]
    both = 2 * width
    small = (length, 2, model // 16, both + LANES)
    n_ring = count - FIRST + 1
    anywhere = pl.BlockSpec(memory_space=pl.ANY)
    inside = pl.BlockSpec(memory_space=pltpu.VMEM)
    dma, vm = pltpu.SemaphoreType.DMA, pltpu.VMEM
    flag = pltpu.SemaphoreType.REGULAR
    scratch = dict(
        back=vm((rows, model + LANES), BF16),
        other_ep=vm((rows, model + LANES), BF16),
        other_tp=vm((rows, model + LANES), BF16),
        mid_dy=vm((rows, model), BF16),
        mid_x2=vm((rows, model), BF16),
        wide_w=vm((model, heads), BF16),
        branch=vm((rows, model), BF16),
        heads=vm((rows, heads), BF16),
        small=vm((LANES, model), F32),
        qs=vm((seqs, each, heads), BF16),
        atts=vm((seqs, each, heads), F32),
        slots=vm((seqs, LINE, 2, each, both), BF16),
        kv_x=vm((seqs, each, both), BF16),
        kv_z=vm((seqs, LINE - 1, 2, each, both), BF16),
        keys=vm((2 * LINE * each, both), BF16),
        bias=vm((2 * LINE * each, each), F32),
        dq=vm((seqs, each, heads), BF16),
        lows=vm((rows, heads), BF16),
        wks=vm((model, width), BF16),
        wvs=vm((model, width), BF16),
        routers=vm((model, LANES), BF16),
        dkv=vm((rows, both), BF16),
        part=vm((rows, model), BF16),
        part_in=vm((rows, model), BF16),
        mix_ep=vm((rows, model), BF16),
        mix_tp=vm((rows, model), BF16),
        held=vm((RING,) + block, BF16),
        spots=vm((RING, 5, depth, wide), BF16),
        kept=vm(block, BF16),
        staged=vm((2, depth, wide), F32),
        zero_in=vm((depth, wide), BF16),
        whole=vm((2, length, 2, depth, wide), BF16),
        came=vm((length, 2, depth, wide), BF16),
        lit=vm((2,) + small, BF16),
        lit_came=vm(small, BF16),
        lit_x=vm((small[0],) + small[2:], BF16),
        lit_spots=vm((5,) + small[2:], BF16),
        ls=dma((28,)),
        ks=dma((1 + early,)),
        xs=dma((n_ring + 2,)),
        xr=dma((n_ring + 2,)),
        zs=dma((n_ring + 1, 6)),
        zr=dma((n_ring + 1, 6)),
        es=dma((4,)),
        er=dma((4,)),
        ts=dma((4,)),
        tr=dma((4,)),
        kxs=dma((2,)),
        kxr=dma((2,)),
        kzs=dma((2, 3)),
        kzr=dma((2, 3)),
        os=dma((count,)),
        free_x=flag,
        free_up=flag,
        free_down=flag,
    )
    return pl.pallas_call(
        functools.partial(back_body, group),
        out_shape=(
            shape_of((rows, model), F32),
            shape_of((rows, model), BF16),
            shape_of((count, depth, wide), F32),
            shape_of((depth, wide), F32),
            shape_of(small[2:], F32),
        ),
        in_specs=[anywhere] * (len(BackIns._fields) - BACK_IN_PLACE)
        + [inside] * BACK_IN_PLACE
        + [anywhere] * 6,
        out_specs=(inside, inside, anywhere, inside, inside),
        scratch_shapes=[scratch[name] for name in BackScratch._fields],
        compiler_params=pltpu.CompilerParams(
            collective_id=1, has_side_effects=True, vmem_limit_bytes=67_043_328
        ),
        name="back_and_sums",
    )(*ins, slots, *chunks)


def results_body(middle, mix, grad, chunk, big, little, out, grad_in, first, second, keys, values, small, both, down):
    out[...] = middle[...] + mix[...].astype(F32)
    grad_in[...] = grad[...]
    half = down.shape[2]
    both[0] = chunk[0, :, : 2 * half].reshape(both.shape[1:])
    down[0] = chunk[0, :, 2 * half :]

    @pl.when(pl.program_id(0) == 0)
    def _():
        tall, width = first.shape[0], keys.shape[1]
        first[...] = big[:tall]
        second[...] = big[tall:]
        keys[...] = little[:, :width]
        values[...] = little[:, width : 2 * width]
        small[...] = little[:, 2 * width :]


def results(middle, mix, grad, chunks, big, little, half):
    rows, model = middle.shape
    count, depth, wide = chunks.shape
    tall, width = big.shape[0] // 2, (little.shape[1] - LANES) // 2
    part = pl.BlockSpec((rows // count, model), lambda e: (e, 0))
    once = lambda shape: pl.BlockSpec(shape, lambda e: (0,) * len(shape))
    whole = [(tall, big.shape[1])] * 2 + [(tall, width)] * 2 + [(tall, LANES)]
    return pl.pallas_call(
        results_body,
        grid=(count,),
        out_shape=[shape_of((rows, model), F32)] * 2
        + [shape_of(shape, F32) for shape in whole]
        + [shape_of((count, depth, 2, half), F32), shape_of((count, depth, half), F32)],
        in_specs=[part] * 3
        + [pl.BlockSpec((1, depth, wide), lambda e: (e, 0, 0)), once(big.shape), once(little.shape)],
        out_specs=[part] * 2
        + [once(shape) for shape in whole]
        + [
            pl.BlockSpec((1, depth, 2, half), lambda e: (e, 0, 0, 0)),
            pl.BlockSpec((1, depth, half), lambda e: (e, 0, 0)),
        ],
        compiler_params=params(),
        name="results",
    )(middle, mix, grad, chunks, big, little)


class FrontIns(NamedTuple):
    q: Any
    kv: Any
    act: Any
    hot: Any
    router: Any
    gain: Any
    place: Any
    w_out: Any
    dy: Any
    w_in: Any


class FrontOuts(NamedTuple):
    slots: Any
    low: Any
    attended: Any
    lse: Any
    middle: Any
    normed: Any
    gates: Any
    x_par: Any
    g_par: Any
    dy_par: Any
    w_flat: Any


class FrontScratch(NamedTuple):
    keys: Any
    bias: Any
    wo: Any
    part: Any
    part_in: Any
    raw: Any
    flat: Any
    ws: Any
    wi: Any
    wf: Any
    us: Any
    ur: Any
    xs: Any
    xr: Any
    ts: Any
    tr: Any
    es: Any
    er: Any


def front_body(group, *refs):
    n_in, n_out = len(FrontIns._fields), len(FrontOuts._fields)
    ins = FrontIns(*refs[:n_in])
    o = FrontOuts(*refs[n_in : n_in + n_out])
    s = FrontScratch(*refs[n_in + n_out :])
    p = Place()
    seqs, rows, _ = ins.q.shape
    experts_here = ins.w_in.shape[0]
    part_of = lambda i: pl.ds(i * rows, rows)

    def fetch(e):
        return pltpu.make_async_copy(ins.w_in.at[e], s.raw.at[e % 2], s.wi.at[e % 2])

    def put(e):
        return pltpu.make_async_copy(s.flat.at[e % 2], o.w_flat.at[e], s.wf.at[e % 2])

    done = []

    def fill(count):
        for _ in range(count):
            e = len(done)
            if e >= experts_here:
                return
            fetch(e).wait()
            if e >= 2:
                put(e - 2).wait()
            s.flat[e % 2] = s.raw[e % 2].reshape(s.flat.shape[1:])
            put(e).start()
            if e + 2 < experts_here:
                fetch(e + 2).start()
            done.append(e)

    def source(i, r):
        return ins.kv.at[i] if r == 0 else o.slots.at[i, r, 0]

    def up_copy(i, r):
        return p.copy("up", source(i, r), o.slots.at[i, r + 1, 0], s.us.at[i, r], s.ur.at[i, r])

    def x_copy(i, r):
        return p.copy("x", source(i, r), o.slots.at[i, r, 1], s.xs.at[i, r], s.xr.at[i, r])

    def tp_copy(i):
        return p.copy("tp", s.part.at[part_of(i)], s.part_in.at[part_of(i)], s.ts.at[i], s.tr.at[i])

    def ep_copies(i):
        at = part_of(i)
        return (
            p.copy("ep", o.normed.at[at], o.x_par.at[at], s.es.at[2 * i], s.er.at[2 * i]),
            p.copy("ep", o.gates.at[at], o.g_par.at[at], s.es.at[2 * i + 1], s.er.at[2 * i + 1]),
        )

    fetch(0).start()
    fetch(1).start()
    wo_load = pltpu.make_async_copy(ins.w_out, s.wo, s.ws.at[0])
    wo_load.start()
    p.greet(("x", "ep", "tp"))
    for i in range(seqs):

        @pl.when(p.z < LINE - 1)
        def _(i=i):
            up_copy(i, 0).start()

        x_copy(i, 0).start()
    dy_copy = p.copy("ep", ins.dy, o.dy_par, s.es.at[2 * seqs], s.er.at[2 * seqs])
    dy_copy.start()
    for i in range(seqs):
        o.slots[i, 0, 0] = ins.kv[i]
        for r in range(1, LINE):

            @pl.when(p.z < r)
            def _(i=i, r=r):
                o.slots[i, r] = jnp.zeros(o.slots.shape[2:], BF16)

    fill(1)
    for r in range(1, LINE):
        for i in range(seqs):
            for z in range(r, LINE):

                @p.at(z)
                def _(i=i, r=r, z=z):
                    up_copy(i, r - 1).wait_recv()
                    if z < LINE - 1:
                        up_copy(i, r).start()
                    x_copy(i, r).start()

        fill(1)
    homes = [(p.z - r, side) for r in range(LINE) for side in (p.side, 1 - p.side)]
    firsts = [jnp.where(a >= 0, (2 * a + b) * rows, 2**24) for a, b in homes]
    for i in range(seqs):
        for r in range(LINE):

            @pl.when(p.z >= r)
            def _(i=i, r=r):
                x_copy(i, r).wait_recv()

        whole = attend_core(
            group,
            ins.q[i],
            ins.place[i],
            [o.slots.at[i, j // 2, j % 2] for j in range(2 * LINE)],
            firsts,
            p.cp * rows,
            s.keys,
            s.bias,
            o.lse.at[i],
            KEY_CHUNK,
        )
        o.attended[i] = whole
        o.low[i] = whole.astype(BF16)
        if i == 0:
            wo_load.wait()
        s.part[part_of(i)] = mm_t(o.low[i], s.wo[...]).astype(BF16)
        tp_copy(i).start()
    fill(1)
    for i in range(seqs):
        at = part_of(i)
        tp_copy(i).wait_recv()
        mid = ins.act[at].astype(F32) + (s.part[at].astype(F32) + s.part_in[at].astype(F32))
        o.middle[at] = mid
        o.normed[at], o.gates[at] = route(mid, ins.gain[...], ins.router[...], ins.hot[at])
        for copy in ep_copies(i):
            copy.start()
        fill(3 if i == 0 else experts_here)
    for i in range(seqs):
        for copy in ep_copies(i):
            copy.wait()
        tp_copy(i).wait_send()
        for r in range(LINE):

            @pl.when(p.z >= r)
            def _(i=i, r=r):
                x_copy(i, r).wait_send()
                if r < LINE - 1:

                    @pl.when(p.z < LINE - 1)
                    def _():
                        up_copy(i, r).wait_send()

    dy_copy.wait()
    for e in done[-2:]:
        put(e).wait()


def front(ins, group):
    v = FrontIns(*ins)
    seqs, each, heads = v.q.shape
    both = v.kv.shape[-1]
    rows, model = v.act.shape
    local, _, _, half = v.w_in.shape
    anywhere = pl.BlockSpec(memory_space=pl.ANY)
    inside = pl.BlockSpec(memory_space=pltpu.VMEM)
    dma, vm = pltpu.SemaphoreType.DMA, pltpu.VMEM
    scratch = dict(
        keys=vm((2 * LINE * each, both), BF16),
        bias=vm((2 * LINE * each, each), F32),
        wo=vm(v.w_out.shape, BF16),
        part=vm((rows, model), BF16),
        part_in=vm((rows, model), BF16),
        raw=vm((2, model, 2, half), BF16),
        flat=vm((2, model, 2 * half), BF16),
        ws=dma((1,)),
        wi=dma((2,)),
        wf=dma((2,)),
        us=dma((seqs, LINE - 1)),
        ur=dma((seqs, LINE - 1)),
        xs=dma((seqs, LINE)),
        xr=dma((seqs, LINE)),
        ts=dma((seqs,)),
        tr=dma((seqs,)),
        es=dma((2 * seqs + 1,)),
        er=dma((2 * seqs + 1,)),
    )
    return pl.pallas_call(
        functools.partial(front_body, group),
        out_shape=(
            shape_of((seqs, LINE, 2, each, both), BF16),
            shape_of((seqs, each, heads), BF16),
            shape_of((seqs, each, heads), F32),
            shape_of((seqs, heads // HEAD // group, group * each), F32),
            shape_of((rows, model), F32),
            shape_of((rows, model), BF16),
            shape_of((rows, LANES), F32),
            shape_of((rows, model), BF16),
            shape_of((rows, LANES), F32),
            shape_of((rows, model), BF16),
            shape_of((local, model, 2 * half), BF16),
        ),
        in_specs=[inside] * 7 + [anywhere] * 3,
        out_specs=(inside,) * 7 + (anywhere,) * 4,
        scratch_shapes=[scratch[name] for name in FrontScratch._fields],
        compiler_params=params(collective_id=3, has_side_effects=True),
        name="front",
    )(*ins)


def on_device(
    activations,
    cotangent,
    positions,
    routes,
    w_query,
    w_key,
    value_weight,
    w_out,
    gain_attn,
    gain_moe,
    w_router,
    w_gate_up,
    w_down,
):
    seqs, rows, model = activations.shape
    total = seqs * rows
    width = w_key.shape[1]
    group = w_query.shape[1] // width
    expert_count = w_router.shape[1]
    local = w_gate_up.shape[0]
    half = w_down.shape[2]
    blocks = lax.axis_size("cp")
    length = blocks // 2
    here = lax.axis_index("cp")
    z, side = here // 2, here % 2
    mine = lax.axis_index("ep")
    act = activations.reshape(total, model)
    dy = cotangent.reshape(total, model)
    gain_one, gain_two = gain_attn.reshape(1, model), gain_moe.reshape(1, model)

    frequency = jnp.power(10000.0, -(jnp.arange(HEAD // 2, dtype=F32) * 2.0 / HEAD))
    angles = positions.reshape(total, 1).astype(F32) * jnp.tile(frequency, 2 * LANES // HEAD)
    cosine, sine = jnp.cos(angles), jnp.sin(angles)

    normed, q, kv = project(act, gain_one, w_query, w_key, value_weight, cosine, sine)
    q = q.reshape(seqs, rows, -1)
    place = positions.reshape(seqs, 1, rows)
    lanes = jnp.arange(LANES, dtype=jnp.int32)
    hot = jnp.sum((routes.reshape(total, -1, 1) == lanes).astype(F32), axis=1)
    router = jnp.pad(w_router, ((0, 0), (0, LANES - expert_count)))
    if length == LINE:
        kv = kv.reshape(seqs, rows, 2 * width)
        ins = (q, kv, act, hot, router, gain_two, place, w_out, dy, w_gate_up)
        slots, low, attended, lse, middle, normed_two, gates, x_par, gates_par, dy_par, w_in = front(ins, group)
        low = low.reshape(total, -1)
    else:
        kv = kv.reshape(1, seqs, rows, 2 * width)
        offset = (here * rows).astype(jnp.int32).reshape(1)
        slots = [lax.all_gather(kv, "cp", axis=0, tiled=True)]
        first = jnp.arange(blocks, dtype=jnp.int32) * rows
        dy_par = swap(dy, "ep")
        low, attended, lse = attend(q, place, slots, first, offset, group)
        low = low.reshape(total, -1)
        part = out_project(low, w_out)
        w_in = w_gate_up.reshape(local, model, 2 * half)
        middle, normed_two, gates = middle_of(act, part, swap(part, "tp"), gain_two, router, hot)
        x_par, gates_par = swap(normed_two, "ep"), swap(gates, "ep")

    early, apart = (EARLY, FIRST) if length == LINE else (0, 0)
    args = (normed_two, x_par, dy, dy_par, gates, gates_par, w_in, w_down)
    chunks, (own_back, par_back, own_mix, par_mix) = experts(early, apart, blocks, *args)
    if length == LINE:
        ins = (
            own_back, par_back, own_mix, par_mix, middle, dy, router, w_out, normed_two, q, attended, act, normed,
            low, w_query, w_key, value_weight, gates, gain_two, gain_one, place, lse, cosine, sine,
        )
        input_grad, mix, expert_grad, big, little = back_and_sums(ins, slots, chunks, group)
        output, input_grad, *plain, small, gate_up_grad, down_grad = results(
            middle, mix, input_grad, expert_grad, big, little, half
        )
        out_grad, query_grad, key_grad, value_grad = plain
        small_grads = small[:, LANES - 2], small[:, LANES - 1], small[:, :expert_count]
    else:
        back = total_of([own_back, swap(par_back, "ep")]).astype(BF16)
        grad_middle, branch, grad_heads, small = middle_back(
            back, swap(back, "tp"), middle, dy, gates, router, gain_two, w_out, normed_two
        )
        seq_cosine, seq_sine = cosine.reshape(seqs, rows, -1), sine.reshape(seqs, rows, -1)
        dq, grads = attend_back(
            q, place, grad_heads.reshape(q.shape), attended, lse, seq_cosine, seq_sine, slots, first, offset, group
        )
        dq = dq.reshape(total, -1)
        kv_sum = lax.psum_scatter(grads[0], "cp", scatter_dimension=0, tiled=True)
        kv_terms = [kv_sum, jnp.zeros_like(kv_sum), jnp.zeros_like(kv_sum)]
        kv_terms = [t.reshape(total, 2 * width) for t in kv_terms]
        spots = jnp.stack([mine, side]).astype(jnp.int32)
        big = weights(spots, blocks, [(branch, low), (normed, dq)], stacked=True)
        normed_part, dkv, gain_row = project_back(act, dq, *kv_terms, cosine, sine, w_query, w_key, value_weight)
        small = jnp.concatenate([small[:expert_count], small[LANES : LANES + 1], gain_row[:1]], axis=0)
        small = jnp.pad(small, ((0, LANES - small.shape[0]), (0, 0)))
        little = weights(spots, blocks, [(normed, dkv)], (small,))
        input_grad = input_of(act, grad_middle, normed_part, swap(normed_part, "tp"), gain_one)
        mix = total_of([own_mix, swap(par_mix, "ep")]).astype(BF16)
        output = middle + total_of([mix, swap(mix, "tp")])

        def spread_sum(keep, send):
            both = total_of([keep, swap(send, "ep")]).astype(BF16)
            return line_sum([both[0], swap(both[1], "cp")], z, length)

        turned = [jnp.swapaxes(v, 0, 1) for v in (chunks[0], swap(chunks[1], "cp"))]
        expert_grad = line_sum(turned, z, length)
        big, little = spread_sum(*big), spread_sum(*little)
        gate_up_grad = expert_grad[:, :, : 2 * half].reshape(local, -1, 2, half)
        down_grad = expert_grad[:, :, 2 * half :]
        tall = big.shape[0] // 2
        out_grad, query_grad = big[:tall], big[tall:]
        key_grad, value_grad = little[:, :width], little[:, width : 2 * width]
        small = little[:, 2 * width :]
        gain_part = small[:, expert_count + 1]
        small_grads = gain_part + swap(gain_part, "tp"), small[:, expert_count], small[:, :expert_count]
    return (
        output.reshape(activations.shape),
        input_grad.reshape(activations.shape),
        query_grad,
        key_grad,
        value_grad,
        out_grad,
        *small_grads,
        gate_up_grad,
        down_grad,
    )


def solution(mesh):
    in_specs = (
        P("ep", "cp", None),
        P("ep", "cp", None),
        P("ep", "cp"),
        P("ep", "cp", None),
        P(None, "tp"),
        P(None, "tp"),
        P(None, "tp"),
        P(None, "tp"),
        P(),
        P(),
        P(),
        P("ep", None, None, "tp"),
        P("ep", None, "tp"),
    )
    out_specs = (
        P("ep", "cp", None),
        P("ep", "cp", None),
        P(("ep", "cp"), "tp"),
        P(("ep", "cp"), "tp"),
        P(("ep", "cp"), "tp"),
        P(("ep", "cp"), "tp"),
        P(("ep", "cp")),
        P(("ep", "cp")),
        P(("ep", "cp"), None),
        P("ep", "cp", None, "tp"),
        P("ep", "cp", "tp"),
    )
    return jax.shard_map(
        on_device, mesh=mesh, in_specs=in_specs, out_specs=out_specs, check_vma=False
    )
```

```python
import functools
from typing import Any, NamedTuple

import jax
import jax.numpy as jnp
from jax import lax
from jax.experimental import pallas as pl
from jax.experimental.pallas import tpu as pltpu
from jax.sharding import PartitionSpec as P

HEAD = 64
EPS = 1e-06
NEG = -1e30
SCALE = 0.125
LANES = 128
KEY_CHUNK = 1024
F32 = jnp.float32
BF16 = jnp.bfloat16
MESH = pl.DeviceIdType.MESH


def mm(a, b):
    return lax.dot_general(a, b, (((1,), (0,)), ((), ())), preferred_element_type=F32)


def mm_t(a, b):
    return lax.dot_general(a, b, (((1,), (1,)), ((), ())), preferred_element_type=F32)


def t_mm(a, b):
    return lax.dot_general(a, b, (((0,), (0,)), ((), ())), preferred_element_type=F32)


def two_parts(v):
    high = v.astype(BF16)
    return high, (v - high.astype(F32)).astype(BF16)


def halves_turned(v, back):
    width = v.shape[1]
    ahead = pltpu.roll(v, width - HEAD // 2, 1)
    behind = pltpu.roll(v, HEAD // 2, 1)
    first = lax.broadcasted_iota(jnp.int32, v.shape, 1) % HEAD < HEAD // 2
    if back:
        return jnp.where(first, ahead, -behind)
    return jnp.where(first, -ahead, behind)


def rope(v, cosine, sine):
    return v * cosine + halves_turned(v, False) * sine


def rope_back(v, cosine, sine):
    return v * cosine + halves_turned(v * sine, True)


def widen(table, width):
    return jnp.concatenate([table] * (width // table.shape[1]), axis=1)


def unit_rows(v):
    scale = lax.rsqrt(jnp.mean(v * v, axis=-1, keepdims=True) + EPS)
    return v * scale, scale


def shape_of(shape, dtype):
    return jax.ShapeDtypeStruct(shape, dtype)


def params(**kw):
    return pltpu.CompilerParams(vmem_limit_bytes=60 * 2**20, **kw)


def cost(flops, moved):
    return pl.CostEstimate(flops=int(flops), bytes_accessed=int(moved), transcendentals=0)


def project_body(act, gain, wq, wk, wv, cosine, sine, normed, q, kv):
    unit, _ = unit_rows(act[...].astype(F32))
    low = (unit * gain[...]).astype(BF16)
    normed[...] = low
    qf = mm(low, wq[...])
    q[...] = rope(qf, widen(cosine[...], qf.shape[1]), widen(sine[...], qf.shape[1])).astype(BF16)
    kf = mm(low, wk[...])
    width = kf.shape[1]
    kv[:, :width] = rope(kf, widen(cosine[...], width), widen(sine[...], width)).astype(BF16)
    kv[:, width:] = mm(low, wv[...]).astype(BF16)


def project(act, gain, wq, wk, wv, cosine, sine):
    rows, model = act.shape
    total = wq.shape[1] + 2 * wk.shape[1]
    return pl.pallas_call(
        project_body,
        out_shape=(
            shape_of((rows, model), BF16),
            shape_of((rows, wq.shape[1]), BF16),
            shape_of((rows, 2 * wk.shape[1]), BF16),
        ),
        compiler_params=params(),
        cost_estimate=cost(2 * rows * model * total, 2 * model * total + 6 * rows * model),
        name="project",
    )(act, gain, wq, wk, wv, cosine, sine)


def fill_keys(firsts, offset, place, slots, keys, bias, rows):
    query = lax.broadcasted_iota(jnp.int32, (rows, rows), 1) + offset
    for at, slot in enumerate(slots):
        keys[at * rows : (at + 1) * rows, :] = slot[...]
        key = lax.broadcasted_iota(jnp.int32, (rows, rows), 0) + firsts[at]
        distance = query - key
        seen = (distance >= 0) & (distance <= place)
        bias[at * rows : (at + 1) * rows, :] = jnp.where(seen, 0.0, NEG)


def single_slots(slots):
    return [slot.at[one, 0] for slot in slots for one in range(slot.shape[0])]


def group_rows(block, head, group):
    return jnp.concatenate(
        [block[:, (head * group + g) * HEAD : (head * group + g + 1) * HEAD] for g in range(group)], axis=0
    )


def attend_core(group, q, place, slots, firsts, offset, keys, bias, lse_ref, most):
    rows = q.shape[0]
    fill_keys(firsts, offset, place, slots, keys, bias, rows)
    total, width = keys.shape[0], keys.shape[1] // 2
    chunk = min(total, most)
    q = (q.astype(F32) * SCALE).astype(BF16)
    pieces = []
    for head in range(width // HEAD):
        q3 = group_rows(q, head, group)
        top = run = out = None
        for low in range(0, total, chunk):
            k = keys[low : low + chunk, head * HEAD : (head + 1) * HEAD]
            v = keys[low : low + chunk, width + head * HEAD : width + (head + 1) * HEAD]
            s = mm_t(k, q3) + widen(bias[low : low + chunk, :], group * rows)
            here = jnp.max(s, axis=0, keepdims=True)
            new = here if top is None else jnp.maximum(top, here)
            p = jnp.exp(s - new)
            part = jnp.sum(p, axis=0, keepdims=True)
            o = t_mm(v, p.astype(BF16))
            if top is None:
                run, out = part, o
            else:
                shrink = jnp.exp(top - new)
                run, out = run * shrink + part, out * shrink + o
            top = new
        out = jnp.transpose(out / run)
        pieces += [out[g * rows : (g + 1) * rows] for g in range(group)]
        lse_ref[head : head + 1, :] = top + jnp.log(run)
    return jnp.concatenate(pieces, axis=1)


def attend_body(group, count, first_ref, offset_ref, q_ref, place_ref, *refs):
    slots = single_slots(refs[:count])
    low_ref, out_ref, lse_ref, keys, bias = refs[count:]
    firsts = [first_ref[i] for i in range(len(slots))]
    whole = attend_core(
        group, q_ref[0], place_ref[0], slots, firsts, offset_ref[0], keys, bias, lse_ref.at[0], KEY_CHUNK
    )
    out_ref[0] = whole
    low_ref[0] = whole.astype(BF16)


def seq_block(shape):
    return pl.BlockSpec((1,) + shape[1:], lambda s, *_: (s,) + (0,) * (len(shape) - 1))


def slot_block(shape):
    return pl.BlockSpec((shape[0], 1) + shape[2:], lambda s, *_: (0, s, 0, 0))


def attend(q, place, slots, first, offset, group):
    seqs, rows, wide = q.shape
    both = slots[0].shape[-1]
    total = rows * sum(slot.shape[0] for slot in slots)
    heads = wide // HEAD // group
    outs = (
        shape_of(q.shape, BF16),
        shape_of(q.shape, F32),
        shape_of((seqs, heads, group * rows), F32),
    )
    return pl.pallas_call(
        functools.partial(attend_body, group, len(slots)),
        out_shape=outs,
        grid_spec=pltpu.PrefetchScalarGridSpec(
            num_scalar_prefetch=2,
            grid=(seqs,),
            in_specs=[seq_block(q.shape), seq_block(place.shape)] + [slot_block(s.shape) for s in slots],
            out_specs=tuple(seq_block(o.shape) for o in outs),
            scratch_shapes=[pltpu.VMEM((total, both), BF16), pltpu.VMEM((total, rows), F32)],
        ),
        compiler_params=params(),
        cost_estimate=cost(2e9 * 4, 20e6),
        name="attend",
    )(first, offset, q, place, *slots)


def attend_back_core(
    group, q, place, go, out, lse_ref, cosine, sine, slots, firsts, offset, keys, bias, keep_grad, most
):
    rows = q.shape[0]
    fill_keys(firsts, offset, place, slots, keys, bias, rows)
    total, width = keys.shape[0], keys.shape[1] // 2
    chunk = min(total, most)
    q = (q.astype(F32) * SCALE).astype(BF16)
    products = go.astype(F32) * out
    ones = jnp.ones((8, HEAD), F32)
    heads = width // HEAD
    q3s = [group_rows(q, head, group) for head in range(heads)]
    g3s = [group_rows(go, head, group) for head in range(heads)]
    deltas = [
        lax.dot_general(
            ones,
            group_rows(products, head, group),
            (((1,), (1,)), ((), ())),
            preferred_element_type=F32,
            precision=lax.Precision.HIGHEST,
        )[:1]
        for head in range(heads)
    ]
    dq = [None] * heads
    for low in range(0, total, chunk):
        dks, dvs = [], []
        for head in range(heads):
            k = keys[low : low + chunk, head * HEAD : (head + 1) * HEAD]
            v = keys[low : low + chunk, width + head * HEAD : width + (head + 1) * HEAD]
            s = mm_t(k, q3s[head]) + widen(bias[low : low + chunk, :], group * rows)
            p = jnp.exp(s - lse_ref[head : head + 1, :])
            dp = mm_t(v, g3s[head])
            ds = (p * (dp - deltas[head])).astype(BF16)
            dks.append(mm(ds, q3s[head]))
            dvs.append(mm(p.astype(BF16), g3s[head]))
            part = t_mm(k, ds)
            dq[head] = part if dq[head] is None else dq[head] + part
        both = jnp.concatenate(dks + dvs, axis=1).astype(BF16)
        for one in range(chunk // rows):
            keep_grad(low // rows + one, both[one * rows : (one + 1) * rows])
    pieces = []
    for head in range(heads):
        back = jnp.transpose(dq[head] * SCALE)
        pieces += [back[g * rows : (g + 1) * rows] for g in range(group)]
    whole = jnp.concatenate(pieces, axis=1)
    return rope_back(whole, widen(cosine, whole.shape[1]), widen(sine, whole.shape[1])).astype(BF16)


def attend_back_body(
    group, count, first_ref, offset_ref, q_ref, place_ref, grad_ref, out_ref, lse_ref, cos_ref, sin_ref, *refs
):
    slots = single_slots(refs[:count])
    dq_ref = refs[count]
    grads = single_slots(refs[count + 1 : 2 * count + 1])
    keys, bias = refs[2 * count + 1 :]

    def keep_grad(at, value):
        grads[at][...] = value

    dq_ref[0] = attend_back_core(
        group,
        q_ref[0],
        place_ref[0],
        grad_ref[0],
        out_ref[0],
        lse_ref.at[0],
        cos_ref[0],
        sin_ref[0],
        slots,
        [first_ref[i] for i in range(len(slots))],
        offset_ref[0],
        keys,
        bias,
        keep_grad,
        KEY_CHUNK,
    )


def attend_back(q, place, grad, out, lse, cosine, sine, slots, first, offset, group):
    seqs, rows, _ = q.shape
    both = slots[0].shape[-1]
    total = rows * sum(slot.shape[0] for slot in slots)
    outs = (shape_of(q.shape, BF16),) + tuple(shape_of(s.shape, BF16) for s in slots)
    ins = (q, place, grad, out, lse, cosine, sine)
    got = pl.pallas_call(
        functools.partial(attend_back_body, group, len(slots)),
        out_shape=outs,
        grid_spec=pltpu.PrefetchScalarGridSpec(
            num_scalar_prefetch=2,
            grid=(seqs,),
            in_specs=[seq_block(a.shape) for a in ins] + [slot_block(s.shape) for s in slots],
            out_specs=(seq_block(outs[0].shape),) + tuple(slot_block(s.shape) for s in slots),
            scratch_shapes=[pltpu.VMEM((total, both), BF16), pltpu.VMEM((total, rows), F32)],
        ),
        compiler_params=params(),
        cost_estimate=cost(2e9 * 8, 30e6),
        name="attend_back",
    )(first, offset, *ins, *slots)
    return got[0], got[1:]


def out_body(low, w_out, part):
    part[...] = mm_t(low[...], w_out[...]).astype(BF16)


def out_project(low, w_out):
    rows, model = low.shape[0], w_out.shape[0]
    return pl.pallas_call(
        out_body,
        out_shape=shape_of((rows, model), BF16),
        compiler_params=params(),
        cost_estimate=cost(2 * rows * model * low.shape[1], 4e6),
        name="out_project",
    )(low, w_out)


def route(mid, gain, router, hot):
    unit, _ = unit_rows(mid)
    low = (unit * gain).astype(BF16)
    chosen = hot > 0.5
    logits = jnp.where(chosen, mm(low, router), NEG)
    up = jnp.where(chosen, jnp.exp(logits - jnp.max(logits, axis=-1, keepdims=True)), 0.0)
    return low, up / jnp.sum(up, axis=-1, keepdims=True)


def middle_body(act, part, other, gain, router, hot, middle, normed, gates):
    mid = act[...].astype(F32) + (part[...].astype(F32) + other[...].astype(F32))
    middle[...] = mid
    normed[...], gates[...] = route(mid, gain[...], router[...], hot[...])


def middle_of(act, part, other, gain, router, hot):
    rows, model = act.shape
    return pl.pallas_call(
        middle_body,
        out_shape=(shape_of((rows, model), F32), shape_of((rows, model), BF16), shape_of((rows, LANES), F32)),
        compiler_params=params(),
        cost_estimate=cost(2 * rows * model * LANES, 12 * rows * model),
        name="middle",
    )(act, part, other, gain, router, hot)


EARLY = 2
FIRST = 1
HALF = 1


def experts_body(early, first, x_own, x_par, dy_own, dy_par, g_own, g_par, w_in, w_out, keep, send, *refs):
    refs = list(refs)
    came, z_kept, z_sent = (refs.pop(0), refs.pop(0), refs.pop(0)) if early else (None, None, None)
    own_back, par_back, own_mix, par_mix, x_turned, dy_order, x_all, dy_all, back, mix, pulls, blocks_of = refs[:12]
    step, steps = pl.program_id(0), pl.num_programs(0)
    rows, model = x_own.shape
    wide = own_back.shape[1] - model
    blocks, depth, _ = blocks_of.shape
    side = lax.axis_index("cp") % 2
    if early:
        leaving, held, spots, es, er, zs, zr = refs[12:]
        p = Place()
        flows = [Flow(p, held.at[i], spots.at[i], zs.at[i], zr.at[i]) for i in range(2)]

    def early_copy(i):
        some = pl.ds(0, blocks // 2 if i < early - 1 else HALF)
        return p.copy("x", leaving.at[i, some], came.at[i, some], es.at[i], er.at[i])

    @pl.when(step == 0)
    def _():
        if early:
            p.greet(("x",))
        x_all[:rows] = x_own[...]
        x_all[rows:] = x_par[...]
        dy_all[:rows] = dy_own[...]
        dy_all[rows:] = dy_par[...]
        for rows_of, ordered in ((x_all, x_turned), (dy_all, dy_order)):
            blocks_of[...] = jnp.transpose(rows_of[...]).reshape(blocks_of.shape)
            for z in range(blocks // 2):
                ordered[z] = blocks_of[2 * z + side]
                ordered[blocks // 2 + z] = blocks_of[2 * z + 1 - side]
        back[...] = jnp.zeros_like(back)
        mix[...] = jnp.zeros_like(mix)
        pulls[...] = jnp.zeros_like(pulls)

    expert = lax.axis_index("ep") * steps + step
    lane = lax.broadcasted_iota(jnp.int32, (2 * rows, wide), 1) == expert
    gate_rows = jnp.concatenate([g_own[...], g_par[...]], axis=0)
    gate = jnp.sum(jnp.where(lane, gate_rows, 0.0), axis=-1, keepdims=True)
    x, dy = x_all[...], dy_all[...]
    w_gu, w_d = w_in[0], w_out[0]
    both = mm(x, w_gu)
    half = both.shape[1] // 2
    g, u = both[:, :half], both[:, half:]
    pull = mm(dy, w_d)
    sig = 1.0 / (1.0 + jnp.exp(-g))
    act = g * sig
    hidden = (act * u).astype(BF16).astype(F32)
    pulls[...] += jnp.where(lane, jnp.sum(hidden * pull, axis=-1, keepdims=True), 0.0)
    weighted = (gate * hidden).astype(BF16)
    pull = gate * pull
    d_g = (pull * u * sig * (1.0 + g * (1.0 - sig))).astype(BF16)
    d_u = (pull * act).astype(BF16)
    d_gu = jnp.concatenate([d_g, d_u], axis=1)
    for i, out in enumerate((keep, send)):
        at = pl.ds(i * (blocks // 2), blocks // 2)
        shape = (model // 2, 2 * rows)
        to = (blocks // 2, depth, -1)
        out[0, :, :, : 2 * half] = mm(x_turned[at].reshape(shape), d_gu).astype(BF16).reshape(to)
        out[0, :, :, 2 * half :] = mm(dy_order[at].reshape(shape), weighted).astype(BF16).reshape(to)
    if early:

        @pl.when(step == 0)
        def _():
            held[0] = keep[0]
            held[1] = send[0]
            for flow in flows:
                flow.open()

        for i in range(early):

            @pl.when(step == first + i)
            def _(i=i):
                leaving[i] = send[0]
                early_copy(i).start()

        for at, work in (
            (2, [lambda: flows[0].second(0)]),
            (3, [lambda: flows[0].second(1)]),
            (4, [flows[0].third]),
            (5, [lambda: flows[1].second(0)]),
            (6, [lambda: flows[1].second(1), flows[1].third]),
        ):

            @pl.when(step == at)
            def _(work=work):
                for one in work:
                    one()

    back[...] += mm_t(d_gu, w_gu)
    mix[...] += mm_t(weighted, w_d)

    @pl.when(step == steps - 1)
    def _():
        own_back[:, :model] = back[:rows].astype(BF16)
        par_back[:, :model] = back[rows:].astype(BF16)
        own_back[:, model:] = pulls[:rows].astype(BF16)
        par_back[:, model:] = pulls[rows:].astype(BF16)
        own_mix[...] = mix[:rows].astype(BF16)
        par_mix[...] = mix[rows:].astype(BF16)
        if early:
            for flow, out in zip(flows, (z_kept, z_sent)):

                def finish(parts, out=out):
                    out[...] = total_of(parts).astype(out.dtype)

                flow.close(finish)
                flow.drain()
            for i in range(early):
                early_copy(i).wait()


def experts(early, first, blocks, x_own, x_par, dy_own, dy_par, g_own, g_par, w_in, w_out):
    rows, model = x_own.shape
    count, _, half = w_out.shape
    depth = model // blocks
    once = lambda shape: pl.BlockSpec(shape, lambda e: (0,) * len(shape))
    whole = (blocks // 2, depth, 3 * half)
    ins = [x_own, x_par, dy_own, dy_par, g_own, g_par]
    apart = first + max(early - 1, 0)
    tail = [shape_of((rows, model + LANES), BF16)] * 2 + [shape_of((rows, model), BF16)] * 2
    outs = [shape_of((count - first,) + whole, BF16), shape_of((count - apart,) + whole, BF16)]
    specs = [
        pl.BlockSpec((1,) + whole, lambda e: (jnp.maximum(e - first, 0), 0, 0, 0)),
        pl.BlockSpec((1,) + whole, lambda e: (jnp.maximum(e - apart, 0), 0, 0, 0)),
    ]
    turned = (blocks, depth, 2 * rows)
    scratch = [
        pltpu.VMEM(turned, BF16),
        pltpu.VMEM(turned, BF16),
        pltpu.VMEM((2 * rows, model), BF16),
        pltpu.VMEM((2 * rows, model), BF16),
        pltpu.VMEM((2 * rows, model), F32),
        pltpu.VMEM((2 * rows, model), F32),
        pltpu.VMEM((2 * rows, LANES), F32),
        pltpu.VMEM(turned, BF16),
    ]
    kind = params()
    if early:
        dma = pltpu.SemaphoreType.DMA
        sums = [shape_of(whole[1:], F32), shape_of(whole[1:], BF16)]
        outs += [shape_of((early,) + whole, BF16)] + sums
        specs += [pl.BlockSpec(memory_space=pl.ANY)] + [once(t.shape) for t in sums]
        scratch += [
            pltpu.VMEM((early,) + whole, BF16),
            pltpu.VMEM((2,) + whole, BF16),
            pltpu.VMEM((2, 5) + whole[1:], BF16),
            dma((early,)),
            dma((early,)),
            dma((2, 6)),
            dma((2, 6)),
        ]
        kind = params(collective_id=2, has_side_effects=True)
    got = pl.pallas_call(
        functools.partial(experts_body, early, first),
        out_shape=tuple(outs + tail),
        grid=(count,),
        in_specs=[once(a.shape) for a in ins]
        + [
            pl.BlockSpec((1, model, 2 * half), lambda e: (e, 0, 0)),
            pl.BlockSpec((1, model, half), lambda e: (e, 0, 0)),
        ],
        out_specs=tuple(specs + [once(t.shape) for t in tail]),
        scratch_shapes=scratch,
        compiler_params=kind,
        cost_estimate=cost(count * 18 * 2 * rows * model * half, count * 12 * model * half),
        name="experts",
    )(*ins, w_in, w_out)
    return got[: len(outs)], got[len(outs) :]


def middle_back_body(mine, other, middle, dy, gates, router, gain, w_out, normed, grad, low, heads, small):
    model = middle.shape[1]
    total = mine[...].astype(F32) + other[...].astype(F32)
    gate, pulls = gates[...], total[:, model:]
    chosen = gate * (pulls - jnp.sum(gate * pulls, axis=-1, keepdims=True))
    high, rest = two_parts(chosen)
    grad_two = total[:, :model] + (mm_t(high, router[...]) + mm_t(rest, router[...]))
    unit, scale = unit_rows(middle[...])
    small[:LANES, :] = t_mm(high, normed[...]) + t_mm(rest, normed[...])
    small[LANES : LANES + 8, :] = jnp.broadcast_to(jnp.sum(grad_two * unit, axis=0, keepdims=True), (8, model))
    scaled = grad_two * gain[...]
    out = dy[...].astype(F32) + scale * (scaled - unit * jnp.mean(scaled * unit, axis=-1, keepdims=True))
    grad[...] = out
    rounded = out.astype(BF16)
    low[...] = rounded
    heads[...] = mm(rounded, w_out[...]).astype(BF16)


def middle_back(mine, other, middle, dy, gates, router, gain, w_out, normed):
    rows, model = middle.shape
    return pl.pallas_call(
        middle_back_body,
        out_shape=(
            shape_of((rows, model), F32),
            shape_of((rows, model), BF16),
            shape_of((rows, w_out.shape[1]), BF16),
            shape_of((LANES + 8, model), F32),
        ),
        compiler_params=params(),
        cost_estimate=cost(2 * rows * model * (w_out.shape[1] + 4 * LANES), 10e6),
        name="middle_back",
    )(mine, other, middle, dy, gates, router, gain, w_out, normed)


def project_back_body(width, act, dq, a, b, c, cosine, sine, wq, wk, wv, part, dkv, gain_row):
    total = a[...].astype(F32) + b[...].astype(F32) + c[...].astype(F32)
    dk = rope_back(total[:, :width], widen(cosine[...], width), widen(sine[...], width)).astype(BF16)
    dv = total[:, width:].astype(BF16)
    dkv[:, :width] = dk
    dkv[:, width:] = dv
    full = mm_t(dq[...], wq[...]) + mm_t(dk, wk[...]) + mm_t(dv, wv[...])
    part[...] = full.astype(BF16)
    unit, _ = unit_rows(act[...].astype(F32))
    gain_row[...] = jnp.broadcast_to(jnp.sum(full * unit, axis=0, keepdims=True), gain_row.shape)


def project_back(act, dq, a, b, c, cosine, sine, wq, wk, wv):
    rows, model = act.shape
    width = wk.shape[1]
    return pl.pallas_call(
        functools.partial(project_back_body, width),
        out_shape=(
            shape_of((rows, model), BF16),
            shape_of((rows, 2 * width), BF16),
            shape_of((8, model), F32),
        ),
        compiler_params=params(),
        cost_estimate=cost(2 * rows * model * (wq.shape[1] + 2 * width), 8e6),
        name="project_back",
    )(act, dq, a, b, c, cosine, sine, wq, wk, wv)


def input_body(act, grad, mine, other, gain, out):
    unit, scale = unit_rows(act[...].astype(F32))
    scaled = (mine[...].astype(F32) + other[...].astype(F32)) * gain[...]
    out[...] = grad[...] + scale * (scaled - unit * jnp.mean(scaled * unit, axis=-1, keepdims=True))


def input_of(act, grad, mine, other, gain):
    return pl.pallas_call(
        input_body,
        out_shape=shape_of(act.shape, F32),
        compiler_params=params(),
        cost_estimate=cost(0, 12 * act.shape[0] * act.shape[1]),
        name="input_grad",
    )(act, grad, mine, other, gain)


def weights_body(blocks, count, stacked, where_ref, *refs):
    lefts = refs[:count]
    rights = refs[count : 2 * count]
    extra = refs[2 * count : -3]
    keep, send, whole = refs[-3:]
    parts = [t_mm(a[...], b[...]).astype(BF16) for a, b in zip(lefts, rights)]
    parts += [jnp.transpose(e[...]).astype(BF16) for e in extra]
    at = down = 0
    for part in parts:
        block = part.reshape(2 * blocks, -1, part.shape[1])
        whole[:, down : down + block.shape[1], at : at + part.shape[1]] = block
        if stacked:
            down += block.shape[1]
        else:
            at += part.shape[1]
    mine, side = where_ref[0], where_ref[1]
    for half, ref in ((mine, keep), (1 - mine, send)):
        for z in range(blocks // 2):
            ref[0, z] = whole[half * blocks + 2 * z + side]
            ref[1, z] = whole[half * blocks + 2 * z + 1 - side]


def weights(where, blocks, pairs, extra=(), stacked=False):
    model = pairs[0][0].shape[1]
    rows = pairs[0][0].shape[0]
    depth = model // (2 * blocks)
    columns = sum(b.shape[1] for _, b in pairs) + sum(e.shape[0] for e in extra)
    tall, wide = (depth * len(pairs), pairs[0][1].shape[1]) if stacked else (depth, columns)
    shape = (2, blocks // 2, tall, wide)
    ins = [a for a, _ in pairs] + [b for _, b in pairs] + list(extra)
    full = lambda a: pl.BlockSpec(a.shape, lambda i, *_: (0,) * len(a.shape))
    return pl.pallas_call(
        functools.partial(weights_body, blocks, len(pairs), stacked),
        out_shape=(shape_of(shape, BF16),) * 2,
        grid_spec=pltpu.PrefetchScalarGridSpec(
            num_scalar_prefetch=1,
            grid=(1,),
            in_specs=[full(a) for a in ins],
            out_specs=(pl.BlockSpec(shape, lambda i, *_: (0, 0, 0, 0)),) * 2,
            scratch_shapes=[pltpu.VMEM((2 * blocks, tall, wide), BF16)],
        ),
        compiler_params=params(),
        cost_estimate=cost(2 * rows * model * columns, 4 * model * columns),
        name="weights",
    )(where, *ins)


def swap(v, axis):
    size = lax.axis_size(axis)
    return lax.ppermute(v, axis, [(i, i ^ 1) for i in range(size)])


def up(v, low, high):
    return lax.ppermute(v, "cp", [(2 * z + s, 2 * z + 2 + s) for z in range(low, high) for s in range(2)])


def down(v, low, high):
    return lax.ppermute(v, "cp", [(2 * z + s, 2 * z - 2 + s) for z in range(low, high) for s in range(2)])


def total_of(terms):
    return functools.reduce(lambda a, b: a + b, [t.astype(F32) for t in terms])


def line_sum(parts, z, length):
    def own(d):
        return [lax.dynamic_index_in_dim(p, jnp.clip(d, 0, length - 1), 0, keepdims=False) for p in parts]

    if length > 4:
        mine = total_of(parts).astype(BF16)
        side = lax.axis_index("cp") % 2
        full = jnp.where(jnp.arange(2).reshape((1, 2) + (1,) * (mine.ndim - 1)) == side, mine[:, None], 0)
        full = full.reshape((2 * length,) + mine.shape[1:])
        return lax.psum_scatter(full, "cp", scatter_dimension=0, tiled=True)[0].astype(F32)
    right = left = None
    for k in range(length - 1):
        far = length - 1 - k
        terms = own(z + far) + ([] if right is None else [right])
        right = up(total_of(terms).astype(BF16), 0, k + 1)
        terms = own(z - far) + ([] if left is None else [left])
        left = down(total_of(terms).astype(BF16), far, length)
    return total_of(own(z) + ([right, left] if length > 1 else []))


LINE = 4
RING = 6


def add_to(ref, at, other):
    ref[at] = (ref[at].astype(F32) + other.astype(F32)).astype(BF16)


class Place:
    def __init__(self):
        self.cp = lax.axis_index("cp")
        self.z, self.side = self.cp // 2, self.cp % 2
        self.ep, self.tp = lax.axis_index("ep"), lax.axis_index("tp")

    def to(self, way):
        if way == "x":
            return {"cp": self.cp + 1 - 2 * self.side}
        if way == "up":
            return {"cp": self.cp + 2}
        if way == "down":
            return {"cp": self.cp - 2}
        return {way: 1 - (self.ep if way == "ep" else self.tp)}

    def signal(self, sem, way):
        pl.semaphore_signal(sem, inc=1, device_id=self.to(way), device_id_type=MESH)

    def signal_line(self, to_down, to_up):
        @pl.when(self.z > 0)
        def _():
            self.signal(to_down, "down")

        @pl.when(self.z < LINE - 1)
        def _():
            self.signal(to_up, "up")

    def greet(self, ways):
        barrier = pltpu.get_barrier_semaphore()
        for way in ways:
            self.signal(barrier, way)
        self.signal_line(barrier, barrier)
        both = jnp.where(self.z > 0, 1, 0) + jnp.where(self.z < LINE - 1, 1, 0)
        pl.semaphore_wait(barrier, len(ways) + both)

    def copy(self, way, src, dst, send, recv):
        return pltpu.make_async_remote_copy(
            src_ref=src, dst_ref=dst, send_sem=send, recv_sem=recv, device_id=self.to(way), device_id_type=MESH
        )

    def at(self, z):
        return pl.when(self.z == z)


LEFT_SPOT = (3, 4, 0)


class Flow:
    def __init__(self, place, held, spots, send, recv, credit=None):
        self.p, self.held, self.spots, self.send, self.recv, self.credit = place, held, spots, send, recv, credit

    def right(self, d):
        return self.p.copy("up", self.held.at[d], self.spots.at[d - 1], self.send.at[d - 1], self.recv.at[d - 1])

    def left(self, d):
        spot = LEFT_SPOT[d]
        return self.p.copy("down", self.held.at[d], self.spots.at[spot], self.send.at[d + 3], self.recv.at[d + 3])

    def allowed(self, way):
        if self.credit is not None:
            pl.semaphore_wait(self.credit[way], 1)

    def open(self):
        @self.p.at(0)
        def _():
            self.allowed("up")
            for d in (3, 2, 1):
                self.right(d).start()

        @self.p.at(3)
        def _():
            self.allowed("down")
            for d in (0, 1, 2):
                self.left(d).start()

    def pass_right(self, d):
        self.right(d).wait_recv()
        add_to(self.held, d, self.spots[d - 1])
        self.right(d).start()

    def pass_left(self, d):
        self.left(d).wait_recv()
        add_to(self.held, d, self.spots[LEFT_SPOT[d]])
        self.left(d).start()

    def second(self, only=None):
        @self.p.at(1)
        def _():
            if only != 1:
                self.allowed("up")
                self.pass_right(3)
            if only != 0:
                self.pass_right(2)

        @self.p.at(2)
        def _():
            if only != 1:
                self.allowed("down")
                self.pass_left(0)
            if only != 0:
                self.pass_left(1)

    def third(self):
        @self.p.at(2)
        def _():
            self.allowed("up")
            self.pass_right(3)

        @self.p.at(1)
        def _():
            self.allowed("down")
            self.pass_left(0)

    def close(self, finish):
        for z in range(LINE):

            @self.p.at(z)
            def _(z=z):
                blocks = [self.held[z]]
                if z > 0:
                    self.right(z).wait_recv()
                    blocks.append(self.spots[z - 1])
                if z < LINE - 1:
                    self.left(z).wait_recv()
                    blocks.append(self.spots[LEFT_SPOT[z]])
                finish(blocks)

    def drain(self):
        for z in range(LINE):

            @self.p.at(z)
            def _(z=z):
                for d in range(z + 1, LINE):
                    self.right(d).wait_send()
                for d in range(z):
                    self.left(d).wait_send()


class BackIns(NamedTuple):
    own_back: Any
    par_back: Any
    own_mix: Any
    par_mix: Any
    middle: Any
    dy: Any
    router: Any
    w_out: Any
    x2: Any
    q: Any
    attended: Any
    act: Any
    normed: Any
    low: Any
    wq: Any
    wk: Any
    wv: Any
    gates: Any
    gain_two: Any
    gain_one: Any
    place: Any
    lse: Any
    cosine: Any
    sine: Any


BACK_IN_PLACE = 7
class BackOuts(NamedTuple):
    grad: Any
    mix: Any
    experts: Any
    big_out: Any
    little_out: Any


class BackScratch(NamedTuple):
    back: Any
    other_ep: Any
    other_tp: Any
    mid_dy: Any
    mid_x2: Any
    wide_w: Any
    branch: Any
    heads: Any
    small: Any
    qs: Any
    atts: Any
    slots: Any
    kv_x: Any
    kv_z: Any
    keys: Any
    bias: Any
    dq: Any
    lows: Any
    wks: Any
    wvs: Any
    routers: Any
    dkv: Any
    part: Any
    part_in: Any
    mix_ep: Any
    mix_tp: Any
    held: Any
    spots: Any
    kept: Any
    staged: Any
    zero_in: Any
    whole: Any
    came: Any
    lit: Any
    lit_came: Any
    lit_x: Any
    lit_spots: Any
    ls: Any
    ks: Any
    xs: Any
    xr: Any
    zs: Any
    zr: Any
    es: Any
    er: Any
    ts: Any
    tr: Any
    kxs: Any
    kxr: Any
    kzs: Any
    kzr: Any
    os: Any
    free_x: Any
    free_up: Any
    free_down: Any


def back_body(group, *refs):
    n_in = len(BackIns._fields) + 6
    ins = BackIns(*refs[: len(BackIns._fields)])
    slots_in = refs[n_in - 6]
    keeps, sends, arrived, z_kept, z_sent = refs[n_in - 5 : n_in]
    o = BackOuts(*refs[n_in : n_in + len(BackOuts._fields)])
    s = BackScratch(*refs[n_in + len(BackOuts._fields) :])
    p = Place()
    early = arrived.shape[0]
    first = FIRST
    count = first + keeps.shape[0]
    seqs, rows, _ = ins.q.shape
    model = ins.middle.shape[1]
    width = ins.wk.shape[1]
    part_of = lambda i: pl.ds(i * rows if isinstance(i, int) else pl.multiple_of(i * rows, rows), rows)

    whole_early = early - 1
    ring = [("here", e) for e in range(first, first + whole_early)] + [("half", first + whole_early)]
    ring += [("x", e) for e in range(first + early, count)] + [("big", 0), ("big", 1)]
    index_of = {item: i for i, item in enumerate(ring)}
    crosses = lambda item: item[0] != "here"

    short = model // 16

    def big_part_of(ref, i):
        return ref.at[i % RING, :, pl.ds(0, short)]

    def big_rows(item):
        return pl.ds(item[1] * short, short)

    def flow(item):
        if item == "little":
            return Flow(p, s.lit_x, s.lit_spots, s.zs.at[len(ring)], s.zr.at[len(ring)])
        i = index_of[item]
        credit = {"up": s.free_up, "down": s.free_down} if i >= RING else None
        if item[0] == "big":
            return Flow(p, big_part_of(s.held, i), big_part_of(s.spots, i), s.zs.at[i], s.zr.at[i], credit)
        return Flow(p, s.held.at[i % RING], s.spots.at[i % RING], s.zs.at[i], s.zr.at[i], credit)

    def x_copy(item):
        if item == "little":
            return p.copy("x", s.lit.at[p.ep, :, 1 - p.side], s.lit_x, s.xs.at[len(ring)], s.xr.at[len(ring)])
        i = index_of[item]
        if item[0] == "half":
            some = pl.ds(HALF, LINE - HALF)
            return p.copy("x", sends.at[0, some], s.held.at[i, some], s.xs.at[i], s.xr.at[i])
        if item[0] == "big":
            src = s.whole.at[p.ep, :, 1 - p.side, big_rows(item)]
            return p.copy("x", src, big_part_of(s.held, i), s.xs.at[i], s.xr.at[i])
        src = sends.at[item[1] - first - whole_early]
        return p.copy("x", src, s.held.at[i % RING], s.xs.at[i], s.xr.at[i])

    def cross(item):
        if item != "little" and index_of[item] >= RING:
            pl.semaphore_wait(s.free_x, 1)
        x_copy(item).start()

    def load_keep(e):
        return pltpu.make_async_copy(keeps.at[e - first], s.kept, s.ks.at[0])

    def load_arrived(e):
        if e == first + whole_early:
            some = pl.ds(0, HALF)
            return pltpu.make_async_copy(
                arrived.at[e - first, some], s.held.at[e - first, some], s.ks.at[1 + e - first]
            )
        return pltpu.make_async_copy(arrived.at[e - first], s.held.at[e - first], s.ks.at[1 + e - first])

    def opened(item):
        if item == "little":
            x_copy(item).wait_recv()
            for d in range(LINE):
                add_to(s.lit_x, d, s.lit[p.ep, d, p.side])
        else:
            held = s.held.at[index_of[item] % RING]
            if item[0] in ("here", "half"):
                load_arrived(item[1]).wait()
            if item[0] != "here":
                x_copy(item).wait_recv()
            if item[0] == "big":
                for d in range(LINE):
                    add_to(big_part_of(s.held, index_of[item]), d, s.whole[p.ep, d, p.side, big_rows(item)])
            else:
                load_keep(item[1]).wait()
                for d in range(LINE):
                    add_to(held, d, s.kept[d])
                if item[1] + 1 < count:
                    load_keep(item[1] + 1).start()
        flow(item).open()

    stored = []

    def store(e):
        return pltpu.make_async_copy(s.staged.at[e % 2], o.experts.at[e], s.os.at[e])

    def finish_expert(e, make):
        if len(stored) >= 2 and e % 2 in [k % 2 for k in stored[-2:]]:
            last = [k for k in stored if k % 2 == e % 2][-1]
            store(last).wait()
            waited.add(last)
        make()
        store(e).start()
        stored.append(e)

    waited = set()

    def closed(item):
        if item == "little":
            def finish(blocks):
                o.little_out[...] = total_of(blocks)

            flow(item).close(finish)
        elif item[0] == "big":
            def finish(blocks):
                o.big_out[big_rows(item)] = total_of(blocks)

            flow(item).close(finish)
        else:
            def finish(blocks):
                s.staged[item[1] % 2] = total_of(blocks)

            finish_expert(item[1], lambda: flow(item).close(finish))

    def freed(item):
        flow(item).drain()
        if item == "little":
            return
        after = index_of[item] + RING
        if after < len(ring):
            if crosses(item):
                x_copy(item).wait_send()
            if crosses(ring[after]):
                p.signal(s.free_x, "x")
            p.signal_line(s.free_up, s.free_down)

    loads = {}

    def load(name, src, dst):
        copy = pltpu.make_async_copy(src, dst, s.ls.at[len(loads)])
        copy.start()
        loads[name] = copy

    def got(*names):
        for name in names:
            loads[name].wait()

    load("back", ins.own_back, s.back)
    load_keep(first).start()
    for e in range(first, first + early):
        load_arrived(e).start()
    load("zero", z_kept, s.staged.at[0])
    load("grad", ins.middle, o.grad)
    load("dy", ins.dy, s.mid_dy)
    load("router", ins.router, s.routers)
    load("x2", ins.x2, s.mid_x2)
    load("w_out", ins.w_out, s.wide_w)
    load("mix", ins.own_mix, o.mix)
    load("q", ins.q, s.qs)
    load("attended", ins.attended, s.atts)
    load("slots", slots_in, s.slots)
    load("low", ins.low, s.lows)
    load("wk", ins.wk, s.wks)
    load("wv", ins.wv, s.wvs)

    p.greet(("x", "ep", "tp"))
    ep_back = p.copy("ep", ins.par_back, s.other_ep, s.es.at[0], s.er.at[0])
    ep_back.start()
    ep_mix = p.copy("ep", ins.par_mix, s.mix_ep, s.es.at[1], s.er.at[1])
    ep_mix.start()
    queue = ring[whole_early:] + ["little"]
    zero_copy = p.copy("x", z_sent, s.zero_in, s.xs.at[len(ring) + 1], s.xr.at[len(ring) + 1])
    zero_copy.start()
    for _ in range(3):
        cross(queue.pop(0))

    got("back")
    ep_back.wait_recv()
    for i in range(seqs):
        s.back[part_of(i)] = (
            s.back[part_of(i)].astype(F32) + s.other_ep[part_of(i)].astype(F32)
        ).astype(BF16)
    tp_back = p.copy("tp", s.back, s.other_tp, s.ts.at[0], s.tr.at[0])
    tp_back.start()
    got("mix")
    ep_mix.wait_recv()
    for i in range(seqs):
        o.mix[part_of(i)] = (o.mix[part_of(i)].astype(F32) + s.mix_ep[part_of(i)].astype(F32)).astype(BF16)

    def step_middle():
        got("grad", "dy", "router", "x2", "w_out")
        tp_back.wait_recv()
        s.small[...] = jnp.zeros_like(s.small)

        @pl.loop(0, seqs)
        def _(i):
            at = pl.ds(pl.multiple_of(i * rows, rows), rows)
            total = s.back[at].astype(F32) + s.other_tp[at].astype(F32)
            gate, pulls = ins.gates[at], total[:, model:]
            chosen = gate * (pulls - jnp.sum(gate * pulls, axis=-1, keepdims=True))
            high, rest = two_parts(chosen)
            grad_two = total[:, :model] + (mm_t(high, s.routers[...]) + mm_t(rest, s.routers[...]))
            unit, scale = unit_rows(o.grad[at])
            s.small[...] += t_mm(high, s.mid_x2[at]) + t_mm(rest, s.mid_x2[at])
            s.small[LANES - 1 :, :] += jnp.sum(grad_two * unit, axis=0, keepdims=True)
            scaled = grad_two * ins.gain_two[...]
            out = s.mid_dy[at].astype(F32) + scale * (
                scaled - unit * jnp.mean(scaled * unit, axis=-1, keepdims=True)
            )
            o.grad[at] = out
            rounded = out.astype(BF16)
            s.branch[at] = rounded
            s.heads[at] = mm(rounded, s.wide_w[...]).astype(BF16)

        load("wq", ins.wq, s.wide_w)
        load("act", ins.act, s.mid_dy)
        load("normed", ins.normed, s.mid_x2)

    tp_mix = p.copy("tp", o.mix, s.mix_tp, s.ts.at[1], s.tr.at[1])

    def step_attend():
        got("q", "attended", "slots")
        homes = [(p.z - r, side) for r in range(LINE) for side in (p.side, 1 - p.side)]
        firsts = [jnp.where(a >= 0, (2 * a + b) * rows, 2**24) for a, b in homes]

        @pl.loop(0, seqs)
        def _(i):
            at = pl.ds(pl.multiple_of(i * rows, rows), rows)

            def keep_grad(j, value):
                s.slots[i, j // 2, j % 2] = value

            s.dq[i] = attend_back_core(
                group,
                s.qs[i],
                ins.place[i],
                s.heads[at],
                s.atts[i],
                ins.lse.at[i],
                ins.cosine[at],
                ins.sine[at],
                [s.slots.at[i, j // 2, j % 2] for j in range(2 * LINE)],
                firsts,
                p.cp * rows,
                s.keys,
                s.bias,
                keep_grad,
                512,
            )

            @p.at(LINE - 1)
            def _():
                for r in range(LINE - 1, 0, -1):
                    kv_down(i, r).start()

    def kv_cross(i):
        return p.copy("x", s.slots.at[i, 0, 1], s.kv_x.at[i], s.kxs.at[i], s.kxr.at[i])

    def kv_down(i, r):
        return p.copy("down", s.slots.at[i, r], s.kv_z.at[i, r - 1], s.kzs.at[i, r - 1], s.kzr.at[i, r - 1])

    def kv_take(i, r):
        kv_down(i, r + 1).wait_recv()
        for way in range(2):
            s.slots[i, r, way] = (s.slots[i, r, way].astype(F32) + s.kv_z[i, r, way].astype(F32)).astype(BF16)

    def keys_pass(i, z):
        @p.at(z)
        def _():
            for r in range(z, 0, -1):
                kv_take(i, r)
                kv_down(i, r).start()

    def keys_cross(i):
        @pl.when(p.z < LINE - 1)
        def _():
            kv_take(i, 0)

        kv_cross(i).start()

    def keys_close(i):
        kv_cross(i).wait_recv()
        s.slots[i, 0, 0] = (s.slots[i, 0, 0].astype(F32) + s.kv_x[i].astype(F32)).astype(BF16)

    def part_copy(i):
        return p.copy("tp", s.part.at[part_of(i)], s.part_in.at[part_of(i)], s.ts.at[2 + i], s.tr.at[2 + i])

    def step_project(i):
        if i == 0:
            got("wq", "wk", "wv", "act", "normed")
        at = part_of(i)
        total = s.slots[i, 0, 0].astype(F32)
        dk = rope_back(total[:, :width], widen(ins.cosine[at], width), widen(ins.sine[at], width)).astype(BF16)
        dv = total[:, width:].astype(BF16)
        s.dkv[at, :width] = dk
        s.dkv[at, width:] = dv
        full = mm_t(s.dq[i], s.wide_w[...]) + mm_t(dk, s.wks[...]) + mm_t(dv, s.wvs[...])
        s.part[at] = full.astype(BF16)
        part_copy(i).start()

    tall = model // 4

    def pieces(make, keep):
        @pl.loop(0, 4)
        def _(piece):
            got_piece = make(pl.ds(pl.multiple_of(piece * tall, tall), tall)).astype(BF16)
            block = got_piece.reshape(4, short, got_piece.shape[1])
            for b in range(4):
                keep(piece // 2, 2 * (piece % 2) + b // 2, b % 2, block[b])

    def big_part(row):
        def keep(half, z, side, value):
            s.whole[half, z, side, row : row + value.shape[0], :] = value

        return keep

    def little_part(column):
        def keep(half, z, side, value):
            s.lit[half, z, side, :, column : column + value.shape[1]] = value

        return keep

    ep_big = p.copy("ep", s.whole.at[1 - p.ep], s.came, s.es.at[2], s.er.at[2])
    ep_lit = p.copy("ep", s.lit.at[1 - p.ep], s.lit_came, s.es.at[3], s.er.at[3])

    def step_out_weight():
        got("low")
        pieces(lambda at: t_mm(s.branch[:, at], s.lows[...]), big_part(0))

    def step_query_weight():
        got("normed")
        loads["normed"] = Done()
        query = jnp.concatenate([s.dq[i] for i in range(seqs)], axis=0)
        pieces(lambda at: t_mm(s.mid_x2[:, at], query), big_part(short))
        ep_big.start()

    def step_key_weight():
        pieces(lambda at: t_mm(s.mid_x2[:, at], s.dkv[...]), little_part(0))
        pieces(lambda at: jnp.transpose(s.small[:, at]), little_part(2 * width))
        ep_lit.start()

    def step_big_cores():
        ep_big.wait_recv()
        for d in range(LINE):
            for side in range(2):
                s.whole[p.ep, d, side] = (
                    s.whole[p.ep, d, side].astype(F32) + s.came[d, side].astype(F32)
                ).astype(BF16)

    def step_little_cores():
        ep_lit.wait_recv()
        for d in range(LINE):
            for side in range(2):
                s.lit[p.ep, d, side] = (
                    s.lit[p.ep, d, side].astype(F32) + s.lit_came[d, side].astype(F32)
                ).astype(BF16)

    def step_input():
        for i in range(seqs):
            at = part_of(i)
            part_copy(i).wait_recv()
            unit, scale = unit_rows(s.mid_dy[at].astype(F32))
            whole = s.part[at].astype(F32) + s.part_in[at].astype(F32)
            gain_row = jnp.sum(whole * unit, axis=0, keepdims=True)
            if i == 0:
                s.small[LANES - 2 : LANES - 1, :] = gain_row
            else:
                s.small[LANES - 2 : LANES - 1, :] += gain_row
            scaled = whole * ins.gain_one[...]
            o.grad[at] = o.grad[at] + scale * (scaled - unit * jnp.mean(scaled * unit, axis=-1, keepdims=True))

    def step_mix():
        tp_mix.wait_recv()
        tp_mix.wait_send()
        for i in range(seqs):
            o.mix[part_of(i)] = (o.mix[part_of(i)].astype(F32) + s.mix_tp[part_of(i)].astype(F32)).astype(BF16)

    line = list(ring) + ["little"]
    stage = {item: 0 for item in line}

    def advance(at, to):
        if not 0 <= at < len(line):
            return
        item = line[at]
        while stage[item] < to:
            now = stage[item]
            if now == 0:
                opened(item)
            elif now == 1:
                flow(item).second()
            elif now == 2:
                flow(item).third()
            elif now == 3:
                closed(item)
            elif now == 4:
                freed(item)
            stage[item] = now + 1

    def turn(at):
        for back in (4, 3, 2, 1, 0):
            advance(at - back, back + 1)

    def add_zero():
        got("zero")
        zero_copy.wait_recv()
        s.staged[0] = s.staged[0] + s.zero_in[...].astype(F32)

    tp_mix.start()
    turn(0)
    finish_expert(0, add_zero)
    turn(1)
    step_middle()
    advance(0, 3)
    advance(1, 2)
    step_attend()
    cross(queue.pop(0))
    step_out_weight()
    step_query_weight()
    turn(2)
    keys_pass(0, 2)
    advance(0, 4)
    advance(1, 3)
    keys_pass(1, 2)
    advance(2, 2)
    step_big_cores()
    step_mix()
    keys_pass(0, 1)
    keys_pass(1, 1)
    turn(3)
    keys_cross(0)
    keys_cross(1)
    cross(queue.pop(0))
    turn(4)
    cross(queue.pop(0))
    keys_close(0)
    step_project(0)
    keys_close(1)
    step_project(1)
    advance(2, 4)
    advance(3, 3)
    advance(4, 2)
    step_input()
    step_key_weight()
    turn(5)
    cross(queue.pop(0))
    step_little_cores()
    for at in range(6, len(line) + 4):
        turn(at)
        if queue:
            cross(queue.pop(0))
    for e in stored:
        if e not in waited:
            store(e).wait()
    for item in line:
        if item == "little" or (crosses(item) and index_of[item] + RING >= len(ring)):
            x_copy(item).wait_send()
    for i in range(seqs):
        kv_cross(i).wait_send()
        part_copy(i).wait_send()
        for z in range(1, LINE):

            @p.at(z)
            def _(z=z):
                for r in range(z, 0, -1):
                    kv_down(i, r).wait_send()

    tp_back.wait_send()
    zero_copy.wait_send()
    for copy in (ep_back, ep_mix, ep_big, ep_lit):
        copy.wait_send()


class Done:
    def wait(self):
        return None


def back_and_sums(ins, slots, chunks, group):
    keeps, _, arrived, *_ = chunks
    _, length, depth, wide = keeps.shape
    early, count = arrived.shape[0], FIRST + keeps.shape[0]
    block = (length, depth, wide)
    v = BackIns(*ins)
    rows, model = v.middle.shape
    seqs, each, heads = v.q.shape
    width = v.wk.shape[1]
    both = 2 * width
    small = (length, 2, model // 16, both + LANES)
    n_ring = count - FIRST + 2
    anywhere = pl.BlockSpec(memory_space=pl.ANY)
    inside = pl.BlockSpec(memory_space=pltpu.VMEM)
    dma, vm = pltpu.SemaphoreType.DMA, pltpu.VMEM
    flag = pltpu.SemaphoreType.REGULAR
    scratch = dict(
        back=vm((rows, model + LANES), BF16),
        other_ep=vm((rows, model + LANES), BF16),
        other_tp=vm((rows, model + LANES), BF16),
        mid_dy=vm((rows, model), BF16),
        mid_x2=vm((rows, model), BF16),
        wide_w=vm((model, heads), BF16),
        branch=vm((rows, model), BF16),
        heads=vm((rows, heads), BF16),
        small=vm((LANES, model), F32),
        qs=vm((seqs, each, heads), BF16),
        atts=vm((seqs, each, heads), F32),
        slots=vm((seqs, LINE, 2, each, both), BF16),
        kv_x=vm((seqs, each, both), BF16),
        kv_z=vm((seqs, LINE - 1, 2, each, both), BF16),
        keys=vm((2 * LINE * each, both), BF16),
        bias=vm((2 * LINE * each, each), F32),
        dq=vm((seqs, each, heads), BF16),
        lows=vm((rows, heads), BF16),
        wks=vm((model, width), BF16),
        wvs=vm((model, width), BF16),
        routers=vm((model, LANES), BF16),
        dkv=vm((rows, both), BF16),
        part=vm((rows, model), BF16),
        part_in=vm((rows, model), BF16),
        mix_ep=vm((rows, model), BF16),
        mix_tp=vm((rows, model), BF16),
        held=vm((RING,) + block, BF16),
        spots=vm((RING, 5, depth, wide), BF16),
        kept=vm(block, BF16),
        staged=vm((2, depth, wide), F32),
        zero_in=vm((depth, wide), BF16),
        whole=vm((2, length, 2, depth, wide), BF16),
        came=vm((length, 2, depth, wide), BF16),
        lit=vm((2,) + small, BF16),
        lit_came=vm(small, BF16),
        lit_x=vm((small[0],) + small[2:], BF16),
        lit_spots=vm((5,) + small[2:], BF16),
        ls=dma((28,)),
        ks=dma((1 + early,)),
        xs=dma((n_ring + 2,)),
        xr=dma((n_ring + 2,)),
        zs=dma((n_ring + 1, 6)),
        zr=dma((n_ring + 1, 6)),
        es=dma((4,)),
        er=dma((4,)),
        ts=dma((4,)),
        tr=dma((4,)),
        kxs=dma((2,)),
        kxr=dma((2,)),
        kzs=dma((2, 3)),
        kzr=dma((2, 3)),
        os=dma((count,)),
        free_x=flag,
        free_up=flag,
        free_down=flag,
    )
    return pl.pallas_call(
        functools.partial(back_body, group),
        out_shape=(
            shape_of((rows, model), F32),
            shape_of((rows, model), BF16),
            shape_of((count, depth, wide), F32),
            shape_of((depth, wide), F32),
            shape_of(small[2:], F32),
        ),
        in_specs=[anywhere] * (len(BackIns._fields) - BACK_IN_PLACE)
        + [inside] * BACK_IN_PLACE
        + [anywhere] * 6,
        out_specs=(inside, inside, anywhere, inside, inside),
        scratch_shapes=[scratch[name] for name in BackScratch._fields],
        compiler_params=pltpu.CompilerParams(
            collective_id=1, has_side_effects=True, vmem_limit_bytes=67_043_328
        ),
        name="back_and_sums",
    )(*ins, slots, *chunks)


def results_body(middle, mix, grad, chunk, big, little, out, grad_in, first, second, keys, values, small, both, down):
    out[...] = middle[...] + mix[...].astype(F32)
    grad_in[...] = grad[...]
    half = down.shape[2]
    both[0] = chunk[0, :, : 2 * half].reshape(both.shape[1:])
    down[0] = chunk[0, :, 2 * half :]

    @pl.when(pl.program_id(0) == 0)
    def _():
        tall, width = first.shape[0], keys.shape[1]
        first[...] = big[:tall]
        second[...] = big[tall:]
        keys[...] = little[:, :width]
        values[...] = little[:, width : 2 * width]
        small[...] = little[:, 2 * width :]


def results(middle, mix, grad, chunks, big, little, half):
    rows, model = middle.shape
    count, depth, wide = chunks.shape
    tall, width = big.shape[0] // 2, (little.shape[1] - LANES) // 2
    part = pl.BlockSpec((rows // count, model), lambda e: (e, 0))
    once = lambda shape: pl.BlockSpec(shape, lambda e: (0,) * len(shape))
    whole = [(tall, big.shape[1])] * 2 + [(tall, width)] * 2 + [(tall, LANES)]
    return pl.pallas_call(
        results_body,
        grid=(count,),
        out_shape=[shape_of((rows, model), F32)] * 2
        + [shape_of(shape, F32) for shape in whole]
        + [shape_of((count, depth, 2, half), F32), shape_of((count, depth, half), F32)],
        in_specs=[part] * 3
        + [pl.BlockSpec((1, depth, wide), lambda e: (e, 0, 0)), once(big.shape), once(little.shape)],
        out_specs=[part] * 2
        + [once(shape) for shape in whole]
        + [
            pl.BlockSpec((1, depth, 2, half), lambda e: (e, 0, 0, 0)),
            pl.BlockSpec((1, depth, half), lambda e: (e, 0, 0)),
        ],
        compiler_params=params(),
        name="results",
    )(middle, mix, grad, chunks, big, little)


class FrontIns(NamedTuple):
    q: Any
    kv: Any
    act: Any
    hot: Any
    router: Any
    gain: Any
    place: Any
    w_out: Any
    dy: Any
    w_in: Any


class FrontOuts(NamedTuple):
    slots: Any
    low: Any
    attended: Any
    lse: Any
    middle: Any
    normed: Any
    gates: Any
    x_par: Any
    g_par: Any
    dy_par: Any
    w_flat: Any


class FrontScratch(NamedTuple):
    keys: Any
    bias: Any
    wo: Any
    part: Any
    part_in: Any
    raw: Any
    flat: Any
    ws: Any
    wi: Any
    wf: Any
    us: Any
    ur: Any
    xs: Any
    xr: Any
    ts: Any
    tr: Any
    es: Any
    er: Any


def front_body(group, *refs):
    n_in, n_out = len(FrontIns._fields), len(FrontOuts._fields)
    ins = FrontIns(*refs[:n_in])
    o = FrontOuts(*refs[n_in : n_in + n_out])
    s = FrontScratch(*refs[n_in + n_out :])
    p = Place()
    seqs, rows, _ = ins.q.shape
    experts_here = ins.w_in.shape[0]
    part_of = lambda i: pl.ds(i * rows if isinstance(i, int) else pl.multiple_of(i * rows, rows), rows)

    def fetch(e):
        return pltpu.make_async_copy(ins.w_in.at[e], s.raw.at[e % 2], s.wi.at[e % 2])

    def put(e):
        return pltpu.make_async_copy(s.flat.at[e % 2], o.w_flat.at[e], s.wf.at[e % 2])

    done = []

    def fill(count):
        for _ in range(count):
            e = len(done)
            if e >= experts_here:
                return
            fetch(e).wait()
            if e >= 2:
                put(e - 2).wait()
            slot, cut = e % 2, s.flat.shape[1] // 4

            @pl.loop(0, 4)
            def _(k):
                at = pl.ds(pl.multiple_of(k * cut, cut), cut)
                s.flat[slot, at] = s.raw[slot, at].reshape(cut, s.flat.shape[2])

            put(e).start()
            if e + 2 < experts_here:
                fetch(e + 2).start()
            done.append(e)

    def source(i, r):
        return ins.kv.at[i] if r == 0 else o.slots.at[i, r, 0]

    def up_copy(i, r):
        return p.copy("up", source(i, r), o.slots.at[i, r + 1, 0], s.us.at[i, r], s.ur.at[i, r])

    def x_copy(i, r):
        return p.copy("x", source(i, r), o.slots.at[i, r, 1], s.xs.at[i, r], s.xr.at[i, r])

    def tp_copy(i):
        return p.copy("tp", s.part.at[part_of(i)], s.part_in.at[part_of(i)], s.ts.at[i], s.tr.at[i])

    def ep_copies(i):
        at = part_of(i)
        return (
            p.copy("ep", o.normed.at[at], o.x_par.at[at], s.es.at[2 * i], s.er.at[2 * i]),
            p.copy("ep", o.gates.at[at], o.g_par.at[at], s.es.at[2 * i + 1], s.er.at[2 * i + 1]),
        )

    fetch(0).start()
    fetch(1).start()
    wo_load = pltpu.make_async_copy(ins.w_out, s.wo, s.ws.at[0])
    wo_load.start()
    p.greet(("x", "ep", "tp"))
    for i in range(seqs):

        @pl.when(p.z < LINE - 1)
        def _(i=i):
            up_copy(i, 0).start()

        x_copy(i, 0).start()
    dy_copy = p.copy("ep", ins.dy, o.dy_par, s.es.at[2 * seqs], s.er.at[2 * seqs])
    dy_copy.start()
    for i in range(seqs):
        o.slots[i, 0, 0] = ins.kv[i]
        for r in range(1, LINE):

            @pl.when(p.z < r)
            def _(i=i, r=r):
                o.slots[i, r] = jnp.zeros(o.slots.shape[2:], BF16)

    fill(1)
    for r in range(1, LINE):
        for i in range(seqs):
            for z in range(r, LINE):

                @p.at(z)
                def _(i=i, r=r, z=z):
                    up_copy(i, r - 1).wait_recv()
                    if z < LINE - 1:
                        up_copy(i, r).start()
                    x_copy(i, r).start()

        fill(1)
    homes = [(p.z - r, side) for r in range(LINE) for side in (p.side, 1 - p.side)]
    firsts = [jnp.where(a >= 0, (2 * a + b) * rows, 2**24) for a, b in homes]
    wo_load.wait()

    @pl.loop(0, seqs)
    def _(i):
        for r in range(LINE):

            @pl.when(p.z >= r)
            def _(r=r):
                x_copy(i, r).wait_recv()

        whole = attend_core(
            group,
            ins.q[i],
            ins.place[i],
            [o.slots.at[i, j // 2, j % 2] for j in range(2 * LINE)],
            firsts,
            p.cp * rows,
            s.keys,
            s.bias,
            o.lse.at[i],
            KEY_CHUNK,
        )
        o.attended[i] = whole
        o.low[i] = whole.astype(BF16)
        s.part[part_of(i)] = mm_t(o.low[i], s.wo[...]).astype(BF16)
        tp_copy(i).start()

    fill(1)
    for i in range(seqs):
        at = part_of(i)
        tp_copy(i).wait_recv()
        mid = ins.act[at].astype(F32) + (s.part[at].astype(F32) + s.part_in[at].astype(F32))
        o.middle[at] = mid
        o.normed[at], o.gates[at] = route(mid, ins.gain[...], ins.router[...], ins.hot[at])
        for copy in ep_copies(i):
            copy.start()
        fill(3 if i == 0 else experts_here)
    for i in range(seqs):
        for copy in ep_copies(i):
            copy.wait()
        tp_copy(i).wait_send()
        for r in range(LINE):

            @pl.when(p.z >= r)
            def _(i=i, r=r):
                x_copy(i, r).wait_send()
                if r < LINE - 1:

                    @pl.when(p.z < LINE - 1)
                    def _():
                        up_copy(i, r).wait_send()

    dy_copy.wait()
    for e in done[-2:]:
        put(e).wait()


def front(ins, group):
    v = FrontIns(*ins)
    seqs, each, heads = v.q.shape
    both = v.kv.shape[-1]
    rows, model = v.act.shape
    local, _, _, half = v.w_in.shape
    anywhere = pl.BlockSpec(memory_space=pl.ANY)
    inside = pl.BlockSpec(memory_space=pltpu.VMEM)
    dma, vm = pltpu.SemaphoreType.DMA, pltpu.VMEM
    scratch = dict(
        keys=vm((2 * LINE * each, both), BF16),
        bias=vm((2 * LINE * each, each), F32),
        wo=vm(v.w_out.shape, BF16),
        part=vm((rows, model), BF16),
        part_in=vm((rows, model), BF16),
        raw=vm((2, model, 2, half), BF16),
        flat=vm((2, model, 2 * half), BF16),
        ws=dma((1,)),
        wi=dma((2,)),
        wf=dma((2,)),
        us=dma((seqs, LINE - 1)),
        ur=dma((seqs, LINE - 1)),
        xs=dma((seqs, LINE)),
        xr=dma((seqs, LINE)),
        ts=dma((seqs,)),
        tr=dma((seqs,)),
        es=dma((2 * seqs + 1,)),
        er=dma((2 * seqs + 1,)),
    )
    return pl.pallas_call(
        functools.partial(front_body, group),
        out_shape=(
            shape_of((seqs, LINE, 2, each, both), BF16),
            shape_of((seqs, each, heads), BF16),
            shape_of((seqs, each, heads), F32),
            shape_of((seqs, heads // HEAD // group, group * each), F32),
            shape_of((rows, model), F32),
            shape_of((rows, model), BF16),
            shape_of((rows, LANES), F32),
            shape_of((rows, model), BF16),
            shape_of((rows, LANES), F32),
            shape_of((rows, model), BF16),
            shape_of((local, model, 2 * half), BF16),
        ),
        in_specs=[inside] * 7 + [anywhere] * 3,
        out_specs=(inside,) * 7 + (anywhere,) * 4,
        scratch_shapes=[scratch[name] for name in FrontScratch._fields],
        compiler_params=params(collective_id=3, has_side_effects=True),
        name="front",
    )(*ins)


def on_device(
    activations,
    cotangent,
    positions,
    routes,
    w_query,
    w_key,
    value_weight,
    w_out,
    gain_attn,
    gain_moe,
    w_router,
    w_gate_up,
    w_down,
):
    seqs, rows, model = activations.shape
    total = seqs * rows
    width = w_key.shape[1]
    group = w_query.shape[1] // width
    expert_count = w_router.shape[1]
    local = w_gate_up.shape[0]
    half = w_down.shape[2]
    blocks = lax.axis_size("cp")
    length = blocks // 2
    here = lax.axis_index("cp")
    z, side = here // 2, here % 2
    mine = lax.axis_index("ep")
    act = activations.reshape(total, model)
    dy = cotangent.reshape(total, model)
    gain_one, gain_two = gain_attn.reshape(1, model), gain_moe.reshape(1, model)

    frequency = jnp.power(10000.0, -(jnp.arange(HEAD // 2, dtype=F32) * 2.0 / HEAD))
    angles = positions.reshape(total, 1).astype(F32) * jnp.tile(frequency, 2 * LANES // HEAD)
    cosine, sine = jnp.cos(angles), jnp.sin(angles)

    normed, q, kv = project(act, gain_one, w_query, w_key, value_weight, cosine, sine)
    q = q.reshape(seqs, rows, -1)
    place = positions.reshape(seqs, 1, rows)
    lanes = jnp.arange(LANES, dtype=jnp.int32)
    hot = jnp.sum((routes.reshape(total, -1, 1) == lanes).astype(F32), axis=1)
    router = jnp.pad(w_router, ((0, 0), (0, LANES - expert_count)))
    if length == LINE:
        kv = kv.reshape(seqs, rows, 2 * width)
        ins = (q, kv, act, hot, router, gain_two, place, w_out, dy, w_gate_up)
        slots, low, attended, lse, middle, normed_two, gates, x_par, gates_par, dy_par, w_in = front(ins, group)
        low = low.reshape(total, -1)
    else:
        kv = kv.reshape(1, seqs, rows, 2 * width)
        offset = (here * rows).astype(jnp.int32).reshape(1)
        slots = [lax.all_gather(kv, "cp", axis=0, tiled=True)]
        first = jnp.arange(blocks, dtype=jnp.int32) * rows
        dy_par = swap(dy, "ep")
        low, attended, lse = attend(q, place, slots, first, offset, group)
        low = low.reshape(total, -1)
        part = out_project(low, w_out)
        w_in = w_gate_up.reshape(local, model, 2 * half)
        middle, normed_two, gates = middle_of(act, part, swap(part, "tp"), gain_two, router, hot)
        x_par, gates_par = swap(normed_two, "ep"), swap(gates, "ep")

    early, apart = (EARLY, FIRST) if length == LINE else (0, 0)
    args = (normed_two, x_par, dy, dy_par, gates, gates_par, w_in, w_down)
    chunks, (own_back, par_back, own_mix, par_mix) = experts(early, apart, blocks, *args)
    if length == LINE:
        ins = (
            own_back, par_back, own_mix, par_mix, middle, dy, router, w_out, normed_two, q, attended, act, normed,
            low, w_query, w_key, value_weight, gates, gain_two, gain_one, place, lse, cosine, sine,
        )
        input_grad, mix, expert_grad, big, little = back_and_sums(ins, slots, chunks, group)
        output, input_grad, *plain, small, gate_up_grad, down_grad = results(
            middle, mix, input_grad, expert_grad, big, little, half
        )
        out_grad, query_grad, key_grad, value_grad = plain
        small_grads = small[:, LANES - 2], small[:, LANES - 1], small[:, :expert_count]
    else:
        back = total_of([own_back, swap(par_back, "ep")]).astype(BF16)
        grad_middle, branch, grad_heads, small = middle_back(
            back, swap(back, "tp"), middle, dy, gates, router, gain_two, w_out, normed_two
        )
        seq_cosine, seq_sine = cosine.reshape(seqs, rows, -1), sine.reshape(seqs, rows, -1)
        dq, grads = attend_back(
            q, place, grad_heads.reshape(q.shape), attended, lse, seq_cosine, seq_sine, slots, first, offset, group
        )
        dq = dq.reshape(total, -1)
        kv_sum = lax.psum_scatter(grads[0], "cp", scatter_dimension=0, tiled=True)
        kv_terms = [kv_sum, jnp.zeros_like(kv_sum), jnp.zeros_like(kv_sum)]
        kv_terms = [t.reshape(total, 2 * width) for t in kv_terms]
        spots = jnp.stack([mine, side]).astype(jnp.int32)
        big = weights(spots, blocks, [(branch, low), (normed, dq)], stacked=True)
        normed_part, dkv, gain_row = project_back(act, dq, *kv_terms, cosine, sine, w_query, w_key, value_weight)
        small = jnp.concatenate([small[:expert_count], small[LANES : LANES + 1], gain_row[:1]], axis=0)
        small = jnp.pad(small, ((0, LANES - small.shape[0]), (0, 0)))
        little = weights(spots, blocks, [(normed, dkv)], (small,))
        input_grad = input_of(act, grad_middle, normed_part, swap(normed_part, "tp"), gain_one)
        mix = total_of([own_mix, swap(par_mix, "ep")]).astype(BF16)
        output = middle + total_of([mix, swap(mix, "tp")])

        def spread_sum(keep, send):
            both = total_of([keep, swap(send, "ep")]).astype(BF16)
            return line_sum([both[0], swap(both[1], "cp")], z, length)

        turned = [jnp.swapaxes(v, 0, 1) for v in (chunks[0], swap(chunks[1], "cp"))]
        expert_grad = line_sum(turned, z, length)
        big, little = spread_sum(*big), spread_sum(*little)
        gate_up_grad = expert_grad[:, :, : 2 * half].reshape(local, -1, 2, half)
        down_grad = expert_grad[:, :, 2 * half :]
        tall = big.shape[0] // 2
        out_grad, query_grad = big[:tall], big[tall:]
        key_grad, value_grad = little[:, :width], little[:, width : 2 * width]
        small = little[:, 2 * width :]
        gain_part = small[:, expert_count + 1]
        small_grads = gain_part + swap(gain_part, "tp"), small[:, expert_count], small[:, :expert_count]
    return (
        output.reshape(activations.shape),
        input_grad.reshape(activations.shape),
        query_grad,
        key_grad,
        value_grad,
        out_grad,
        *small_grads,
        gate_up_grad,
        down_grad,
    )


def solution(mesh):
    in_specs = (
        P("ep", "cp", None),
        P("ep", "cp", None),
        P("ep", "cp"),
        P("ep", "cp", None),
        P(None, "tp"),
        P(None, "tp"),
        P(None, "tp"),
        P(None, "tp"),
        P(),
        P(),
        P(),
        P("ep", None, None, "tp"),
        P("ep", None, "tp"),
    )
    out_specs = (
        P("ep", "cp", None),
        P("ep", "cp", None),
        P(("ep", "cp"), "tp"),
        P(("ep", "cp"), "tp"),
        P(("ep", "cp"), "tp"),
        P(("ep", "cp"), "tp"),
        P(("ep", "cp")),
        P(("ep", "cp")),
        P(("ep", "cp"), None),
        P("ep", "cp", None, "tp"),
        P("ep", "cp", "tp"),
    )
    return jax.shard_map(
        on_device, mesh=mesh, in_specs=in_specs, out_specs=out_specs, check_vma=False
    )
```

```python
import functools
from typing import Any, NamedTuple

import jax
import jax.numpy as jnp
from jax import lax
from jax.experimental import pallas as pl
from jax.experimental.pallas import tpu as pltpu
from jax.sharding import PartitionSpec as P

HEAD = 64
EPS = 1e-06
NEG = -1e30
SCALE = 0.125
LANES = 128
KEY_CHUNK = 1024
F32 = jnp.float32
BF16 = jnp.bfloat16
MESH = pl.DeviceIdType.MESH


def mm(a, b):
    return lax.dot_general(a, b, (((1,), (0,)), ((), ())), preferred_element_type=F32)


def mm_t(a, b):
    return lax.dot_general(a, b, (((1,), (1,)), ((), ())), preferred_element_type=F32)


def t_mm(a, b):
    return lax.dot_general(a, b, (((0,), (0,)), ((), ())), preferred_element_type=F32)


def two_parts(v):
    high = v.astype(BF16)
    return high, (v - high.astype(F32)).astype(BF16)


def halves_turned(v, back):
    width = v.shape[1]
    ahead = pltpu.roll(v, width - HEAD // 2, 1)
    behind = pltpu.roll(v, HEAD // 2, 1)
    first = lax.broadcasted_iota(jnp.int32, v.shape, 1) % HEAD < HEAD // 2
    if back:
        return jnp.where(first, ahead, -behind)
    return jnp.where(first, -ahead, behind)


def rope(v, cosine, sine):
    return v * cosine + halves_turned(v, False) * sine


def rope_back(v, cosine, sine):
    return v * cosine + halves_turned(v * sine, True)


def widen(table, width):
    return jnp.concatenate([table] * (width // table.shape[1]), axis=1)


def unit_rows(v):
    scale = lax.rsqrt(jnp.mean(v * v, axis=-1, keepdims=True) + EPS)
    return v * scale, scale


def shape_of(shape, dtype):
    return jax.ShapeDtypeStruct(shape, dtype)


def params(**kw):
    return pltpu.CompilerParams(vmem_limit_bytes=60 * 2**20, **kw)


def cost(flops, moved):
    return pl.CostEstimate(flops=int(flops), bytes_accessed=int(moved), transcendentals=0)


def project_body(act, gain, wq, wk, wv, cosine, sine, normed, q, kv):
    unit, _ = unit_rows(act[...].astype(F32))
    low = (unit * gain[...]).astype(BF16)
    normed[...] = low
    qf = mm(low, wq[...])
    q[...] = rope(qf, widen(cosine[...], qf.shape[1]), widen(sine[...], qf.shape[1])).astype(BF16)
    kf = mm(low, wk[...])
    width = kf.shape[1]
    kv[:, :width] = rope(kf, widen(cosine[...], width), widen(sine[...], width)).astype(BF16)
    kv[:, width:] = mm(low, wv[...]).astype(BF16)


def project(act, gain, wq, wk, wv, cosine, sine):
    rows, model = act.shape
    total = wq.shape[1] + 2 * wk.shape[1]
    return pl.pallas_call(
        project_body,
        out_shape=(
            shape_of((rows, model), BF16),
            shape_of((rows, wq.shape[1]), BF16),
            shape_of((rows, 2 * wk.shape[1]), BF16),
        ),
        compiler_params=params(),
        cost_estimate=cost(2 * rows * model * total, 2 * model * total + 6 * rows * model),
        name="project",
    )(act, gain, wq, wk, wv, cosine, sine)


def fill_keys(firsts, offset, place, slots, keys, bias, rows):
    query = lax.broadcasted_iota(jnp.int32, (rows, rows), 1) + offset
    for at, slot in enumerate(slots):
        keys[at * rows : (at + 1) * rows, :] = slot[...]
        key = lax.broadcasted_iota(jnp.int32, (rows, rows), 0) + firsts[at]
        distance = query - key
        seen = (distance >= 0) & (distance <= place)
        bias[at * rows : (at + 1) * rows, :] = jnp.where(seen, 0.0, NEG)


def single_slots(slots):
    return [slot.at[one, 0] for slot in slots for one in range(slot.shape[0])]


def group_rows(block, head, group):
    return jnp.concatenate(
        [block[:, (head * group + g) * HEAD : (head * group + g + 1) * HEAD] for g in range(group)], axis=0
    )


def pair_lanes(pair, width, start=0):
    return pl.ds(pl.multiple_of(start + pair * width, LANES), width)


def attend_core(group, q_ref, place, slots, firsts, offset, keys, bias, lse_ref, most, out_ref, low_ref):
    rows = q_ref.shape[0]
    fill_keys(firsts, offset, place, slots, keys, bias, rows)
    total, width = keys.shape[0], keys.shape[1] // 2
    chunk = min(total, most)
    two, many = 2 * HEAD, 2 * HEAD * group

    @pl.loop(0, width // two)
    def _(pair):
        q = (q_ref[:, pair_lanes(pair, many)].astype(F32) * SCALE).astype(BF16)
        pieces = []
        for head in range(2):
            mine = slice(head * HEAD, (head + 1) * HEAD)
            q3 = group_rows(q, head, group)
            top = run = out = None
            for low in range(0, total, chunk):
                k = keys[low : low + chunk, pair_lanes(pair, two)][:, mine]
                v = keys[low : low + chunk, pair_lanes(pair, two, width)][:, mine]
                s = mm_t(k, q3) + widen(bias[low : low + chunk, :], group * rows)
                here = jnp.max(s, axis=0, keepdims=True)
                new = here if top is None else jnp.maximum(top, here)
                p = jnp.exp(s - new)
                part = jnp.sum(p, axis=0, keepdims=True)
                o = t_mm(v, p.astype(BF16))
                if top is None:
                    run, out = part, o
                else:
                    shrink = jnp.exp(top - new)
                    run, out = run * shrink + part, out * shrink + o
                top = new
            out = jnp.transpose(out / run)
            pieces += [out[g * rows : (g + 1) * rows] for g in range(group)]
            lse_ref[pl.ds(2 * pair + head, 1), :] = top + jnp.log(run)
        whole = jnp.concatenate(pieces, axis=1)
        out_ref[:, pair_lanes(pair, many)] = whole
        low_ref[:, pair_lanes(pair, many)] = whole.astype(BF16)


def attend_body(group, count, first_ref, offset_ref, q_ref, place_ref, *refs):
    slots = single_slots(refs[:count])
    low_ref, out_ref, lse_ref, keys, bias = refs[count:]
    firsts = [first_ref[i] for i in range(len(slots))]
    attend_core(
        group,
        q_ref.at[0],
        place_ref[0],
        slots,
        firsts,
        offset_ref[0],
        keys,
        bias,
        lse_ref.at[0],
        KEY_CHUNK,
        out_ref.at[0],
        low_ref.at[0],
    )


def seq_block(shape):
    return pl.BlockSpec((1,) + shape[1:], lambda s, *_: (s,) + (0,) * (len(shape) - 1))


def slot_block(shape):
    return pl.BlockSpec((shape[0], 1) + shape[2:], lambda s, *_: (0, s, 0, 0))


def attend(q, place, slots, first, offset, group):
    seqs, rows, wide = q.shape
    both = slots[0].shape[-1]
    total = rows * sum(slot.shape[0] for slot in slots)
    heads = wide // HEAD // group
    outs = (
        shape_of(q.shape, BF16),
        shape_of(q.shape, F32),
        shape_of((seqs, heads, group * rows), F32),
    )
    return pl.pallas_call(
        functools.partial(attend_body, group, len(slots)),
        out_shape=outs,
        grid_spec=pltpu.PrefetchScalarGridSpec(
            num_scalar_prefetch=2,
            grid=(seqs,),
            in_specs=[seq_block(q.shape), seq_block(place.shape)] + [slot_block(s.shape) for s in slots],
            out_specs=tuple(seq_block(o.shape) for o in outs),
            scratch_shapes=[pltpu.VMEM((total, both), BF16), pltpu.VMEM((total, rows), F32)],
        ),
        compiler_params=params(),
        cost_estimate=cost(2e9 * 4, 20e6),
        name="attend",
    )(first, offset, q, place, *slots)


def attend_back_core(
    group, q_ref, place, go_ref, out_ref, lse_ref, cosine, sine, slots, firsts, offset, keys, bias, grads, dq_ref, most
):
    rows = q_ref.shape[0]
    fill_keys(firsts, offset, place, slots, keys, bias, rows)
    total, width = keys.shape[0], keys.shape[1] // 2
    chunk = min(total, most)
    two, many = 2 * HEAD, 2 * HEAD * group

    @pl.loop(0, width // two)
    def _(pair):
        here = pair_lanes(pair, many)
        q = (q_ref[:, here].astype(F32) * SCALE).astype(BF16)
        go = go_ref[:, here]
        products = go.astype(F32) * out_ref[:, here]
        ones = jnp.ones((8, HEAD), F32)
        q3s = [group_rows(q, head, group) for head in range(2)]
        g3s = [group_rows(go, head, group) for head in range(2)]
        deltas = [
            lax.dot_general(
                ones,
                group_rows(products, head, group),
                (((1,), (1,)), ((), ())),
                preferred_element_type=F32,
                precision=lax.Precision.HIGHEST,
            )[:1]
            for head in range(2)
        ]
        dq = [None] * 2
        for low in range(0, total, chunk):
            dks, dvs = [], []
            for head in range(2):
                mine = slice(head * HEAD, (head + 1) * HEAD)
                k = keys[low : low + chunk, pair_lanes(pair, two)][:, mine]
                v = keys[low : low + chunk, pair_lanes(pair, two, width)][:, mine]
                s = mm_t(k, q3s[head]) + widen(bias[low : low + chunk, :], group * rows)
                p = jnp.exp(s - lse_ref[pl.ds(2 * pair + head, 1), :])
                dp = mm_t(v, g3s[head])
                ds = (p * (dp - deltas[head])).astype(BF16)
                dks.append(mm(ds, q3s[head]))
                dvs.append(mm(p.astype(BF16), g3s[head]))
                part = t_mm(k, ds)
                dq[head] = part if dq[head] is None else dq[head] + part
            for made, start in ((dks, 0), (dvs, width)):
                both = jnp.concatenate(made, axis=1).astype(BF16)
                for one in range(chunk // rows):
                    grad = grads[low // rows + one]
                    grad[:, pair_lanes(pair, two, start)] = both[one * rows : (one + 1) * rows]
        pieces = []
        for head in range(2):
            back = jnp.transpose(dq[head] * SCALE)
            pieces += [back[g * rows : (g + 1) * rows] for g in range(group)]
        whole = jnp.concatenate(pieces, axis=1)
        dq_ref[:, here] = rope_back(whole, widen(cosine, many), widen(sine, many)).astype(BF16)


def attend_back_body(
    group, count, first_ref, offset_ref, q_ref, place_ref, grad_ref, out_ref, lse_ref, cos_ref, sin_ref, *refs
):
    slots = single_slots(refs[:count])
    dq_ref = refs[count]
    grads = single_slots(refs[count + 1 : 2 * count + 1])
    keys, bias = refs[2 * count + 1 :]

    attend_back_core(
        group,
        q_ref.at[0],
        place_ref[0],
        grad_ref.at[0],
        out_ref.at[0],
        lse_ref.at[0],
        cos_ref[0],
        sin_ref[0],
        slots,
        [first_ref[i] for i in range(len(slots))],
        offset_ref[0],
        keys,
        bias,
        grads,
        dq_ref.at[0],
        KEY_CHUNK,
    )


def attend_back(q, place, grad, out, lse, cosine, sine, slots, first, offset, group):
    seqs, rows, _ = q.shape
    both = slots[0].shape[-1]
    total = rows * sum(slot.shape[0] for slot in slots)
    outs = (shape_of(q.shape, BF16),) + tuple(shape_of(s.shape, BF16) for s in slots)
    ins = (q, place, grad, out, lse, cosine, sine)
    got = pl.pallas_call(
        functools.partial(attend_back_body, group, len(slots)),
        out_shape=outs,
        grid_spec=pltpu.PrefetchScalarGridSpec(
            num_scalar_prefetch=2,
            grid=(seqs,),
            in_specs=[seq_block(a.shape) for a in ins] + [slot_block(s.shape) for s in slots],
            out_specs=(seq_block(outs[0].shape),) + tuple(slot_block(s.shape) for s in slots),
            scratch_shapes=[pltpu.VMEM((total, both), BF16), pltpu.VMEM((total, rows), F32)],
        ),
        compiler_params=params(),
        cost_estimate=cost(2e9 * 8, 30e6),
        name="attend_back",
    )(first, offset, *ins, *slots)
    return got[0], got[1:]


def out_body(low, w_out, part):
    part[...] = mm_t(low[...], w_out[...]).astype(BF16)


def out_project(low, w_out):
    rows, model = low.shape[0], w_out.shape[0]
    return pl.pallas_call(
        out_body,
        out_shape=shape_of((rows, model), BF16),
        compiler_params=params(),
        cost_estimate=cost(2 * rows * model * low.shape[1], 4e6),
        name="out_project",
    )(low, w_out)


def route(mid, gain, logits_of, hot):
    unit, _ = unit_rows(mid)
    low = (unit * gain).astype(BF16)
    chosen = hot > 0.5
    logits = jnp.where(chosen, logits_of(low), NEG)
    up = jnp.where(chosen, jnp.exp(logits - jnp.max(logits, axis=-1, keepdims=True)), 0.0)
    return low, up / jnp.sum(up, axis=-1, keepdims=True)


def middle_body(act, part, other, gain, router, hot, middle, normed, gates):
    mid = act[...].astype(F32) + (part[...].astype(F32) + other[...].astype(F32))
    middle[...] = mid
    normed[...], gates[...] = route(mid, gain[...], lambda v: mm(v, router[...]), hot[...])


def middle_of(act, part, other, gain, router, hot):
    rows, model = act.shape
    return pl.pallas_call(
        middle_body,
        out_shape=(shape_of((rows, model), F32), shape_of((rows, model), BF16), shape_of((rows, LANES), F32)),
        compiler_params=params(),
        cost_estimate=cost(2 * rows * model * LANES, 12 * rows * model),
        name="middle",
    )(act, part, other, gain, router, hot)


EARLY = 2
FIRST = 1
HALF = 1


def experts_body(early, first, x_own, x_par, dy_own, dy_par, g_own, g_par, w_in, w_out, keep, send, *refs):
    refs = list(refs)
    came, z_kept, z_sent = (refs.pop(0), refs.pop(0), refs.pop(0)) if early else (None, None, None)
    own_back, par_back, own_mix, par_mix, x_turned, dy_order, x_all, dy_all, back, mix, pulls, blocks_of = refs[:12]
    step, steps = pl.program_id(0), pl.num_programs(0)
    rows, model = x_own.shape
    wide = own_back.shape[1] - model
    blocks, depth, _ = blocks_of.shape
    side = lax.axis_index("cp") % 2
    if early:
        leaving, held, spots, es, er, zs, zr = refs[12:]
        p = Place()
        flows = [Flow(p, held.at[i], spots.at[i], zs.at[i], zr.at[i]) for i in range(2)]

    def early_copy(i):
        some = pl.ds(0, blocks // 2 if i < early - 1 else HALF)
        return p.copy("x", leaving.at[i, some], came.at[i, some], es.at[i], er.at[i])

    @pl.when(step == 0)
    def _():
        if early:
            p.greet(("x",))
        x_all[:rows] = x_own[...]
        x_all[rows:] = x_par[...]
        dy_all[:rows] = dy_own[...]
        dy_all[rows:] = dy_par[...]
        for rows_of, ordered in ((x_all, x_turned), (dy_all, dy_order)):
            blocks_of[...] = jnp.transpose(rows_of[...]).reshape(blocks_of.shape)
            for z in range(blocks // 2):
                ordered[z] = blocks_of[2 * z + side]
                ordered[blocks // 2 + z] = blocks_of[2 * z + 1 - side]
        back[...] = jnp.zeros_like(back)
        mix[...] = jnp.zeros_like(mix)
        pulls[...] = jnp.zeros_like(pulls)

    expert = lax.axis_index("ep") * steps + step
    lane = lax.broadcasted_iota(jnp.int32, (2 * rows, wide), 1) == expert
    gate_rows = jnp.concatenate([g_own[...], g_par[...]], axis=0)
    gate = jnp.sum(jnp.where(lane, gate_rows, 0.0), axis=-1, keepdims=True)
    x, dy = x_all[...], dy_all[...]
    w_gu, w_d = w_in[0], w_out[0]
    both = mm(x, w_gu)
    half = both.shape[1] // 2
    g, u = both[:, :half], both[:, half:]
    pull = mm(dy, w_d)
    sig = 1.0 / (1.0 + jnp.exp(-g))
    act = g * sig
    hidden = (act * u).astype(BF16).astype(F32)
    pulls[...] += jnp.where(lane, jnp.sum(hidden * pull, axis=-1, keepdims=True), 0.0)
    weighted = (gate * hidden).astype(BF16)
    pull = gate * pull
    d_g = (pull * u * sig * (1.0 + g * (1.0 - sig))).astype(BF16)
    d_u = (pull * act).astype(BF16)
    d_gu = jnp.concatenate([d_g, d_u], axis=1)
    for i, out in enumerate((keep, send)):
        at = pl.ds(i * (blocks // 2), blocks // 2)
        shape = (model // 2, 2 * rows)
        to = (blocks // 2, depth, -1)
        out[0, :, :, : 2 * half] = mm(x_turned[at].reshape(shape), d_gu).astype(BF16).reshape(to)
        out[0, :, :, 2 * half :] = mm(dy_order[at].reshape(shape), weighted).astype(BF16).reshape(to)
    if early:

        @pl.when(step == 0)
        def _():
            held[0] = keep[0]
            held[1] = send[0]
            for flow in flows:
                flow.open()

        for i in range(early):

            @pl.when(step == first + i)
            def _(i=i):
                leaving[i] = send[0]
                early_copy(i).start()

        for at, work in (
            (2, [lambda: flows[0].second(0)]),
            (3, [lambda: flows[0].second(1)]),
            (4, [flows[0].third]),
            (5, [lambda: flows[1].second(0)]),
            (6, [lambda: flows[1].second(1), flows[1].third]),
        ):

            @pl.when(step == at)
            def _(work=work):
                for one in work:
                    one()

    back[...] += mm_t(d_gu, w_gu)
    mix[...] += mm_t(weighted, w_d)

    @pl.when(step == steps - 1)
    def _():
        own_back[:, :model] = back[:rows].astype(BF16)
        par_back[:, :model] = back[rows:].astype(BF16)
        own_back[:, model:] = pulls[:rows].astype(BF16)
        par_back[:, model:] = pulls[rows:].astype(BF16)
        own_mix[...] = mix[:rows].astype(BF16)
        par_mix[...] = mix[rows:].astype(BF16)
        if early:
            for flow, out in zip(flows, (z_kept, z_sent)):

                def finish(parts, out=out):
                    sum_into(out, *parts)

                flow.close(finish)
                flow.drain()
            for i in range(early):
                early_copy(i).wait()


def experts(early, first, blocks, x_own, x_par, dy_own, dy_par, g_own, g_par, w_in, w_out):
    rows, model = x_own.shape
    count, _, half = w_out.shape
    depth = model // blocks
    once = lambda shape: pl.BlockSpec(shape, lambda e: (0,) * len(shape))
    whole = (blocks // 2, depth, 3 * half)
    ins = [x_own, x_par, dy_own, dy_par, g_own, g_par]
    apart = first + max(early - 1, 0)
    tail = [shape_of((rows, model + LANES), BF16)] * 2 + [shape_of((rows, model), BF16)] * 2
    outs = [shape_of((count - first,) + whole, BF16), shape_of((count - apart,) + whole, BF16)]
    specs = [
        pl.BlockSpec((1,) + whole, lambda e: (jnp.maximum(e - first, 0), 0, 0, 0)),
        pl.BlockSpec((1,) + whole, lambda e: (jnp.maximum(e - apart, 0), 0, 0, 0)),
    ]
    turned = (blocks, depth, 2 * rows)
    scratch = [
        pltpu.VMEM(turned, BF16),
        pltpu.VMEM(turned, BF16),
        pltpu.VMEM((2 * rows, model), BF16),
        pltpu.VMEM((2 * rows, model), BF16),
        pltpu.VMEM((2 * rows, model), F32),
        pltpu.VMEM((2 * rows, model), F32),
        pltpu.VMEM((2 * rows, LANES), F32),
        pltpu.VMEM(turned, BF16),
    ]
    kind = params()
    if early:
        dma = pltpu.SemaphoreType.DMA
        sums = [shape_of(whole[1:], F32), shape_of(whole[1:], BF16)]
        outs += [shape_of((early,) + whole, BF16)] + sums
        specs += [pl.BlockSpec(memory_space=pl.ANY)] + [once(t.shape) for t in sums]
        scratch += [
            pltpu.VMEM((early,) + whole, BF16),
            pltpu.VMEM((2,) + whole, BF16),
            pltpu.VMEM((2, 5) + whole[1:], BF16),
            dma((early,)),
            dma((early,)),
            dma((2, 6)),
            dma((2, 6)),
        ]
        kind = params(collective_id=2, has_side_effects=True)
    got = pl.pallas_call(
        functools.partial(experts_body, early, first),
        out_shape=tuple(outs + tail),
        grid=(count,),
        in_specs=[once(a.shape) for a in ins]
        + [
            pl.BlockSpec((1, model, 2 * half), lambda e: (e, 0, 0)),
            pl.BlockSpec((1, model, half), lambda e: (e, 0, 0)),
        ],
        out_specs=tuple(specs + [once(t.shape) for t in tail]),
        scratch_shapes=scratch,
        compiler_params=kind,
        cost_estimate=cost(count * 18 * 2 * rows * model * half, count * 12 * model * half),
        name="experts",
    )(*ins, w_in, w_out)
    return got[: len(outs)], got[len(outs) :]


def middle_back_body(mine, other, middle, dy, gates, router, gain, w_out, normed, grad, low, heads, small):
    model = middle.shape[1]
    total = mine[...].astype(F32) + other[...].astype(F32)
    gate, pulls = gates[...], total[:, model:]
    chosen = gate * (pulls - jnp.sum(gate * pulls, axis=-1, keepdims=True))
    high, rest = two_parts(chosen)
    grad_two = total[:, :model] + (mm_t(high, router[...]) + mm_t(rest, router[...]))
    unit, scale = unit_rows(middle[...])
    small[:LANES, :] = t_mm(high, normed[...]) + t_mm(rest, normed[...])
    small[LANES : LANES + 8, :] = jnp.broadcast_to(jnp.sum(grad_two * unit, axis=0, keepdims=True), (8, model))
    scaled = grad_two * gain[...]
    out = dy[...].astype(F32) + scale * (scaled - unit * jnp.mean(scaled * unit, axis=-1, keepdims=True))
    grad[...] = out
    rounded = out.astype(BF16)
    low[...] = rounded
    heads[...] = mm(rounded, w_out[...]).astype(BF16)


def middle_back(mine, other, middle, dy, gates, router, gain, w_out, normed):
    rows, model = middle.shape
    return pl.pallas_call(
        middle_back_body,
        out_shape=(
            shape_of((rows, model), F32),
            shape_of((rows, model), BF16),
            shape_of((rows, w_out.shape[1]), BF16),
            shape_of((LANES + 8, model), F32),
        ),
        compiler_params=params(),
        cost_estimate=cost(2 * rows * model * (w_out.shape[1] + 4 * LANES), 10e6),
        name="middle_back",
    )(mine, other, middle, dy, gates, router, gain, w_out, normed)


def project_back_body(width, act, dq, a, b, c, cosine, sine, wq, wk, wv, part, dkv, gain_row):
    total = a[...].astype(F32) + b[...].astype(F32) + c[...].astype(F32)
    dk = rope_back(total[:, :width], widen(cosine[...], width), widen(sine[...], width)).astype(BF16)
    dv = total[:, width:].astype(BF16)
    dkv[:, :width] = dk
    dkv[:, width:] = dv
    full = mm_t(dq[...], wq[...]) + mm_t(dk, wk[...]) + mm_t(dv, wv[...])
    part[...] = full.astype(BF16)
    unit, _ = unit_rows(act[...].astype(F32))
    gain_row[...] = jnp.broadcast_to(jnp.sum(full * unit, axis=0, keepdims=True), gain_row.shape)


def project_back(act, dq, a, b, c, cosine, sine, wq, wk, wv):
    rows, model = act.shape
    width = wk.shape[1]
    return pl.pallas_call(
        functools.partial(project_back_body, width),
        out_shape=(
            shape_of((rows, model), BF16),
            shape_of((rows, 2 * width), BF16),
            shape_of((8, model), F32),
        ),
        compiler_params=params(),
        cost_estimate=cost(2 * rows * model * (wq.shape[1] + 2 * width), 8e6),
        name="project_back",
    )(act, dq, a, b, c, cosine, sine, wq, wk, wv)


def input_body(act, grad, mine, other, gain, out):
    unit, scale = unit_rows(act[...].astype(F32))
    scaled = (mine[...].astype(F32) + other[...].astype(F32)) * gain[...]
    out[...] = grad[...] + scale * (scaled - unit * jnp.mean(scaled * unit, axis=-1, keepdims=True))


def input_of(act, grad, mine, other, gain):
    return pl.pallas_call(
        input_body,
        out_shape=shape_of(act.shape, F32),
        compiler_params=params(),
        cost_estimate=cost(0, 12 * act.shape[0] * act.shape[1]),
        name="input_grad",
    )(act, grad, mine, other, gain)


def weights_body(blocks, count, stacked, where_ref, *refs):
    lefts = refs[:count]
    rights = refs[count : 2 * count]
    extra = refs[2 * count : -3]
    keep, send, whole = refs[-3:]
    parts = [t_mm(a[...], b[...]).astype(BF16) for a, b in zip(lefts, rights)]
    parts += [jnp.transpose(e[...]).astype(BF16) for e in extra]
    at = down = 0
    for part in parts:
        block = part.reshape(2 * blocks, -1, part.shape[1])
        whole[:, down : down + block.shape[1], at : at + part.shape[1]] = block
        if stacked:
            down += block.shape[1]
        else:
            at += part.shape[1]
    mine, side = where_ref[0], where_ref[1]
    for half, ref in ((mine, keep), (1 - mine, send)):
        for z in range(blocks // 2):
            ref[0, z] = whole[half * blocks + 2 * z + side]
            ref[1, z] = whole[half * blocks + 2 * z + 1 - side]


def weights(where, blocks, pairs, extra=(), stacked=False):
    model = pairs[0][0].shape[1]
    rows = pairs[0][0].shape[0]
    depth = model // (2 * blocks)
    columns = sum(b.shape[1] for _, b in pairs) + sum(e.shape[0] for e in extra)
    tall, wide = (depth * len(pairs), pairs[0][1].shape[1]) if stacked else (depth, columns)
    shape = (2, blocks // 2, tall, wide)
    ins = [a for a, _ in pairs] + [b for _, b in pairs] + list(extra)
    full = lambda a: pl.BlockSpec(a.shape, lambda i, *_: (0,) * len(a.shape))
    return pl.pallas_call(
        functools.partial(weights_body, blocks, len(pairs), stacked),
        out_shape=(shape_of(shape, BF16),) * 2,
        grid_spec=pltpu.PrefetchScalarGridSpec(
            num_scalar_prefetch=1,
            grid=(1,),
            in_specs=[full(a) for a in ins],
            out_specs=(pl.BlockSpec(shape, lambda i, *_: (0, 0, 0, 0)),) * 2,
            scratch_shapes=[pltpu.VMEM((2 * blocks, tall, wide), BF16)],
        ),
        compiler_params=params(),
        cost_estimate=cost(2 * rows * model * columns, 4 * model * columns),
        name="weights",
    )(where, *ins)


def swap(v, axis):
    size = lax.axis_size(axis)
    return lax.ppermute(v, axis, [(i, i ^ 1) for i in range(size)])


def up(v, low, high):
    return lax.ppermute(v, "cp", [(2 * z + s, 2 * z + 2 + s) for z in range(low, high) for s in range(2)])


def down(v, low, high):
    return lax.ppermute(v, "cp", [(2 * z + s, 2 * z - 2 + s) for z in range(low, high) for s in range(2)])


def total_of(terms):
    return functools.reduce(lambda a, b: a + b, [t.astype(F32) for t in terms])


def line_sum(parts, z, length):
    def own(d):
        return [lax.dynamic_index_in_dim(p, jnp.clip(d, 0, length - 1), 0, keepdims=False) for p in parts]

    if length > 4:
        mine = total_of(parts).astype(BF16)
        side = lax.axis_index("cp") % 2
        full = jnp.where(jnp.arange(2).reshape((1, 2) + (1,) * (mine.ndim - 1)) == side, mine[:, None], 0)
        full = full.reshape((2 * length,) + mine.shape[1:])
        return lax.psum_scatter(full, "cp", scatter_dimension=0, tiled=True)[0].astype(F32)
    right = left = None
    for k in range(length - 1):
        far = length - 1 - k
        terms = own(z + far) + ([] if right is None else [right])
        right = up(total_of(terms).astype(BF16), 0, k + 1)
        terms = own(z - far) + ([] if left is None else [left])
        left = down(total_of(terms).astype(BF16), far, length)
    return total_of(own(z) + ([right, left] if length > 1 else []))


LINE = 4
RING = 6


def sum_into(out, *parts):
    few = 48 if out.shape[0] % 48 == 0 else out.shape[0]

    @pl.loop(0, out.shape[0] // few)
    def _(k):
        at = pl.ds(pl.multiple_of(k * few, few), few)
        out[at] = total_of([part[at] for part in parts]).astype(out.dtype)


def add_into(ref, other):
    sum_into(ref, ref, other)


class Place:
    def __init__(self):
        self.cp = lax.axis_index("cp")
        self.z, self.side = self.cp // 2, self.cp % 2
        self.ep, self.tp = lax.axis_index("ep"), lax.axis_index("tp")

    def to(self, way):
        if way == "x":
            return {"cp": self.cp + 1 - 2 * self.side}
        if way == "up":
            return {"cp": self.cp + 2}
        if way == "down":
            return {"cp": self.cp - 2}
        return {way: 1 - (self.ep if way == "ep" else self.tp)}

    def signal(self, sem, way):
        pl.semaphore_signal(sem, inc=1, device_id=self.to(way), device_id_type=MESH)

    def signal_line(self, to_down, to_up):
        @pl.when(self.z > 0)
        def _():
            self.signal(to_down, "down")

        @pl.when(self.z < LINE - 1)
        def _():
            self.signal(to_up, "up")

    def greet(self, ways):
        barrier = pltpu.get_barrier_semaphore()
        for way in ways:
            self.signal(barrier, way)
        self.signal_line(barrier, barrier)
        both = jnp.where(self.z > 0, 1, 0) + jnp.where(self.z < LINE - 1, 1, 0)
        pl.semaphore_wait(barrier, len(ways) + both)

    def copy(self, way, src, dst, send, recv):
        return pltpu.make_async_remote_copy(
            src_ref=src, dst_ref=dst, send_sem=send, recv_sem=recv, device_id=self.to(way), device_id_type=MESH
        )

    def at(self, z):
        return pl.when(self.z == z)


LEFT_SPOT = (3, 4, 0)


class Flow:
    def __init__(self, place, held, spots, send, recv, credit=None):
        self.p, self.held, self.spots, self.send, self.recv, self.credit = place, held, spots, send, recv, credit

    def right(self, d):
        return self.p.copy("up", self.held.at[d], self.spots.at[d - 1], self.send.at[d - 1], self.recv.at[d - 1])

    def left(self, d):
        spot = LEFT_SPOT[d]
        return self.p.copy("down", self.held.at[d], self.spots.at[spot], self.send.at[d + 3], self.recv.at[d + 3])

    def allowed(self, way):
        if self.credit is not None:
            pl.semaphore_wait(self.credit[way], 1)

    def open(self):
        @self.p.at(0)
        def _():
            self.allowed("up")
            for d in (3, 2, 1):
                self.right(d).start()

        @self.p.at(3)
        def _():
            self.allowed("down")
            for d in (0, 1, 2):
                self.left(d).start()

    def pass_right(self, d):
        self.right(d).wait_recv()
        add_into(self.held.at[d], self.spots.at[d - 1])
        self.right(d).start()

    def pass_left(self, d):
        self.left(d).wait_recv()
        add_into(self.held.at[d], self.spots.at[LEFT_SPOT[d]])
        self.left(d).start()

    def second(self, only=None):
        @self.p.at(1)
        def _():
            if only != 1:
                self.allowed("up")
                self.pass_right(3)
            if only != 0:
                self.pass_right(2)

        @self.p.at(2)
        def _():
            if only != 1:
                self.allowed("down")
                self.pass_left(0)
            if only != 0:
                self.pass_left(1)

    def third(self):
        @self.p.at(2)
        def _():
            self.allowed("up")
            self.pass_right(3)

        @self.p.at(1)
        def _():
            self.allowed("down")
            self.pass_left(0)

    def close(self, finish):
        for z in range(LINE):

            @self.p.at(z)
            def _(z=z):
                blocks = [self.held.at[z]]
                if z > 0:
                    self.right(z).wait_recv()
                    blocks.append(self.spots.at[z - 1])
                if z < LINE - 1:
                    self.left(z).wait_recv()
                    blocks.append(self.spots.at[LEFT_SPOT[z]])
                finish(blocks)

    def drain(self):
        for z in range(LINE):

            @self.p.at(z)
            def _(z=z):
                for d in range(z + 1, LINE):
                    self.right(d).wait_send()
                for d in range(z):
                    self.left(d).wait_send()


class BackIns(NamedTuple):
    own_back: Any
    par_back: Any
    own_mix: Any
    par_mix: Any
    middle: Any
    dy: Any
    router: Any
    w_out: Any
    x2: Any
    q: Any
    attended: Any
    act: Any
    normed: Any
    low: Any
    wq: Any
    wk: Any
    wv: Any
    gates: Any
    gain_two: Any
    gain_one: Any
    place: Any
    lse: Any
    cosine: Any
    sine: Any


BACK_IN_PLACE = 7
class BackOuts(NamedTuple):
    grad: Any
    mix: Any
    experts: Any
    big_out: Any
    little_out: Any


class BackScratch(NamedTuple):
    back: Any
    other_ep: Any
    other_tp: Any
    mid_dy: Any
    mid_x2: Any
    wide_w: Any
    branch: Any
    heads: Any
    small: Any
    qs: Any
    atts: Any
    slots: Any
    kv_x: Any
    kv_z: Any
    keys: Any
    bias: Any
    dq: Any
    lows: Any
    wks: Any
    wvs: Any
    routers: Any
    dkv: Any
    part: Any
    part_in: Any
    mix_ep: Any
    mix_tp: Any
    held: Any
    spots: Any
    kept: Any
    staged: Any
    zero_in: Any
    whole: Any
    came: Any
    lit: Any
    lit_came: Any
    lit_x: Any
    lit_spots: Any
    ls: Any
    ks: Any
    xs: Any
    xr: Any
    zs: Any
    zr: Any
    es: Any
    er: Any
    ts: Any
    tr: Any
    kxs: Any
    kxr: Any
    kzs: Any
    kzr: Any
    os: Any
    free_x: Any
    free_up: Any
    free_down: Any


def back_body(group, *refs):
    n_in = len(BackIns._fields) + 6
    ins = BackIns(*refs[: len(BackIns._fields)])
    slots_in = refs[n_in - 6]
    keeps, sends, arrived, z_kept, z_sent = refs[n_in - 5 : n_in]
    o = BackOuts(*refs[n_in : n_in + len(BackOuts._fields)])
    s = BackScratch(*refs[n_in + len(BackOuts._fields) :])
    p = Place()
    early = arrived.shape[0]
    first = FIRST
    count = first + keeps.shape[0]
    seqs, rows, _ = ins.q.shape
    model = ins.middle.shape[1]
    width = ins.wk.shape[1]
    part_of = lambda i: pl.ds(i * rows if isinstance(i, int) else pl.multiple_of(i * rows, rows), rows)

    whole_early = early - 1
    ring = [("here", e) for e in range(first, first + whole_early)] + [("half", first + whole_early)]
    ring += [("x", e) for e in range(first + early, count)] + [("big", 0), ("big", 1)]
    index_of = {item: i for i, item in enumerate(ring)}
    crosses = lambda item: item[0] != "here"

    short = model // 16

    def big_part_of(ref, i):
        return ref.at[i % RING, :, pl.ds(0, short)]

    def big_rows(item):
        return pl.ds(item[1] * short, short)

    def flow(item):
        if item == "little":
            return Flow(p, s.lit_x, s.lit_spots, s.zs.at[len(ring)], s.zr.at[len(ring)])
        i = index_of[item]
        credit = {"up": s.free_up, "down": s.free_down} if i >= RING else None
        if item[0] == "big":
            return Flow(p, big_part_of(s.held, i), big_part_of(s.spots, i), s.zs.at[i], s.zr.at[i], credit)
        return Flow(p, s.held.at[i % RING], s.spots.at[i % RING], s.zs.at[i], s.zr.at[i], credit)

    def x_copy(item):
        if item == "little":
            return p.copy("x", s.lit.at[p.ep, :, 1 - p.side], s.lit_x, s.xs.at[len(ring)], s.xr.at[len(ring)])
        i = index_of[item]
        if item[0] == "half":
            some = pl.ds(HALF, LINE - HALF)
            return p.copy("x", sends.at[0, some], s.held.at[i, some], s.xs.at[i], s.xr.at[i])
        if item[0] == "big":
            src = s.whole.at[p.ep, :, 1 - p.side, big_rows(item)]
            return p.copy("x", src, big_part_of(s.held, i), s.xs.at[i], s.xr.at[i])
        src = sends.at[item[1] - first - whole_early]
        return p.copy("x", src, s.held.at[i % RING], s.xs.at[i], s.xr.at[i])

    def cross(item):
        if item != "little" and index_of[item] >= RING:
            pl.semaphore_wait(s.free_x, 1)
        x_copy(item).start()

    def load_keep(e):
        return pltpu.make_async_copy(keeps.at[e - first], s.kept, s.ks.at[0])

    def load_arrived(e):
        if e == first + whole_early:
            some = pl.ds(0, HALF)
            return pltpu.make_async_copy(
                arrived.at[e - first, some], s.held.at[e - first, some], s.ks.at[1 + e - first]
            )
        return pltpu.make_async_copy(arrived.at[e - first], s.held.at[e - first], s.ks.at[1 + e - first])

    def opened(item):
        if item == "little":
            x_copy(item).wait_recv()
            for d in range(LINE):
                add_into(s.lit_x.at[d], s.lit.at[p.ep, d, p.side])
        else:
            held = s.held.at[index_of[item] % RING]
            if item[0] in ("here", "half"):
                load_arrived(item[1]).wait()
            if item[0] != "here":
                x_copy(item).wait_recv()
            if item[0] == "big":
                for d in range(LINE):
                    add_into(
                        big_part_of(s.held, index_of[item]).at[d], s.whole.at[p.ep, d, p.side, big_rows(item)]
                    )
            else:
                load_keep(item[1]).wait()
                for d in range(LINE):
                    add_into(held.at[d], s.kept.at[d])
                if item[1] + 1 < count:
                    load_keep(item[1] + 1).start()
        flow(item).open()

    stored = []

    def store(e):
        return pltpu.make_async_copy(s.staged.at[e % 2], o.experts.at[e], s.os.at[e])

    def finish_expert(e, make):
        if len(stored) >= 2 and e % 2 in [k % 2 for k in stored[-2:]]:
            last = [k for k in stored if k % 2 == e % 2][-1]
            store(last).wait()
            waited.add(last)
        make()
        store(e).start()
        stored.append(e)

    waited = set()

    def closed(item):
        if item == "little":
            def finish(blocks):
                sum_into(o.little_out, *blocks)

            flow(item).close(finish)
        elif item[0] == "big":
            def finish(blocks):
                sum_into(o.big_out.at[big_rows(item)], *blocks)

            flow(item).close(finish)
        else:
            def finish(blocks):
                sum_into(s.staged.at[item[1] % 2], *blocks)

            finish_expert(item[1], lambda: flow(item).close(finish))

    def freed(item):
        flow(item).drain()
        if item == "little":
            return
        after = index_of[item] + RING
        if after < len(ring):
            if crosses(item):
                x_copy(item).wait_send()
            if crosses(ring[after]):
                p.signal(s.free_x, "x")
            p.signal_line(s.free_up, s.free_down)

    loads = {}

    def load(name, src, dst):
        copy = pltpu.make_async_copy(src, dst, s.ls.at[len(loads)])
        copy.start()
        loads[name] = copy

    def got(*names):
        for name in names:
            loads[name].wait()

    load("back", ins.own_back, s.back)
    load_keep(first).start()
    for e in range(first, first + early):
        load_arrived(e).start()
    load("zero", z_kept, s.staged.at[0])
    load("grad", ins.middle, o.grad)
    load("dy", ins.dy, s.mid_dy)
    load("router", ins.router, s.routers)
    load("x2", ins.x2, s.mid_x2)
    load("w_out", ins.w_out, s.wide_w)
    load("mix", ins.own_mix, o.mix)
    load("q", ins.q, s.qs)
    load("attended", ins.attended, s.atts)
    load("slots", slots_in, s.slots)
    load("low", ins.low, s.lows)
    load("wk", ins.wk, s.wks)
    load("wv", ins.wv, s.wvs)

    p.greet(("x", "ep", "tp"))
    ep_back = p.copy("ep", ins.par_back, s.other_ep, s.es.at[0], s.er.at[0])
    ep_back.start()
    ep_mix = p.copy("ep", ins.par_mix, s.mix_ep, s.es.at[1], s.er.at[1])
    ep_mix.start()
    queue = ring[whole_early:] + ["little"]
    zero_copy = p.copy("x", z_sent, s.zero_in, s.xs.at[len(ring) + 1], s.xr.at[len(ring) + 1])
    zero_copy.start()
    for _ in range(3):
        cross(queue.pop(0))

    got("back")
    ep_back.wait_recv()
    for i in range(seqs):
        s.back[part_of(i)] = (
            s.back[part_of(i)].astype(F32) + s.other_ep[part_of(i)].astype(F32)
        ).astype(BF16)
    tp_back = p.copy("tp", s.back, s.other_tp, s.ts.at[0], s.tr.at[0])
    tp_back.start()
    got("mix")
    ep_mix.wait_recv()
    for i in range(seqs):
        o.mix[part_of(i)] = (o.mix[part_of(i)].astype(F32) + s.mix_ep[part_of(i)].astype(F32)).astype(BF16)

    def step_middle():
        got("grad", "dy", "router", "x2", "w_out")
        tp_back.wait_recv()
        s.small[...] = jnp.zeros_like(s.small)

        @pl.loop(0, seqs)
        def _(i):
            at = pl.ds(pl.multiple_of(i * rows, rows), rows)
            total = s.back[at].astype(F32) + s.other_tp[at].astype(F32)
            gate, pulls = ins.gates[at], total[:, model:]
            chosen = gate * (pulls - jnp.sum(gate * pulls, axis=-1, keepdims=True))
            high, rest = two_parts(chosen)
            grad_two = total[:, :model] + (mm(high, s.routers[...]) + mm(rest, s.routers[...]))
            unit, scale = unit_rows(o.grad[at])
            s.small[...] += t_mm(high, s.mid_x2[at]) + t_mm(rest, s.mid_x2[at])
            s.small[LANES - 1 :, :] += jnp.sum(grad_two * unit, axis=0, keepdims=True)
            scaled = grad_two * ins.gain_two[...]
            out = s.mid_dy[at].astype(F32) + scale * (
                scaled - unit * jnp.mean(scaled * unit, axis=-1, keepdims=True)
            )
            o.grad[at] = out
            rounded = out.astype(BF16)
            s.branch[at] = rounded
            s.heads[at] = mm(rounded, s.wide_w[...]).astype(BF16)

        load("wq", ins.wq, s.wide_w)
        load("act", ins.act, s.mid_dy)
        load("normed", ins.normed, s.mid_x2)

    tp_mix = p.copy("tp", o.mix, s.mix_tp, s.ts.at[1], s.tr.at[1])

    def step_attend():
        got("q", "attended", "slots")
        homes = [(p.z - r, side) for r in range(LINE) for side in (p.side, 1 - p.side)]
        firsts = [jnp.where(a >= 0, (2 * a + b) * rows, 2**24) for a, b in homes]

        @pl.loop(0, seqs)
        def _(i):
            at = pl.ds(pl.multiple_of(i * rows, rows), rows)

            singles = [s.slots.at[i, j // 2, j % 2] for j in range(2 * LINE)]
            attend_back_core(
                group,
                s.qs.at[i],
                ins.place[i],
                s.heads.at[at],
                s.atts.at[i],
                ins.lse.at[i],
                ins.cosine[at],
                ins.sine[at],
                singles,
                firsts,
                p.cp * rows,
                s.keys,
                s.bias,
                singles,
                s.dq.at[i],
                512,
            )

            @p.at(LINE - 1)
            def _():
                for r in range(LINE - 1, 0, -1):
                    kv_down(i, r).start()

    def kv_cross(i):
        return p.copy("x", s.slots.at[i, 0, 1], s.kv_x.at[i], s.kxs.at[i], s.kxr.at[i])

    def kv_down(i, r):
        return p.copy("down", s.slots.at[i, r], s.kv_z.at[i, r - 1], s.kzs.at[i, r - 1], s.kzr.at[i, r - 1])

    def kv_take(i, r):
        kv_down(i, r + 1).wait_recv()
        for way in range(2):
            s.slots[i, r, way] = (s.slots[i, r, way].astype(F32) + s.kv_z[i, r, way].astype(F32)).astype(BF16)

    def keys_pass(i, z):
        @p.at(z)
        def _():
            for r in range(z, 0, -1):
                kv_take(i, r)
                kv_down(i, r).start()

    def keys_cross(i):
        @pl.when(p.z < LINE - 1)
        def _():
            kv_take(i, 0)

        kv_cross(i).start()

    def keys_close(i):
        kv_cross(i).wait_recv()
        s.slots[i, 0, 0] = (s.slots[i, 0, 0].astype(F32) + s.kv_x[i].astype(F32)).astype(BF16)

    def part_copy(i):
        return p.copy("tp", s.part.at[part_of(i)], s.part_in.at[part_of(i)], s.ts.at[2 + i], s.tr.at[2 + i])

    def step_project(i):
        if i == 0:
            got("wq", "wk", "wv", "act", "normed")
        at = part_of(i)
        total = s.slots[i, 0, 0].astype(F32)
        dk = rope_back(total[:, :width], widen(ins.cosine[at], width), widen(ins.sine[at], width)).astype(BF16)
        dv = total[:, width:].astype(BF16)
        s.dkv[at, :width] = dk
        s.dkv[at, width:] = dv
        full = mm_t(s.dq[i], s.wide_w[...]) + mm_t(dk, s.wks[...]) + mm_t(dv, s.wvs[...])
        s.part[at] = full.astype(BF16)
        part_copy(i).start()

    tall = model // 4

    def pieces(make, keep):
        @pl.loop(0, 4)
        def _(piece):
            got_piece = make(pl.ds(pl.multiple_of(piece * tall, tall), tall)).astype(BF16)
            block = got_piece.reshape(4, short, got_piece.shape[1])
            for b in range(4):
                keep(piece // 2, 2 * (piece % 2) + b // 2, b % 2, block[b])

    def big_part(row):
        def keep(half, z, side, value):
            s.whole[half, z, side, row : row + value.shape[0], :] = value

        return keep

    def little_part(column):
        def keep(half, z, side, value):
            s.lit[half, z, side, :, column : column + value.shape[1]] = value

        return keep

    ep_big = p.copy("ep", s.whole.at[1 - p.ep], s.came, s.es.at[2], s.er.at[2])
    ep_lit = p.copy("ep", s.lit.at[1 - p.ep], s.lit_came, s.es.at[3], s.er.at[3])

    def step_out_weight():
        got("low")
        pieces(lambda at: t_mm(s.branch[:, at], s.lows[...]), big_part(0))

    def step_query_weight():
        got("normed")
        loads["normed"] = Done()
        query = jnp.concatenate([s.dq[i] for i in range(seqs)], axis=0)
        pieces(lambda at: t_mm(s.mid_x2[:, at], query), big_part(short))
        ep_big.start()

    def step_key_weight():
        pieces(lambda at: t_mm(s.mid_x2[:, at], s.dkv[...]), little_part(0))
        pieces(lambda at: jnp.transpose(s.small[:, at]), little_part(2 * width))
        ep_lit.start()

    def step_big_cores():
        ep_big.wait_recv()
        for side in range(2):

            @pl.loop(0, LINE)
            def _(d):
                add_into(s.whole.at[p.ep, d, side], s.came.at[d, side])

    def step_little_cores():
        ep_lit.wait_recv()
        for side in range(2):

            @pl.loop(0, LINE)
            def _(d):
                add_into(s.lit.at[p.ep, d, side], s.lit_came.at[d, side])

    def step_input():
        for i in range(seqs):
            at = part_of(i)
            part_copy(i).wait_recv()
            unit, scale = unit_rows(s.mid_dy[at].astype(F32))
            whole = s.part[at].astype(F32) + s.part_in[at].astype(F32)
            gain_row = jnp.sum(whole * unit, axis=0, keepdims=True)
            if i == 0:
                s.small[LANES - 2 : LANES - 1, :] = gain_row
            else:
                s.small[LANES - 2 : LANES - 1, :] += gain_row
            scaled = whole * ins.gain_one[...]
            o.grad[at] = o.grad[at] + scale * (scaled - unit * jnp.mean(scaled * unit, axis=-1, keepdims=True))

    def step_mix():
        tp_mix.wait_recv()
        tp_mix.wait_send()
        for i in range(seqs):
            o.mix[part_of(i)] = (o.mix[part_of(i)].astype(F32) + s.mix_tp[part_of(i)].astype(F32)).astype(BF16)

    line = list(ring) + ["little"]
    stage = {item: 0 for item in line}

    def advance(at, to):
        if not 0 <= at < len(line):
            return
        item = line[at]
        while stage[item] < to:
            now = stage[item]
            if now == 0:
                opened(item)
            elif now == 1:
                flow(item).second()
            elif now == 2:
                flow(item).third()
            elif now == 3:
                closed(item)
            elif now == 4:
                freed(item)
            stage[item] = now + 1

    def turn(at):
        for back in (4, 3, 2, 1, 0):
            advance(at - back, back + 1)

    def add_zero():
        got("zero")
        zero_copy.wait_recv()
        s.staged[0] = s.staged[0] + s.zero_in[...].astype(F32)

    tp_mix.start()
    turn(0)
    finish_expert(0, add_zero)
    turn(1)
    step_middle()
    advance(0, 3)
    advance(1, 2)
    step_attend()
    cross(queue.pop(0))
    step_out_weight()
    step_query_weight()
    turn(2)
    keys_pass(0, 2)
    advance(0, 4)
    advance(1, 3)
    keys_pass(1, 2)
    advance(2, 2)
    step_big_cores()
    step_mix()
    keys_pass(0, 1)
    keys_pass(1, 1)
    turn(3)
    keys_cross(0)
    keys_cross(1)
    cross(queue.pop(0))
    turn(4)
    cross(queue.pop(0))
    keys_close(0)
    step_project(0)
    keys_close(1)
    step_project(1)
    advance(2, 4)
    advance(3, 3)
    advance(4, 2)
    step_input()
    step_key_weight()
    turn(5)
    cross(queue.pop(0))
    step_little_cores()
    for at in range(6, len(line) + 4):
        turn(at)
        if queue:
            cross(queue.pop(0))
    for e in stored:
        if e not in waited:
            store(e).wait()
    for item in line:
        if item == "little" or (crosses(item) and index_of[item] + RING >= len(ring)):
            x_copy(item).wait_send()
    for i in range(seqs):
        kv_cross(i).wait_send()
        part_copy(i).wait_send()
        for z in range(1, LINE):

            @p.at(z)
            def _(z=z):
                for r in range(z, 0, -1):
                    kv_down(i, r).wait_send()

    tp_back.wait_send()
    zero_copy.wait_send()
    for copy in (ep_back, ep_mix, ep_big, ep_lit):
        copy.wait_send()


class Done:
    def wait(self):
        return None


def back_and_sums(ins, slots, chunks, group):
    keeps, _, arrived, *_ = chunks
    _, length, depth, wide = keeps.shape
    early, count = arrived.shape[0], FIRST + keeps.shape[0]
    block = (length, depth, wide)
    v = BackIns(*ins)
    rows, model = v.middle.shape
    seqs, each, heads = v.q.shape
    width = v.wk.shape[1]
    both = 2 * width
    small = (length, 2, model // 16, both + LANES)
    n_ring = count - FIRST + 2
    anywhere = pl.BlockSpec(memory_space=pl.ANY)
    inside = pl.BlockSpec(memory_space=pltpu.VMEM)
    dma, vm = pltpu.SemaphoreType.DMA, pltpu.VMEM
    flag = pltpu.SemaphoreType.REGULAR
    scratch = dict(
        back=vm((rows, model + LANES), BF16),
        other_ep=vm((rows, model + LANES), BF16),
        other_tp=vm((rows, model + LANES), BF16),
        mid_dy=vm((rows, model), BF16),
        mid_x2=vm((rows, model), BF16),
        wide_w=vm((model, heads), BF16),
        branch=vm((rows, model), BF16),
        heads=vm((rows, heads), BF16),
        small=vm((LANES, model), F32),
        qs=vm((seqs, each, heads), BF16),
        atts=vm((seqs, each, heads), F32),
        slots=vm((seqs, LINE, 2, each, both), BF16),
        kv_x=vm((seqs, each, both), BF16),
        kv_z=vm((seqs, LINE - 1, 2, each, both), BF16),
        keys=vm((2 * LINE * each, both), BF16),
        bias=vm((2 * LINE * each, each), F32),
        dq=vm((seqs, each, heads), BF16),
        lows=vm((rows, heads), BF16),
        wks=vm((model, width), BF16),
        wvs=vm((model, width), BF16),
        routers=vm((LANES, model), BF16),
        dkv=vm((rows, both), BF16),
        part=vm((rows, model), BF16),
        part_in=vm((rows, model), BF16),
        mix_ep=vm((rows, model), BF16),
        mix_tp=vm((rows, model), BF16),
        held=vm((RING,) + block, BF16),
        spots=vm((RING, 5, depth, wide), BF16),
        kept=vm(block, BF16),
        staged=vm((2, depth, wide), F32),
        zero_in=vm((depth, wide), BF16),
        whole=vm((2, length, 2, depth, wide), BF16),
        came=vm((length, 2, depth, wide), BF16),
        lit=vm((2,) + small, BF16),
        lit_came=vm(small, BF16),
        lit_x=vm((small[0],) + small[2:], BF16),
        lit_spots=vm((5,) + small[2:], BF16),
        ls=dma((28,)),
        ks=dma((1 + early,)),
        xs=dma((n_ring + 2,)),
        xr=dma((n_ring + 2,)),
        zs=dma((n_ring + 1, 6)),
        zr=dma((n_ring + 1, 6)),
        es=dma((4,)),
        er=dma((4,)),
        ts=dma((4,)),
        tr=dma((4,)),
        kxs=dma((2,)),
        kxr=dma((2,)),
        kzs=dma((2, 3)),
        kzr=dma((2, 3)),
        os=dma((count,)),
        free_x=flag,
        free_up=flag,
        free_down=flag,
    )
    return pl.pallas_call(
        functools.partial(back_body, group),
        out_shape=(
            shape_of((rows, model), F32),
            shape_of((rows, model), BF16),
            shape_of((count, depth, wide), F32),
            shape_of((depth, wide), F32),
            shape_of(small[2:], F32),
        ),
        in_specs=[anywhere] * (len(BackIns._fields) - BACK_IN_PLACE)
        + [inside] * BACK_IN_PLACE
        + [anywhere] * 6,
        out_specs=(inside, inside, anywhere, inside, inside),
        scratch_shapes=[scratch[name] for name in BackScratch._fields],
        compiler_params=pltpu.CompilerParams(
            collective_id=1, has_side_effects=True, vmem_limit_bytes=67_043_328
        ),
        name="back_and_sums",
    )(*ins, slots, *chunks)


def results_body(middle, mix, grad, chunk, big, little, out, grad_in, first, second, keys, values, small, both, down):
    out[...] = middle[...] + mix[...].astype(F32)
    grad_in[...] = grad[...]
    half = down.shape[2]
    both[0] = chunk[0, :, : 2 * half].reshape(both.shape[1:])
    down[0] = chunk[0, :, 2 * half :]

    @pl.when(pl.program_id(0) == 0)
    def _():
        tall, width = first.shape[0], keys.shape[1]
        first[...] = big[:tall]
        second[...] = big[tall:]
        keys[...] = little[:, :width]
        values[...] = little[:, width : 2 * width]
        small[...] = little[:, 2 * width :]


def results(middle, mix, grad, chunks, big, little, half):
    rows, model = middle.shape
    count, depth, wide = chunks.shape
    tall, width = big.shape[0] // 2, (little.shape[1] - LANES) // 2
    part = pl.BlockSpec((rows // count, model), lambda e: (e, 0))
    once = lambda shape: pl.BlockSpec(shape, lambda e: (0,) * len(shape))
    whole = [(tall, big.shape[1])] * 2 + [(tall, width)] * 2 + [(tall, LANES)]
    return pl.pallas_call(
        results_body,
        grid=(count,),
        out_shape=[shape_of((rows, model), F32)] * 2
        + [shape_of(shape, F32) for shape in whole]
        + [shape_of((count, depth, 2, half), F32), shape_of((count, depth, half), F32)],
        in_specs=[part] * 3
        + [pl.BlockSpec((1, depth, wide), lambda e: (e, 0, 0)), once(big.shape), once(little.shape)],
        out_specs=[part] * 2
        + [once(shape) for shape in whole]
        + [
            pl.BlockSpec((1, depth, 2, half), lambda e: (e, 0, 0, 0)),
            pl.BlockSpec((1, depth, half), lambda e: (e, 0, 0)),
        ],
        compiler_params=params(),
        name="results",
    )(middle, mix, grad, chunks, big, little)


class FrontIns(NamedTuple):
    q: Any
    kv: Any
    act: Any
    routes: Any
    router: Any
    gain: Any
    place: Any
    w_out: Any
    dy: Any
    w_in: Any


class FrontOuts(NamedTuple):
    slots: Any
    low: Any
    attended: Any
    lse: Any
    middle: Any
    normed: Any
    gates: Any
    router: Any
    x_par: Any
    g_par: Any
    dy_par: Any
    w_flat: Any


class FrontScratch(NamedTuple):
    keys: Any
    bias: Any
    wo: Any
    part: Any
    part_in: Any
    raw: Any
    flat: Any
    ws: Any
    wi: Any
    wf: Any
    us: Any
    ur: Any
    xs: Any
    xr: Any
    ts: Any
    tr: Any
    es: Any
    er: Any


def front_body(group, *refs):
    n_in, n_out = len(FrontIns._fields), len(FrontOuts._fields)
    ins = FrontIns(*refs[:n_in])
    o = FrontOuts(*refs[n_in : n_in + n_out])
    s = FrontScratch(*refs[n_in + n_out :])
    p = Place()
    seqs, rows, _ = ins.q.shape
    experts_here = ins.w_in.shape[0]
    part_of = lambda i: pl.ds(i * rows if isinstance(i, int) else pl.multiple_of(i * rows, rows), rows)

    def fetch(e):
        return pltpu.make_async_copy(ins.w_in.at[e], s.raw.at[e % 2], s.wi.at[e % 2])

    def put(e):
        return pltpu.make_async_copy(s.flat.at[e % 2], o.w_flat.at[e], s.wf.at[e % 2])

    done = []

    def fill(count):
        for _ in range(count):
            e = len(done)
            if e >= experts_here:
                return
            fetch(e).wait()
            if e >= 2:
                put(e - 2).wait()
            slot, cut = e % 2, s.flat.shape[1] // 4

            @pl.loop(0, 4)
            def _(k):
                at = pl.ds(pl.multiple_of(k * cut, cut), cut)
                s.flat[slot, at] = s.raw[slot, at].reshape(cut, s.flat.shape[2])

            put(e).start()
            if e + 2 < experts_here:
                fetch(e + 2).start()
            done.append(e)

    def source(i, r):
        return ins.kv.at[i] if r == 0 else o.slots.at[i, r, 0]

    def up_copy(i, r):
        return p.copy("up", source(i, r), o.slots.at[i, r + 1, 0], s.us.at[i, r], s.ur.at[i, r])

    def x_copy(i, r):
        return p.copy("x", source(i, r), o.slots.at[i, r, 1], s.xs.at[i, r], s.xr.at[i, r])

    def tp_copy(i):
        return p.copy("tp", s.part.at[part_of(i)], s.part_in.at[part_of(i)], s.ts.at[i], s.tr.at[i])

    def ep_copies(i):
        at = part_of(i)
        return (
            p.copy("ep", o.normed.at[at], o.x_par.at[at], s.es.at[2 * i], s.er.at[2 * i]),
            p.copy("ep", o.gates.at[at], o.g_par.at[at], s.es.at[2 * i + 1], s.er.at[2 * i + 1]),
        )

    fetch(0).start()
    fetch(1).start()
    o.router[...] = jnp.zeros_like(o.router)
    o.router[: ins.router.shape[0]] = ins.router[...]
    wo_load = pltpu.make_async_copy(ins.w_out, s.wo, s.ws.at[0])
    wo_load.start()
    p.greet(("x", "ep", "tp"))
    for i in range(seqs):

        @pl.when(p.z < LINE - 1)
        def _(i=i):
            up_copy(i, 0).start()

        x_copy(i, 0).start()
    dy_copy = p.copy("ep", ins.dy, o.dy_par, s.es.at[2 * seqs], s.er.at[2 * seqs])
    dy_copy.start()
    for i in range(seqs):
        o.slots[i, 0, 0] = ins.kv[i]
        for r in range(1, LINE):

            @pl.when(p.z < r)
            def _(i=i, r=r):
                o.slots[i, r] = jnp.zeros(o.slots.shape[2:], BF16)

    fill(1)
    for r in range(1, LINE):
        for i in range(seqs):
            for z in range(r, LINE):

                @p.at(z)
                def _(i=i, r=r, z=z):
                    up_copy(i, r - 1).wait_recv()
                    if z < LINE - 1:
                        up_copy(i, r).start()
                    x_copy(i, r).start()

        fill(1)
    homes = [(p.z - r, side) for r in range(LINE) for side in (p.side, 1 - p.side)]
    firsts = [jnp.where(a >= 0, (2 * a + b) * rows, 2**24) for a, b in homes]
    wo_load.wait()

    @pl.loop(0, seqs)
    def _(i):
        for r in range(LINE):

            @pl.when(p.z >= r)
            def _(r=r):
                x_copy(i, r).wait_recv()

        attend_core(
            group,
            ins.q.at[i],
            ins.place[i],
            [o.slots.at[i, j // 2, j % 2] for j in range(2 * LINE)],
            firsts,
            p.cp * rows,
            s.keys,
            s.bias,
            o.lse.at[i],
            KEY_CHUNK,
            o.attended.at[i],
            o.low.at[i],
        )
        s.part[part_of(i)] = mm_t(o.low[i], s.wo[...]).astype(BF16)
        tp_copy(i).start()

    fill(1)
    for i in range(seqs):
        at = part_of(i)
        tp_copy(i).wait_recv()
        mid = ins.act[at].astype(F32) + (s.part[at].astype(F32) + s.part_in[at].astype(F32))
        o.middle[at] = mid
        expert = lax.broadcasted_iota(jnp.int32, (LANES, rows), 0)
        hot = sum(jnp.where(ins.routes[i, k : k + 1, :] == expert, 1.0, 0.0) for k in range(ins.routes.shape[1]))
        o.normed[at], o.gates[at] = route(
            mid, ins.gain[...], lambda v: mm_t(v, o.router[...]), jnp.transpose(hot)
        )
        for copy in ep_copies(i):
            copy.start()
        fill(3 if i == 0 else experts_here)
    for i in range(seqs):
        for copy in ep_copies(i):
            copy.wait()
        tp_copy(i).wait_send()
        for r in range(LINE):

            @pl.when(p.z >= r)
            def _(i=i, r=r):
                x_copy(i, r).wait_send()
                if r < LINE - 1:

                    @pl.when(p.z < LINE - 1)
                    def _():
                        up_copy(i, r).wait_send()

    dy_copy.wait()
    for e in done[-2:]:
        put(e).wait()


def front(ins, group):
    v = FrontIns(*ins)
    seqs, each, heads = v.q.shape
    both = v.kv.shape[-1]
    rows, model = v.act.shape
    local, _, _, half = v.w_in.shape
    anywhere = pl.BlockSpec(memory_space=pl.ANY)
    inside = pl.BlockSpec(memory_space=pltpu.VMEM)
    dma, vm = pltpu.SemaphoreType.DMA, pltpu.VMEM
    scratch = dict(
        keys=vm((2 * LINE * each, both), BF16),
        bias=vm((2 * LINE * each, each), F32),
        wo=vm(v.w_out.shape, BF16),
        part=vm((rows, model), BF16),
        part_in=vm((rows, model), BF16),
        raw=vm((2, model, 2, half), BF16),
        flat=vm((2, model, 2 * half), BF16),
        ws=dma((1,)),
        wi=dma((2,)),
        wf=dma((2,)),
        us=dma((seqs, LINE - 1)),
        ur=dma((seqs, LINE - 1)),
        xs=dma((seqs, LINE)),
        xr=dma((seqs, LINE)),
        ts=dma((seqs,)),
        tr=dma((seqs,)),
        es=dma((2 * seqs + 1,)),
        er=dma((2 * seqs + 1,)),
    )
    return pl.pallas_call(
        functools.partial(front_body, group),
        out_shape=(
            shape_of((seqs, LINE, 2, each, both), BF16),
            shape_of((seqs, each, heads), BF16),
            shape_of((seqs, each, heads), F32),
            shape_of((seqs, heads // HEAD // group, group * each), F32),
            shape_of((rows, model), F32),
            shape_of((rows, model), BF16),
            shape_of((rows, LANES), F32),
            shape_of((LANES, model), BF16),
            shape_of((rows, model), BF16),
            shape_of((rows, LANES), F32),
            shape_of((rows, model), BF16),
            shape_of((local, model, 2 * half), BF16),
        ),
        in_specs=[inside] * 7 + [anywhere] * 3,
        out_specs=(inside,) * 8 + (anywhere,) * 4,
        scratch_shapes=[scratch[name] for name in FrontScratch._fields],
        compiler_params=params(collective_id=3, has_side_effects=True),
        name="front",
    )(*ins)


def on_device(
    activations,
    cotangent,
    positions,
    routes,
    w_query,
    w_key,
    value_weight,
    w_out,
    gain_attn,
    gain_moe,
    w_router,
    w_gate_up,
    w_down,
):
    seqs, rows, model = activations.shape
    total = seqs * rows
    width = w_key.shape[1]
    group = w_query.shape[1] // width
    expert_count = w_router.shape[1]
    local = w_gate_up.shape[0]
    half = w_down.shape[2]
    blocks = lax.axis_size("cp")
    length = blocks // 2
    here = lax.axis_index("cp")
    z, side = here // 2, here % 2
    mine = lax.axis_index("ep")
    act = activations.reshape(total, model)
    dy = cotangent.reshape(total, model)
    gains = jnp.stack([gain_attn, gain_moe])
    gain_one, gain_two = gains[:1], gains[1:]

    frequency = jnp.power(10000.0, -(jnp.arange(HEAD // 2, dtype=F32) * 2.0 / HEAD))
    angles = positions.reshape(total, 1).astype(F32) * jnp.tile(frequency, 2 * LANES // HEAD)
    cosine, sine = jnp.cos(angles), jnp.sin(angles)

    normed, q, kv = project(act, gain_one, w_query, w_key, value_weight, cosine, sine)
    q = q.reshape(seqs, rows, -1)
    place = positions.reshape(seqs, 1, rows)
    if length == LINE:
        kv = kv.reshape(seqs, rows, 2 * width)
        ins = (q, kv, act, jnp.swapaxes(routes, 1, 2), w_router.T, gain_two, place, w_out, dy, w_gate_up)
        got = FrontOuts(*front(ins, group))
        slots, low, attended, lse, middle, normed_two, gates, router, x_par, gates_par, dy_par, w_in = got
        low = low.reshape(total, -1)
    else:
        lanes = jnp.arange(LANES, dtype=jnp.int32)
        hot = jnp.sum((routes.reshape(total, -1, 1) == lanes).astype(F32), axis=1)
        router = jnp.pad(w_router, ((0, 0), (0, LANES - expert_count)))
        kv = kv.reshape(1, seqs, rows, 2 * width)
        offset = (here * rows).astype(jnp.int32).reshape(1)
        slots = [lax.all_gather(kv, "cp", axis=0, tiled=True)]
        first = jnp.arange(blocks, dtype=jnp.int32) * rows
        dy_par = swap(dy, "ep")
        low, attended, lse = attend(q, place, slots, first, offset, group)
        low = low.reshape(total, -1)
        part = out_project(low, w_out)
        w_in = w_gate_up.reshape(local, model, 2 * half)
        middle, normed_two, gates = middle_of(act, part, swap(part, "tp"), gain_two, router, hot)
        x_par, gates_par = swap(normed_two, "ep"), swap(gates, "ep")

    early, apart = (EARLY, FIRST) if length == LINE else (0, 0)
    args = (normed_two, x_par, dy, dy_par, gates, gates_par, w_in, w_down)
    chunks, (own_back, par_back, own_mix, par_mix) = experts(early, apart, blocks, *args)
    if length == LINE:
        ins = (
            own_back, par_back, own_mix, par_mix, middle, dy, router, w_out, normed_two, q, attended, act, normed,
            low, w_query, w_key, value_weight, gates, gain_two, gain_one, place, lse, cosine, sine,
        )
        input_grad, mix, expert_grad, big, little = back_and_sums(ins, slots, chunks, group)
        output, input_grad, *plain, small, gate_up_grad, down_grad = results(
            middle, mix, input_grad, expert_grad, big, little, half
        )
        out_grad, query_grad, key_grad, value_grad = plain
        small_grads = small[:, LANES - 2], small[:, LANES - 1], small[:, :expert_count]
    else:
        back = total_of([own_back, swap(par_back, "ep")]).astype(BF16)
        grad_middle, branch, grad_heads, small = middle_back(
            back, swap(back, "tp"), middle, dy, gates, router, gain_two, w_out, normed_two
        )
        seq_cosine, seq_sine = cosine.reshape(seqs, rows, -1), sine.reshape(seqs, rows, -1)
        dq, grads = attend_back(
            q, place, grad_heads.reshape(q.shape), attended, lse, seq_cosine, seq_sine, slots, first, offset, group
        )
        dq = dq.reshape(total, -1)
        kv_sum = lax.psum_scatter(grads[0], "cp", scatter_dimension=0, tiled=True)
        kv_terms = [kv_sum, jnp.zeros_like(kv_sum), jnp.zeros_like(kv_sum)]
        kv_terms = [t.reshape(total, 2 * width) for t in kv_terms]
        spots = jnp.stack([mine, side]).astype(jnp.int32)
        big = weights(spots, blocks, [(branch, low), (normed, dq)], stacked=True)
        normed_part, dkv, gain_row = project_back(act, dq, *kv_terms, cosine, sine, w_query, w_key, value_weight)
        small = jnp.concatenate([small[:expert_count], small[LANES : LANES + 1], gain_row[:1]], axis=0)
        small = jnp.pad(small, ((0, LANES - small.shape[0]), (0, 0)))
        little = weights(spots, blocks, [(normed, dkv)], (small,))
        input_grad = input_of(act, grad_middle, normed_part, swap(normed_part, "tp"), gain_one)
        mix = total_of([own_mix, swap(par_mix, "ep")]).astype(BF16)
        output = middle + total_of([mix, swap(mix, "tp")])

        def spread_sum(keep, send):
            both = total_of([keep, swap(send, "ep")]).astype(BF16)
            return line_sum([both[0], swap(both[1], "cp")], z, length)

        turned = [jnp.swapaxes(v, 0, 1) for v in (chunks[0], swap(chunks[1], "cp"))]
        expert_grad = line_sum(turned, z, length)
        big, little = spread_sum(*big), spread_sum(*little)
        gate_up_grad = expert_grad[:, :, : 2 * half].reshape(local, -1, 2, half)
        down_grad = expert_grad[:, :, 2 * half :]
        tall = big.shape[0] // 2
        out_grad, query_grad = big[:tall], big[tall:]
        key_grad, value_grad = little[:, :width], little[:, width : 2 * width]
        small = little[:, 2 * width :]
        gain_part = small[:, expert_count + 1]
        small_grads = gain_part + swap(gain_part, "tp"), small[:, expert_count], small[:, :expert_count]
    return (
        output.reshape(activations.shape),
        input_grad.reshape(activations.shape),
        query_grad,
        key_grad,
        value_grad,
        out_grad,
        *small_grads,
        gate_up_grad,
        down_grad,
    )


def solution(mesh):
    in_specs = (
        P("ep", "cp", None),
        P("ep", "cp", None),
        P("ep", "cp"),
        P("ep", "cp", None),
        P(None, "tp"),
        P(None, "tp"),
        P(None, "tp"),
        P(None, "tp"),
        P(),
        P(),
        P(),
        P("ep", None, None, "tp"),
        P("ep", None, "tp"),
    )
    out_specs = (
        P("ep", "cp", None),
        P("ep", "cp", None),
        P(("ep", "cp"), "tp"),
        P(("ep", "cp"), "tp"),
        P(("ep", "cp"), "tp"),
        P(("ep", "cp"), "tp"),
        P(("ep", "cp")),
        P(("ep", "cp")),
        P(("ep", "cp"), None),
        P("ep", "cp", None, "tp"),
        P("ep", "cp", "tp"),
    )
    return jax.shard_map(
        on_device, mesh=mesh, in_specs=in_specs, out_specs=out_specs, check_vma=False
    )
```

```python
import functools
from typing import Any, NamedTuple

import jax
import jax.numpy as jnp
from jax import lax
from jax.experimental import pallas as pl
from jax.experimental.pallas import tpu as pltpu
from jax.sharding import PartitionSpec as P

HEAD = 64
EPS = 1e-06
NEG = -1e30
SCALE = 0.125
LANES = 128
KEY_CHUNK = 1024
F32 = jnp.float32
BF16 = jnp.bfloat16
MESH = pl.DeviceIdType.MESH


def mm(a, b):
    return lax.dot_general(a, b, (((1,), (0,)), ((), ())), preferred_element_type=F32)


def mm_t(a, b):
    return lax.dot_general(a, b, (((1,), (1,)), ((), ())), preferred_element_type=F32)


def t_mm(a, b):
    return lax.dot_general(a, b, (((0,), (0,)), ((), ())), preferred_element_type=F32)


def two_parts(v):
    high = v.astype(BF16)
    return high, (v - high.astype(F32)).astype(BF16)


def halves_turned(v, back):
    width = v.shape[1]
    ahead = pltpu.roll(v, width - HEAD // 2, 1)
    behind = pltpu.roll(v, HEAD // 2, 1)
    first = lax.broadcasted_iota(jnp.int32, v.shape, 1) % HEAD < HEAD // 2
    if back:
        return jnp.where(first, ahead, -behind)
    return jnp.where(first, -ahead, behind)


def rope(v, cosine, sine):
    return v * cosine + halves_turned(v, False) * sine


def rope_back(v, cosine, sine):
    return v * cosine + halves_turned(v * sine, True)


def widen(table, width):
    return jnp.concatenate([table] * (width // table.shape[1]), axis=1)


def unit_rows(v):
    scale = lax.rsqrt(jnp.mean(v * v, axis=-1, keepdims=True) + EPS)
    return v * scale, scale


def shape_of(shape, dtype):
    return jax.ShapeDtypeStruct(shape, dtype)


def params(**kw):
    return pltpu.CompilerParams(vmem_limit_bytes=60 * 2**20, **kw)


def cost(flops, moved):
    return pl.CostEstimate(flops=int(flops), bytes_accessed=int(moved), transcendentals=0)


def project_body(act, gain, wq, wk, wv, cosine, sine, normed, q, kv):
    unit, _ = unit_rows(act[...].astype(F32))
    low = (unit * gain[:1]).astype(BF16)
    normed[...] = low
    qf = mm(low, wq[...])
    q[...] = rope(qf, widen(cosine[...], qf.shape[1]), widen(sine[...], qf.shape[1])).astype(BF16)
    kf = mm(low, wk[...])
    width = kf.shape[1]
    kv[:, :width] = rope(kf, widen(cosine[...], width), widen(sine[...], width)).astype(BF16)
    kv[:, width:] = mm(low, wv[...]).astype(BF16)


def project(act, gain, wq, wk, wv, cosine, sine):
    rows, model = act.shape
    total = wq.shape[1] + 2 * wk.shape[1]
    return pl.pallas_call(
        project_body,
        out_shape=(
            shape_of((rows, model), BF16),
            shape_of((rows, wq.shape[1]), BF16),
            shape_of((rows, 2 * wk.shape[1]), BF16),
        ),
        compiler_params=params(),
        cost_estimate=cost(2 * rows * model * total, 2 * model * total + 6 * rows * model),
        name="project",
    )(act, gain, wq, wk, wv, cosine, sine)


def fill_keys(firsts, offset, place, slots, keys, bias, rows):
    query = lax.broadcasted_iota(jnp.int32, (rows, rows), 1) + offset
    for at, slot in enumerate(slots):
        keys[at * rows : (at + 1) * rows, :] = slot[...]
        key = lax.broadcasted_iota(jnp.int32, (rows, rows), 0) + firsts[at]
        distance = query - key
        seen = (distance >= 0) & (distance <= place)
        bias[at * rows : (at + 1) * rows, :] = jnp.where(seen, 0.0, NEG)


def single_slots(slots):
    return [slot.at[one, 0] for slot in slots for one in range(slot.shape[0])]


def group_rows(block, head, group):
    return jnp.concatenate(
        [block[:, (head * group + g) * HEAD : (head * group + g + 1) * HEAD] for g in range(group)], axis=0
    )


def pair_lanes(pair, width, start=0):
    return pl.ds(pl.multiple_of(start + pair * width, LANES), width)


def attend_core(group, q_ref, place, slots, firsts, offset, keys, bias, lse_ref, most, out_ref, low_ref):
    rows = q_ref.shape[0]
    fill_keys(firsts, offset, place, slots, keys, bias, rows)
    total, width = keys.shape[0], keys.shape[1] // 2
    chunk = min(total, most)
    two, many = 2 * HEAD, 2 * HEAD * group

    @pl.loop(0, width // two)
    def _(pair):
        q = (q_ref[:, pair_lanes(pair, many)].astype(F32) * SCALE).astype(BF16)
        pieces = []
        for head in range(2):
            mine = slice(head * HEAD, (head + 1) * HEAD)
            q3 = group_rows(q, head, group)
            top = run = out = None
            for low in range(0, total, chunk):
                k = keys[low : low + chunk, pair_lanes(pair, two)][:, mine]
                v = keys[low : low + chunk, pair_lanes(pair, two, width)][:, mine]
                s = mm_t(k, q3) + widen(bias[low : low + chunk, :], group * rows)
                here = jnp.max(s, axis=0, keepdims=True)
                new = here if top is None else jnp.maximum(top, here)
                p = jnp.exp(s - new)
                part = jnp.sum(p, axis=0, keepdims=True)
                o = t_mm(v, p.astype(BF16))
                if top is None:
                    run, out = part, o
                else:
                    shrink = jnp.exp(top - new)
                    run, out = run * shrink + part, out * shrink + o
                top = new
            out = jnp.transpose(out / run)
            pieces += [out[g * rows : (g + 1) * rows] for g in range(group)]
            lse_ref[pl.ds(2 * pair + head, 1), :] = top + jnp.log(run)
        whole = jnp.concatenate(pieces, axis=1)
        out_ref[:, pair_lanes(pair, many)] = whole
        low_ref[:, pair_lanes(pair, many)] = whole.astype(BF16)


def attend_body(group, count, first_ref, offset_ref, q_ref, place_ref, *refs):
    slots = single_slots(refs[:count])
    low_ref, out_ref, lse_ref, keys, bias = refs[count:]
    firsts = [first_ref[i] for i in range(len(slots))]
    attend_core(
        group,
        q_ref.at[0],
        place_ref[0],
        slots,
        firsts,
        offset_ref[0],
        keys,
        bias,
        lse_ref.at[0],
        KEY_CHUNK,
        out_ref.at[0],
        low_ref.at[0],
    )


def seq_block(shape):
    return pl.BlockSpec((1,) + shape[1:], lambda s, *_: (s,) + (0,) * (len(shape) - 1))


def slot_block(shape):
    return pl.BlockSpec((shape[0], 1) + shape[2:], lambda s, *_: (0, s, 0, 0))


def attend(q, place, slots, first, offset, group):
    seqs, rows, wide = q.shape
    both = slots[0].shape[-1]
    total = rows * sum(slot.shape[0] for slot in slots)
    heads = wide // HEAD // group
    outs = (
        shape_of(q.shape, BF16),
        shape_of(q.shape, F32),
        shape_of((seqs, heads, group * rows), F32),
    )
    return pl.pallas_call(
        functools.partial(attend_body, group, len(slots)),
        out_shape=outs,
        grid_spec=pltpu.PrefetchScalarGridSpec(
            num_scalar_prefetch=2,
            grid=(seqs,),
            in_specs=[seq_block(q.shape), seq_block(place.shape)] + [slot_block(s.shape) for s in slots],
            out_specs=tuple(seq_block(o.shape) for o in outs),
            scratch_shapes=[pltpu.VMEM((total, both), BF16), pltpu.VMEM((total, rows), F32)],
        ),
        compiler_params=params(),
        cost_estimate=cost(2e9 * 4, 20e6),
        name="attend",
    )(first, offset, q, place, *slots)


def attend_back_core(
    group, q_ref, place, go_ref, out_ref, lse_ref, cosine, sine, slots, firsts, offset, keys, bias, grads, dq_ref, most
):
    rows = q_ref.shape[0]
    fill_keys(firsts, offset, place, slots, keys, bias, rows)
    total, width = keys.shape[0], keys.shape[1] // 2
    chunk = min(total, most)
    two, many = 2 * HEAD, 2 * HEAD * group

    @pl.loop(0, width // two)
    def _(pair):
        here = pair_lanes(pair, many)
        q = (q_ref[:, here].astype(F32) * SCALE).astype(BF16)
        go = go_ref[:, here]
        products = go.astype(F32) * out_ref[:, here]
        ones = jnp.ones((8, HEAD), F32)
        q3s = [group_rows(q, head, group) for head in range(2)]
        g3s = [group_rows(go, head, group) for head in range(2)]
        deltas = [
            lax.dot_general(
                ones,
                group_rows(products, head, group),
                (((1,), (1,)), ((), ())),
                preferred_element_type=F32,
                precision=lax.Precision.HIGHEST,
            )[:1]
            for head in range(2)
        ]
        dq = [None] * 2
        for low in range(0, total, chunk):
            dks, dvs = [], []
            for head in range(2):
                mine = slice(head * HEAD, (head + 1) * HEAD)
                k = keys[low : low + chunk, pair_lanes(pair, two)][:, mine]
                v = keys[low : low + chunk, pair_lanes(pair, two, width)][:, mine]
                s = mm_t(k, q3s[head]) + widen(bias[low : low + chunk, :], group * rows)
                p = jnp.exp(s - lse_ref[pl.ds(2 * pair + head, 1), :])
                dp = mm_t(v, g3s[head])
                ds = (p * (dp - deltas[head])).astype(BF16)
                dks.append(mm(ds, q3s[head]))
                dvs.append(mm(p.astype(BF16), g3s[head]))
                part = t_mm(k, ds)
                dq[head] = part if dq[head] is None else dq[head] + part
            for made, start in ((dks, 0), (dvs, width)):
                both = jnp.concatenate(made, axis=1).astype(BF16)
                for one in range(chunk // rows):
                    grad = grads[low // rows + one]
                    grad[:, pair_lanes(pair, two, start)] = both[one * rows : (one + 1) * rows]
        pieces = []
        for head in range(2):
            back = jnp.transpose(dq[head] * SCALE)
            pieces += [back[g * rows : (g + 1) * rows] for g in range(group)]
        whole = jnp.concatenate(pieces, axis=1)
        dq_ref[:, here] = rope_back(whole, widen(cosine, many), widen(sine, many)).astype(BF16)


def attend_back_body(
    group, count, first_ref, offset_ref, q_ref, place_ref, grad_ref, out_ref, lse_ref, cos_ref, sin_ref, *refs
):
    slots = single_slots(refs[:count])
    dq_ref = refs[count]
    grads = single_slots(refs[count + 1 : 2 * count + 1])
    keys, bias = refs[2 * count + 1 :]

    attend_back_core(
        group,
        q_ref.at[0],
        place_ref[0],
        grad_ref.at[0],
        out_ref.at[0],
        lse_ref.at[0],
        cos_ref[0],
        sin_ref[0],
        slots,
        [first_ref[i] for i in range(len(slots))],
        offset_ref[0],
        keys,
        bias,
        grads,
        dq_ref.at[0],
        KEY_CHUNK,
    )


def attend_back(q, place, grad, out, lse, cosine, sine, slots, first, offset, group):
    seqs, rows, _ = q.shape
    both = slots[0].shape[-1]
    total = rows * sum(slot.shape[0] for slot in slots)
    outs = (shape_of(q.shape, BF16),) + tuple(shape_of(s.shape, BF16) for s in slots)
    ins = (q, place, grad, out, lse, cosine, sine)
    got = pl.pallas_call(
        functools.partial(attend_back_body, group, len(slots)),
        out_shape=outs,
        grid_spec=pltpu.PrefetchScalarGridSpec(
            num_scalar_prefetch=2,
            grid=(seqs,),
            in_specs=[seq_block(a.shape) for a in ins] + [slot_block(s.shape) for s in slots],
            out_specs=(seq_block(outs[0].shape),) + tuple(slot_block(s.shape) for s in slots),
            scratch_shapes=[pltpu.VMEM((total, both), BF16), pltpu.VMEM((total, rows), F32)],
        ),
        compiler_params=params(),
        cost_estimate=cost(2e9 * 8, 30e6),
        name="attend_back",
    )(first, offset, *ins, *slots)
    return got[0], got[1:]


def out_body(low, w_out, part):
    part[...] = mm_t(low[...], w_out[...]).astype(BF16)


def out_project(low, w_out):
    rows, model = low.shape[0], w_out.shape[0]
    return pl.pallas_call(
        out_body,
        out_shape=shape_of((rows, model), BF16),
        compiler_params=params(),
        cost_estimate=cost(2 * rows * model * low.shape[1], 4e6),
        name="out_project",
    )(low, w_out)


def route(mid, gain, logits_of, hot):
    unit, _ = unit_rows(mid)
    low = (unit * gain).astype(BF16)
    chosen = hot > 0.5
    logits = jnp.where(chosen, logits_of(low), NEG)
    up = jnp.where(chosen, jnp.exp(logits - jnp.max(logits, axis=-1, keepdims=True)), 0.0)
    return low, up / jnp.sum(up, axis=-1, keepdims=True)


def middle_body(act, part, other, gain, router, hot, middle, normed, gates):
    mid = act[...].astype(F32) + (part[...].astype(F32) + other[...].astype(F32))
    middle[...] = mid
    normed[...], gates[...] = route(mid, gain[...], lambda v: mm(v, router[...]), hot[...])


def middle_of(act, part, other, gain, router, hot):
    rows, model = act.shape
    return pl.pallas_call(
        middle_body,
        out_shape=(shape_of((rows, model), F32), shape_of((rows, model), BF16), shape_of((rows, LANES), F32)),
        compiler_params=params(),
        cost_estimate=cost(2 * rows * model * LANES, 12 * rows * model),
        name="middle",
    )(act, part, other, gain, router, hot)


EARLY = 2
FIRST = 1
HALF = 1


def experts_body(early, first, x_own, x_par, dy_own, dy_par, g_own, g_par, w_in, w_out, keep, send, *refs):
    refs = list(refs)
    came, z_kept, z_sent = (refs.pop(0), refs.pop(0), refs.pop(0)) if early else (None, None, None)
    own_back, par_back, own_mix, par_mix, x_turned, dy_order, x_all, dy_all, back, mix, pulls, blocks_of = refs[:12]
    step, steps = pl.program_id(0), pl.num_programs(0)
    rows, model = x_own.shape
    wide = own_back.shape[1] - model
    blocks, depth, _ = blocks_of.shape
    side = lax.axis_index("cp") % 2
    if early:
        leaving, held, spots, es, er, zs, zr = refs[12:]
        p = Place()
        flows = [Flow(p, held.at[i], spots.at[i], zs.at[i], zr.at[i]) for i in range(2)]

    def early_copy(i):
        some = pl.ds(0, blocks // 2 if i < early - 1 else HALF)
        return p.copy("x", leaving.at[i, some], came.at[i, some], es.at[i], er.at[i])

    @pl.when(step == 0)
    def _():
        if early:
            p.greet(("x",))
        x_all[:rows] = x_own[...]
        x_all[rows:] = x_par[...]
        dy_all[:rows] = dy_own[...]
        dy_all[rows:] = dy_par[...]
        for rows_of, ordered in ((x_all, x_turned), (dy_all, dy_order)):
            blocks_of[...] = jnp.transpose(rows_of[...]).reshape(blocks_of.shape)
            for z in range(blocks // 2):
                ordered[z] = blocks_of[2 * z + side]
                ordered[blocks // 2 + z] = blocks_of[2 * z + 1 - side]
        back[...] = jnp.zeros_like(back)
        mix[...] = jnp.zeros_like(mix)
        pulls[...] = jnp.zeros_like(pulls)

    expert = lax.axis_index("ep") * steps + step
    lane = lax.broadcasted_iota(jnp.int32, (2 * rows, wide), 1) == expert
    gate_rows = jnp.concatenate([g_own[...], g_par[...]], axis=0)
    gate = jnp.sum(jnp.where(lane, gate_rows, 0.0), axis=-1, keepdims=True)
    x, dy = x_all[...], dy_all[...]
    w_gu, w_d = w_in[0], w_out[0]
    both = mm(x, w_gu)
    half = both.shape[1] // 2
    g, u = both[:, :half], both[:, half:]
    pull = mm(dy, w_d)
    sig = 1.0 / (1.0 + jnp.exp(-g))
    act = g * sig
    hidden = (act * u).astype(BF16).astype(F32)
    pulls[...] += jnp.where(lane, jnp.sum(hidden * pull, axis=-1, keepdims=True), 0.0)
    weighted = (gate * hidden).astype(BF16)
    pull = gate * pull
    d_g = (pull * u * sig * (1.0 + g * (1.0 - sig))).astype(BF16)
    d_u = (pull * act).astype(BF16)
    d_gu = jnp.concatenate([d_g, d_u], axis=1)
    for i, out in enumerate((keep, send)):
        at = pl.ds(i * (blocks // 2), blocks // 2)
        shape = (model // 2, 2 * rows)
        to = (blocks // 2, depth, -1)
        out[0, :, :, : 2 * half] = mm(x_turned[at].reshape(shape), d_gu).astype(BF16).reshape(to)
        out[0, :, :, 2 * half :] = mm(dy_order[at].reshape(shape), weighted).astype(BF16).reshape(to)
    if early:

        @pl.when(step == 0)
        def _():
            held[0] = keep[0]
            held[1] = send[0]
            for flow in flows:
                flow.open()

        for i in range(early):

            @pl.when(step == first + i)
            def _(i=i):
                leaving[i] = send[0]
                early_copy(i).start()

        for at, work in (
            (2, [lambda: flows[0].second(0)]),
            (3, [lambda: flows[0].second(1)]),
            (4, [flows[0].third]),
            (5, [lambda: flows[1].second(0)]),
            (6, [lambda: flows[1].second(1), flows[1].third]),
        ):

            @pl.when(step == at)
            def _(work=work):
                for one in work:
                    one()

    back[...] += mm_t(d_gu, w_gu)
    mix[...] += mm_t(weighted, w_d)

    @pl.when(step == steps - 1)
    def _():
        own_back[:, :model] = back[:rows].astype(BF16)
        par_back[:, :model] = back[rows:].astype(BF16)
        own_back[:, model:] = pulls[:rows].astype(BF16)
        par_back[:, model:] = pulls[rows:].astype(BF16)
        own_mix[...] = mix[:rows].astype(BF16)
        par_mix[...] = mix[rows:].astype(BF16)
        if early:
            for flow, out in zip(flows, (z_kept, z_sent)):

                def finish(parts, out=out):
                    sum_into(out, *parts)

                flow.close(finish)
                flow.drain()
            for i in range(early):
                early_copy(i).wait()


def experts(early, first, blocks, x_own, x_par, dy_own, dy_par, g_own, g_par, w_in, w_out):
    rows, model = x_own.shape
    count, _, half = w_out.shape
    depth = model // blocks
    once = lambda shape: pl.BlockSpec(shape, lambda e: (0,) * len(shape))
    whole = (blocks // 2, depth, 3 * half)
    ins = [x_own, x_par, dy_own, dy_par, g_own, g_par]
    apart = first + max(early - 1, 0)
    tail = [shape_of((rows, model + LANES), BF16)] * 2 + [shape_of((rows, model), BF16)] * 2
    outs = [shape_of((count - first,) + whole, BF16), shape_of((count - apart,) + whole, BF16)]
    specs = [
        pl.BlockSpec((1,) + whole, lambda e: (jnp.maximum(e - first, 0), 0, 0, 0)),
        pl.BlockSpec((1,) + whole, lambda e: (jnp.maximum(e - apart, 0), 0, 0, 0)),
    ]
    turned = (blocks, depth, 2 * rows)
    scratch = [
        pltpu.VMEM(turned, BF16),
        pltpu.VMEM(turned, BF16),
        pltpu.VMEM((2 * rows, model), BF16),
        pltpu.VMEM((2 * rows, model), BF16),
        pltpu.VMEM((2 * rows, model), F32),
        pltpu.VMEM((2 * rows, model), F32),
        pltpu.VMEM((2 * rows, LANES), F32),
        pltpu.VMEM(turned, BF16),
    ]
    kind = params()
    if early:
        dma = pltpu.SemaphoreType.DMA
        sums = [shape_of(whole[1:], F32), shape_of(whole[1:], BF16)]
        outs += [shape_of((early,) + whole, BF16)] + sums
        specs += [pl.BlockSpec(memory_space=pl.ANY)] + [once(t.shape) for t in sums]
        scratch += [
            pltpu.VMEM((early,) + whole, BF16),
            pltpu.VMEM((2,) + whole, BF16),
            pltpu.VMEM((2, 5) + whole[1:], BF16),
            dma((early,)),
            dma((early,)),
            dma((2, 6)),
            dma((2, 6)),
        ]
        kind = params(collective_id=2, has_side_effects=True)
    got = pl.pallas_call(
        functools.partial(experts_body, early, first),
        out_shape=tuple(outs + tail),
        grid=(count,),
        in_specs=[once(a.shape) for a in ins]
        + [
            pl.BlockSpec((1, model, 2 * half), lambda e: (e, 0, 0)),
            pl.BlockSpec((1, model, half), lambda e: (e, 0, 0)),
        ],
        out_specs=tuple(specs + [once(t.shape) for t in tail]),
        scratch_shapes=scratch,
        compiler_params=kind,
        cost_estimate=cost(count * 18 * 2 * rows * model * half, count * 12 * model * half),
        name="experts",
    )(*ins, w_in, w_out)
    return got[: len(outs)], got[len(outs) :]


def middle_back_body(mine, other, middle, dy, gates, router, gain, w_out, normed, grad, low, heads, small):
    model = middle.shape[1]
    total = mine[...].astype(F32) + other[...].astype(F32)
    gate, pulls = gates[...], total[:, model:]
    chosen = gate * (pulls - jnp.sum(gate * pulls, axis=-1, keepdims=True))
    high, rest = two_parts(chosen)
    grad_two = total[:, :model] + (mm_t(high, router[...]) + mm_t(rest, router[...]))
    unit, scale = unit_rows(middle[...])
    small[:LANES, :] = t_mm(high, normed[...]) + t_mm(rest, normed[...])
    small[LANES : LANES + 8, :] = jnp.broadcast_to(jnp.sum(grad_two * unit, axis=0, keepdims=True), (8, model))
    scaled = grad_two * gain[...]
    out = dy[...].astype(F32) + scale * (scaled - unit * jnp.mean(scaled * unit, axis=-1, keepdims=True))
    grad[...] = out
    rounded = out.astype(BF16)
    low[...] = rounded
    heads[...] = mm(rounded, w_out[...]).astype(BF16)


def middle_back(mine, other, middle, dy, gates, router, gain, w_out, normed):
    rows, model = middle.shape
    return pl.pallas_call(
        middle_back_body,
        out_shape=(
            shape_of((rows, model), F32),
            shape_of((rows, model), BF16),
            shape_of((rows, w_out.shape[1]), BF16),
            shape_of((LANES + 8, model), F32),
        ),
        compiler_params=params(),
        cost_estimate=cost(2 * rows * model * (w_out.shape[1] + 4 * LANES), 10e6),
        name="middle_back",
    )(mine, other, middle, dy, gates, router, gain, w_out, normed)


def project_back_body(width, act, dq, a, b, c, cosine, sine, wq, wk, wv, part, dkv, gain_row):
    total = a[...].astype(F32) + b[...].astype(F32) + c[...].astype(F32)
    dk = rope_back(total[:, :width], widen(cosine[...], width), widen(sine[...], width)).astype(BF16)
    dv = total[:, width:].astype(BF16)
    dkv[:, :width] = dk
    dkv[:, width:] = dv
    full = mm_t(dq[...], wq[...]) + mm_t(dk, wk[...]) + mm_t(dv, wv[...])
    part[...] = full.astype(BF16)
    unit, _ = unit_rows(act[...].astype(F32))
    gain_row[...] = jnp.broadcast_to(jnp.sum(full * unit, axis=0, keepdims=True), gain_row.shape)


def project_back(act, dq, a, b, c, cosine, sine, wq, wk, wv):
    rows, model = act.shape
    width = wk.shape[1]
    return pl.pallas_call(
        functools.partial(project_back_body, width),
        out_shape=(
            shape_of((rows, model), BF16),
            shape_of((rows, 2 * width), BF16),
            shape_of((8, model), F32),
        ),
        compiler_params=params(),
        cost_estimate=cost(2 * rows * model * (wq.shape[1] + 2 * width), 8e6),
        name="project_back",
    )(act, dq, a, b, c, cosine, sine, wq, wk, wv)


def input_body(act, grad, mine, other, gain, out):
    unit, scale = unit_rows(act[...].astype(F32))
    scaled = (mine[...].astype(F32) + other[...].astype(F32)) * gain[...]
    out[...] = grad[...] + scale * (scaled - unit * jnp.mean(scaled * unit, axis=-1, keepdims=True))


def input_of(act, grad, mine, other, gain):
    return pl.pallas_call(
        input_body,
        out_shape=shape_of(act.shape, F32),
        compiler_params=params(),
        cost_estimate=cost(0, 12 * act.shape[0] * act.shape[1]),
        name="input_grad",
    )(act, grad, mine, other, gain)


def weights_body(blocks, count, stacked, where_ref, *refs):
    lefts = refs[:count]
    rights = refs[count : 2 * count]
    extra = refs[2 * count : -3]
    keep, send, whole = refs[-3:]
    parts = [t_mm(a[...], b[...]).astype(BF16) for a, b in zip(lefts, rights)]
    parts += [jnp.transpose(e[...]).astype(BF16) for e in extra]
    at = down = 0
    for part in parts:
        block = part.reshape(2 * blocks, -1, part.shape[1])
        whole[:, down : down + block.shape[1], at : at + part.shape[1]] = block
        if stacked:
            down += block.shape[1]
        else:
            at += part.shape[1]
    mine, side = where_ref[0], where_ref[1]
    for half, ref in ((mine, keep), (1 - mine, send)):
        for z in range(blocks // 2):
            ref[0, z] = whole[half * blocks + 2 * z + side]
            ref[1, z] = whole[half * blocks + 2 * z + 1 - side]


def weights(where, blocks, pairs, extra=(), stacked=False):
    model = pairs[0][0].shape[1]
    rows = pairs[0][0].shape[0]
    depth = model // (2 * blocks)
    columns = sum(b.shape[1] for _, b in pairs) + sum(e.shape[0] for e in extra)
    tall, wide = (depth * len(pairs), pairs[0][1].shape[1]) if stacked else (depth, columns)
    shape = (2, blocks // 2, tall, wide)
    ins = [a for a, _ in pairs] + [b for _, b in pairs] + list(extra)
    full = lambda a: pl.BlockSpec(a.shape, lambda i, *_: (0,) * len(a.shape))
    return pl.pallas_call(
        functools.partial(weights_body, blocks, len(pairs), stacked),
        out_shape=(shape_of(shape, BF16),) * 2,
        grid_spec=pltpu.PrefetchScalarGridSpec(
            num_scalar_prefetch=1,
            grid=(1,),
            in_specs=[full(a) for a in ins],
            out_specs=(pl.BlockSpec(shape, lambda i, *_: (0, 0, 0, 0)),) * 2,
            scratch_shapes=[pltpu.VMEM((2 * blocks, tall, wide), BF16)],
        ),
        compiler_params=params(),
        cost_estimate=cost(2 * rows * model * columns, 4 * model * columns),
        name="weights",
    )(where, *ins)


def swap(v, axis):
    size = lax.axis_size(axis)
    return lax.ppermute(v, axis, [(i, i ^ 1) for i in range(size)])


def up(v, low, high):
    return lax.ppermute(v, "cp", [(2 * z + s, 2 * z + 2 + s) for z in range(low, high) for s in range(2)])


def down(v, low, high):
    return lax.ppermute(v, "cp", [(2 * z + s, 2 * z - 2 + s) for z in range(low, high) for s in range(2)])


def total_of(terms):
    return functools.reduce(lambda a, b: a + b, [t.astype(F32) for t in terms])


def line_sum(parts, z, length):
    def own(d):
        return [lax.dynamic_index_in_dim(p, jnp.clip(d, 0, length - 1), 0, keepdims=False) for p in parts]

    if length > 4:
        mine = total_of(parts).astype(BF16)
        side = lax.axis_index("cp") % 2
        full = jnp.where(jnp.arange(2).reshape((1, 2) + (1,) * (mine.ndim - 1)) == side, mine[:, None], 0)
        full = full.reshape((2 * length,) + mine.shape[1:])
        return lax.psum_scatter(full, "cp", scatter_dimension=0, tiled=True)[0].astype(F32)
    right = left = None
    for k in range(length - 1):
        far = length - 1 - k
        terms = own(z + far) + ([] if right is None else [right])
        right = up(total_of(terms).astype(BF16), 0, k + 1)
        terms = own(z - far) + ([] if left is None else [left])
        left = down(total_of(terms).astype(BF16), far, length)
    return total_of(own(z) + ([right, left] if length > 1 else []))


LINE = 4
RING = 6


def sum_into(out, *parts):
    few = 48 if out.shape[0] % 48 == 0 else out.shape[0]

    @pl.loop(0, out.shape[0] // few)
    def _(k):
        at = pl.ds(pl.multiple_of(k * few, few), few)
        out[at] = total_of([part[at] for part in parts]).astype(out.dtype)


def add_into(ref, other):
    sum_into(ref, ref, other)


class Place:
    def __init__(self):
        self.cp = lax.axis_index("cp")
        self.z, self.side = self.cp // 2, self.cp % 2
        self.ep, self.tp = lax.axis_index("ep"), lax.axis_index("tp")

    def to(self, way):
        if way == "x":
            return {"cp": self.cp + 1 - 2 * self.side}
        if way == "up":
            return {"cp": self.cp + 2}
        if way == "down":
            return {"cp": self.cp - 2}
        return {way: 1 - (self.ep if way == "ep" else self.tp)}

    def signal(self, sem, way):
        pl.semaphore_signal(sem, inc=1, device_id=self.to(way), device_id_type=MESH)

    def signal_line(self, to_down, to_up):
        @pl.when(self.z > 0)
        def _():
            self.signal(to_down, "down")

        @pl.when(self.z < LINE - 1)
        def _():
            self.signal(to_up, "up")

    def greet(self, ways):
        barrier = pltpu.get_barrier_semaphore()
        for way in ways:
            self.signal(barrier, way)
        self.signal_line(barrier, barrier)
        both = jnp.where(self.z > 0, 1, 0) + jnp.where(self.z < LINE - 1, 1, 0)
        pl.semaphore_wait(barrier, len(ways) + both)

    def copy(self, way, src, dst, send, recv):
        return pltpu.make_async_remote_copy(
            src_ref=src, dst_ref=dst, send_sem=send, recv_sem=recv, device_id=self.to(way), device_id_type=MESH
        )

    def at(self, z):
        return pl.when(self.z == z)


LEFT_SPOT = (3, 4, 0)


class Flow:
    def __init__(self, place, held, spots, send, recv, credit=None):
        self.p, self.held, self.spots, self.send, self.recv, self.credit = place, held, spots, send, recv, credit

    def right(self, d):
        return self.p.copy("up", self.held.at[d], self.spots.at[d - 1], self.send.at[d - 1], self.recv.at[d - 1])

    def left(self, d):
        spot = LEFT_SPOT[d]
        return self.p.copy("down", self.held.at[d], self.spots.at[spot], self.send.at[d + 3], self.recv.at[d + 3])

    def allowed(self, way):
        if self.credit is not None:
            pl.semaphore_wait(self.credit[way], 1)

    def open(self):
        @self.p.at(0)
        def _():
            self.allowed("up")
            for d in (3, 2, 1):
                self.right(d).start()

        @self.p.at(3)
        def _():
            self.allowed("down")
            for d in (0, 1, 2):
                self.left(d).start()

    def pass_right(self, d):
        self.right(d).wait_recv()
        add_into(self.held.at[d], self.spots.at[d - 1])
        self.right(d).start()

    def pass_left(self, d):
        self.left(d).wait_recv()
        add_into(self.held.at[d], self.spots.at[LEFT_SPOT[d]])
        self.left(d).start()

    def second(self, only=None):
        @self.p.at(1)
        def _():
            if only != 1:
                self.allowed("up")
                self.pass_right(3)
            if only != 0:
                self.pass_right(2)

        @self.p.at(2)
        def _():
            if only != 1:
                self.allowed("down")
                self.pass_left(0)
            if only != 0:
                self.pass_left(1)

    def third(self):
        @self.p.at(2)
        def _():
            self.allowed("up")
            self.pass_right(3)

        @self.p.at(1)
        def _():
            self.allowed("down")
            self.pass_left(0)

    def close(self, finish):
        for z in range(LINE):

            @self.p.at(z)
            def _(z=z):
                blocks = [self.held.at[z]]
                if z > 0:
                    self.right(z).wait_recv()
                    blocks.append(self.spots.at[z - 1])
                if z < LINE - 1:
                    self.left(z).wait_recv()
                    blocks.append(self.spots.at[LEFT_SPOT[z]])
                finish(blocks)

    def drain(self):
        for z in range(LINE):

            @self.p.at(z)
            def _(z=z):
                for d in range(z + 1, LINE):
                    self.right(d).wait_send()
                for d in range(z):
                    self.left(d).wait_send()


class BackIns(NamedTuple):
    own_back: Any
    par_back: Any
    own_mix: Any
    par_mix: Any
    middle: Any
    dy: Any
    router: Any
    w_out: Any
    x2: Any
    q: Any
    attended: Any
    act: Any
    normed: Any
    low: Any
    wq: Any
    wk: Any
    wv: Any
    gates: Any
    gains: Any
    place: Any
    lse: Any
    cosine: Any
    sine: Any


BACK_IN_PLACE = 6
class BackOuts(NamedTuple):
    grad: Any
    mix: Any
    experts: Any
    big_out: Any
    little_out: Any


class BackScratch(NamedTuple):
    back: Any
    other_ep: Any
    other_tp: Any
    mid_dy: Any
    mid_x2: Any
    wide_w: Any
    branch: Any
    heads: Any
    small: Any
    qs: Any
    atts: Any
    slots: Any
    kv_x: Any
    kv_z: Any
    keys: Any
    bias: Any
    dq: Any
    lows: Any
    wks: Any
    wvs: Any
    routers: Any
    dkv: Any
    part: Any
    part_in: Any
    mix_ep: Any
    mix_tp: Any
    held: Any
    spots: Any
    kept: Any
    staged: Any
    zero_in: Any
    whole: Any
    came: Any
    lit: Any
    lit_came: Any
    lit_x: Any
    lit_spots: Any
    ls: Any
    ks: Any
    xs: Any
    xr: Any
    zs: Any
    zr: Any
    es: Any
    er: Any
    ts: Any
    tr: Any
    kxs: Any
    kxr: Any
    kzs: Any
    kzr: Any
    os: Any
    free_x: Any
    free_up: Any
    free_down: Any


def back_body(group, *refs):
    n_in = len(BackIns._fields) + 6
    ins = BackIns(*refs[: len(BackIns._fields)])
    slots_in = refs[n_in - 6]
    keeps, sends, arrived, z_kept, z_sent = refs[n_in - 5 : n_in]
    o = BackOuts(*refs[n_in : n_in + len(BackOuts._fields)])
    s = BackScratch(*refs[n_in + len(BackOuts._fields) :])
    p = Place()
    early = arrived.shape[0]
    first = FIRST
    count = first + keeps.shape[0]
    seqs, rows, _ = ins.q.shape
    model = ins.middle.shape[1]
    width = ins.wk.shape[1]
    part_of = lambda i: pl.ds(i * rows if isinstance(i, int) else pl.multiple_of(i * rows, rows), rows)

    whole_early = early - 1
    ring = [("here", e) for e in range(first, first + whole_early)] + [("half", first + whole_early)]
    ring += [("x", e) for e in range(first + early, count)] + [("big", 0), ("big", 1)]
    index_of = {item: i for i, item in enumerate(ring)}
    crosses = lambda item: item[0] != "here"

    short = model // 16

    def big_part_of(ref, i):
        return ref.at[i % RING, :, pl.ds(0, short)]

    def lit_columns(item):
        return pl.ds(0, 3 * LANES) if item[1] == 0 else pl.ds(3 * LANES, 2 * width - 2 * LANES)

    def big_rows(item):
        return pl.ds(item[1] * short, short)

    def flow(item):
        if item[0] == "lit":
            k, cols = len(ring) + item[1], lit_columns(item)
            return Flow(p, s.lit_x.at[:, :, cols], s.lit_spots.at[:, :, cols], s.zs.at[k], s.zr.at[k])
        i = index_of[item]
        credit = {"up": s.free_up, "down": s.free_down} if i >= RING else None
        if item[0] == "big":
            return Flow(p, big_part_of(s.held, i), big_part_of(s.spots, i), s.zs.at[i], s.zr.at[i], credit)
        return Flow(p, s.held.at[i % RING], s.spots.at[i % RING], s.zs.at[i], s.zr.at[i], credit)

    def x_copy(item):
        if item[0] == "lit":
            k, cols = len(ring) + item[1], lit_columns(item)
            src = s.lit.at[p.ep, :, 1 - p.side, :, cols]
            return p.copy("x", src, s.lit_x.at[:, :, cols], s.xs.at[k], s.xr.at[k])
        i = index_of[item]
        if item[0] == "half":
            some = pl.ds(HALF, LINE - HALF)
            return p.copy("x", sends.at[0, some], s.held.at[i, some], s.xs.at[i], s.xr.at[i])
        if item[0] == "big":
            src = s.whole.at[p.ep, :, 1 - p.side, big_rows(item)]
            return p.copy("x", src, big_part_of(s.held, i), s.xs.at[i], s.xr.at[i])
        src = sends.at[item[1] - first - whole_early]
        return p.copy("x", src, s.held.at[i % RING], s.xs.at[i], s.xr.at[i])

    def cross(item):
        if item[0] != "lit" and index_of[item] >= RING:
            pl.semaphore_wait(s.free_x, 1)
        x_copy(item).start()

    def load_keep(e):
        return pltpu.make_async_copy(keeps.at[e - first], s.kept, s.ks.at[0])

    def load_arrived(e):
        if e == first + whole_early:
            some = pl.ds(0, HALF)
            return pltpu.make_async_copy(
                arrived.at[e - first, some], s.held.at[e - first, some], s.ks.at[1 + e - first]
            )
        return pltpu.make_async_copy(arrived.at[e - first], s.held.at[e - first], s.ks.at[1 + e - first])

    def opened(item):
        if item[0] == "lit":
            cols = lit_columns(item)
            x_copy(item).wait_recv()
            for d in range(LINE):
                add_into(s.lit_x.at[d, :, cols], s.lit.at[p.ep, d, p.side, :, cols])
        else:
            held = s.held.at[index_of[item] % RING]
            if item[0] in ("here", "half"):
                load_arrived(item[1]).wait()
            if item[0] != "here":
                x_copy(item).wait_recv()
            if item[0] == "big":
                for d in range(LINE):
                    add_into(
                        big_part_of(s.held, index_of[item]).at[d], s.whole.at[p.ep, d, p.side, big_rows(item)]
                    )
            else:
                load_keep(item[1]).wait()
                for d in range(LINE):
                    add_into(held.at[d], s.kept.at[d])
                if item[1] + 1 < count:
                    load_keep(item[1] + 1).start()
        flow(item).open()

    stored = []

    def store(e):
        return pltpu.make_async_copy(s.staged.at[e % 2], o.experts.at[e], s.os.at[e])

    def finish_expert(e, make):
        if len(stored) >= 2 and e % 2 in [k % 2 for k in stored[-2:]]:
            last = [k for k in stored if k % 2 == e % 2][-1]
            store(last).wait()
            waited.add(last)
        make()
        store(e).start()
        stored.append(e)

    waited = set()

    def closed(item):
        if item[0] == "lit":
            def finish(blocks):
                sum_into(o.little_out.at[:, lit_columns(item)], *blocks)

            flow(item).close(finish)
        elif item[0] == "big":
            def finish(blocks):
                sum_into(o.big_out.at[big_rows(item)], *blocks)

            flow(item).close(finish)
        else:
            def finish(blocks):
                sum_into(s.staged.at[item[1] % 2], *blocks)

            finish_expert(item[1], lambda: flow(item).close(finish))

    def freed(item):
        flow(item).drain()
        if item[0] == "lit":
            return
        after = index_of[item] + RING
        if after < len(ring):
            if crosses(item):
                x_copy(item).wait_send()
            if crosses(ring[after]):
                p.signal(s.free_x, "x")
            p.signal_line(s.free_up, s.free_down)

    loads = {}

    def load(name, src, dst):
        copy = pltpu.make_async_copy(src, dst, s.ls.at[len(loads)])
        copy.start()
        loads[name] = copy

    def got(*names):
        for name in names:
            loads[name].wait()

    load("back", ins.own_back, s.back)
    load_keep(first).start()
    for e in range(first, first + early):
        load_arrived(e).start()
    load("zero", z_kept, s.staged.at[0])
    load("grad", ins.middle, o.grad)
    load("dy", ins.dy, s.mid_dy)
    load("router", ins.router, s.routers)
    load("x2", ins.x2, s.mid_x2)
    load("w_out", ins.w_out, s.wide_w)
    load("mix", ins.own_mix, o.mix)
    load("q", ins.q, s.qs)
    load("attended", ins.attended, s.atts)
    load("slots", slots_in, s.slots)
    load("low", ins.low, s.lows)
    load("wk", ins.wk, s.wks)
    load("wv", ins.wv, s.wvs)

    p.greet(("x", "ep", "tp"))
    ep_back = p.copy("ep", ins.par_back, s.other_ep, s.es.at[0], s.er.at[0])
    ep_back.start()
    ep_mix = p.copy("ep", ins.par_mix, s.mix_ep, s.es.at[1], s.er.at[1])
    ep_mix.start()
    lits = [("lit", 0), ("lit", 1)]
    queue = ring[whole_early:] + lits
    zero_copy = p.copy("x", z_sent, s.zero_in, s.xs.at[len(ring) + 2], s.xr.at[len(ring) + 2])
    zero_copy.start()
    for _ in range(3):
        cross(queue.pop(0))

    got("back")
    ep_back.wait_recv()
    for i in range(seqs):
        s.back[part_of(i)] = (
            s.back[part_of(i)].astype(F32) + s.other_ep[part_of(i)].astype(F32)
        ).astype(BF16)
    tp_back = p.copy("tp", s.back, s.other_tp, s.ts.at[0], s.tr.at[0])
    tp_back.start()
    got("mix")
    ep_mix.wait_recv()
    for i in range(seqs):
        o.mix[part_of(i)] = (o.mix[part_of(i)].astype(F32) + s.mix_ep[part_of(i)].astype(F32)).astype(BF16)

    def step_middle():
        got("grad", "dy", "router", "x2", "w_out")
        tp_back.wait_recv()
        s.small[...] = jnp.zeros_like(s.small)

        @pl.loop(0, seqs)
        def _(i):
            at = pl.ds(pl.multiple_of(i * rows, rows), rows)
            total = s.back[at].astype(F32) + s.other_tp[at].astype(F32)
            gate, pulls = ins.gates[at], total[:, model:]
            chosen = gate * (pulls - jnp.sum(gate * pulls, axis=-1, keepdims=True))
            high, rest = two_parts(chosen)
            grad_two = total[:, :model] + (mm(high, s.routers[...]) + mm(rest, s.routers[...]))
            unit, scale = unit_rows(o.grad[at])
            s.small[...] += t_mm(high, s.mid_x2[at]) + t_mm(rest, s.mid_x2[at])
            s.small[LANES - 1 :, :] += jnp.sum(grad_two * unit, axis=0, keepdims=True)
            scaled = grad_two * ins.gains[1:]
            out = s.mid_dy[at].astype(F32) + scale * (
                scaled - unit * jnp.mean(scaled * unit, axis=-1, keepdims=True)
            )
            o.grad[at] = out
            rounded = out.astype(BF16)
            s.branch[at] = rounded
            s.heads[at] = mm(rounded, s.wide_w[...]).astype(BF16)

        load("wq", ins.wq, s.wide_w)
        load("act", ins.act, s.mid_dy)
        load("normed", ins.normed, s.mid_x2)

    tp_mix = p.copy("tp", o.mix, s.mix_tp, s.ts.at[1], s.tr.at[1])

    def step_attend():
        got("q", "attended", "slots")
        homes = [(p.z - r, side) for r in range(LINE) for side in (p.side, 1 - p.side)]
        firsts = [jnp.where(a >= 0, (2 * a + b) * rows, 2**24) for a, b in homes]

        @pl.loop(0, seqs)
        def _(i):
            at = pl.ds(pl.multiple_of(i * rows, rows), rows)

            singles = [s.slots.at[i, j // 2, j % 2] for j in range(2 * LINE)]
            attend_back_core(
                group,
                s.qs.at[i],
                ins.place[i],
                s.heads.at[at],
                s.atts.at[i],
                ins.lse.at[i],
                ins.cosine[at],
                ins.sine[at],
                singles,
                firsts,
                p.cp * rows,
                s.keys,
                s.bias,
                singles,
                s.dq.at[i],
                512,
            )

            @p.at(LINE - 1)
            def _():
                for r in range(LINE - 1, 0, -1):
                    kv_down(i, r).start()

    def kv_cross(i):
        return p.copy("x", s.slots.at[i, 0, 1], s.kv_x.at[i], s.kxs.at[i], s.kxr.at[i])

    def kv_down(i, r):
        return p.copy("down", s.slots.at[i, r], s.kv_z.at[i, r - 1], s.kzs.at[i, r - 1], s.kzr.at[i, r - 1])

    def kv_take(i, r):
        kv_down(i, r + 1).wait_recv()
        for way in range(2):
            s.slots[i, r, way] = (s.slots[i, r, way].astype(F32) + s.kv_z[i, r, way].astype(F32)).astype(BF16)

    def keys_pass(i, z):
        @p.at(z)
        def _():
            for r in range(z, 0, -1):
                kv_take(i, r)
                kv_down(i, r).start()

    def keys_cross(i):
        @pl.when(p.z < LINE - 1)
        def _():
            kv_take(i, 0)

        kv_cross(i).start()

    def keys_close(i):
        kv_cross(i).wait_recv()
        s.slots[i, 0, 0] = (s.slots[i, 0, 0].astype(F32) + s.kv_x[i].astype(F32)).astype(BF16)

    def part_copy(i):
        return p.copy("tp", s.part.at[part_of(i)], s.part_in.at[part_of(i)], s.ts.at[2 + i], s.tr.at[2 + i])

    def step_project(i):
        if i == 0:
            got("wq", "wk", "wv", "act", "normed")
        at = part_of(i)
        total = s.slots[i, 0, 0].astype(F32)
        dk = rope_back(total[:, :width], widen(ins.cosine[at], width), widen(ins.sine[at], width)).astype(BF16)
        dv = total[:, width:].astype(BF16)
        s.dkv[at, :width] = dk
        s.dkv[at, width:] = dv
        full = mm_t(s.dq[i], s.wide_w[...]) + mm_t(dk, s.wks[...]) + mm_t(dv, s.wvs[...])
        s.part[at] = full.astype(BF16)
        part_copy(i).start()

    tall = model // 4

    def pieces(make, keep):
        @pl.loop(0, 4)
        def _(piece):
            got_piece = make(pl.ds(pl.multiple_of(piece * tall, tall), tall)).astype(BF16)
            block = got_piece.reshape(4, short, got_piece.shape[1])
            for b in range(4):
                keep(piece // 2, 2 * (piece % 2) + b // 2, b % 2, block[b])

    def big_part(row):
        def keep(half, z, side, value):
            s.whole[half, z, side, row : row + value.shape[0], :] = value

        return keep

    def little_part(column):
        def keep(half, z, side, value):
            s.lit[half, z, side, :, column : column + value.shape[1]] = value

        return keep

    ep_big = p.copy("ep", s.whole.at[1 - p.ep], s.came, s.es.at[2], s.er.at[2])
    ep_lit = p.copy("ep", s.lit.at[1 - p.ep], s.lit_came, s.es.at[3], s.er.at[3])

    def step_out_weight():
        got("low")
        pieces(lambda at: t_mm(s.branch[:, at], s.lows[...]), big_part(0))

    def step_query_weight():
        got("normed")
        loads["normed"] = Done()
        query = jnp.concatenate([s.dq[i] for i in range(seqs)], axis=0)
        pieces(lambda at: t_mm(s.mid_x2[:, at], query), big_part(short))
        ep_big.start()

    def step_key_weight():
        pieces(lambda at: t_mm(s.mid_x2[:, at], s.dkv[...]), little_part(0))
        pieces(lambda at: jnp.transpose(s.small[:, at]), little_part(2 * width))
        ep_lit.start()

    def step_big_cores():
        ep_big.wait_recv()
        for side in range(2):

            @pl.loop(0, LINE)
            def _(d):
                add_into(s.whole.at[p.ep, d, side], s.came.at[d, side])

    def step_little_cores():
        ep_lit.wait_recv()
        for side in range(2):

            @pl.loop(0, LINE)
            def _(d):
                add_into(s.lit.at[p.ep, d, side], s.lit_came.at[d, side])

    def step_input():
        for i in range(seqs):
            at = part_of(i)
            part_copy(i).wait_recv()
            unit, scale = unit_rows(s.mid_dy[at].astype(F32))
            whole = s.part[at].astype(F32) + s.part_in[at].astype(F32)
            gain_row = jnp.sum(whole * unit, axis=0, keepdims=True)
            if i == 0:
                s.small[LANES - 2 : LANES - 1, :] = gain_row
            else:
                s.small[LANES - 2 : LANES - 1, :] += gain_row
            scaled = whole * ins.gains[:1]
            o.grad[at] = o.grad[at] + scale * (scaled - unit * jnp.mean(scaled * unit, axis=-1, keepdims=True))

    def step_mix():
        tp_mix.wait_recv()
        tp_mix.wait_send()
        for i in range(seqs):
            o.mix[part_of(i)] = (o.mix[part_of(i)].astype(F32) + s.mix_tp[part_of(i)].astype(F32)).astype(BF16)

    line = list(ring) + lits
    stage = {item: 0 for item in line}

    def advance(at, to):
        if not 0 <= at < len(line):
            return
        item = line[at]
        while stage[item] < to:
            now = stage[item]
            if now == 0:
                opened(item)
            elif now == 1:
                flow(item).second()
            elif now == 2:
                flow(item).third()
            elif now == 3:
                closed(item)
            elif now == 4:
                freed(item)
            stage[item] = now + 1

    def turn(at):
        for back in (4, 3, 2, 1, 0):
            advance(at - back, back + 1)

    def add_zero():
        got("zero")
        zero_copy.wait_recv()
        s.staged[0] = s.staged[0] + s.zero_in[...].astype(F32)

    tp_mix.start()
    turn(0)
    finish_expert(0, add_zero)
    turn(1)
    step_middle()
    advance(0, 3)
    advance(1, 2)
    step_attend()
    cross(queue.pop(0))
    step_out_weight()
    step_query_weight()
    turn(2)
    keys_pass(0, 2)
    advance(0, 4)
    advance(1, 3)
    keys_pass(1, 2)
    advance(2, 2)
    step_big_cores()
    step_mix()
    keys_pass(0, 1)
    keys_pass(1, 1)
    turn(3)
    keys_cross(0)
    keys_cross(1)
    cross(queue.pop(0))
    turn(4)
    cross(queue.pop(0))
    keys_close(0)
    step_project(0)
    keys_close(1)
    step_project(1)
    advance(2, 4)
    advance(3, 3)
    advance(4, 2)
    step_input()
    step_key_weight()
    turn(5)
    cross(queue.pop(0))
    step_little_cores()
    for at in range(6, len(line) + 4):
        turn(at)
        if queue:
            cross(queue.pop(0))
    for e in stored:
        if e not in waited:
            store(e).wait()
    for item in line:
        if item[0] == "lit" or (crosses(item) and index_of[item] + RING >= len(ring)):
            x_copy(item).wait_send()
    for i in range(seqs):
        kv_cross(i).wait_send()
        part_copy(i).wait_send()
        for z in range(1, LINE):

            @p.at(z)
            def _(z=z):
                for r in range(z, 0, -1):
                    kv_down(i, r).wait_send()

    tp_back.wait_send()
    zero_copy.wait_send()
    for copy in (ep_back, ep_mix, ep_big, ep_lit):
        copy.wait_send()


class Done:
    def wait(self):
        return None


def back_and_sums(ins, slots, chunks, group):
    keeps, _, arrived, *_ = chunks
    _, length, depth, wide = keeps.shape
    early, count = arrived.shape[0], FIRST + keeps.shape[0]
    block = (length, depth, wide)
    v = BackIns(*ins)
    rows, model = v.middle.shape
    seqs, each, heads = v.q.shape
    width = v.wk.shape[1]
    both = 2 * width
    small = (length, 2, model // 16, both + LANES)
    n_ring = count - FIRST + 2
    anywhere = pl.BlockSpec(memory_space=pl.ANY)
    inside = pl.BlockSpec(memory_space=pltpu.VMEM)
    dma, vm = pltpu.SemaphoreType.DMA, pltpu.VMEM
    flag = pltpu.SemaphoreType.REGULAR
    scratch = dict(
        back=vm((rows, model + LANES), BF16),
        other_ep=vm((rows, model + LANES), BF16),
        other_tp=vm((rows, model + LANES), BF16),
        mid_dy=vm((rows, model), BF16),
        mid_x2=vm((rows, model), BF16),
        wide_w=vm((model, heads), BF16),
        branch=vm((rows, model), BF16),
        heads=vm((rows, heads), BF16),
        small=vm((LANES, model), F32),
        qs=vm((seqs, each, heads), BF16),
        atts=vm((seqs, each, heads), F32),
        slots=vm((seqs, LINE, 2, each, both), BF16),
        kv_x=vm((seqs, each, both), BF16),
        kv_z=vm((seqs, LINE - 1, 2, each, both), BF16),
        keys=vm((2 * LINE * each, both), BF16),
        bias=vm((2 * LINE * each, each), F32),
        dq=vm((seqs, each, heads), BF16),
        lows=vm((rows, heads), BF16),
        wks=vm((model, width), BF16),
        wvs=vm((model, width), BF16),
        routers=vm((LANES, model), BF16),
        dkv=vm((rows, both), BF16),
        part=vm((rows, model), BF16),
        part_in=vm((rows, model), BF16),
        mix_ep=vm((rows, model), BF16),
        mix_tp=vm((rows, model), BF16),
        held=vm((RING,) + block, BF16),
        spots=vm((RING, 5, depth, wide), BF16),
        kept=vm(block, BF16),
        staged=vm((2, depth, wide), F32),
        zero_in=vm((depth, wide), BF16),
        whole=vm((2, length, 2, depth, wide), BF16),
        came=vm((length, 2, depth, wide), BF16),
        lit=vm((2,) + small, BF16),
        lit_came=vm(small, BF16),
        lit_x=vm((small[0],) + small[2:], BF16),
        lit_spots=vm((5,) + small[2:], BF16),
        ls=dma((28,)),
        ks=dma((1 + early,)),
        xs=dma((n_ring + 3,)),
        xr=dma((n_ring + 3,)),
        zs=dma((n_ring + 2, 6)),
        zr=dma((n_ring + 2, 6)),
        es=dma((4,)),
        er=dma((4,)),
        ts=dma((4,)),
        tr=dma((4,)),
        kxs=dma((2,)),
        kxr=dma((2,)),
        kzs=dma((2, 3)),
        kzr=dma((2, 3)),
        os=dma((count,)),
        free_x=flag,
        free_up=flag,
        free_down=flag,
    )
    return pl.pallas_call(
        functools.partial(back_body, group),
        out_shape=(
            shape_of((rows, model), F32),
            shape_of((rows, model), BF16),
            shape_of((count, depth, wide), F32),
            shape_of((depth, wide), F32),
            shape_of(small[2:], F32),
        ),
        in_specs=[anywhere] * (len(BackIns._fields) - BACK_IN_PLACE)
        + [inside] * BACK_IN_PLACE
        + [anywhere] * 6,
        out_specs=(inside, inside, anywhere, inside, inside),
        scratch_shapes=[scratch[name] for name in BackScratch._fields],
        compiler_params=pltpu.CompilerParams(
            collective_id=1, has_side_effects=True, vmem_limit_bytes=67_043_328
        ),
        name="back_and_sums",
    )(*ins, slots, *chunks)


def results_body(
    middle, mix, grad, chunk, big, little, out, grad_in, first, second, keys, values, router, one, two, both, down
):
    out[...] = middle[...] + mix[...].astype(F32)
    grad_in[...] = grad[...]
    half = down.shape[2]
    both[0] = chunk[0, :, : 2 * half].reshape(both.shape[1:])
    down[0] = chunk[0, :, 2 * half :]

    @pl.when(pl.program_id(0) == 0)
    def _():
        tall, width = first.shape[0], keys.shape[1]
        first[...] = big[:tall]
        second[...] = big[tall:]
        keys[...] = little[:, :width]
        values[...] = little[:, width : 2 * width]
        small = jnp.transpose(little[:, 2 * width :])
        router[...] = small[: router.shape[0]]
        one[...] = small[LANES - 2 : LANES - 1]
        two[...] = small[LANES - 1 :]


def results(middle, mix, grad, chunks, big, little, half, expert_count):
    rows, model = middle.shape
    count, depth, wide = chunks.shape
    tall, width = big.shape[0] // 2, (little.shape[1] - LANES) // 2
    part = pl.BlockSpec((rows // count, model), lambda e: (e, 0))
    once = lambda shape: pl.BlockSpec(shape, lambda e: (0,) * len(shape))
    whole = [(tall, big.shape[1])] * 2 + [(tall, width)] * 2 + [(expert_count, tall), (1, tall), (1, tall)]
    return pl.pallas_call(
        results_body,
        grid=(count,),
        out_shape=[shape_of((rows, model), F32)] * 2
        + [shape_of(shape, F32) for shape in whole]
        + [shape_of((count, depth, 2, half), F32), shape_of((count, depth, half), F32)],
        in_specs=[part] * 3
        + [pl.BlockSpec((1, depth, wide), lambda e: (e, 0, 0)), once(big.shape), once(little.shape)],
        out_specs=[part] * 2
        + [once(shape) for shape in whole]
        + [
            pl.BlockSpec((1, depth, 2, half), lambda e: (e, 0, 0, 0)),
            pl.BlockSpec((1, depth, half), lambda e: (e, 0, 0)),
        ],
        compiler_params=params(),
        name="results",
    )(middle, mix, grad, chunks, big, little)


class FrontIns(NamedTuple):
    q: Any
    kv: Any
    act: Any
    routes: Any
    router: Any
    gain: Any
    place: Any
    w_out: Any
    dy: Any
    w_in: Any


class FrontOuts(NamedTuple):
    slots: Any
    low: Any
    attended: Any
    lse: Any
    middle: Any
    normed: Any
    gates: Any
    router: Any
    x_par: Any
    g_par: Any
    dy_par: Any
    w_flat: Any


class FrontScratch(NamedTuple):
    keys: Any
    bias: Any
    wo: Any
    part: Any
    part_in: Any
    raw: Any
    flat: Any
    ws: Any
    wi: Any
    wf: Any
    us: Any
    ur: Any
    xs: Any
    xr: Any
    ts: Any
    tr: Any
    es: Any
    er: Any


def front_body(group, *refs):
    n_in, n_out = len(FrontIns._fields), len(FrontOuts._fields)
    ins = FrontIns(*refs[:n_in])
    o = FrontOuts(*refs[n_in : n_in + n_out])
    s = FrontScratch(*refs[n_in + n_out :])
    p = Place()
    seqs, rows, _ = ins.q.shape
    experts_here = ins.w_in.shape[0]
    part_of = lambda i: pl.ds(i * rows if isinstance(i, int) else pl.multiple_of(i * rows, rows), rows)

    def fetch(e):
        return pltpu.make_async_copy(ins.w_in.at[e], s.raw.at[e % 2], s.wi.at[e % 2])

    def put(e):
        return pltpu.make_async_copy(s.flat.at[e % 2], o.w_flat.at[e], s.wf.at[e % 2])

    done = []

    def fill(count):
        for _ in range(count):
            e = len(done)
            if e >= experts_here:
                return
            fetch(e).wait()
            if e >= 2:
                put(e - 2).wait()
            slot, cut = e % 2, s.flat.shape[1] // 4

            @pl.loop(0, 4)
            def _(k):
                at = pl.ds(pl.multiple_of(k * cut, cut), cut)
                s.flat[slot, at] = s.raw[slot, at].reshape(cut, s.flat.shape[2])

            put(e).start()
            if e + 2 < experts_here:
                fetch(e + 2).start()
            done.append(e)

    def source(i, r):
        return ins.kv.at[i] if r == 0 else o.slots.at[i, r, 0]

    def up_copy(i, r):
        return p.copy("up", source(i, r), o.slots.at[i, r + 1, 0], s.us.at[i, r], s.ur.at[i, r])

    def x_copy(i, r):
        return p.copy("x", source(i, r), o.slots.at[i, r, 1], s.xs.at[i, r], s.xr.at[i, r])

    def tp_copy(i):
        return p.copy("tp", s.part.at[part_of(i)], s.part_in.at[part_of(i)], s.ts.at[i], s.tr.at[i])

    def ep_copies(i):
        at = part_of(i)
        return (
            p.copy("ep", o.normed.at[at], o.x_par.at[at], s.es.at[2 * i], s.er.at[2 * i]),
            p.copy("ep", o.gates.at[at], o.g_par.at[at], s.es.at[2 * i + 1], s.er.at[2 * i + 1]),
        )

    fetch(0).start()
    fetch(1).start()
    o.router[...] = jnp.zeros_like(o.router)
    o.router[: ins.router.shape[0]] = ins.router[...]
    wo_load = pltpu.make_async_copy(ins.w_out, s.wo, s.ws.at[0])
    wo_load.start()
    p.greet(("x", "ep", "tp"))
    for i in range(seqs):

        @pl.when(p.z < LINE - 1)
        def _(i=i):
            up_copy(i, 0).start()

        x_copy(i, 0).start()
    dy_copy = p.copy("ep", ins.dy, o.dy_par, s.es.at[2 * seqs], s.er.at[2 * seqs])
    dy_copy.start()
    for i in range(seqs):
        o.slots[i, 0, 0] = ins.kv[i]
        for r in range(1, LINE):

            @pl.when(p.z < r)
            def _(i=i, r=r):
                o.slots[i, r] = jnp.zeros(o.slots.shape[2:], BF16)

    fill(1)
    for r in range(1, LINE):
        for i in range(seqs):
            for z in range(r, LINE):

                @p.at(z)
                def _(i=i, r=r, z=z):
                    up_copy(i, r - 1).wait_recv()
                    if z < LINE - 1:
                        up_copy(i, r).start()
                    x_copy(i, r).start()

        fill(1)
    homes = [(p.z - r, side) for r in range(LINE) for side in (p.side, 1 - p.side)]
    firsts = [jnp.where(a >= 0, (2 * a + b) * rows, 2**24) for a, b in homes]
    wo_load.wait()

    @pl.loop(0, seqs)
    def _(i):
        for r in range(LINE):

            @pl.when(p.z >= r)
            def _(r=r):
                x_copy(i, r).wait_recv()

        attend_core(
            group,
            ins.q.at[i],
            ins.place[i],
            [o.slots.at[i, j // 2, j % 2] for j in range(2 * LINE)],
            firsts,
            p.cp * rows,
            s.keys,
            s.bias,
            o.lse.at[i],
            KEY_CHUNK,
            o.attended.at[i],
            o.low.at[i],
        )
        s.part[part_of(i)] = mm_t(o.low[i], s.wo[...]).astype(BF16)
        tp_copy(i).start()

    fill(1)
    for i in range(seqs):
        at = part_of(i)
        tp_copy(i).wait_recv()
        mid = ins.act[at].astype(F32) + (s.part[at].astype(F32) + s.part_in[at].astype(F32))
        o.middle[at] = mid
        expert = lax.broadcasted_iota(jnp.int32, (LANES, rows), 0)
        hot = sum(jnp.where(ins.routes[i, k : k + 1, :] == expert, 1.0, 0.0) for k in range(ins.routes.shape[1]))
        o.normed[at], o.gates[at] = route(
            mid, ins.gain[1:], lambda v: mm_t(v, o.router[...]), jnp.transpose(hot)
        )
        for copy in ep_copies(i):
            copy.start()
        fill(3 if i == 0 else experts_here)
    for i in range(seqs):
        for copy in ep_copies(i):
            copy.wait()
        tp_copy(i).wait_send()
        for r in range(LINE):

            @pl.when(p.z >= r)
            def _(i=i, r=r):
                x_copy(i, r).wait_send()
                if r < LINE - 1:

                    @pl.when(p.z < LINE - 1)
                    def _():
                        up_copy(i, r).wait_send()

    dy_copy.wait()
    for e in done[-2:]:
        put(e).wait()


def front(ins, group):
    v = FrontIns(*ins)
    seqs, each, heads = v.q.shape
    both = v.kv.shape[-1]
    rows, model = v.act.shape
    local, _, _, half = v.w_in.shape
    anywhere = pl.BlockSpec(memory_space=pl.ANY)
    inside = pl.BlockSpec(memory_space=pltpu.VMEM)
    dma, vm = pltpu.SemaphoreType.DMA, pltpu.VMEM
    scratch = dict(
        keys=vm((2 * LINE * each, both), BF16),
        bias=vm((2 * LINE * each, each), F32),
        wo=vm(v.w_out.shape, BF16),
        part=vm((rows, model), BF16),
        part_in=vm((rows, model), BF16),
        raw=vm((2, model, 2, half), BF16),
        flat=vm((2, model, 2 * half), BF16),
        ws=dma((1,)),
        wi=dma((2,)),
        wf=dma((2,)),
        us=dma((seqs, LINE - 1)),
        ur=dma((seqs, LINE - 1)),
        xs=dma((seqs, LINE)),
        xr=dma((seqs, LINE)),
        ts=dma((seqs,)),
        tr=dma((seqs,)),
        es=dma((2 * seqs + 1,)),
        er=dma((2 * seqs + 1,)),
    )
    return pl.pallas_call(
        functools.partial(front_body, group),
        out_shape=(
            shape_of((seqs, LINE, 2, each, both), BF16),
            shape_of((seqs, each, heads), BF16),
            shape_of((seqs, each, heads), F32),
            shape_of((seqs, heads // HEAD // group, group * each), F32),
            shape_of((rows, model), F32),
            shape_of((rows, model), BF16),
            shape_of((rows, LANES), F32),
            shape_of((LANES, model), BF16),
            shape_of((rows, model), BF16),
            shape_of((rows, LANES), F32),
            shape_of((rows, model), BF16),
            shape_of((local, model, 2 * half), BF16),
        ),
        in_specs=[inside] * 7 + [anywhere] * 3,
        out_specs=(inside,) * 8 + (anywhere,) * 4,
        scratch_shapes=[scratch[name] for name in FrontScratch._fields],
        compiler_params=params(collective_id=3, has_side_effects=True),
        name="front",
    )(*ins)


def on_device(
    activations,
    cotangent,
    positions,
    routes,
    w_query,
    w_key,
    value_weight,
    w_out,
    gain_attn,
    gain_moe,
    w_router,
    w_gate_up,
    w_down,
):
    seqs, rows, model = activations.shape
    total = seqs * rows
    width = w_key.shape[1]
    group = w_query.shape[1] // width
    expert_count = w_router.shape[1]
    local = w_gate_up.shape[0]
    half = w_down.shape[2]
    blocks = lax.axis_size("cp")
    length = blocks // 2
    here = lax.axis_index("cp")
    z, side = here // 2, here % 2
    mine = lax.axis_index("ep")
    act = activations.reshape(total, model)
    dy = cotangent.reshape(total, model)
    gains = jnp.where(lax.broadcasted_iota(jnp.int32, (2, model), 0) == 0, gain_attn, gain_moe)
    gain_one, gain_two = gains[:1], gains[1:]

    frequency = jnp.power(10000.0, -(jnp.arange(HEAD // 2, dtype=F32) * 2.0 / HEAD))
    angles = positions.reshape(total, 1).astype(F32) * jnp.tile(frequency, 2 * LANES // HEAD)
    cosine, sine = jnp.cos(angles), jnp.sin(angles)

    normed, q, kv = project(act, gains, w_query, w_key, value_weight, cosine, sine)
    q = q.reshape(seqs, rows, -1)
    place = positions.reshape(seqs, 1, rows)
    if length == LINE:
        kv = kv.reshape(seqs, rows, 2 * width)
        ins = (q, kv, act, jnp.swapaxes(routes, 1, 2), w_router.T, gains, place, w_out, dy, w_gate_up)
        got = FrontOuts(*front(ins, group))
        slots, low, attended, lse, middle, normed_two, gates, router, x_par, gates_par, dy_par, w_in = got
        low = low.reshape(total, -1)
    else:
        lanes = jnp.arange(LANES, dtype=jnp.int32)
        hot = jnp.sum((routes.reshape(total, -1, 1) == lanes).astype(F32), axis=1)
        router = jnp.pad(w_router, ((0, 0), (0, LANES - expert_count)))
        kv = kv.reshape(1, seqs, rows, 2 * width)
        offset = (here * rows).astype(jnp.int32).reshape(1)
        slots = [lax.all_gather(kv, "cp", axis=0, tiled=True)]
        first = jnp.arange(blocks, dtype=jnp.int32) * rows
        dy_par = swap(dy, "ep")
        low, attended, lse = attend(q, place, slots, first, offset, group)
        low = low.reshape(total, -1)
        part = out_project(low, w_out)
        w_in = w_gate_up.reshape(local, model, 2 * half)
        middle, normed_two, gates = middle_of(act, part, swap(part, "tp"), gain_two, router, hot)
        x_par, gates_par = swap(normed_two, "ep"), swap(gates, "ep")

    early, apart = (EARLY, FIRST) if length == LINE else (0, 0)
    args = (normed_two, x_par, dy, dy_par, gates, gates_par, w_in, w_down)
    chunks, (own_back, par_back, own_mix, par_mix) = experts(early, apart, blocks, *args)
    if length == LINE:
        ins = (
            own_back, par_back, own_mix, par_mix, middle, dy, router, w_out, normed_two, q, attended, act, normed,
            low, w_query, w_key, value_weight, gates, gains, place, lse, cosine, sine,
        )
        input_grad, mix, expert_grad, big, little = back_and_sums(ins, slots, chunks, group)
        output, input_grad, *plain, gate_up_grad, down_grad = results(
            middle, mix, input_grad, expert_grad, big, little, half, expert_count
        )
        out_grad, query_grad, key_grad, value_grad, router_grad, one, two = plain
        small_grads = one.reshape(-1), two.reshape(-1), router_grad.T
    else:
        back = total_of([own_back, swap(par_back, "ep")]).astype(BF16)
        grad_middle, branch, grad_heads, small = middle_back(
            back, swap(back, "tp"), middle, dy, gates, router, gain_two, w_out, normed_two
        )
        seq_cosine, seq_sine = cosine.reshape(seqs, rows, -1), sine.reshape(seqs, rows, -1)
        dq, grads = attend_back(
            q, place, grad_heads.reshape(q.shape), attended, lse, seq_cosine, seq_sine, slots, first, offset, group
        )
        dq = dq.reshape(total, -1)
        kv_sum = lax.psum_scatter(grads[0], "cp", scatter_dimension=0, tiled=True)
        kv_terms = [kv_sum, jnp.zeros_like(kv_sum), jnp.zeros_like(kv_sum)]
        kv_terms = [t.reshape(total, 2 * width) for t in kv_terms]
        spots = jnp.stack([mine, side]).astype(jnp.int32)
        big = weights(spots, blocks, [(branch, low), (normed, dq)], stacked=True)
        normed_part, dkv, gain_row = project_back(act, dq, *kv_terms, cosine, sine, w_query, w_key, value_weight)
        small = jnp.concatenate([small[:expert_count], small[LANES : LANES + 1], gain_row[:1]], axis=0)
        small = jnp.pad(small, ((0, LANES - small.shape[0]), (0, 0)))
        little = weights(spots, blocks, [(normed, dkv)], (small,))
        input_grad = input_of(act, grad_middle, normed_part, swap(normed_part, "tp"), gain_one)
        mix = total_of([own_mix, swap(par_mix, "ep")]).astype(BF16)
        output = middle + total_of([mix, swap(mix, "tp")])

        def spread_sum(keep, send):
            both = total_of([keep, swap(send, "ep")]).astype(BF16)
            return line_sum([both[0], swap(both[1], "cp")], z, length)

        turned = [jnp.swapaxes(v, 0, 1) for v in (chunks[0], swap(chunks[1], "cp"))]
        expert_grad = line_sum(turned, z, length)
        big, little = spread_sum(*big), spread_sum(*little)
        gate_up_grad = expert_grad[:, :, : 2 * half].reshape(local, -1, 2, half)
        down_grad = expert_grad[:, :, 2 * half :]
        tall = big.shape[0] // 2
        out_grad, query_grad = big[:tall], big[tall:]
        key_grad, value_grad = little[:, :width], little[:, width : 2 * width]
        small = little[:, 2 * width :]
        gain_part = small[:, expert_count + 1]
        small_grads = gain_part + swap(gain_part, "tp"), small[:, expert_count], small[:, :expert_count]
    return (
        output.reshape(activations.shape),
        input_grad.reshape(activations.shape),
        query_grad,
        key_grad,
        value_grad,
        out_grad,
        *small_grads,
        gate_up_grad,
        down_grad,
    )


def solution(mesh):
    in_specs = (
        P("ep", "cp", None),
        P("ep", "cp", None),
        P("ep", "cp"),
        P("ep", "cp", None),
        P(None, "tp"),
        P(None, "tp"),
        P(None, "tp"),
        P(None, "tp"),
        P(),
        P(),
        P(),
        P("ep", None, None, "tp"),
        P("ep", None, "tp"),
    )
    out_specs = (
        P("ep", "cp", None),
        P("ep", "cp", None),
        P(("ep", "cp"), "tp"),
        P(("ep", "cp"), "tp"),
        P(("ep", "cp"), "tp"),
        P(("ep", "cp"), "tp"),
        P(("ep", "cp")),
        P(("ep", "cp")),
        P(("ep", "cp"), None),
        P("ep", "cp", None, "tp"),
        P("ep", "cp", "tp"),
    )
    return jax.shard_map(
        on_device, mesh=mesh, in_specs=in_specs, out_specs=out_specs, check_vma=False
    )
```

```python
import functools
from typing import Any, NamedTuple

import jax
import jax.numpy as jnp
from jax import lax
from jax.experimental import pallas as pl
from jax.experimental.pallas import tpu as pltpu
from jax.sharding import PartitionSpec as P

HEAD = 64
EPS = 1e-06
NEG = -1e30
SCALE = 0.125
LANES = 128
KEY_CHUNK = 1024
F32 = jnp.float32
BF16 = jnp.bfloat16
MESH = pl.DeviceIdType.MESH


def mm(a, b):
    return lax.dot_general(a, b, (((1,), (0,)), ((), ())), preferred_element_type=F32)


def mm_t(a, b):
    return lax.dot_general(a, b, (((1,), (1,)), ((), ())), preferred_element_type=F32)


def t_mm(a, b):
    return lax.dot_general(a, b, (((0,), (0,)), ((), ())), preferred_element_type=F32)


def two_parts(v):
    high = v.astype(BF16)
    return high, (v - high.astype(F32)).astype(BF16)


def halves_turned(v, back):
    width = v.shape[1]
    ahead = pltpu.roll(v, width - HEAD // 2, 1)
    behind = pltpu.roll(v, HEAD // 2, 1)
    first = lax.broadcasted_iota(jnp.int32, v.shape, 1) % HEAD < HEAD // 2
    if back:
        return jnp.where(first, ahead, -behind)
    return jnp.where(first, -ahead, behind)


def rope(v, cosine, sine):
    return v * cosine + halves_turned(v, False) * sine


def rope_back(v, cosine, sine):
    return v * cosine + halves_turned(v * sine, True)


def widen(table, width):
    return jnp.concatenate([table] * (width // table.shape[1]), axis=1)


def unit_rows(v):
    scale = lax.rsqrt(jnp.mean(v * v, axis=-1, keepdims=True) + EPS)
    return v * scale, scale


def shape_of(shape, dtype):
    return jax.ShapeDtypeStruct(shape, dtype)


def params(**kw):
    return pltpu.CompilerParams(vmem_limit_bytes=60 * 2**20, **kw)


def cost(flops, moved):
    return pl.CostEstimate(flops=int(flops), bytes_accessed=int(moved), transcendentals=0)


def project_body(act, gain, wq, wk, wv, cosine, sine, normed, q, kv):
    unit, _ = unit_rows(act[...].astype(F32))
    low = (unit * gain[:1]).astype(BF16)
    normed[...] = low
    qf = mm(low, wq[...])
    q[...] = rope(qf, widen(cosine[...], qf.shape[1]), widen(sine[...], qf.shape[1])).astype(BF16)
    kf = mm(low, wk[...])
    width = kf.shape[1]
    kv[:, :width] = rope(kf, widen(cosine[...], width), widen(sine[...], width)).astype(BF16)
    kv[:, width:] = mm(low, wv[...]).astype(BF16)


def project(act, gain, wq, wk, wv, cosine, sine):
    rows, model = act.shape
    total = wq.shape[1] + 2 * wk.shape[1]
    return pl.pallas_call(
        project_body,
        out_shape=(
            shape_of((rows, model), BF16),
            shape_of((rows, wq.shape[1]), BF16),
            shape_of((rows, 2 * wk.shape[1]), BF16),
        ),
        compiler_params=params(),
        cost_estimate=cost(2 * rows * model * total, 2 * model * total + 6 * rows * model),
        name="project",
    )(act, gain, wq, wk, wv, cosine, sine)


def fill_keys(firsts, offset, place, slots, keys, bias, rows):
    query = lax.broadcasted_iota(jnp.int32, (rows, rows), 1) + offset
    for at, slot in enumerate(slots):
        keys[at * rows : (at + 1) * rows, :] = slot[...]
        key = lax.broadcasted_iota(jnp.int32, (rows, rows), 0) + firsts[at]
        distance = query - key
        seen = (distance >= 0) & (distance <= place)
        bias[at * rows : (at + 1) * rows, :] = jnp.where(seen, 0.0, NEG)


def single_slots(slots):
    return [slot.at[one, 0] for slot in slots for one in range(slot.shape[0])]


def group_rows(block, head, group):
    return jnp.concatenate(
        [block[:, (head * group + g) * HEAD : (head * group + g + 1) * HEAD] for g in range(group)], axis=0
    )


def pair_lanes(pair, width, start=0):
    return pl.ds(pl.multiple_of(start + pair * width, LANES), width)


def attend_core(group, q_ref, place, slots, firsts, offset, keys, bias, lse_ref, most, out_ref, low_ref):
    rows = q_ref.shape[0]
    fill_keys(firsts, offset, place, slots, keys, bias, rows)
    total, width = keys.shape[0], keys.shape[1] // 2
    chunk = min(total, most)
    two, many = 2 * HEAD, 2 * HEAD * group

    @pl.loop(0, width // two)
    def _(pair):
        q = (q_ref[:, pair_lanes(pair, many)].astype(F32) * SCALE).astype(BF16)
        pieces = []
        for head in range(2):
            mine = slice(head * HEAD, (head + 1) * HEAD)
            q3 = group_rows(q, head, group)
            top = run = out = None
            for low in range(0, total, chunk):
                k = keys[low : low + chunk, pair_lanes(pair, two)][:, mine]
                v = keys[low : low + chunk, pair_lanes(pair, two, width)][:, mine]
                s = mm_t(k, q3) + widen(bias[low : low + chunk, :], group * rows)
                here = jnp.max(s, axis=0, keepdims=True)
                new = here if top is None else jnp.maximum(top, here)
                p = jnp.exp(s - new)
                part = jnp.sum(p, axis=0, keepdims=True)
                o = t_mm(v, p.astype(BF16))
                if top is None:
                    run, out = part, o
                else:
                    shrink = jnp.exp(top - new)
                    run, out = run * shrink + part, out * shrink + o
                top = new
            out = jnp.transpose(out / run)
            pieces += [out[g * rows : (g + 1) * rows] for g in range(group)]
            lse_ref[pl.ds(2 * pair + head, 1), :] = top + jnp.log(run)
        whole = jnp.concatenate(pieces, axis=1)
        out_ref[:, pair_lanes(pair, many)] = whole
        low_ref[:, pair_lanes(pair, many)] = whole.astype(BF16)


def attend_body(group, count, first_ref, offset_ref, q_ref, place_ref, *refs):
    slots = single_slots(refs[:count])
    low_ref, out_ref, lse_ref, keys, bias = refs[count:]
    firsts = [first_ref[i] for i in range(len(slots))]
    attend_core(
        group,
        q_ref.at[0],
        place_ref[0],
        slots,
        firsts,
        offset_ref[0],
        keys,
        bias,
        lse_ref.at[0],
        KEY_CHUNK,
        out_ref.at[0],
        low_ref.at[0],
    )


def seq_block(shape):
    return pl.BlockSpec((1,) + shape[1:], lambda s, *_: (s,) + (0,) * (len(shape) - 1))


def slot_block(shape):
    return pl.BlockSpec((shape[0], 1) + shape[2:], lambda s, *_: (0, s, 0, 0))


def attend(q, place, slots, first, offset, group):
    seqs, rows, wide = q.shape
    both = slots[0].shape[-1]
    total = rows * sum(slot.shape[0] for slot in slots)
    heads = wide // HEAD // group
    outs = (
        shape_of(q.shape, BF16),
        shape_of(q.shape, F32),
        shape_of((seqs, heads, group * rows), F32),
    )
    return pl.pallas_call(
        functools.partial(attend_body, group, len(slots)),
        out_shape=outs,
        grid_spec=pltpu.PrefetchScalarGridSpec(
            num_scalar_prefetch=2,
            grid=(seqs,),
            in_specs=[seq_block(q.shape), seq_block(place.shape)] + [slot_block(s.shape) for s in slots],
            out_specs=tuple(seq_block(o.shape) for o in outs),
            scratch_shapes=[pltpu.VMEM((total, both), BF16), pltpu.VMEM((total, rows), F32)],
        ),
        compiler_params=params(),
        cost_estimate=cost(2e9 * 4, 20e6),
        name="attend",
    )(first, offset, q, place, *slots)


def attend_back_core(
    group, q_ref, place, go_ref, out_ref, lse_ref, cosine, sine, slots, firsts, offset, keys, bias, grads, dq_ref, most
):
    rows = q_ref.shape[0]
    fill_keys(firsts, offset, place, slots, keys, bias, rows)
    total, width = keys.shape[0], keys.shape[1] // 2
    chunk = min(total, most)
    two, many = 2 * HEAD, 2 * HEAD * group

    @pl.loop(0, width // two)
    def _(pair):
        here = pair_lanes(pair, many)
        q = (q_ref[:, here].astype(F32) * SCALE).astype(BF16)
        go = go_ref[:, here]
        products = go.astype(F32) * out_ref[:, here]
        ones = jnp.ones((8, HEAD), F32)
        q3s = [group_rows(q, head, group) for head in range(2)]
        g3s = [group_rows(go, head, group) for head in range(2)]
        deltas = [
            lax.dot_general(
                ones,
                group_rows(products, head, group),
                (((1,), (1,)), ((), ())),
                preferred_element_type=F32,
                precision=lax.Precision.HIGHEST,
            )[:1]
            for head in range(2)
        ]
        dq = [None] * 2
        for low in range(0, total, chunk):
            dks, dvs = [], []
            for head in range(2):
                mine = slice(head * HEAD, (head + 1) * HEAD)
                k = keys[low : low + chunk, pair_lanes(pair, two)][:, mine]
                v = keys[low : low + chunk, pair_lanes(pair, two, width)][:, mine]
                s = mm_t(k, q3s[head]) + widen(bias[low : low + chunk, :], group * rows)
                p = jnp.exp(s - lse_ref[pl.ds(2 * pair + head, 1), :])
                dp = mm_t(v, g3s[head])
                ds = (p * (dp - deltas[head])).astype(BF16)
                dks.append(mm(ds, q3s[head]))
                dvs.append(mm(p.astype(BF16), g3s[head]))
                part = t_mm(k, ds)
                dq[head] = part if dq[head] is None else dq[head] + part
            for made, start in ((dks, 0), (dvs, width)):
                both = jnp.concatenate(made, axis=1).astype(BF16)
                for one in range(chunk // rows):
                    grad = grads[low // rows + one]
                    grad[:, pair_lanes(pair, two, start)] = both[one * rows : (one + 1) * rows]
        pieces = []
        for head in range(2):
            back = jnp.transpose(dq[head] * SCALE)
            pieces += [back[g * rows : (g + 1) * rows] for g in range(group)]
        whole = jnp.concatenate(pieces, axis=1)
        dq_ref[:, here] = rope_back(whole, widen(cosine, many), widen(sine, many)).astype(BF16)


def attend_back_body(
    group, count, first_ref, offset_ref, q_ref, place_ref, grad_ref, out_ref, lse_ref, cos_ref, sin_ref, *refs
):
    slots = single_slots(refs[:count])
    dq_ref = refs[count]
    grads = single_slots(refs[count + 1 : 2 * count + 1])
    keys, bias = refs[2 * count + 1 :]

    attend_back_core(
        group,
        q_ref.at[0],
        place_ref[0],
        grad_ref.at[0],
        out_ref.at[0],
        lse_ref.at[0],
        cos_ref[0],
        sin_ref[0],
        slots,
        [first_ref[i] for i in range(len(slots))],
        offset_ref[0],
        keys,
        bias,
        grads,
        dq_ref.at[0],
        KEY_CHUNK,
    )


def attend_back(q, place, grad, out, lse, cosine, sine, slots, first, offset, group):
    seqs, rows, _ = q.shape
    both = slots[0].shape[-1]
    total = rows * sum(slot.shape[0] for slot in slots)
    outs = (shape_of(q.shape, BF16),) + tuple(shape_of(s.shape, BF16) for s in slots)
    ins = (q, place, grad, out, lse, cosine, sine)
    got = pl.pallas_call(
        functools.partial(attend_back_body, group, len(slots)),
        out_shape=outs,
        grid_spec=pltpu.PrefetchScalarGridSpec(
            num_scalar_prefetch=2,
            grid=(seqs,),
            in_specs=[seq_block(a.shape) for a in ins] + [slot_block(s.shape) for s in slots],
            out_specs=(seq_block(outs[0].shape),) + tuple(slot_block(s.shape) for s in slots),
            scratch_shapes=[pltpu.VMEM((total, both), BF16), pltpu.VMEM((total, rows), F32)],
        ),
        compiler_params=params(),
        cost_estimate=cost(2e9 * 8, 30e6),
        name="attend_back",
    )(first, offset, *ins, *slots)
    return got[0], got[1:]


def out_body(low, w_out, part):
    part[...] = mm_t(low[...], w_out[...]).astype(BF16)


def out_project(low, w_out):
    rows, model = low.shape[0], w_out.shape[0]
    return pl.pallas_call(
        out_body,
        out_shape=shape_of((rows, model), BF16),
        compiler_params=params(),
        cost_estimate=cost(2 * rows * model * low.shape[1], 4e6),
        name="out_project",
    )(low, w_out)


def route(mid, gain, logits_of, hot):
    unit, _ = unit_rows(mid)
    low = (unit * gain).astype(BF16)
    chosen = hot > 0.5
    logits = jnp.where(chosen, logits_of(low), NEG)
    up = jnp.where(chosen, jnp.exp(logits - jnp.max(logits, axis=-1, keepdims=True)), 0.0)
    return low, up / jnp.sum(up, axis=-1, keepdims=True)


def middle_body(act, part, other, gain, router, hot, middle, normed, gates):
    mid = act[...].astype(F32) + (part[...].astype(F32) + other[...].astype(F32))
    middle[...] = mid
    normed[...], gates[...] = route(mid, gain[...], lambda v: mm(v, router[...]), hot[...])


def middle_of(act, part, other, gain, router, hot):
    rows, model = act.shape
    return pl.pallas_call(
        middle_body,
        out_shape=(shape_of((rows, model), F32), shape_of((rows, model), BF16), shape_of((rows, LANES), F32)),
        compiler_params=params(),
        cost_estimate=cost(2 * rows * model * LANES, 12 * rows * model),
        name="middle",
    )(act, part, other, gain, router, hot)


def ordered_turn(rows_of, blocks_of, ordered, side):
    blocks_of[...] = jnp.transpose(rows_of[...]).reshape(blocks_of.shape)
    count = blocks_of.shape[0] // 2
    for z in range(count):
        ordered[z] = blocks_of[2 * z + side]
        ordered[count + z] = blocks_of[2 * z + 1 - side]


EARLY = 2
FIRST = 1
HALF = 2


def experts_body(early, first, x_all, dy_all, dy_order, gates, w_in, w_out, keep, send, *refs):
    refs = list(refs)
    came, z_kept, z_sent = (refs.pop(0), refs.pop(0), refs.pop(0)) if early else (None, None, None)
    own_back, par_back, own_mix, par_mix, x_turned, back, mix, pulls, blocks_of = refs[:9]
    step, steps = pl.program_id(0), pl.num_programs(0)
    rows, model = own_mix.shape
    wide = own_back.shape[1] - model
    blocks, depth, _ = blocks_of.shape
    side = lax.axis_index("cp") % 2
    if early:
        leaving, held, spots, es, er, zs, zr = refs[9:]
        p = Place()
        flows = [Flow(p, held.at[i], spots.at[i], zs.at[i], zr.at[i]) for i in range(2)]

    def early_copy(i):
        some = pl.ds(0, blocks // 2 if i < early - 1 else HALF)
        return p.copy("x", leaving.at[i, some], came.at[i, some], es.at[i], er.at[i])

    @pl.when(step == 0)
    def _():
        if early:
            p.greet(("x",))
        ordered_turn(x_all, blocks_of, x_turned, side)
        back[...] = jnp.zeros_like(back)
        mix[...] = jnp.zeros_like(mix)
        pulls[...] = jnp.zeros_like(pulls)

    expert = lax.axis_index("ep") * steps + step
    lane = lax.broadcasted_iota(jnp.int32, (2 * rows, wide), 1) == expert
    gate = jnp.sum(jnp.where(lane, gates[...], 0.0), axis=-1, keepdims=True)
    x, dy = x_all[...], dy_all[...]
    w_gu, w_d = w_in[0], w_out[0]
    both = mm(x, w_gu)
    half = both.shape[1] // 2
    g, u = both[:, :half], both[:, half:]
    pull = mm(dy, w_d)
    sig = 1.0 / (1.0 + jnp.exp(-g))
    act = g * sig
    hidden = (act * u).astype(BF16).astype(F32)
    pulls[...] += jnp.where(lane, jnp.sum(hidden * pull, axis=-1, keepdims=True), 0.0)
    weighted = (gate * hidden).astype(BF16)
    pull = gate * pull
    d_g = (pull * u * sig * (1.0 + g * (1.0 - sig))).astype(BF16)
    d_u = (pull * act).astype(BF16)
    d_gu = jnp.concatenate([d_g, d_u], axis=1)
    for i, out in enumerate((keep, send)):
        at = pl.ds(i * (blocks // 2), blocks // 2)
        shape = (model // 2, 2 * rows)
        to = (blocks // 2, depth, -1)
        out[0, :, :, : 2 * half] = mm(x_turned[at].reshape(shape), d_gu).astype(BF16).reshape(to)
        out[0, :, :, 2 * half :] = mm(dy_order[at].reshape(shape), weighted).astype(BF16).reshape(to)
    if early:

        @pl.when(step == 0)
        def _():
            held[0] = keep[0]
            held[1] = send[0]
            for flow in flows:
                flow.open()

        for i in range(early):

            @pl.when(step == first + i)
            def _(i=i):
                leaving[i] = send[0]
                early_copy(i).start()

        for at, work in (
            (2, [lambda: flows[0].second(0)]),
            (3, [lambda: flows[0].second(1)]),
            (4, [flows[0].third]),
            (5, [lambda: flows[1].second(0)]),
            (6, [lambda: flows[1].second(1), flows[1].third]),
        ):

            @pl.when(step == at)
            def _(work=work):
                for one in work:
                    one()

    back[...] += mm_t(d_gu, w_gu)
    mix[...] += mm_t(weighted, w_d)

    @pl.when(step == steps - 1)
    def _():
        own_back[:, :model] = back[:rows].astype(BF16)
        par_back[:, :model] = back[rows:].astype(BF16)
        own_back[:, model:] = pulls[:rows].astype(BF16)
        par_back[:, model:] = pulls[rows:].astype(BF16)
        own_mix[...] = mix[:rows].astype(BF16)
        par_mix[...] = mix[rows:].astype(BF16)
        if early:
            for flow, out in zip(flows, (z_kept, z_sent)):

                def finish(parts, out=out):
                    sum_into(out, *parts)

                flow.close(finish)
                flow.drain()
            for i in range(early):
                early_copy(i).wait()


def experts(early, first, blocks, x_all, dy_all, dy_order, gates, w_in, w_out):
    rows, model = x_all.shape[0] // 2, x_all.shape[1]
    count, _, half = w_out.shape
    depth = model // blocks
    once = lambda shape: pl.BlockSpec(shape, lambda e: (0,) * len(shape))
    whole = (blocks // 2, depth, 3 * half)
    ins = [x_all, dy_all, dy_order, gates]
    apart = first + max(early - 1, 0)
    tail = [shape_of((rows, model + LANES), BF16)] * 2 + [shape_of((rows, model), BF16)] * 2
    outs = [shape_of((count - first,) + whole, BF16), shape_of((count - apart,) + whole, BF16)]
    specs = [
        pl.BlockSpec((1,) + whole, lambda e: (jnp.maximum(e - first, 0), 0, 0, 0)),
        pl.BlockSpec((1,) + whole, lambda e: (jnp.maximum(e - apart, 0), 0, 0, 0)),
    ]
    turned = (blocks, depth, 2 * rows)
    scratch = [
        pltpu.VMEM(turned, BF16),
        pltpu.VMEM((2 * rows, model), F32),
        pltpu.VMEM((2 * rows, model), F32),
        pltpu.VMEM((2 * rows, LANES), F32),
        pltpu.VMEM(turned, BF16),
    ]
    kind = params()
    if early:
        dma = pltpu.SemaphoreType.DMA
        sums = [shape_of(whole[1:], F32), shape_of(whole[1:], BF16)]
        outs += [shape_of((early,) + whole, BF16)] + sums
        specs += [pl.BlockSpec(memory_space=pl.ANY)] + [once(t.shape) for t in sums]
        scratch += [
            pltpu.VMEM((early,) + whole, BF16),
            pltpu.VMEM((2,) + whole, BF16),
            pltpu.VMEM((2, 5) + whole[1:], BF16),
            dma((early,)),
            dma((early,)),
            dma((2, 6)),
            dma((2, 6)),
        ]
        kind = params(collective_id=2, has_side_effects=True)
    got = pl.pallas_call(
        functools.partial(experts_body, early, first),
        out_shape=tuple(outs + tail),
        grid=(count,),
        in_specs=[once(a.shape) for a in ins]
        + [
            pl.BlockSpec((1, model, 2 * half), lambda e: (e, 0, 0)),
            pl.BlockSpec((1, model, half), lambda e: (e, 0, 0)),
        ],
        out_specs=tuple(specs + [once(t.shape) for t in tail]),
        scratch_shapes=scratch,
        compiler_params=kind,
        cost_estimate=cost(count * 18 * 2 * rows * model * half, count * 12 * model * half),
        name="experts",
    )(*ins, w_in, w_out)
    return got[: len(outs)], got[len(outs) :]


def middle_back_body(mine, other, middle, dy, gates, router, gain, w_out, normed, grad, low, heads, small):
    model = middle.shape[1]
    total = mine[...].astype(F32) + other[...].astype(F32)
    gate, pulls = gates[...], total[:, model:]
    chosen = gate * (pulls - jnp.sum(gate * pulls, axis=-1, keepdims=True))
    high, rest = two_parts(chosen)
    grad_two = total[:, :model] + (mm_t(high, router[...]) + mm_t(rest, router[...]))
    unit, scale = unit_rows(middle[...])
    small[:LANES, :] = t_mm(high, normed[...]) + t_mm(rest, normed[...])
    small[LANES : LANES + 8, :] = jnp.broadcast_to(jnp.sum(grad_two * unit, axis=0, keepdims=True), (8, model))
    scaled = grad_two * gain[...]
    out = dy[...].astype(F32) + scale * (scaled - unit * jnp.mean(scaled * unit, axis=-1, keepdims=True))
    grad[...] = out
    rounded = out.astype(BF16)
    low[...] = rounded
    heads[...] = mm(rounded, w_out[...]).astype(BF16)


def middle_back(mine, other, middle, dy, gates, router, gain, w_out, normed):
    rows, model = middle.shape
    return pl.pallas_call(
        middle_back_body,
        out_shape=(
            shape_of((rows, model), F32),
            shape_of((rows, model), BF16),
            shape_of((rows, w_out.shape[1]), BF16),
            shape_of((LANES + 8, model), F32),
        ),
        compiler_params=params(),
        cost_estimate=cost(2 * rows * model * (w_out.shape[1] + 4 * LANES), 10e6),
        name="middle_back",
    )(mine, other, middle, dy, gates, router, gain, w_out, normed)


def project_back_body(width, act, dq, a, b, c, cosine, sine, wq, wk, wv, part, dkv, gain_row):
    total = a[...].astype(F32) + b[...].astype(F32) + c[...].astype(F32)
    dk = rope_back(total[:, :width], widen(cosine[...], width), widen(sine[...], width)).astype(BF16)
    dv = total[:, width:].astype(BF16)
    dkv[:, :width] = dk
    dkv[:, width:] = dv
    full = mm_t(dq[...], wq[...]) + mm_t(dk, wk[...]) + mm_t(dv, wv[...])
    part[...] = full.astype(BF16)
    unit, _ = unit_rows(act[...].astype(F32))
    gain_row[...] = jnp.broadcast_to(jnp.sum(full * unit, axis=0, keepdims=True), gain_row.shape)


def project_back(act, dq, a, b, c, cosine, sine, wq, wk, wv):
    rows, model = act.shape
    width = wk.shape[1]
    return pl.pallas_call(
        functools.partial(project_back_body, width),
        out_shape=(
            shape_of((rows, model), BF16),
            shape_of((rows, 2 * width), BF16),
            shape_of((8, model), F32),
        ),
        compiler_params=params(),
        cost_estimate=cost(2 * rows * model * (wq.shape[1] + 2 * width), 8e6),
        name="project_back",
    )(act, dq, a, b, c, cosine, sine, wq, wk, wv)


def input_body(act, grad, mine, other, gain, out):
    unit, scale = unit_rows(act[...].astype(F32))
    scaled = (mine[...].astype(F32) + other[...].astype(F32)) * gain[...]
    out[...] = grad[...] + scale * (scaled - unit * jnp.mean(scaled * unit, axis=-1, keepdims=True))


def input_of(act, grad, mine, other, gain):
    return pl.pallas_call(
        input_body,
        out_shape=shape_of(act.shape, F32),
        compiler_params=params(),
        cost_estimate=cost(0, 12 * act.shape[0] * act.shape[1]),
        name="input_grad",
    )(act, grad, mine, other, gain)


def weights_body(blocks, count, stacked, where_ref, *refs):
    lefts = refs[:count]
    rights = refs[count : 2 * count]
    extra = refs[2 * count : -3]
    keep, send, whole = refs[-3:]
    parts = [t_mm(a[...], b[...]).astype(BF16) for a, b in zip(lefts, rights)]
    parts += [jnp.transpose(e[...]).astype(BF16) for e in extra]
    at = down = 0
    for part in parts:
        block = part.reshape(2 * blocks, -1, part.shape[1])
        whole[:, down : down + block.shape[1], at : at + part.shape[1]] = block
        if stacked:
            down += block.shape[1]
        else:
            at += part.shape[1]
    mine, side = where_ref[0], where_ref[1]
    for half, ref in ((mine, keep), (1 - mine, send)):
        for z in range(blocks // 2):
            ref[0, z] = whole[half * blocks + 2 * z + side]
            ref[1, z] = whole[half * blocks + 2 * z + 1 - side]


def weights(where, blocks, pairs, extra=(), stacked=False):
    model = pairs[0][0].shape[1]
    rows = pairs[0][0].shape[0]
    depth = model // (2 * blocks)
    columns = sum(b.shape[1] for _, b in pairs) + sum(e.shape[0] for e in extra)
    tall, wide = (depth * len(pairs), pairs[0][1].shape[1]) if stacked else (depth, columns)
    shape = (2, blocks // 2, tall, wide)
    ins = [a for a, _ in pairs] + [b for _, b in pairs] + list(extra)
    full = lambda a: pl.BlockSpec(a.shape, lambda i, *_: (0,) * len(a.shape))
    return pl.pallas_call(
        functools.partial(weights_body, blocks, len(pairs), stacked),
        out_shape=(shape_of(shape, BF16),) * 2,
        grid_spec=pltpu.PrefetchScalarGridSpec(
            num_scalar_prefetch=1,
            grid=(1,),
            in_specs=[full(a) for a in ins],
            out_specs=(pl.BlockSpec(shape, lambda i, *_: (0, 0, 0, 0)),) * 2,
            scratch_shapes=[pltpu.VMEM((2 * blocks, tall, wide), BF16)],
        ),
        compiler_params=params(),
        cost_estimate=cost(2 * rows * model * columns, 4 * model * columns),
        name="weights",
    )(where, *ins)


def swap(v, axis):
    size = lax.axis_size(axis)
    return lax.ppermute(v, axis, [(i, i ^ 1) for i in range(size)])


def up(v, low, high):
    return lax.ppermute(v, "cp", [(2 * z + s, 2 * z + 2 + s) for z in range(low, high) for s in range(2)])


def down(v, low, high):
    return lax.ppermute(v, "cp", [(2 * z + s, 2 * z - 2 + s) for z in range(low, high) for s in range(2)])


def total_of(terms):
    return functools.reduce(lambda a, b: a + b, [t.astype(F32) for t in terms])


def line_sum(parts, z, length):
    def own(d):
        return [lax.dynamic_index_in_dim(p, jnp.clip(d, 0, length - 1), 0, keepdims=False) for p in parts]

    if length > 4:
        mine = total_of(parts).astype(BF16)
        side = lax.axis_index("cp") % 2
        full = jnp.where(jnp.arange(2).reshape((1, 2) + (1,) * (mine.ndim - 1)) == side, mine[:, None], 0)
        full = full.reshape((2 * length,) + mine.shape[1:])
        return lax.psum_scatter(full, "cp", scatter_dimension=0, tiled=True)[0].astype(F32)
    right = left = None
    for k in range(length - 1):
        far = length - 1 - k
        terms = own(z + far) + ([] if right is None else [right])
        right = up(total_of(terms).astype(BF16), 0, k + 1)
        terms = own(z - far) + ([] if left is None else [left])
        left = down(total_of(terms).astype(BF16), far, length)
    return total_of(own(z) + ([right, left] if length > 1 else []))


LINE = 4
RING = 6


def sum_into(out, *parts):
    few = 48 if out.shape[0] % 48 == 0 else out.shape[0]

    @pl.loop(0, out.shape[0] // few)
    def _(k):
        at = pl.ds(pl.multiple_of(k * few, few), few)
        out[at] = total_of([part[at] for part in parts]).astype(out.dtype)


def add_into(ref, other):
    sum_into(ref, ref, other)


class Place:
    def __init__(self):
        self.cp = lax.axis_index("cp")
        self.z, self.side = self.cp // 2, self.cp % 2
        self.ep, self.tp = lax.axis_index("ep"), lax.axis_index("tp")

    def to(self, way):
        if way == "x":
            return {"cp": self.cp + 1 - 2 * self.side}
        if way == "up":
            return {"cp": self.cp + 2}
        if way == "down":
            return {"cp": self.cp - 2}
        return {way: 1 - (self.ep if way == "ep" else self.tp)}

    def signal(self, sem, way):
        pl.semaphore_signal(sem, inc=1, device_id=self.to(way), device_id_type=MESH)

    def signal_line(self, to_down, to_up):
        @pl.when(self.z > 0)
        def _():
            self.signal(to_down, "down")

        @pl.when(self.z < LINE - 1)
        def _():
            self.signal(to_up, "up")

    def greet(self, ways):
        barrier = pltpu.get_barrier_semaphore()
        for way in ways:
            self.signal(barrier, way)
        self.signal_line(barrier, barrier)
        both = jnp.where(self.z > 0, 1, 0) + jnp.where(self.z < LINE - 1, 1, 0)
        pl.semaphore_wait(barrier, len(ways) + both)

    def copy(self, way, src, dst, send, recv):
        return pltpu.make_async_remote_copy(
            src_ref=src, dst_ref=dst, send_sem=send, recv_sem=recv, device_id=self.to(way), device_id_type=MESH
        )

    def at(self, z):
        return pl.when(self.z == z)


LEFT_SPOT = (3, 4, 0)


class Flow:
    def __init__(self, place, held, spots, send, recv, credit=None):
        self.p, self.held, self.spots, self.send, self.recv, self.credit = place, held, spots, send, recv, credit

    def right(self, d):
        return self.p.copy("up", self.held.at[d], self.spots.at[d - 1], self.send.at[d - 1], self.recv.at[d - 1])

    def left(self, d):
        spot = LEFT_SPOT[d]
        return self.p.copy("down", self.held.at[d], self.spots.at[spot], self.send.at[d + 3], self.recv.at[d + 3])

    def allowed(self, way):
        if self.credit is not None:
            pl.semaphore_wait(self.credit[way], 1)

    def open(self):
        @self.p.at(0)
        def _():
            self.allowed("up")
            for d in (3, 2, 1):
                self.right(d).start()

        @self.p.at(3)
        def _():
            self.allowed("down")
            for d in (0, 1, 2):
                self.left(d).start()

    def pass_right(self, d):
        self.right(d).wait_recv()
        add_into(self.held.at[d], self.spots.at[d - 1])
        self.right(d).start()

    def pass_left(self, d):
        self.left(d).wait_recv()
        add_into(self.held.at[d], self.spots.at[LEFT_SPOT[d]])
        self.left(d).start()

    def second(self, only=None):
        @self.p.at(1)
        def _():
            if only != 1:
                self.allowed("up")
                self.pass_right(3)
            if only != 0:
                self.pass_right(2)

        @self.p.at(2)
        def _():
            if only != 1:
                self.allowed("down")
                self.pass_left(0)
            if only != 0:
                self.pass_left(1)

    def third(self):
        @self.p.at(2)
        def _():
            self.allowed("up")
            self.pass_right(3)

        @self.p.at(1)
        def _():
            self.allowed("down")
            self.pass_left(0)

    def close(self, finish):
        for z in range(LINE):

            @self.p.at(z)
            def _(z=z):
                blocks = [self.held.at[z]]
                if z > 0:
                    self.right(z).wait_recv()
                    blocks.append(self.spots.at[z - 1])
                if z < LINE - 1:
                    self.left(z).wait_recv()
                    blocks.append(self.spots.at[LEFT_SPOT[z]])
                finish(blocks)

    def drain(self):
        for z in range(LINE):

            @self.p.at(z)
            def _(z=z):
                for d in range(z + 1, LINE):
                    self.right(d).wait_send()
                for d in range(z):
                    self.left(d).wait_send()


class BackIns(NamedTuple):
    own_back: Any
    par_back: Any
    own_mix: Any
    par_mix: Any
    middle: Any
    dy: Any
    router: Any
    w_out: Any
    x2: Any
    q: Any
    attended: Any
    act: Any
    normed: Any
    low: Any
    wq: Any
    wk: Any
    wv: Any
    gates: Any
    gains: Any
    place: Any
    lse: Any
    cosine: Any
    sine: Any


BACK_IN_PLACE = 6
class BackOuts(NamedTuple):
    grad: Any
    mix: Any
    experts: Any
    big_out: Any
    little_out: Any


class BackScratch(NamedTuple):
    back: Any
    other_ep: Any
    other_tp: Any
    mid_dy: Any
    mid_x2: Any
    wide_w: Any
    branch: Any
    heads: Any
    small: Any
    qs: Any
    atts: Any
    slots: Any
    kv_x: Any
    kv_z: Any
    keys: Any
    bias: Any
    dq: Any
    lows: Any
    wks: Any
    wvs: Any
    routers: Any
    dkv: Any
    part: Any
    part_in: Any
    mix_ep: Any
    mix_tp: Any
    held: Any
    spots: Any
    kept: Any
    staged: Any
    zero_in: Any
    whole: Any
    came: Any
    lit: Any
    lit_came: Any
    lit_x: Any
    lit_spots: Any
    ls: Any
    ks: Any
    xs: Any
    xr: Any
    zs: Any
    zr: Any
    es: Any
    er: Any
    ts: Any
    tr: Any
    kxs: Any
    kxr: Any
    kzs: Any
    kzr: Any
    os: Any
    free_x: Any
    free_up: Any
    free_down: Any


def back_body(group, *refs):
    n_in = len(BackIns._fields) + 6
    ins = BackIns(*refs[: len(BackIns._fields)])
    slots_in = refs[n_in - 6]
    keeps, sends, arrived, z_kept, z_sent = refs[n_in - 5 : n_in]
    o = BackOuts(*refs[n_in : n_in + len(BackOuts._fields)])
    s = BackScratch(*refs[n_in + len(BackOuts._fields) :])
    p = Place()
    early = arrived.shape[0]
    first = FIRST
    count = first + keeps.shape[0]
    seqs, rows, _ = ins.q.shape
    model = ins.middle.shape[1]
    width = ins.wk.shape[1]
    part_of = lambda i: pl.ds(i * rows if isinstance(i, int) else pl.multiple_of(i * rows, rows), rows)

    whole_early = early - 1
    ring = [("here", e) for e in range(first, first + whole_early)] + [("half", first + whole_early)]
    ring += [("x", e) for e in range(first + early, count)] + [("big", 0), ("big", 1)]
    index_of = {item: i for i, item in enumerate(ring)}
    crosses = lambda item: item[0] != "here"

    short = model // 16

    def big_part_of(ref, i):
        return ref.at[i % RING, :, pl.ds(0, short)]

    def lit_columns(item):
        return pl.ds(0, 3 * LANES) if item[1] == 0 else pl.ds(3 * LANES, 2 * width - 2 * LANES)

    def big_rows(item):
        return pl.ds(item[1] * short, short)

    def flow(item):
        if item[0] == "lit":
            k, cols = len(ring) + item[1], lit_columns(item)
            return Flow(p, s.lit_x.at[:, :, cols], s.lit_spots.at[:, :, cols], s.zs.at[k], s.zr.at[k])
        i = index_of[item]
        credit = {"up": s.free_up, "down": s.free_down} if i >= RING else None
        if item[0] == "big":
            return Flow(p, big_part_of(s.held, i), big_part_of(s.spots, i), s.zs.at[i], s.zr.at[i], credit)
        return Flow(p, s.held.at[i % RING], s.spots.at[i % RING], s.zs.at[i], s.zr.at[i], credit)

    def x_copy(item):
        if item[0] == "lit":
            k, cols = len(ring) + item[1], lit_columns(item)
            src = s.lit.at[p.ep, :, 1 - p.side, :, cols]
            return p.copy("x", src, s.lit_x.at[:, :, cols], s.xs.at[k], s.xr.at[k])
        i = index_of[item]
        if item[0] == "half":
            some = pl.ds(HALF, LINE - HALF)
            return p.copy("x", sends.at[0, some], s.held.at[i, some], s.xs.at[i], s.xr.at[i])
        if item[0] == "big":
            src = s.whole.at[p.ep, :, 1 - p.side, big_rows(item)]
            return p.copy("x", src, big_part_of(s.held, i), s.xs.at[i], s.xr.at[i])
        src = sends.at[item[1] - first - whole_early]
        return p.copy("x", src, s.held.at[i % RING], s.xs.at[i], s.xr.at[i])

    def cross(item):
        if item[0] != "lit" and index_of[item] >= RING:
            pl.semaphore_wait(s.free_x, 1)
        x_copy(item).start()

    def load_keep(e):
        return pltpu.make_async_copy(keeps.at[e - first], s.kept, s.ks.at[0])

    def load_arrived(e):
        if e == first + whole_early:
            some = pl.ds(0, HALF)
            return pltpu.make_async_copy(
                arrived.at[e - first, some], s.held.at[e - first, some], s.ks.at[1 + e - first]
            )
        return pltpu.make_async_copy(arrived.at[e - first], s.held.at[e - first], s.ks.at[1 + e - first])

    def opened(item):
        if item[0] == "lit":
            cols = lit_columns(item)
            x_copy(item).wait_recv()
            for d in range(LINE):
                add_into(s.lit_x.at[d, :, cols], s.lit.at[p.ep, d, p.side, :, cols])
        else:
            held = s.held.at[index_of[item] % RING]
            if item[0] in ("here", "half"):
                load_arrived(item[1]).wait()
            if item[0] != "here":
                x_copy(item).wait_recv()
            if item[0] == "big":
                for d in range(LINE):
                    add_into(
                        big_part_of(s.held, index_of[item]).at[d], s.whole.at[p.ep, d, p.side, big_rows(item)]
                    )
            else:
                load_keep(item[1]).wait()
                for d in range(LINE):
                    add_into(held.at[d], s.kept.at[d])
                if item[1] + 1 < count:
                    load_keep(item[1] + 1).start()
        flow(item).open()

    stored = []

    def store(e):
        return pltpu.make_async_copy(s.staged.at[e % 2], o.experts.at[e], s.os.at[e])

    def finish_expert(e, make):
        if len(stored) >= 2 and e % 2 in [k % 2 for k in stored[-2:]]:
            last = [k for k in stored if k % 2 == e % 2][-1]
            store(last).wait()
            waited.add(last)
        make()
        store(e).start()
        stored.append(e)

    waited = set()

    def closed(item):
        if item[0] == "lit":
            def finish(blocks):
                sum_into(o.little_out.at[:, lit_columns(item)], *blocks)

            flow(item).close(finish)
        elif item[0] == "big":
            def finish(blocks):
                sum_into(o.big_out.at[big_rows(item)], *blocks)

            flow(item).close(finish)
        else:
            def finish(blocks):
                sum_into(s.staged.at[item[1] % 2], *blocks)

            finish_expert(item[1], lambda: flow(item).close(finish))

    def freed(item):
        flow(item).drain()
        if item[0] == "lit":
            return
        after = index_of[item] + RING
        if after < len(ring):
            if crosses(item):
                x_copy(item).wait_send()
            if crosses(ring[after]):
                p.signal(s.free_x, "x")
            p.signal_line(s.free_up, s.free_down)

    loads = {}

    def load(name, src, dst):
        copy = pltpu.make_async_copy(src, dst, s.ls.at[len(loads)])
        copy.start()
        loads[name] = copy

    def got(*names):
        for name in names:
            loads[name].wait()

    load("back", ins.own_back, s.back)
    load_keep(first).start()
    for e in range(first, first + early):
        load_arrived(e).start()
    load("zero", z_kept, s.staged.at[0])
    load("grad", ins.middle, o.grad)
    load("dy", ins.dy, s.mid_dy)
    load("router", ins.router, s.routers)
    load("x2", ins.x2.at[pl.ds(0, seqs * rows)], s.mid_x2)
    load("w_out", ins.w_out, s.wide_w)
    load("mix", ins.own_mix, o.mix)
    load("q", ins.q, s.qs)
    load("attended", ins.attended, s.atts)
    load("slots", slots_in, s.slots)
    load("low", ins.low, s.lows)
    load("wk", ins.wk, s.wks)
    load("wv", ins.wv, s.wvs)

    p.greet(("x", "ep", "tp"))
    ep_back = p.copy("ep", ins.par_back, s.other_ep, s.es.at[0], s.er.at[0])
    ep_back.start()
    ep_mix = p.copy("ep", ins.par_mix, s.mix_ep, s.es.at[1], s.er.at[1])
    ep_mix.start()
    lits = [("lit", 0), ("lit", 1)]
    queue = ring[whole_early:] + lits
    zero_copy = p.copy("x", z_sent, s.zero_in, s.xs.at[len(ring) + 2], s.xr.at[len(ring) + 2])
    zero_copy.start()
    for _ in range(3):
        cross(queue.pop(0))

    got("back")
    ep_back.wait_recv()
    for i in range(seqs):
        s.back[part_of(i)] = (
            s.back[part_of(i)].astype(F32) + s.other_ep[part_of(i)].astype(F32)
        ).astype(BF16)
    tp_back = p.copy("tp", s.back, s.other_tp, s.ts.at[0], s.tr.at[0])
    tp_back.start()
    got("mix")
    ep_mix.wait_recv()
    for i in range(seqs):
        o.mix[part_of(i)] = (o.mix[part_of(i)].astype(F32) + s.mix_ep[part_of(i)].astype(F32)).astype(BF16)

    def step_middle():
        got("grad", "dy", "router", "x2", "w_out")
        tp_back.wait_recv()
        s.small[...] = jnp.zeros_like(s.small)

        @pl.loop(0, seqs)
        def _(i):
            at = pl.ds(pl.multiple_of(i * rows, rows), rows)
            total = s.back[at].astype(F32) + s.other_tp[at].astype(F32)
            gate, pulls = ins.gates[at], total[:, model:]
            chosen = gate * (pulls - jnp.sum(gate * pulls, axis=-1, keepdims=True))
            high, rest = two_parts(chosen)
            grad_two = total[:, :model] + (mm(high, s.routers[...]) + mm(rest, s.routers[...]))
            unit, scale = unit_rows(o.grad[at])
            s.small[...] += t_mm(high, s.mid_x2[at]) + t_mm(rest, s.mid_x2[at])
            s.small[LANES - 1 :, :] += jnp.sum(grad_two * unit, axis=0, keepdims=True)
            scaled = grad_two * ins.gains[1:]
            out = s.mid_dy[at].astype(F32) + scale * (
                scaled - unit * jnp.mean(scaled * unit, axis=-1, keepdims=True)
            )
            o.grad[at] = out
            rounded = out.astype(BF16)
            s.branch[at] = rounded
            s.heads[at] = mm(rounded, s.wide_w[...]).astype(BF16)

        load("wq", ins.wq, s.wide_w)
        load("act", ins.act, s.mid_dy)
        load("normed", ins.normed, s.mid_x2)

    tp_mix = p.copy("tp", o.mix, s.mix_tp, s.ts.at[1], s.tr.at[1])

    def step_attend():
        got("q", "attended", "slots")
        homes = [(p.z - r, side) for r in range(LINE) for side in (p.side, 1 - p.side)]
        firsts = [jnp.where(a >= 0, (2 * a + b) * rows, 2**24) for a, b in homes]

        @pl.loop(0, seqs)
        def _(i):
            at = pl.ds(pl.multiple_of(i * rows, rows), rows)

            singles = [s.slots.at[i, j // 2, j % 2] for j in range(2 * LINE)]
            attend_back_core(
                group,
                s.qs.at[i],
                ins.place[i],
                s.heads.at[at],
                s.atts.at[i],
                ins.lse.at[i],
                ins.cosine[at],
                ins.sine[at],
                singles,
                firsts,
                p.cp * rows,
                s.keys,
                s.bias,
                singles,
                s.dq.at[i],
                512,
            )

            @p.at(LINE - 1)
            def _():
                for r in range(LINE - 1, 0, -1):
                    kv_down(i, r).start()

    def kv_cross(i):
        return p.copy("x", s.slots.at[i, 0, 1], s.kv_x.at[i], s.kxs.at[i], s.kxr.at[i])

    def kv_down(i, r):
        return p.copy("down", s.slots.at[i, r], s.kv_z.at[i, r - 1], s.kzs.at[i, r - 1], s.kzr.at[i, r - 1])

    def kv_take(i, r):
        kv_down(i, r + 1).wait_recv()
        for way in range(2):
            s.slots[i, r, way] = (s.slots[i, r, way].astype(F32) + s.kv_z[i, r, way].astype(F32)).astype(BF16)

    def keys_pass(i, z):
        @p.at(z)
        def _():
            for r in range(z, 0, -1):
                kv_take(i, r)
                kv_down(i, r).start()

    def keys_cross(i):
        @pl.when(p.z < LINE - 1)
        def _():
            kv_take(i, 0)

        kv_cross(i).start()

    def keys_close(i):
        kv_cross(i).wait_recv()
        s.slots[i, 0, 0] = (s.slots[i, 0, 0].astype(F32) + s.kv_x[i].astype(F32)).astype(BF16)

    def part_copy(i):
        return p.copy("tp", s.part.at[part_of(i)], s.part_in.at[part_of(i)], s.ts.at[2 + i], s.tr.at[2 + i])

    def step_project(i):
        if i == 0:
            got("wq", "wk", "wv", "act", "normed")
        at = part_of(i)
        total = s.slots[i, 0, 0].astype(F32)
        dk = rope_back(total[:, :width], widen(ins.cosine[at], width), widen(ins.sine[at], width)).astype(BF16)
        dv = total[:, width:].astype(BF16)
        s.dkv[at, :width] = dk
        s.dkv[at, width:] = dv
        full = mm_t(s.dq[i], s.wide_w[...]) + mm_t(dk, s.wks[...]) + mm_t(dv, s.wvs[...])
        s.part[at] = full.astype(BF16)
        part_copy(i).start()

    tall = model // 4

    def pieces(make, keep):
        @pl.loop(0, 4)
        def _(piece):
            got_piece = make(pl.ds(pl.multiple_of(piece * tall, tall), tall)).astype(BF16)
            block = got_piece.reshape(4, short, got_piece.shape[1])
            for b in range(4):
                keep(piece // 2, 2 * (piece % 2) + b // 2, b % 2, block[b])

    def big_part(row):
        def keep(half, z, side, value):
            s.whole[half, z, side, row : row + value.shape[0], :] = value

        return keep

    def little_part(column):
        def keep(half, z, side, value):
            s.lit[half, z, side, :, column : column + value.shape[1]] = value

        return keep

    ep_big = p.copy("ep", s.whole.at[1 - p.ep], s.came, s.es.at[2], s.er.at[2])
    ep_lit = p.copy("ep", s.lit.at[1 - p.ep], s.lit_came, s.es.at[3], s.er.at[3])

    def step_out_weight():
        got("low")
        pieces(lambda at: t_mm(s.branch[:, at], s.lows[...]), big_part(0))

    def step_query_weight():
        got("normed")
        loads["normed"] = Done()
        query = jnp.concatenate([s.dq[i] for i in range(seqs)], axis=0)
        pieces(lambda at: t_mm(s.mid_x2[:, at], query), big_part(short))
        ep_big.start()

    def step_key_weight():
        pieces(lambda at: t_mm(s.mid_x2[:, at], s.dkv[...]), little_part(0))
        pieces(lambda at: jnp.transpose(s.small[:, at]), little_part(2 * width))
        ep_lit.start()

    def step_big_cores():
        ep_big.wait_recv()
        for side in range(2):

            @pl.loop(0, LINE)
            def _(d):
                add_into(s.whole.at[p.ep, d, side], s.came.at[d, side])

    def step_little_cores():
        ep_lit.wait_recv()
        for side in range(2):

            @pl.loop(0, LINE)
            def _(d):
                add_into(s.lit.at[p.ep, d, side], s.lit_came.at[d, side])

    def step_input():
        for i in range(seqs):
            at = part_of(i)
            part_copy(i).wait_recv()
            unit, scale = unit_rows(s.mid_dy[at].astype(F32))
            whole = s.part[at].astype(F32) + s.part_in[at].astype(F32)
            gain_row = jnp.sum(whole * unit, axis=0, keepdims=True)
            if i == 0:
                s.small[LANES - 2 : LANES - 1, :] = gain_row
            else:
                s.small[LANES - 2 : LANES - 1, :] += gain_row
            scaled = whole * ins.gains[:1]
            o.grad[at] = o.grad[at] + scale * (scaled - unit * jnp.mean(scaled * unit, axis=-1, keepdims=True))

    def step_mix():
        tp_mix.wait_recv()
        tp_mix.wait_send()
        for i in range(seqs):
            o.mix[part_of(i)] = (o.mix[part_of(i)].astype(F32) + s.mix_tp[part_of(i)].astype(F32)).astype(BF16)

    line = list(ring) + lits
    stage = {item: 0 for item in line}

    def advance(at, to):
        if not 0 <= at < len(line):
            return
        item = line[at]
        while stage[item] < to:
            now = stage[item]
            if now == 0:
                opened(item)
            elif now == 1:
                flow(item).second()
            elif now == 2:
                flow(item).third()
            elif now == 3:
                closed(item)
            elif now == 4:
                freed(item)
            stage[item] = now + 1

    def turn(at):
        for back in (4, 3, 2, 1, 0):
            advance(at - back, back + 1)

    def add_zero():
        got("zero")
        zero_copy.wait_recv()
        s.staged[0] = s.staged[0] + s.zero_in[...].astype(F32)

    tp_mix.start()
    turn(0)
    finish_expert(0, add_zero)
    turn(1)
    step_middle()
    advance(0, 3)
    advance(1, 2)
    step_attend()
    cross(queue.pop(0))
    step_out_weight()
    step_query_weight()
    turn(2)
    keys_pass(0, 2)
    advance(0, 4)
    advance(1, 3)
    keys_pass(1, 2)
    advance(2, 2)
    step_big_cores()
    step_mix()
    keys_pass(0, 1)
    keys_pass(1, 1)
    turn(3)
    keys_cross(0)
    keys_cross(1)
    cross(queue.pop(0))
    turn(4)
    cross(queue.pop(0))
    keys_close(0)
    step_project(0)
    keys_close(1)
    step_project(1)
    advance(2, 4)
    advance(3, 3)
    advance(4, 2)
    step_input()
    step_key_weight()
    turn(5)
    cross(queue.pop(0))
    step_little_cores()
    for at in range(6, len(line) + 4):
        turn(at)
        if queue:
            cross(queue.pop(0))
    for e in stored:
        if e not in waited:
            store(e).wait()
    for item in line:
        if item[0] == "lit" or (crosses(item) and index_of[item] + RING >= len(ring)):
            x_copy(item).wait_send()
    for i in range(seqs):
        kv_cross(i).wait_send()
        part_copy(i).wait_send()
        for z in range(1, LINE):

            @p.at(z)
            def _(z=z):
                for r in range(z, 0, -1):
                    kv_down(i, r).wait_send()

    tp_back.wait_send()
    zero_copy.wait_send()
    for copy in (ep_back, ep_mix, ep_big, ep_lit):
        copy.wait_send()


class Done:
    def wait(self):
        return None


def back_and_sums(ins, slots, chunks, group):
    keeps, _, arrived, *_ = chunks
    _, length, depth, wide = keeps.shape
    early, count = arrived.shape[0], FIRST + keeps.shape[0]
    block = (length, depth, wide)
    v = BackIns(*ins)
    rows, model = v.middle.shape
    seqs, each, heads = v.q.shape
    width = v.wk.shape[1]
    both = 2 * width
    small = (length, 2, model // 16, both + LANES)
    n_ring = count - FIRST + 2
    anywhere = pl.BlockSpec(memory_space=pl.ANY)
    inside = pl.BlockSpec(memory_space=pltpu.VMEM)
    dma, vm = pltpu.SemaphoreType.DMA, pltpu.VMEM
    flag = pltpu.SemaphoreType.REGULAR
    scratch = dict(
        back=vm((rows, model + LANES), BF16),
        other_ep=vm((rows, model + LANES), BF16),
        other_tp=vm((rows, model + LANES), BF16),
        mid_dy=vm((rows, model), BF16),
        mid_x2=vm((rows, model), BF16),
        wide_w=vm((model, heads), BF16),
        branch=vm((rows, model), BF16),
        heads=vm((rows, heads), BF16),
        small=vm((LANES, model), F32),
        qs=vm((seqs, each, heads), BF16),
        atts=vm((seqs, each, heads), F32),
        slots=vm((seqs, LINE, 2, each, both), BF16),
        kv_x=vm((seqs, each, both), BF16),
        kv_z=vm((seqs, LINE - 1, 2, each, both), BF16),
        keys=vm((2 * LINE * each, both), BF16),
        bias=vm((2 * LINE * each, each), F32),
        dq=vm((seqs, each, heads), BF16),
        lows=vm((rows, heads), BF16),
        wks=vm((model, width), BF16),
        wvs=vm((model, width), BF16),
        routers=vm((LANES, model), BF16),
        dkv=vm((rows, both), BF16),
        part=vm((rows, model), BF16),
        part_in=vm((rows, model), BF16),
        mix_ep=vm((rows, model), BF16),
        mix_tp=vm((rows, model), BF16),
        held=vm((RING,) + block, BF16),
        spots=vm((RING, 5, depth, wide), BF16),
        kept=vm(block, BF16),
        staged=vm((2, depth, wide), F32),
        zero_in=vm((depth, wide), BF16),
        whole=vm((2, length, 2, depth, wide), BF16),
        came=vm((length, 2, depth, wide), BF16),
        lit=vm((2,) + small, BF16),
        lit_came=vm(small, BF16),
        lit_x=vm((small[0],) + small[2:], BF16),
        lit_spots=vm((5,) + small[2:], BF16),
        ls=dma((28,)),
        ks=dma((1 + early,)),
        xs=dma((n_ring + 3,)),
        xr=dma((n_ring + 3,)),
        zs=dma((n_ring + 2, 6)),
        zr=dma((n_ring + 2, 6)),
        es=dma((4,)),
        er=dma((4,)),
        ts=dma((4,)),
        tr=dma((4,)),
        kxs=dma((2,)),
        kxr=dma((2,)),
        kzs=dma((2, 3)),
        kzr=dma((2, 3)),
        os=dma((count,)),
        free_x=flag,
        free_up=flag,
        free_down=flag,
    )
    return pl.pallas_call(
        functools.partial(back_body, group),
        out_shape=(
            shape_of((rows, model), F32),
            shape_of((rows, model), BF16),
            shape_of((count, depth, wide), F32),
            shape_of((depth, wide), F32),
            shape_of(small[2:], F32),
        ),
        in_specs=[anywhere] * (len(BackIns._fields) - BACK_IN_PLACE)
        + [inside] * BACK_IN_PLACE
        + [anywhere] * 6,
        out_specs=(inside, inside, anywhere, inside, inside),
        scratch_shapes=[scratch[name] for name in BackScratch._fields],
        compiler_params=pltpu.CompilerParams(
            collective_id=1, has_side_effects=True, vmem_limit_bytes=67_043_328
        ),
        name="back_and_sums",
    )(*ins, slots, *chunks)


def results_body(
    middle, mix, grad, chunk, big, little, out, grad_in, first, second, keys, values, router, one, two, both, down
):
    out[...] = middle[...] + mix[...].astype(F32)
    grad_in[...] = grad[...]
    half = down.shape[2]
    for one_chunk in range(chunk.shape[0]):
        both[one_chunk] = chunk[one_chunk, :, : 2 * half].reshape(both.shape[1:])
        down[one_chunk] = chunk[one_chunk, :, 2 * half :]

    @pl.when(pl.program_id(0) == 0)
    def _():
        tall, width = first.shape[0], keys.shape[1]
        first[...] = big[:tall]
        second[...] = big[tall:]
        keys[...] = little[:, :width]
        values[...] = little[:, width : 2 * width]
        small = jnp.transpose(little[:, 2 * width :])
        router[...] = small[: router.shape[0]]
        one[...] = small[LANES - 2 : LANES - 1]
        two[...] = small[LANES - 1 :]


def results(middle, mix, grad, chunks, big, little, half, expert_count):
    rows, model = middle.shape
    count, depth, wide = chunks.shape
    tall, width = big.shape[0] // 2, (little.shape[1] - LANES) // 2
    per = 2 if count % 2 == 0 else 1
    part = pl.BlockSpec((rows * per // count, model), lambda e: (e, 0))
    once = lambda shape: pl.BlockSpec(shape, lambda e: (0,) * len(shape))
    whole = [(tall, big.shape[1])] * 2 + [(tall, width)] * 2 + [(expert_count, tall), (1, tall), (1, tall)]
    return pl.pallas_call(
        results_body,
        grid=(count // per,),
        out_shape=[shape_of((rows, model), F32)] * 2
        + [shape_of(shape, F32) for shape in whole]
        + [shape_of((count, depth, 2, half), F32), shape_of((count, depth, half), F32)],
        in_specs=[part] * 3
        + [pl.BlockSpec((per, depth, wide), lambda e: (e, 0, 0)), once(big.shape), once(little.shape)],
        out_specs=[part] * 2
        + [once(shape) for shape in whole]
        + [
            pl.BlockSpec((per, depth, 2, half), lambda e: (e, 0, 0, 0)),
            pl.BlockSpec((per, depth, half), lambda e: (e, 0, 0)),
        ],
        compiler_params=params(),
        name="results",
    )(middle, mix, grad, chunks, big, little)


class FrontIns(NamedTuple):
    act: Any
    routes: Any
    router: Any
    gain: Any
    place: Any
    cosine: Any
    sine: Any
    w_out: Any
    dy: Any
    w_in: Any
    wq: Any
    wk: Any
    wv: Any


class FrontOuts(NamedTuple):
    slots: Any
    low: Any
    attended: Any
    lse: Any
    middle: Any
    q: Any
    normed: Any
    x_all: Any
    gates: Any
    router: Any
    dy_all: Any
    dy_order: Any
    w_flat: Any


class FrontScratch(NamedTuple):
    kv: Any
    wqs: Any
    wks: Any
    wvs: Any
    blocks: Any
    keys: Any
    bias: Any
    wo: Any
    part: Any
    part_in: Any
    raw: Any
    flat: Any
    ws: Any
    wi: Any
    wf: Any
    us: Any
    ur: Any
    xs: Any
    xr: Any
    ts: Any
    tr: Any
    es: Any
    er: Any


def front_body(group, *refs):
    n_in, n_out = len(FrontIns._fields), len(FrontOuts._fields)
    ins = FrontIns(*refs[:n_in])
    o = FrontOuts(*refs[n_in : n_in + n_out])
    s = FrontScratch(*refs[n_in + n_out :])
    p = Place()
    seqs, _, rows = ins.place.shape
    total = seqs * rows
    width = ins.wk.shape[1]
    experts_here = ins.w_in.shape[0]
    part_of = lambda i: pl.ds(i * rows if isinstance(i, int) else pl.multiple_of(i * rows, rows), rows)

    def fetch(e):
        return pltpu.make_async_copy(ins.w_in.at[e], s.raw.at[e % 2], s.wi.at[e % 2])

    def put(e):
        return pltpu.make_async_copy(s.flat.at[e % 2], o.w_flat.at[e], s.wf.at[e % 2])

    done = []

    def fill(count):
        for _ in range(count):
            e = len(done)
            if e >= experts_here:
                return
            fetch(e).wait()
            if e >= 2:
                put(e - 2).wait()
            slot, cut = e % 2, s.flat.shape[1] // 4

            @pl.loop(0, 4)
            def _(k):
                at = pl.ds(pl.multiple_of(k * cut, cut), cut)
                s.flat[slot, at] = s.raw[slot, at].reshape(cut, s.flat.shape[2])

            put(e).start()
            if e + 2 < experts_here:
                fetch(e + 2).start()
            done.append(e)

    def source(i, r):
        return s.kv.at[i] if r == 0 else o.slots.at[i, r, 0]

    def up_copy(i, r):
        return p.copy("up", source(i, r), o.slots.at[i, r + 1, 0], s.us.at[i, r], s.ur.at[i, r])

    def x_copy(i, r):
        return p.copy("x", source(i, r), o.slots.at[i, r, 1], s.xs.at[i, r], s.xr.at[i, r])

    def tp_copy(i):
        return p.copy("tp", s.part.at[part_of(i)], s.part_in.at[part_of(i)], s.ts.at[i], s.tr.at[i])

    def ep_copies(i):
        at, there = part_of(i), pl.ds(total + i * rows, rows)
        return (
            p.copy("ep", o.x_all.at[at], o.x_all.at[there], s.es.at[2 * i], s.er.at[2 * i]),
            p.copy("ep", o.gates.at[at], o.gates.at[there], s.es.at[2 * i + 1], s.er.at[2 * i + 1]),
        )

    weights_in = [
        pltpu.make_async_copy(src, dst, s.ws.at[1 + k])
        for k, (src, dst) in enumerate(((ins.wq, s.wqs), (ins.wk, s.wks), (ins.wv, s.wvs)))
    ]
    for copy in weights_in:
        copy.start()
    dy_here = pltpu.make_async_copy(ins.dy, o.dy_all.at[pl.ds(0, total)], s.ws.at[4])
    dy_here.start()
    fetch(0).start()
    fetch(1).start()
    o.router[...] = jnp.zeros_like(o.router)
    o.router[: ins.router.shape[0]] = ins.router[...]
    wo_load = pltpu.make_async_copy(ins.w_out, s.wo, s.ws.at[0])
    wo_load.start()
    unit, _ = unit_rows(ins.act[...].astype(F32))
    o.normed[...] = (unit * ins.gain[:1]).astype(BF16)
    for copy in weights_in:
        copy.wait()
    kf = mm(o.normed[...], s.wks[...])
    kf = rope(kf, widen(ins.cosine[...], width), widen(ins.sine[...], width)).astype(BF16)
    vf = mm(o.normed[...], s.wvs[...]).astype(BF16)
    for i in range(seqs):
        s.kv[i, :, :width] = kf[i * rows : (i + 1) * rows]
        s.kv[i, :, width:] = vf[i * rows : (i + 1) * rows]
    p.greet(("x", "ep", "tp"))
    for i in range(seqs):

        @pl.when(p.z < LINE - 1)
        def _(i=i):
            up_copy(i, 0).start()

        x_copy(i, 0).start()
    dy_copy = p.copy("ep", ins.dy, o.dy_all.at[pl.ds(total, total)], s.es.at[2 * seqs], s.er.at[2 * seqs])
    dy_copy.start()
    qf = mm(o.normed[...], s.wqs[...])
    qf = rope(qf, widen(ins.cosine[...], qf.shape[1]), widen(ins.sine[...], qf.shape[1])).astype(BF16)
    for i in range(seqs):
        o.q[i] = qf[i * rows : (i + 1) * rows]
    for i in range(seqs):
        o.slots[i, 0, 0] = s.kv[i]
        for r in range(1, LINE):

            @pl.when(p.z < r)
            def _(i=i, r=r):
                o.slots[i, r] = jnp.zeros(o.slots.shape[2:], BF16)

    fill(1)
    for r in range(1, LINE):
        for i in range(seqs):
            for z in range(r, LINE):

                @p.at(z)
                def _(i=i, r=r, z=z):
                    up_copy(i, r - 1).wait_recv()
                    if z < LINE - 1:
                        up_copy(i, r).start()
                    x_copy(i, r).start()

        fill(1)
    homes = [(p.z - r, side) for r in range(LINE) for side in (p.side, 1 - p.side)]
    firsts = [jnp.where(a >= 0, (2 * a + b) * rows, 2**24) for a, b in homes]
    wo_load.wait()

    @pl.loop(0, seqs)
    def _(i):
        for r in range(LINE):

            @pl.when(p.z >= r)
            def _(r=r):
                x_copy(i, r).wait_recv()

        attend_core(
            group,
            o.q.at[i],
            ins.place[i],
            [o.slots.at[i, j // 2, j % 2] for j in range(2 * LINE)],
            firsts,
            p.cp * rows,
            s.keys,
            s.bias,
            o.lse.at[i],
            KEY_CHUNK,
            o.attended.at[i],
            o.low.at[i],
        )
        s.part[part_of(i)] = mm_t(o.low[i], s.wo[...]).astype(BF16)
        tp_copy(i).start()

    dy_here.wait()
    dy_copy.wait_recv()
    ordered_turn(o.dy_all, s.blocks, o.dy_order, p.side)
    fill(1)
    for i in range(seqs):
        at = part_of(i)
        tp_copy(i).wait_recv()
        mid = ins.act[at].astype(F32) + (s.part[at].astype(F32) + s.part_in[at].astype(F32))
        o.middle[at] = mid
        expert = lax.broadcasted_iota(jnp.int32, (LANES, rows), 0)
        hot = sum(jnp.where(ins.routes[i, k : k + 1, :] == expert, 1.0, 0.0) for k in range(ins.routes.shape[1]))
        o.x_all[at], o.gates[at] = route(
            mid, ins.gain[1:], lambda v: mm_t(v, o.router[...]), jnp.transpose(hot)
        )
        for copy in ep_copies(i):
            copy.start()
        fill(3 if i == 0 else experts_here)
    for i in range(seqs):
        for copy in ep_copies(i):
            copy.wait()
        tp_copy(i).wait_send()
        for r in range(LINE):

            @pl.when(p.z >= r)
            def _(i=i, r=r):
                x_copy(i, r).wait_send()
                if r < LINE - 1:

                    @pl.when(p.z < LINE - 1)
                    def _():
                        up_copy(i, r).wait_send()

    dy_copy.wait_send()
    for e in done[-2:]:
        put(e).wait()


def front(ins, group, blocks):
    v = FrontIns(*ins)
    seqs, _, each = v.place.shape
    heads, both = v.wq.shape[1], 2 * v.wk.shape[1]
    rows, model = v.act.shape
    local, _, _, half = v.w_in.shape
    turned = (blocks, model // blocks, 2 * rows)
    anywhere = pl.BlockSpec(memory_space=pl.ANY)
    inside = pl.BlockSpec(memory_space=pltpu.VMEM)
    dma, vm = pltpu.SemaphoreType.DMA, pltpu.VMEM
    scratch = dict(
        kv=vm((seqs, each, both), BF16),
        wqs=vm(v.wq.shape, BF16),
        wks=vm(v.wk.shape, BF16),
        wvs=vm(v.wv.shape, BF16),
        blocks=vm(turned, BF16),
        keys=vm((2 * LINE * each, both), BF16),
        bias=vm((2 * LINE * each, each), F32),
        wo=vm(v.w_out.shape, BF16),
        part=vm((rows, model), BF16),
        part_in=vm((rows, model), BF16),
        raw=vm((2, model, 2, half), BF16),
        flat=vm((2, model, 2 * half), BF16),
        ws=dma((5,)),
        wi=dma((2,)),
        wf=dma((2,)),
        us=dma((seqs, LINE - 1)),
        ur=dma((seqs, LINE - 1)),
        xs=dma((seqs, LINE)),
        xr=dma((seqs, LINE)),
        ts=dma((seqs,)),
        tr=dma((seqs,)),
        es=dma((2 * seqs + 1,)),
        er=dma((2 * seqs + 1,)),
    )
    return pl.pallas_call(
        functools.partial(front_body, group),
        out_shape=(
            shape_of((seqs, LINE, 2, each, both), BF16),
            shape_of((seqs, each, heads), BF16),
            shape_of((seqs, each, heads), F32),
            shape_of((seqs, heads // HEAD // group, group * each), F32),
            shape_of((rows, model), F32),
            shape_of((seqs, each, heads), BF16),
            shape_of((rows, model), BF16),
            shape_of((2 * rows, model), BF16),
            shape_of((2 * rows, LANES), F32),
            shape_of((LANES, model), BF16),
            shape_of((2 * rows, model), BF16),
            shape_of(turned, BF16),
            shape_of((local, model, 2 * half), BF16),
        ),
        in_specs=[inside] * 7 + [anywhere] * 6,
        out_specs=(inside,) * 12 + (anywhere,),
        scratch_shapes=[scratch[name] for name in FrontScratch._fields],
        compiler_params=params(collective_id=3, has_side_effects=True),
        name="front",
    )(*ins)


def on_device(
    activations,
    cotangent,
    positions,
    routes,
    w_query,
    w_key,
    value_weight,
    w_out,
    gain_attn,
    gain_moe,
    w_router,
    w_gate_up,
    w_down,
):
    seqs, rows, model = activations.shape
    total = seqs * rows
    width = w_key.shape[1]
    group = w_query.shape[1] // width
    expert_count = w_router.shape[1]
    local = w_gate_up.shape[0]
    half = w_down.shape[2]
    blocks = lax.axis_size("cp")
    length = blocks // 2
    here = lax.axis_index("cp")
    z, side = here // 2, here % 2
    mine = lax.axis_index("ep")
    act = activations.reshape(total, model)
    dy = cotangent.reshape(total, model)
    gains = jnp.where(lax.broadcasted_iota(jnp.int32, (2, model), 0) == 0, gain_attn, gain_moe)
    gain_one, gain_two = gains[:1], gains[1:]

    frequency = jnp.power(10000.0, -(jnp.arange(HEAD // 2, dtype=F32) * 2.0 / HEAD))
    angles = positions.reshape(total, 1).astype(F32) * jnp.tile(frequency, 2 * LANES // HEAD)
    cosine, sine = jnp.cos(angles), jnp.sin(angles)

    place = positions.reshape(seqs, 1, rows)
    if length == LINE:
        ins = (
            act, jnp.swapaxes(routes, 1, 2), w_router.T, gains, place, cosine, sine, w_out, dy, w_gate_up, w_query,
            w_key, value_weight,
        )
        got = FrontOuts(*front(ins, group, blocks))
        slots, low, attended, lse, middle, q, normed, x_all, gates, router, dy_all, dy_order, w_in = got
        low, x_own = low.reshape(total, -1), x_all
    else:
        normed, q, kv = project(act, gains, w_query, w_key, value_weight, cosine, sine)
        q = q.reshape(seqs, rows, -1)
        lanes = jnp.arange(LANES, dtype=jnp.int32)
        hot = jnp.sum((routes.reshape(total, -1, 1) == lanes).astype(F32), axis=1)
        router = jnp.pad(w_router, ((0, 0), (0, LANES - expert_count)))
        kv = kv.reshape(1, seqs, rows, 2 * width)
        offset = (here * rows).astype(jnp.int32).reshape(1)
        slots = [lax.all_gather(kv, "cp", axis=0, tiled=True)]
        first = jnp.arange(blocks, dtype=jnp.int32) * rows
        low, attended, lse = attend(q, place, slots, first, offset, group)
        low = low.reshape(total, -1)
        part = out_project(low, w_out)
        w_in = w_gate_up.reshape(local, model, 2 * half)
        middle, x_own, gates_own = middle_of(act, part, swap(part, "tp"), gain_two, router, hot)
        x_all = jnp.concatenate([x_own, swap(x_own, "ep")])
        gates = jnp.concatenate([gates_own, swap(gates_own, "ep")])
        dy_all = jnp.concatenate([dy, swap(dy, "ep")])
        order = 2 * jnp.arange(length)
        order = jnp.concatenate([order + side, order + 1 - side])
        dy_order = jnp.take(dy_all.T.reshape(blocks, -1, 2 * total), order, axis=0)

    early, apart = (EARLY, FIRST) if length == LINE else (0, 0)
    args = (x_all, dy_all, dy_order, gates, w_in, w_down)
    chunks, (own_back, par_back, own_mix, par_mix) = experts(early, apart, blocks, *args)
    if length == LINE:
        ins = (
            own_back, par_back, own_mix, par_mix, middle, dy, router, w_out, x_own, q, attended, act, normed,
            low, w_query, w_key, value_weight, gates, gains, place, lse, cosine, sine,
        )
        input_grad, mix, expert_grad, big, little = back_and_sums(ins, slots, chunks, group)
        output, input_grad, *plain, gate_up_grad, down_grad = results(
            middle, mix, input_grad, expert_grad, big, little, half, expert_count
        )
        out_grad, query_grad, key_grad, value_grad, router_grad, one, two = plain
        small_grads = one.reshape(-1), two.reshape(-1), router_grad.T
    else:
        back = total_of([own_back, swap(par_back, "ep")]).astype(BF16)
        grad_middle, branch, grad_heads, small = middle_back(
            back, swap(back, "tp"), middle, dy, gates_own, router, gain_two, w_out, x_own
        )
        seq_cosine, seq_sine = cosine.reshape(seqs, rows, -1), sine.reshape(seqs, rows, -1)
        dq, grads = attend_back(
            q, place, grad_heads.reshape(q.shape), attended, lse, seq_cosine, seq_sine, slots, first, offset, group
        )
        dq = dq.reshape(total, -1)
        kv_sum = lax.psum_scatter(grads[0], "cp", scatter_dimension=0, tiled=True)
        kv_terms = [kv_sum, jnp.zeros_like(kv_sum), jnp.zeros_like(kv_sum)]
        kv_terms = [t.reshape(total, 2 * width) for t in kv_terms]
        spots = jnp.stack([mine, side]).astype(jnp.int32)
        big = weights(spots, blocks, [(branch, low), (normed, dq)], stacked=True)
        normed_part, dkv, gain_row = project_back(act, dq, *kv_terms, cosine, sine, w_query, w_key, value_weight)
        small = jnp.concatenate([small[:expert_count], small[LANES : LANES + 1], gain_row[:1]], axis=0)
        small = jnp.pad(small, ((0, LANES - small.shape[0]), (0, 0)))
        little = weights(spots, blocks, [(normed, dkv)], (small,))
        input_grad = input_of(act, grad_middle, normed_part, swap(normed_part, "tp"), gain_one)
        mix = total_of([own_mix, swap(par_mix, "ep")]).astype(BF16)
        output = middle + total_of([mix, swap(mix, "tp")])

        def spread_sum(keep, send):
            both = total_of([keep, swap(send, "ep")]).astype(BF16)
            return line_sum([both[0], swap(both[1], "cp")], z, length)

        turned = [jnp.swapaxes(v, 0, 1) for v in (chunks[0], swap(chunks[1], "cp"))]
        expert_grad = line_sum(turned, z, length)
        big, little = spread_sum(*big), spread_sum(*little)
        gate_up_grad = expert_grad[:, :, : 2 * half].reshape(local, -1, 2, half)
        down_grad = expert_grad[:, :, 2 * half :]
        tall = big.shape[0] // 2
        out_grad, query_grad = big[:tall], big[tall:]
        key_grad, value_grad = little[:, :width], little[:, width : 2 * width]
        small = little[:, 2 * width :]
        gain_part = small[:, expert_count + 1]
        small_grads = gain_part + swap(gain_part, "tp"), small[:, expert_count], small[:, :expert_count]
    return (
        output.reshape(activations.shape),
        input_grad.reshape(activations.shape),
        query_grad,
        key_grad,
        value_grad,
        out_grad,
        *small_grads,
        gate_up_grad,
        down_grad,
    )


def solution(mesh):
    in_specs = (
        P("ep", "cp", None),
        P("ep", "cp", None),
        P("ep", "cp"),
        P("ep", "cp", None),
        P(None, "tp"),
        P(None, "tp"),
        P(None, "tp"),
        P(None, "tp"),
        P(),
        P(),
        P(),
        P("ep", None, None, "tp"),
        P("ep", None, "tp"),
    )
    out_specs = (
        P("ep", "cp", None),
        P("ep", "cp", None),
        P(("ep", "cp"), "tp"),
        P(("ep", "cp"), "tp"),
        P(("ep", "cp"), "tp"),
        P(("ep", "cp"), "tp"),
        P(("ep", "cp")),
        P(("ep", "cp")),
        P(("ep", "cp"), None),
        P("ep", "cp", None, "tp"),
        P("ep", "cp", "tp"),
    )
    return jax.shard_map(
        on_device, mesh=mesh, in_specs=in_specs, out_specs=out_specs, check_vma=False
    )
```
